32 devices in a mesh: fsdp: 2 (over y), blk: 4 (over x, core), head: 4 (over z).
Axes of the slice: x: 2, y: 2, z: 4, core: 2. Of those that a mesh axis runs over, the one named last changes fastest.
Arguments:
- tokens: bfloat16 [4096, 2048], P(('fsdp', 'blk', 'head')), may hold values from -8 to 8
- w_query: bfloat16 [2048, 2048], P(('fsdp', 'blk'), 'head'), may hold values from -0.125 to 0.125
- w_key: bfloat16 [2048, 256], P(('fsdp', 'blk')), may hold values from -0.125 to 0.125
- w_value: bfloat16 [2048, 256], P(('fsdp', 'blk')), may hold values from -0.125 to 0.125
- w_out: bfloat16 [2048, 2048], P(('fsdp', 'blk'), 'head'), may hold values from -0.75 to 0.75
- w_gate: bfloat16 [2048, 5632], P(('fsdp', 'blk'), 'head'), may hold values from -0.125 to 0.125
- w_up: bfloat16 [2048, 5632], P(('fsdp', 'blk'), 'head'), may hold values from -0.125 to 0.125
- w_down: bfloat16 [2048, 5632], P(('fsdp', 'blk'), 'head'), may hold values from -0.078125 to 0.078125
- gain_attn: bfloat16 [2048], P(('fsdp', 'blk')), may hold values from 0.5 to 1.5
- gain_mlp: bfloat16 [2048], P(('fsdp', 'blk')), may hold values from 0.5 to 1.5
- stretch_order: int32 [8], replicated, may hold values from 0 to 7, each once
- cotangent: bfloat16 [4096, 2048], P(('fsdp', 'blk', 'head')), may hold values from -6 to 6
Outputs:
- layer_out: bfloat16 [4096, 2048], P(('fsdp', 'blk', 'head'))
- grad_tokens: bfloat16 [4096, 2048], P(('fsdp', 'blk', 'head'))
- grad_query: float32 [2048, 2048], P(('fsdp', 'blk'), 'head')
- grad_key: float32 [2048, 256], P(('fsdp', 'blk'))
- grad_value: float32 [2048, 256], P(('fsdp', 'blk'))
- grad_out: float32 [2048, 2048], P(('fsdp', 'blk'), 'head')
- grad_gate: float32 [2048, 5632], P(('fsdp', 'blk'), 'head')
- grad_up: float32 [2048, 5632], P(('fsdp', 'blk'), 'head')
- grad_down: float32 [2048, 5632], P(('fsdp', 'blk'), 'head')
- grad_gain_attn: float32 [2048], P(('fsdp', 'blk'))
- grad_gain_mlp: float32 [2048], P(('fsdp', 'blk'))
The draws below stay inside these ranges and needn't reach their ends.
Inputs may be any that keep to these rules, and one draw needn't show every extreme that they name: A permutation: stored stretch c holds positions stretch_order[c] * 256 to stretch_order[c] * 256 + 255 of its sequence.
All inputs are finite; a program needn't handle non-finite values.
Results may differ from the reference program's by a relative error of at most 0.025.
Values may be sent and summed in bfloat16 or wider, within the bound.
A program may use at most 192 MiB of HBM per device.

```python
import math
import jax
import jax.numpy as jnp
from jax import lax

D = 2048
H = 32
KV = 4
HD = 64
FF = 5632
SEQ = 2048
STRETCH = 256
TOKENS = 4096
N_FSDP = 2
N_BLK = 4
N_HEAD = 4


def levels(stream_key, dims, split, low, high):
    gain, own = 1.0, jax.random.fold_in(stream_key, 6)
    for dim, blocks in split:
        draws = jnp.exp(jax.random.uniform(jax.random.fold_in(own, dim), (blocks,), jnp.float32, low / len(split), high / len(split)))
        gain = gain * jnp.repeat(draws, dims[dim] // blocks).reshape([-1 if axis == dim else 1 for axis in range(len(dims))])
    return gain


def centred(key, extent, scale, bound, pieces=(), kind=jnp.bfloat16):
    drawn = scale * jax.random.normal(key, extent, jnp.float32)
    if pieces:
        drawn = drawn * levels(key, extent, pieces, -0.22, 0.18)
    return jnp.clip(drawn, -bound, bound).astype(kind)


def setup_inputs(seed: int = 0) -> dict:
    arg_keys = jax.random.split(jax.random.key(seed), 13)
    return {
        "tokens": centred(arg_keys[0], (TOKENS, D), 1.0, 8.0, ((0, 32),)),
        "w_query": centred(arg_keys[1], (D, H * HD), D ** -0.5, 0.125, ((0, 8), (1, 4))),
        "w_key": centred(arg_keys[2], (D, KV * HD), D ** -0.5, 0.125, ((0, 8),)),
        "w_value": centred(arg_keys[3], (D, KV * HD), D ** -0.5, 0.125, ((0, 8),)),
        "w_out": centred(arg_keys[4], (D, H * HD), HD ** -0.5, 0.75, ((0, 8), (1, 4))),
        "w_gate": centred(arg_keys[5], (D, FF), D ** -0.5, 0.125, ((0, 8), (1, 4))),
        "w_up": centred(arg_keys[6], (D, FF), D ** -0.5, 0.125, ((0, 8), (1, 4))),
        "w_down": centred(arg_keys[7], (D, FF), FF ** -0.5, 0.078125, ((0, 8), (1, 4))),
        "gain_attn": jnp.clip(1.0 + 0.1 * jax.random.normal(arg_keys[8], (D,), jnp.float32), 0.5, 1.5).astype(jnp.bfloat16),
        "gain_mlp": jnp.clip(1.0 + 0.1 * jax.random.normal(arg_keys[9], (D,), jnp.float32), 0.5, 1.5).astype(jnp.bfloat16),
        "stretch_order": jax.random.permutation(arg_keys[10], 2 * N_BLK).astype(jnp.int32),
        "cotangent": centred(arg_keys[11], (TOKENS, D), 1.0, 6.0, ((0, 32),)),
    }


@jax.custom_vjp
def low(v):
    return lax.optimization_barrier(v.astype(jnp.bfloat16)).astype(jnp.float32)

@jax.custom_vjp
def low_back(v):
    return v

def low_keep(v):
    return (low(v), None)

def low_pass(kept, grad):
    return (grad,)

def back_keep(v):
    return (v, None)

def back_low(kept, grad):
    return (low(grad),)
low.defvjp(low_keep, low_pass)
low_back.defvjp(back_keep, back_low)
norm_epsilon = 1e-05
rope_base = 10000.0
masked_value = -1e+30
highest = lax.Precision.HIGHEST

def storage_positions(stretch_order):
    indices = jnp.arange(SEQ, dtype=jnp.int32)
    return stretch_order[indices // STRETCH] * STRETCH + indices % STRETCH

def rope_tables(positions):
    half_dim = HD // 2
    frequency = rope_base ** (-(jnp.arange(half_dim, dtype=jnp.float32) * (2.0 / HD)))
    angles = positions.astype(jnp.float32)[:, None] * frequency[None, :]
    return (jnp.cos(angles), jnp.sin(angles))

def rotate(values, cosine, sine_table):
    half_dim = HD // 2
    first_half = values[..., :half_dim]
    second_half = values[..., half_dim:]
    cos_rows = cosine[:, None, :]
    sin_rows = sine_table[:, None, :]
    return jnp.concatenate([first_half * cos_rows - second_half * sin_rows, second_half * cos_rows + first_half * sin_rows], axis=-1)

def rms_norm(values, gain_vector):
    inverse = lax.rsqrt(lax.optimization_barrier(jnp.mean(values * values, axis=-1, keepdims=True)) + norm_epsilon)
    return values * inverse * gain_vector

def forward(tokens, w_query, w_key, w_value, w_out, w_gate, w_up, w_down, gain_attn, gain_mlp, cosine, sine_table, positions):
    total_rows = tokens.shape[0]
    repeats = N_HEAD // KV
    per_group = H // N_HEAD
    score_scale = 1.0 / math.sqrt(HD)
    normed = low(rms_norm(tokens, gain_attn))
    query_lin = low_back(jnp.dot(normed, w_query, precision=highest))
    key_lin = jnp.dot(normed, w_key, precision=highest).reshape(total_rows, KV, HD)
    value_lin = jnp.dot(normed, w_value, precision=highest).reshape(total_rows, KV, HD)
    query_rot = low_back(low(rotate(query_lin.reshape(total_rows, H, HD), cosine, sine_table)))
    key_slot_lin = low_back(jnp.repeat(key_lin, repeats, axis=1))
    key_slots = low_back(low(rotate(key_slot_lin, cosine, sine_table))).reshape(N_FSDP, SEQ, N_HEAD, HD)
    value_slots = low_back(low(jnp.repeat(value_lin, repeats, axis=1))).reshape(N_FSDP, SEQ, N_HEAD, HD)
    block_count = N_FSDP * 2 * N_BLK
    query_blocks = query_rot.reshape(block_count, STRETCH, H, HD)
    sequence_ids = jnp.arange(block_count, dtype=jnp.int32) // (2 * N_BLK)
    query_positions = jnp.tile(positions.reshape(2 * N_BLK, STRETCH), (N_FSDP, 1))

    def one_block(block_item):
        query_block, sequence_id, block_positions = block_item
        keys_all = jnp.repeat(key_slots[sequence_id], per_group, axis=1)
        values_all = jnp.repeat(value_slots[sequence_id], per_group, axis=1)
        scores = low_back(jnp.einsum('qhd,khd->hqk', query_block, keys_all, precision=highest) * score_scale)
        allowed = block_positions[:, None] >= positions[None, :]
        scores = jnp.where(allowed[None], scores, masked_value)
        probabilities = jax.nn.softmax(scores, axis=-1)
        return jnp.einsum('hqk,khd->qhd', low(probabilities), values_all, precision=highest)
    attended = lax.map(jax.checkpoint(one_block), (query_blocks, sequence_ids, query_positions))
    attended = low_back(low(attended.reshape(total_rows, H * HD)))
    hidden_one = tokens + low_back(jnp.dot(attended, w_out.T, precision=highest))
    normed_two = low(rms_norm(hidden_one, gain_mlp))
    gate_proj = low_back(jnp.dot(normed_two, w_gate, precision=highest))
    up_proj = low_back(jnp.dot(normed_two, w_up, precision=highest))
    hidden = low(jax.nn.silu(gate_proj) * up_proj)
    return hidden_one + low_back(jnp.dot(hidden, w_down.T, precision=highest))

def reference(tokens, w_query, w_key, w_value, w_out, w_gate, w_up, w_down, gain_attn, gain_mlp, stretch_order, cotangent):
    positions = storage_positions(stretch_order)
    cosine, sine_table = rope_tables(positions)
    cos_rows = jnp.tile(cosine, (N_FSDP, 1))
    sin_rows = jnp.tile(sine_table, (N_FSDP, 1))
    floats = tuple((source.astype(jnp.float32) for source in (tokens, w_query, w_key, w_value, w_out, w_gate, w_up, w_down, gain_attn, gain_mlp)))

    def layer_forward(*arrays):
        return forward(*arrays, cos_rows, sin_rows, positions)
    output, pullback = jax.vjp(layer_forward, *floats)
    gradients = pullback(cotangent.astype(jnp.float32))
    return (output.astype(jnp.bfloat16), gradients[0].astype(jnp.bfloat16), gradients[1], gradients[2], gradients[3], gradients[4], gradients[5], gradients[6], gradients[7], gradients[8], gradients[9])
```

```python
import math

import jax
import jax.numpy as jnp
from jax import lax
from jax.experimental import pallas as pl
from jax.experimental.pallas import tpu as pltpu
from jax.sharding import PartitionSpec as P

H = 32
KV = 4
HD = 64


norm_epsilon = 1e-05
rope_base = 10000.0
masked_value = -1e30


def rope_tables(positions, head_dim):
    half_dim = head_dim // 2
    frequency = rope_base ** (-(jnp.arange(half_dim, dtype=jnp.float32) * (2.0 / head_dim)))
    angles = positions.astype(jnp.float32)[:, None] * frequency[None, :]
    return (jnp.cos(angles), jnp.sin(angles))


def rotate(values, cosine, sine_table):
    half_dim = values.shape[-1] // 2
    first_half = values[..., :half_dim]
    second_half = values[..., half_dim:]
    cos_rows = cosine[:, None, :]
    sin_rows = sine_table[:, None, :]
    return jnp.concatenate(
        [
            first_half * cos_rows - second_half * sin_rows,
            second_half * cos_rows + first_half * sin_rows,
        ],
        axis=-1,
    )


def unrotate(values, cosine, sine_table):
    half_dim = values.shape[-1] // 2
    first_half = values[..., :half_dim]
    second_half = values[..., half_dim:]
    cos_rows = cosine[:, None, :]
    sin_rows = sine_table[:, None, :]
    return jnp.concatenate(
        [
            first_half * cos_rows + second_half * sin_rows,
            second_half * cos_rows - first_half * sin_rows,
        ],
        axis=-1,
    )


def stretch_positions(stretch_order, first_row, row_span, stretch_rows):
    storage = first_row + jnp.arange(row_span, dtype=jnp.int32)
    stretch_index = storage // stretch_rows
    match_table = (
        stretch_index[:, None] == jnp.arange(stretch_order.shape[0], dtype=jnp.int32)[None, :]
    )
    stretch_base = jnp.sum(jnp.where(match_table, stretch_order[None, :], 0), axis=1)
    return stretch_base * stretch_rows + storage % stretch_rows


def norm_input_grad(values, inverse, gain_vector, grad_normed):
    scaled = grad_normed * gain_vector
    inner = jnp.mean(scaled * values, axis=-1, keepdims=True)
    return inverse * scaled - values * inverse * inverse * inverse * inner


def gain_grad(values, inverse, grad_normed):
    return jnp.sum(grad_normed * values * inverse, axis=0)


def fold_block(
    state_now, keys_block, values_block, key_positions, query_heads, query_positions, score_scale
):
    running_max, running_sum, running_out = state_now
    scores = (
        jnp.einsum("qhd,kd->hqk", query_heads, keys_block, preferred_element_type=jnp.float32)
        * score_scale
    )
    allowed = (query_positions[:, None] >= key_positions[None, :])[None]
    scores = jnp.where(allowed, scores, masked_value)
    new_max = jnp.maximum(running_max, jnp.max(scores, axis=-1))
    weights = jnp.where(allowed, jnp.exp(scores - new_max[..., None]), 0.0)
    factor = jnp.exp(running_max - new_max)
    running_sum = running_sum * factor + jnp.sum(weights, axis=-1)
    running_out = running_out * factor[..., None] + jnp.einsum(
        "hqk,kd->hqd",
        weights.astype(jnp.bfloat16),
        values_block,
        preferred_element_type=jnp.float32,
    )
    return (new_max, running_sum, running_out)


def local(
    tokens,
    w_query,
    w_key,
    w_value,
    w_out,
    w_gate,
    w_up,
    w_down,
    gain_attn,
    gain_mlp,
    stretch_order,
    cotangent,
):
    row_count = tokens.shape[0]
    groups = lax.axis_size("head")
    blocks = lax.axis_size("blk")
    local_heads = H // groups
    repeats = groups // KV
    head_rows = row_count * groups
    stretch_rows = head_rows // 2
    score_scale = 1.0 / math.sqrt(HD)
    contract_last = (((1,), (1,)), ((), ()))
    contract_first = (((0,), (0,)), ((), ()))
    head_index = lax.axis_index("head")
    own_first = head_index * row_count
    block_first = lax.axis_index("blk") * head_rows
    positions = stretch_positions(stretch_order, block_first + own_first, row_count, stretch_rows)
    query_positions = stretch_positions(stretch_order, block_first, head_rows, stretch_rows)
    cos_own, sin_own = rope_tables(positions, HD)
    cos_block, sin_block = rope_tables(query_positions, HD)

    def layer_weights():
        return (
            lax.all_gather(w_query, ("fsdp", "blk"), axis=0, tiled=True),
            lax.all_gather(w_key, ("fsdp", "blk"), axis=0, tiled=True),
            lax.all_gather(w_value, ("fsdp", "blk"), axis=0, tiled=True),
            lax.all_gather(w_out, ("fsdp", "blk"), axis=0, tiled=True),
            lax.all_gather(w_gate, ("fsdp", "blk"), axis=0, tiled=True),
            lax.all_gather(w_up, ("fsdp", "blk"), axis=0, tiled=True),
            lax.all_gather(w_down, ("fsdp", "blk"), axis=0, tiled=True),
            lax.all_gather(gain_attn, ("fsdp", "blk"), axis=0, tiled=True),
            lax.all_gather(gain_mlp, ("fsdp", "blk"), axis=0, tiled=True),
        )

    def gather_query(columns):
        return lax.all_gather(columns, "head", axis=1, tiled=True)

    (
        query_cols,
        key_full,
        value_full,
        out_cols,
        gate_cols,
        up_cols,
        down_cols,
        gain_one,
        gain_two,
    ) = layer_weights()
    tokens_float = tokens.astype(jnp.float32)
    inv_attn = lax.rsqrt(
        jnp.mean(tokens_float * tokens_float, axis=-1, keepdims=True) + norm_epsilon
    )
    normed = (tokens_float * inv_attn * gain_one.astype(jnp.float32)).astype(jnp.bfloat16)
    normed_rows, cotangent_rows = (
        lax.all_gather(normed, "head", axis=0, tiled=True),
        lax.all_gather(cotangent, "head", axis=0, tiled=True),
    )
    query_all = gather_query(query_cols)
    query_lin = jnp.dot(normed, query_all, preferred_element_type=jnp.float32).reshape(
        row_count, H, HD
    )
    key_lin = jnp.dot(normed, key_full, preferred_element_type=jnp.float32).reshape(
        row_count, KV, HD
    )
    value_lin = jnp.dot(normed, value_full, preferred_element_type=jnp.float32).reshape(
        row_count, KV, HD
    )
    query_rot = rotate(query_lin, cos_own, sin_own).astype(jnp.bfloat16).reshape(row_count, H * HD)
    key_rot = rotate(key_lin, cos_own, sin_own).astype(jnp.bfloat16)
    key_slots = jnp.repeat(key_rot, repeats, axis=1).reshape(row_count, groups * HD)
    value_slots = jnp.repeat(value_lin.astype(jnp.bfloat16), repeats, axis=1).reshape(
        row_count, groups * HD
    )
    query_recv, key_own, value_own = (
        lax.all_to_all(query_rot, "head", split_axis=1, concat_axis=0, tiled=True),
        lax.all_to_all(key_slots, "head", split_axis=1, concat_axis=0, tiled=True),
        lax.all_to_all(value_slots, "head", split_axis=1, concat_axis=0, tiled=True),
    )
    query_heads = query_recv.reshape(head_rows, local_heads, HD)
    initial = (
        jnp.full((local_heads, head_rows), masked_value, jnp.float32),
        jnp.zeros((local_heads, head_rows), jnp.float32),
        jnp.zeros((local_heads, head_rows, HD), jnp.float32),
    )
    state_now = initial
    keys_piece = lax.all_gather(key_own, "blk", axis=0, tiled=True)
    values_piece = lax.all_gather(value_own, "blk", axis=0, tiled=True)
    piece_rows = keys_piece.shape[0]

    def scan_step(state_inner, step_index):
        offset = step_index * head_rows
        keys_block = lax.dynamic_slice_in_dim(keys_piece, offset, head_rows, 0)
        values_block = lax.dynamic_slice_in_dim(values_piece, offset, head_rows, 0)
        key_positions = stretch_positions(stretch_order, offset, head_rows, stretch_rows)
        return (
            fold_block(
                state_inner,
                keys_block,
                values_block,
                key_positions,
                query_heads,
                query_positions,
                score_scale,
            ),
            None,
        )

    state_now, unused = lax.scan(
        scan_step, state_now, jnp.arange(piece_rows // head_rows, dtype=jnp.int32)
    )
    running_max, running_sum, running_out = state_now
    attended_float = running_out / running_sum[..., None]
    log_sum = running_max + jnp.log(running_sum)
    attended_heads = (
        attended_float.astype(jnp.bfloat16).transpose(1, 0, 2).reshape(head_rows, local_heads * HD)
    )
    branch = lax.dot_general(
        attended_heads, out_cols, contract_last, preferred_element_type=jnp.float32
    )
    own_branch = lax.dynamic_slice_in_dim(branch, own_first, row_count, 0)
    partial_value = lax.dynamic_update_slice_in_dim(branch, own_branch + tokens_float, own_first, 0)
    hidden_rows = lax.psum(partial_value.astype(jnp.bfloat16), "head").astype(jnp.float32)
    inv_mlp = lax.rsqrt(jnp.mean(hidden_rows * hidden_rows, axis=-1, keepdims=True) + norm_epsilon)
    normed_two_rows = (hidden_rows * inv_mlp * gain_two.astype(jnp.float32)).astype(jnp.bfloat16)
    gate_proj = jnp.dot(normed_two_rows, gate_cols, preferred_element_type=jnp.float32)
    up_proj = jnp.dot(normed_two_rows, up_cols, preferred_element_type=jnp.float32)
    gate_sigmoid = jax.nn.sigmoid(gate_proj)
    gate_silu = gate_proj * gate_sigmoid
    hidden = (gate_silu * up_proj).astype(jnp.bfloat16)
    hidden_own = lax.dynamic_slice_in_dim(hidden_rows, own_first, row_count, 0)
    output_float = hidden_own + lax.psum_scatter(
        lax.dot_general(
            hidden, down_cols, contract_last, preferred_element_type=jnp.float32
        ).astype(jnp.bfloat16),
        "head",
        scatter_dimension=0,
        tiled=True,
    ).astype(jnp.float32)
    layer_low = output_float.astype(jnp.bfloat16)
    (
        query_cols,
        key_full,
        value_full,
        out_cols,
        gate_cols,
        up_cols,
        down_cols,
        gain_one,
        gain_two,
    ) = layer_weights()
    query_all = gather_query(query_cols)
    grad_hidden = jnp.dot(cotangent_rows, down_cols, preferred_element_type=jnp.float32)
    grad_gate_rows = (
        grad_hidden * up_proj * gate_sigmoid * (1.0 + gate_proj * (1.0 - gate_sigmoid))
    ).astype(jnp.bfloat16)
    grad_up_rows = (grad_hidden * gate_silu).astype(jnp.bfloat16)
    grad_w_down = lax.dot_general(
        cotangent_rows, hidden, contract_first, preferred_element_type=jnp.float32
    )
    grad_w_gate = lax.dot_general(
        normed_two_rows, grad_gate_rows, contract_first, preferred_element_type=jnp.float32
    )
    grad_w_up = lax.dot_general(
        normed_two_rows, grad_up_rows, contract_first, preferred_element_type=jnp.float32
    )
    normed_two_part = lax.dot_general(
        grad_gate_rows, gate_cols, contract_last, preferred_element_type=jnp.float32
    )
    normed_two_part = normed_two_part + lax.dot_general(
        grad_up_rows, up_cols, contract_last, preferred_element_type=jnp.float32
    )
    grad_normed_two = lax.psum(normed_two_part.astype(jnp.bfloat16), "head").astype(jnp.float32)
    gain_two_float = gain_two.astype(jnp.float32)
    grad_hidden_rows = cotangent_rows.astype(jnp.float32) + norm_input_grad(
        hidden_rows, inv_mlp, gain_two_float, grad_normed_two
    )
    own_grad_two = lax.dynamic_slice_in_dim(grad_normed_two, own_first, row_count, 0)
    own_inv_mlp = lax.dynamic_slice_in_dim(inv_mlp, own_first, row_count, 0)
    grad_gain_two = gain_grad(hidden_own, own_inv_mlp, own_grad_two)
    grad_low_rows = grad_hidden_rows.astype(jnp.bfloat16)
    grad_w_out = lax.dot_general(
        grad_low_rows, attended_heads, contract_first, preferred_element_type=jnp.float32
    )
    grad_heads = (
        jnp.dot(grad_low_rows, out_cols, preferred_element_type=jnp.float32)
        .astype(jnp.bfloat16)
        .reshape(head_rows, local_heads, HD)
    )
    keys_all, values_all = (
        lax.all_gather(key_own, "blk", axis=0, tiled=True),
        lax.all_gather(value_own, "blk", axis=0, tiled=True),
    )
    row_delta = jnp.sum(grad_heads.astype(jnp.float32).transpose(1, 0, 2) * attended_float, axis=-1)

    def back_block(grad_query_acc, block_index):
        offset = block_index * head_rows
        keys_block = lax.dynamic_slice_in_dim(keys_all, offset, head_rows, 0)
        values_block = lax.dynamic_slice_in_dim(values_all, offset, head_rows, 0)
        key_positions = stretch_positions(stretch_order, offset, head_rows, stretch_rows)
        scores = (
            jnp.einsum("qhd,kd->hqk", query_heads, keys_block, preferred_element_type=jnp.float32)
            * score_scale
        )
        allowed = (query_positions[:, None] >= key_positions[None, :])[None]
        probs_block = jnp.where(allowed, jnp.exp(scores - log_sum[..., None]), 0.0)
        grad_probs = jnp.einsum(
            "qhd,kd->hqk", grad_heads, values_block, preferred_element_type=jnp.float32
        )
        grad_scores = (probs_block * (grad_probs - row_delta[..., None])).astype(jnp.bfloat16)
        grad_query_acc = grad_query_acc + jnp.einsum(
            "hqk,kd->qhd", grad_scores, keys_block, preferred_element_type=jnp.float32
        )
        grad_key_part = (
            jnp.einsum("hqk,qhd->kd", grad_scores, query_heads, preferred_element_type=jnp.float32)
            * score_scale
        )
        grad_value_part = jnp.einsum(
            "hqk,qhd->kd",
            probs_block.astype(jnp.bfloat16),
            grad_heads,
            preferred_element_type=jnp.float32,
        )
        return (grad_query_acc, (grad_key_part, grad_value_part))

    grad_query_acc, (key_terms, value_terms) = lax.scan(
        back_block,
        jnp.zeros((head_rows, local_heads, HD), jnp.float32),
        jnp.arange(blocks, dtype=jnp.int32),
    )
    grad_key_sum, grad_value_sum = (
        lax.psum_scatter(
            key_terms.reshape(blocks * head_rows, HD).astype(jnp.bfloat16),
            "blk",
            scatter_dimension=0,
            tiled=True,
        ).astype(jnp.float32),
        lax.psum_scatter(
            value_terms.reshape(blocks * head_rows, HD).astype(jnp.bfloat16),
            "blk",
            scatter_dimension=0,
            tiled=True,
        ).astype(jnp.float32),
    )
    grad_query_rot = (grad_query_acc * score_scale).astype(jnp.bfloat16)
    grad_query_lin_heads = (
        unrotate(grad_query_rot.astype(jnp.float32), cos_block, sin_block)
        .astype(jnp.bfloat16)
        .reshape(head_rows, local_heads * HD)
    )
    key_slot_grad = grad_key_sum.astype(jnp.bfloat16)
    value_slot_grad = grad_value_sum.astype(jnp.bfloat16)
    grad_w_query = lax.dot_general(
        normed_rows, grad_query_lin_heads, contract_first, preferred_element_type=jnp.float32
    )
    query_back, key_back, value_back = (
        lax.all_to_all(grad_query_lin_heads, "head", split_axis=0, concat_axis=1, tiled=True),
        lax.all_to_all(key_slot_grad, "head", split_axis=0, concat_axis=1, tiled=True),
        lax.all_to_all(value_slot_grad, "head", split_axis=0, concat_axis=1, tiled=True),
    )
    key_slot_lin = (
        unrotate(key_back.astype(jnp.float32).reshape(row_count, groups, HD), cos_own, sin_own)
        .astype(jnp.bfloat16)
        .reshape(row_count, KV, repeats, HD)
    )
    value_slot_lin = value_back.reshape(row_count, KV, repeats, HD)
    grad_w_key = jnp.einsum(
        "td,tjrc->djc", normed, key_slot_lin, preferred_element_type=jnp.float32
    ).reshape(-1, KV * HD)
    grad_w_value = jnp.einsum(
        "td,tjrc->djc", normed, value_slot_lin, preferred_element_type=jnp.float32
    ).reshape(-1, KV * HD)
    grad_normed = lax.dot_general(
        query_back, query_all, contract_last, preferred_element_type=jnp.float32
    )
    grad_normed = grad_normed + jnp.einsum(
        "tjrc,djc->td",
        key_slot_lin,
        key_full.reshape(-1, KV, HD),
        preferred_element_type=jnp.float32,
    )
    grad_normed = grad_normed + jnp.einsum(
        "tjrc,djc->td",
        value_slot_lin,
        value_full.reshape(-1, KV, HD),
        preferred_element_type=jnp.float32,
    )
    gain_one_float = gain_one.astype(jnp.float32)
    grad_input_norm = norm_input_grad(tokens_float, inv_attn, gain_one_float, grad_normed)
    grad_gain_one = gain_grad(tokens_float, inv_attn, grad_normed)
    grad_hidden_own = lax.dynamic_slice_in_dim(grad_hidden_rows, own_first, row_count, 0)
    grad_tokens = (grad_hidden_own + grad_input_norm).astype(jnp.bfloat16)
    head_sums = (
        lax.psum(grad_w_key.astype(jnp.bfloat16), "head").astype(jnp.float32),
        lax.psum(grad_w_value.astype(jnp.bfloat16), "head").astype(jnp.float32),
        lax.psum(grad_gain_one.astype(jnp.bfloat16), "head").astype(jnp.float32),
        lax.psum(grad_gain_two.astype(jnp.bfloat16), "head").astype(jnp.float32),
    )
    reduced = (
        lax.psum_scatter(
            grad_w_query.astype(jnp.bfloat16), ("fsdp", "blk"), scatter_dimension=0, tiled=True
        ).astype(jnp.float32),
        lax.psum_scatter(
            head_sums[0].astype(jnp.bfloat16), ("fsdp", "blk"), scatter_dimension=0, tiled=True
        ).astype(jnp.float32),
        lax.psum_scatter(
            head_sums[1].astype(jnp.bfloat16), ("fsdp", "blk"), scatter_dimension=0, tiled=True
        ).astype(jnp.float32),
        lax.psum_scatter(
            grad_w_out.astype(jnp.bfloat16), ("fsdp", "blk"), scatter_dimension=0, tiled=True
        ).astype(jnp.float32),
        lax.psum_scatter(
            grad_w_gate.astype(jnp.bfloat16), ("fsdp", "blk"), scatter_dimension=0, tiled=True
        ).astype(jnp.float32),
        lax.psum_scatter(
            grad_w_up.astype(jnp.bfloat16), ("fsdp", "blk"), scatter_dimension=0, tiled=True
        ).astype(jnp.float32),
        lax.psum_scatter(
            grad_w_down.astype(jnp.bfloat16), ("fsdp", "blk"), scatter_dimension=0, tiled=True
        ).astype(jnp.float32),
        lax.psum_scatter(
            head_sums[2].astype(jnp.bfloat16), ("fsdp", "blk"), scatter_dimension=0, tiled=True
        ).astype(jnp.float32),
        lax.psum_scatter(
            head_sums[3].astype(jnp.bfloat16), ("fsdp", "blk"), scatter_dimension=0, tiled=True
        ).astype(jnp.float32),
    )
    return (
        layer_low,
        grad_tokens,
        reduced[0],
        reduced[1],
        reduced[2],
        reduced[3],
        reduced[4],
        reduced[5],
        reduced[6],
        reduced[7],
        reduced[8],
    )


MESH = pl.DeviceIdType.MESH
f32, bf16 = jnp.float32, jnp.bfloat16
VM = pl.BlockSpec(memory_space=pltpu.VMEM)
HB = pl.BlockSpec(memory_space=pl.ANY)


def dma_sems(n):
    return [pltpu.SemaphoreType.DMA((n,)), pltpu.SemaphoreType.DMA((n,))]


class Here:
    def __init__(self, send_sem, recv_sem):
        self.y = lax.axis_index("fsdp")
        blk = lax.axis_index("blk")
        self.x, self.c = blk // 2, blk % 2
        self.z = lax.axis_index("head")
        self.send_sem, self.recv_sem, self.used = send_sem, recv_sem, 0

    def plane(self, i):
        y = 1 - self.y if i & 4 else self.y
        x = 1 - self.x if i & 2 else self.x
        c = 1 - self.c if i & 1 else self.c
        return {"fsdp": y, "blk": x * 2 + c}

    def up(self):
        return {"head": self.z + 1}

    def down(self):
        return {"head": self.z - 1}

    def copy(self, src, dst, device):
        k = self.used
        self.used += 1
        return self.again(k, src, dst, device)

    def slot(self):
        self.used += 1
        return self.used - 1

    def again(self, k, src, dst, device):
        return pltpu.make_async_remote_copy(
            src_ref=src,
            dst_ref=dst,
            send_sem=self.send_sem.at[k],
            recv_sem=self.recv_sem.at[k],
            device_id=device,
            device_id_type=MESH,
        )

    def local(self, src, dst):
        k = self.used
        self.used += 1
        return pltpu.make_async_copy(src, dst, self.send_sem.at[k])

    def enter(self, offsets, along_z=True, all_z=False):
        bar = pltpu.get_barrier_semaphore()
        for i in offsets:
            pl.semaphore_signal(bar, inc=1, device_id=self.plane(i), device_id_type=MESH)
        if all_z:
            for d in (1, 2, 3):
                pl.semaphore_signal(
                    bar, inc=1, device_id={"head": (self.z + d) % 4}, device_id_type=MESH
                )
            pl.semaphore_wait(bar, len(offsets) + 3)
            return
        if along_z:

            @pl.when(self.z > 0)
            def _():
                pl.semaphore_signal(bar, inc=1, device_id=self.down(), device_id_type=MESH)

            @pl.when(self.z < 3)
            def _():
                pl.semaphore_signal(bar, inc=1, device_id=self.up(), device_id_type=MESH)

        peers = len(offsets)
        if along_z:
            peers = peers + jnp.where(self.z > 0, 1, 0) + jnp.where(self.z < 3, 1, 0)
        pl.semaphore_wait(bar, peers)


def drive(*tasks):
    waiting = [(0.0, i, task) for i, task in enumerate(tasks)]
    while waiting:
        waiting.sort(key=lambda item: item[:2])
        _, i, task = waiting.pop(0)
        at = next(task, None)
        if at is not None:
            waiting.append((at, i, task))


def z_gather(me, src, dst, unit, begin=0.0):
    rows = src.shape[0]
    z = me.z

    def block(j):
        return dst.at[pl.ds(pl.multiple_of(j * rows, rows), rows)]

    ups = [me.slot() for _ in range(3)]
    downs = [me.slot() for _ in range(3)]
    if begin:
        yield begin

    @pl.when(z < 3)
    def _():
        me.again(ups[0], src, block(z), me.up()).start()

    @pl.when(z > 0)
    def _():
        me.again(downs[0], src, block(z), me.down()).start()

    own = me.local(src, block(z))
    own.start()
    for j in (1, 2, 3):
        yield begin + unit * j

        @pl.when(z >= j)
        def _():
            me.again(ups[j - 1], block(z - j), block(z - j), me.up()).wait_recv()

        if j < 3:

            @pl.when((z >= j) & (z < 3))
            def _():
                me.again(ups[j], block(z - j), block(z - j), me.up()).start()

        @pl.when(z <= 3 - j)
        def _():
            me.again(downs[j - 1], block(z + j), block(z + j), me.down()).wait_recv()

        if j < 3:

            @pl.when((z <= 3 - j) & (z > 0))
            def _():
                me.again(downs[j], block(z + j), block(z + j), me.down()).start()

    yield begin + unit * 3.2
    own.wait()
    for j in (0, 1, 2):

        @pl.when((z >= j) & (z < 3))
        def _():
            me.again(ups[j], block(z - j), block(z - j), me.up()).wait_send()

        @pl.when((z <= 3 - j) & (z > 0))
        def _():
            me.again(downs[j], block(z + j), block(z + j), me.down()).wait_send()


def plane_gather(me, src, dst, unit, begin=0.0):
    rows = src.shape[0]
    half = rows // 2

    def block(i):
        return dst.at[pl.ds(i * rows, rows)]

    def part(i, h):
        return dst.at[pl.ds(i * rows + h * half, half)]

    if begin:
        yield begin
    to_x = me.copy(src, block(2), me.plane(2))
    to_y = me.copy(src, block(4), me.plane(4))
    to_c = me.copy(src, block(1), me.plane(1))
    own = me.local(src, block(0))
    for copy in (to_x, to_y, to_c, own):
        copy.start()
    yield begin + unit
    to_x.wait_recv()
    x_on = me.copy(part(2, 0), part(6, 0), me.plane(4))
    x_core = me.copy(block(2), block(3), me.plane(1))
    x_on.start()
    x_core.start()
    to_y.wait_recv()
    y_on = me.copy(part(4, 1), part(6, 1), me.plane(2))
    y_core = me.copy(block(4), block(5), me.plane(1))
    y_on.start()
    y_core.start()
    yield begin + unit * 1.5
    x_on.wait_recv()
    d0_core = me.copy(part(6, 0), part(7, 0), me.plane(1))
    d0_core.start()
    y_on.wait_recv()
    d1_core = me.copy(part(6, 1), part(7, 1), me.plane(1))
    d1_core.start()
    yield begin + unit * 1.7
    own.wait()
    for copy in (to_c, x_core, y_core, d0_core, d1_core):
        copy.wait_recv()
    for copy in (to_x, to_y, to_c, x_on, x_core, y_on, y_core, d0_core, d1_core):
        copy.wait_send()


def add_rows(dst, a, b, step=32):
    rows = a.shape[0]

    def body(i, _):
        at = pl.ds(pl.multiple_of(i * step, step), step)
        dst[at, :] = (a[at, :].astype(f32) + b[at, :].astype(f32)).astype(dst.dtype)
        return 0

    lax.fori_loop(0, rows // step, body, 0)


def z_reduce_all(me, part, total, inbox, across, partial, out, unit, chunks=8, begin=0.0):
    rows = part.shape[0] // chunks
    z = me.z
    end = (z == 0) | (z == 3)
    middle = (z == 1) | (z == 2)
    inward = {"head": jnp.where(z < 2, z + 1, z - 1)}
    outward = {"head": jnp.where(z < 2, z - 1, z + 1)}
    first = [me.slot() for _ in range(chunks)]
    second = [me.slot() for _ in range(chunks)]
    third = [me.slot() for _ in range(chunks)]
    store = [me.slot() for _ in range(chunks)]

    def at(ref, k):
        return ref.at[pl.ds(k * rows, rows)]

    def put(k):
        return pltpu.make_async_copy(at(total, k), at(out, k), me.send_sem.at[store[k]])

    if begin:
        yield begin

    @pl.when(end)
    def _():
        for k in range(chunks):
            me.again(first[k], at(part, k), at(inbox, k), inward).start()

    hop = unit / chunks
    for k in range(chunks + 2):
        yield begin + hop * (k + 1) + 2.0

        @pl.when(middle)
        def _():
            if k < chunks:
                me.again(first[k], at(part, k), at(inbox, k), inward).wait_recv()
                add_rows(at(partial, k), at(part, k), at(inbox, k))
                me.again(second[k], at(partial, k), at(across, k), inward).start()
            if 1 <= k <= chunks:
                j = k - 1
                me.again(second[j], at(partial, j), at(across, j), inward).wait_recv()
                add_rows(at(total, j), at(partial, j), at(across, j))
                me.again(third[j], at(total, j), at(total, j), outward).start()
                put(j).start()

        @pl.when(end)
        def _():
            if k >= 2:
                j = k - 2
                me.again(third[j], at(total, j), at(total, j), outward).wait_recv()
                put(j).start()

    yield begin + unit + hop * 3

    @pl.when(end)
    def _():
        for k in range(chunks):
            me.again(first[k], at(part, k), at(inbox, k), inward).wait_send()

    @pl.when(middle)
    def _():
        for k in range(chunks):
            me.again(second[k], at(partial, k), at(across, k), inward).wait_send()
            me.again(third[k], at(total, k), at(total, k), outward).wait_send()

    for k in range(chunks):
        put(k).wait()


def z_reduce_scatter(me, part, from_below, from_above, sums_up, sums_down, own, unit, begin=0.0):
    rows = part.shape[0] // 4
    z = me.z
    ups = [me.slot() for _ in range(4)]
    downs = [me.slot() for _ in range(4)]

    def at(ref, j):
        return ref.at[pl.ds(j * rows, rows)]

    if begin:
        yield begin

    @pl.when(z == 0)
    def _():
        for j in (3, 2, 1):
            me.again(ups[j], at(part, j), at(from_below, j), me.up()).start()

    @pl.when(z == 3)
    def _():
        for j in (0, 1, 2):
            me.again(downs[j], at(part, j), at(from_above, j), me.down()).start()

    for step, j in enumerate((3, 2)):
        for stop in range(1, j):
            yield begin + unit * (3 - j + stop) + 1.0

            @pl.when(z == stop)
            def _():
                me.again(ups[j], at(part, j), at(from_below, j), me.up()).wait_recv()
                add_rows(at(sums_up, j), at(part, j), at(from_below, j))
                me.again(ups[j], at(sums_up, j), at(from_below, j), me.up()).start()

            @pl.when(z == 3 - stop)
            def _():
                i = 3 - j
                me.again(downs[i], at(part, i), at(from_above, i), me.down()).wait_recv()
                add_rows(at(sums_down, i), at(part, i), at(from_above, i))
                me.again(downs[i], at(sums_down, i), at(from_above, i), me.down()).start()

    yield begin + unit * 3 + 1.5
    for j in range(4):

        @pl.when(z == j)
        def _():
            if j > 0:
                me.again(ups[j], at(part, j), at(from_below, j), me.up()).wait_recv()
            if j < 3:
                me.again(downs[j], at(part, j), at(from_above, j), me.down()).wait_recv()

            def body(i, _):
                span = pl.ds(pl.multiple_of(i * 32, 32), 32)
                there = pl.ds(pl.multiple_of(j * rows + i * 32, 32), 32)
                value = part[there, :].astype(f32)
                if j > 0:
                    value = value + from_below[there, :].astype(f32)
                if j < 3:
                    value = value + from_above[there, :].astype(f32)
                own[span, :] = value
                return 0

            lax.fori_loop(0, rows // 32, body, 0)
            for i in range(4):
                if i > j:
                    me.again(ups[i], at(part, i), at(from_below, i), me.up()).wait_send()
                if i < j:
                    me.again(downs[i], at(part, i), at(from_above, i), me.down()).wait_send()


def plane_scatter_scratch(rows, cols):
    half = rows // 2
    return [
        pltpu.VMEM((4, rows, cols), bf16),
        pltpu.VMEM((4, rows, cols), bf16),
        pltpu.VMEM((2, half, cols), bf16),
        pltpu.VMEM((2, half, cols), bf16),
        pltpu.VMEM((half, cols), bf16),
        pltpu.VMEM((half, cols), bf16),
    ]


def plane_scatter(me, src, out, scratch, unit, begin=0.0):
    held, other, over_x, over_y, last_y, last_x = scratch
    rows = out.shape[0]
    half = rows // 2

    def block(i):
        return src.at[pl.ds(i * rows, rows)]

    first, second = pl.ds(0, half), pl.ds(half, half)
    if begin:
        yield begin
    loads, cores = {}, {}
    for i in (6, 2, 4, 0):
        cores[i] = me.copy(block(i + 1), other.at[i // 2], me.plane(1))
        cores[i].start()
        loads[i] = me.local(block(i), held.at[i // 2])
        loads[i].start()
    yield begin + 3.0
    for i in (6, 2, 4, 0):
        loads[i].wait()
        cores[i].wait_recv()
        add_rows(held.at[i // 2], held.at[i // 2], other.at[i // 2])
        if i == 6:
            six_x = me.copy(held.at[3, first], over_x.at[1], me.plane(2))
            six_y = me.copy(held.at[3, second], over_y.at[1], me.plane(4))
            six_x.start()
            six_y.start()
        if i == 2:
            two_x = me.copy(held.at[1, first], over_x.at[0], me.plane(2))
            two_x.start()
        if i == 4:
            four_y = me.copy(held.at[2, second], over_y.at[0], me.plane(4))
            four_y.start()
    yield begin + 4.0 + unit * 0.5
    six_x.wait_recv()
    add_rows(held.at[2, first], held.at[2, first], over_x.at[1])
    to_y = me.copy(held.at[2, first], last_y, me.plane(4))
    to_y.start()
    six_y.wait_recv()
    add_rows(held.at[1, second], held.at[1, second], over_y.at[1])
    to_x = me.copy(held.at[1, second], last_x, me.plane(2))
    to_x.start()
    yield begin + 5.0 + unit * 1.5
    two_x.wait_recv()
    four_y.wait_recv()
    to_y.wait_recv()
    to_x.wait_recv()

    def body(i, _):
        at = pl.ds(pl.multiple_of(i * 32, 32), 32)
        low = pl.ds(pl.multiple_of(half + i * 32, 32), 32)
        out[at, :] = (
            held[0, at, :].astype(f32) + over_x[0, at, :].astype(f32) + last_y[at, :].astype(f32)
        ).astype(out.dtype)
        out[low, :] = (
            held[0, low, :].astype(f32) + over_y[0, at, :].astype(f32) + last_x[at, :].astype(f32)
        ).astype(out.dtype)
        return 0

    lax.fori_loop(0, half // 32, body, 0)
    for i in (6, 2, 4, 0):
        cores[i].wait_send()
    for copy in (six_x, six_y, two_x, four_y, to_y, to_x):
        copy.wait_send()


def params(number, vmem=60 * 2**20):
    return pltpu.CompilerParams(
        collective_id=number, has_side_effects=True, vmem_limit_bytes=vmem
    )


def shape(dims, kind=bf16):
    return jax.ShapeDtypeStruct(dims, kind)


def first_kernel(tok, wqkv, gains, wo, wg, tok_all, wqkv_all, gains_all, wo_all, wg_all, ss, rs):
    me = Here(ss, rs)
    me.enter((1, 2, 4))
    drive(
        z_gather(me, tok, tok_all, 11.3),
        plane_gather(me, wqkv, wqkv_all, 7.0),
        plane_gather(me, gains, gains_all, 7.1),
        plane_gather(me, wo, wo_all, 12.0, 0.1),
        plane_gather(me, wg, wg_all, 27.0, 0.2),
    )


def first(tok, wqkv, gains, wo, wg):
    def grown(a, n):
        return shape((a.shape[0] * n,) + a.shape[1:])

    return pl.pallas_call(
        first_kernel,
        out_shape=(grown(tok, 4), grown(wqkv, 8), grown(gains, 8), grown(wo, 8), grown(wg, 8)),
        in_specs=[VM] * 5,
        out_specs=[HB] * 5,
        scratch_shapes=dma_sems(64),
        compiler_params=params(1),
        name="gather_first",
    )(tok, wqkv, gains, wo, wg)


def attention_forward(me, q_t, kv_own, kv, v_t, key_pos, query_pos, out_t, log_sum, kv_all, per):
    heads, hd, rows = q_t.shape
    blocks = kv.shape[0] // rows

    def block(i):
        return kv.at[pl.ds(i * rows, rows)]

    copies = [me.copy(kv_own, block(i), me.plane(i)) for i in (1, 2, 3)]
    for copy in copies:
        copy.start()
    own = me.local(kv_own, block(0))
    own.start()
    yield 0.2
    own.wait()
    for copy in copies:
        copy.wait_recv()
    save = me.local(kv, kv_all)
    save.start()
    for i in range(blocks):
        v_t[:, i * rows : (i + 1) * rows] = kv[i * rows : (i + 1) * rows, :].astype(f32).T[hd:, :].astype(bf16)

    def head(h, _):
        q = q_t[h]
        limit = query_pos[0:1, :]

        def step(i, state):
            top, total, acc = state
            at = pl.ds(pl.multiple_of(i * rows, rows), rows)
            s = jnp.dot(kv[at, 0:hd], q, preferred_element_type=f32)
            pos = key_pos[at, :]
            pos = jnp.concatenate([pos] * (rows // 128), axis=1)
            s = jnp.where(pos <= limit, s, masked_value)
            new = jnp.maximum(top, jnp.max(s, axis=0, keepdims=True))
            p = jnp.exp(s - new)
            factor = jnp.exp(top - new)
            total = total * factor + jnp.sum(p, axis=0, keepdims=True)
            acc = acc * factor + jnp.dot(v_t[:, at], p.astype(bf16), preferred_element_type=f32)
            return new, total, acc

        top, total, acc = lax.fori_loop(
            0,
            blocks,
            step,
            (
                jnp.full((1, rows), masked_value, f32),
                jnp.zeros((1, rows), f32),
                jnp.zeros((hd, rows), f32),
            ),
        )
        out_t[h] = acc / total
        log_sum[h] = top + jnp.log(total)
        return 0

    for h in range(0, heads, 2):
        yield 6.0 + per * h
        lax.fori_loop(h, h + 2, head, 0)
    yield 6.0 + per * heads
    save.wait()
    for copy in copies:
        copy.wait_send()


def second_kernel(q_t, kv_own, key_pos, query_pos, cot, wu, out_t, log_sum, kv_all, cot_all, wu_all, kv, v_t, ss, rs):
    me = Here(ss, rs)
    me.enter((1, 2, 3, 4))
    drive(
        attention_forward(me, q_t, kv_own, kv, v_t, key_pos, query_pos, out_t, log_sum, kv_all, 3.5),
        z_gather(me, cot, cot_all, 11.3, 0.1),
        plane_gather(me, wu, wu_all, 15.5, 0.3),
    )


def second(q_t, kv_own, key_pos, query_pos, cot, wu):
    heads, hd, rows = q_t.shape
    keys = key_pos.shape[0]
    return pl.pallas_call(
        second_kernel,
        out_shape=(
            shape((heads, hd, rows), f32),
            shape((heads, 1, rows), f32),
            shape((keys, 2 * hd)),
            shape((cot.shape[0] * 4, cot.shape[1])),
            shape((wu.shape[0] * 8, wu.shape[1])),
        ),
        in_specs=[VM] * 6,
        out_specs=[VM, VM, HB, HB, HB],
        scratch_shapes=[pltpu.VMEM((keys, 2 * hd), bf16), pltpu.VMEM((hd, keys), bf16)] + dma_sems(32),
        compiler_params=params(2),
        name="attention_forward",
    )(q_t, kv_own, key_pos, query_pos, cot, wu)


def third_kernel(part, wd, total_out, wd_all, total, inbox, across, partial, ss, rs):
    me = Here(ss, rs)
    me.enter((1, 2, 4))
    drive(
        z_reduce_all(me, part, total, inbox, across, partial, total_out, 45.0),
        plane_gather(me, wd, wd_all, 15.5, 0.1),
    )


def third(part, wd):
    rows = pltpu.VMEM(part.shape, bf16)
    return pl.pallas_call(
        third_kernel,
        out_shape=(shape(part.shape), shape((wd.shape[0] * 8, wd.shape[1]))),
        in_specs=[VM] * 2,
        out_specs=[HB] * 2,
        scratch_shapes=[rows] * 4 + dma_sems(64),
        compiler_params=params(3),
        name="sum_branch",
    )(part, wd)


def fourth_kernel(part, dwd, total_out, dwd_own, total, inbox, across, partial, *rest):
    *scratch, ss, rs = rest
    me = Here(ss, rs)
    me.enter((1, 2, 4))
    drive(
        z_reduce_all(me, part, total, inbox, across, partial, total_out, 45.0),
        plane_scatter(me, dwd, dwd_own, scratch, 15.5, 0.1),
    )


def fourth(part, dwd):
    rows = pltpu.VMEM(part.shape, bf16)
    own = (dwd.shape[0] // 8, dwd.shape[1])
    return pl.pallas_call(
        fourth_kernel,
        out_shape=(shape(part.shape), shape(own, f32)),
        in_specs=[VM, HB],
        out_specs=[HB, VM],
        scratch_shapes=[rows] * 4 + plane_scatter_scratch(*own) + dma_sems(64),
        compiler_params=params(4),
        name="sum_grad_normed_two",
    )(part, dwd)


def attention_backward(me, q_t, q_n, g_t, g_n, kv_all, log_sum, delta, key_pos, query_pos, dq_t, dkv_own, kv, k_t, dk, dv, dkv, came, per):
    heads, hd, rows = q_t.shape
    blocks = kv.shape[0] // rows
    load = me.local(kv_all, kv)
    load.start()
    dk[...] = jnp.zeros_like(dk)
    dv[...] = jnp.zeros_like(dv)
    load.wait()
    for i in range(blocks):
        k_t[:, i * rows : (i + 1) * rows] = kv[i * rows : (i + 1) * rows, :].astype(f32).T[:hd, :].astype(bf16)

    def head(h, _):
        q, g = q_t[h], g_t[h]
        limit = query_pos[0:1, :]

        def step(i, acc):
            at = pl.ds(pl.multiple_of(i * rows, rows), rows)
            both = kv[at, :]
            s = jnp.dot(both[:, 0:hd], q, preferred_element_type=f32)
            pos = key_pos[at, :]
            pos = jnp.concatenate([pos] * (rows // 128), axis=1)
            s = jnp.where(pos <= limit, s, masked_value)
            p = jnp.exp(s - log_sum[h])
            dp = jnp.dot(both[:, hd:], g, preferred_element_type=f32)
            ds = (p * (dp - delta[h])).astype(bf16)
            dv[at, :] += jnp.dot(p.astype(bf16), g_n[h], preferred_element_type=f32)
            dk[at, :] += jnp.dot(ds, q_n[h], preferred_element_type=f32)
            return acc + jnp.dot(k_t[:, at], ds, preferred_element_type=f32)

        acc = lax.fori_loop(0, blocks, step, jnp.zeros((hd, rows), f32))
        dq_t[h] = (acc * (1.0 / math.sqrt(hd))).astype(bf16)
        return 0

    for h in range(0, heads, 2):
        yield 0.3 + per * h
        lax.fori_loop(h, h + 2, head, 0)
    for i in range(blocks):
        at = slice(i * rows, (i + 1) * rows)
        dkv[at, :] = jnp.concatenate([dk[at, :], dv[at, :]], axis=1).astype(bf16)
    copies = [
        me.copy(dkv.at[pl.ds(i * rows, rows)], came.at[i - 1], me.plane(i)) for i in (1, 2, 3)
    ]
    for copy in copies:
        copy.start()
    yield 0.3 + per * heads + 8.0
    for copy in copies:
        copy.wait_recv()
    value = dkv[0:rows, :].astype(f32)
    for i in range(blocks - 1):
        value = value + came[i].astype(f32)
    dkv_own[...] = value
    for copy in copies:
        copy.wait_send()


def fifth_kernel(
    q_t, q_n, g_t, g_n, kv_all, log_sum, delta, key_pos, query_pos, out_part, dwg, dwu,
    dq_t, dkv_own, out_own, dwg_own, dwu_own,
    kv, k_t, dk, dv, dkv, came, below, above, sums_up, sums_down, *rest
):
    *scratch, ss, rs = rest
    me = Here(ss, rs)
    me.enter((1, 2, 3, 4))
    drive(
        plane_scatter(me, dwg, dwg_own, scratch[:6], 15.5),
        plane_scatter(me, dwu, dwu_own, scratch[6:], 15.5, 18.0),
        z_reduce_scatter(me, out_part, below, above, sums_up, sums_down, out_own, 11.3),
        attention_backward(
            me, q_t, q_n, g_t, g_n, kv_all, log_sum, delta, key_pos, query_pos,
            dq_t, dkv_own, kv, k_t, dk, dv, dkv, came, 6.0,
        ),
    )


def fifth(q_t, q_n, g_t, g_n, kv_all, log_sum, delta, key_pos, query_pos, out_part, dwg, dwu):
    heads, hd, rows = q_t.shape
    keys = key_pos.shape[0]
    own = (dwg.shape[0] // 8, dwg.shape[1])
    part = pltpu.VMEM(out_part.shape, bf16)
    return pl.pallas_call(
        fifth_kernel,
        out_shape=(
            shape((heads, hd, rows)),
            shape((rows, 2 * hd), f32),
            shape((out_part.shape[0] // 4, out_part.shape[1]), f32),
            shape(own, f32),
            shape(own, f32),
        ),
        in_specs=[VM] * 4 + [HB] + [VM] * 5 + [HB] * 2,
        out_specs=[VM] * 5,
        scratch_shapes=[
            pltpu.VMEM((keys, 2 * hd), bf16),
            pltpu.VMEM((hd, keys), bf16),
            pltpu.VMEM((keys, hd), f32),
            pltpu.VMEM((keys, hd), f32),
            pltpu.VMEM((keys, 2 * hd), bf16),
            pltpu.VMEM((keys // rows - 1, rows, 2 * hd), bf16),
            part, part, part, part,
        ]
        + plane_scatter_scratch(*own) * 2
        + dma_sems(64),
        compiler_params=params(5),
        name="attention_backward",
    )(q_t, q_n, g_t, g_n, kv_all, log_sum, delta, key_pos, query_pos, out_part, dwg, dwu)


def gain_sums(me, src, out, came, mine, came_z):
    n = src.shape[0] // 8
    copies = [me.copy(src.at[pl.ds(i * 8, 8)], came.at[i - 1], me.plane(i)) for i in range(1, n)]
    for copy in copies:
        copy.start()
    yield 4.0
    value = src[0:8, :]
    for i, copy in enumerate(copies):
        copy.wait_recv()
        value = value + came[i]
    mine[...] = value
    again = [
        me.copy(mine, came_z.at[d - 1], {"head": (me.z + d) % 4}) for d in (1, 2, 3)
    ]
    for copy in again:
        copy.start()
    yield 8.0
    for d, copy in enumerate(again):
        copy.wait_recv()
        value = value + came_z[d]
    out[...] = value
    for copy in copies + again:
        copy.wait_send()


def sixth_kernel(
    part, dwqkv, dwo, gains,
    own, dwq_own, dwkv_all, dwo_own, gains_out,
    below, above, sums_up, sums_down, dwqkv_own, dwkv_own, came_kv, came, mine, came_z, *rest
):
    *scratch, ss, rs = rest
    me = Here(ss, rs)
    me.enter(tuple(range(1, 8)), all_z=True)
    wide = dwq_own.shape[1]

    def weights():
        yield from plane_scatter(me, dwqkv, dwqkv_own, scratch[:6], 7.0, 0.1)
        dwq_own[...] = dwqkv_own[:, :wide]
        dwkv_own[...] = dwqkv_own[:, wide:].astype(bf16)
        copies = [
            me.copy(dwkv_own, came_kv.at[d - 1], {"head": (me.z + d) % 4}) for d in (1, 2, 3)
        ]
        for copy in copies:
            copy.start()
        yield 30.0
        for copy in copies:
            copy.wait_recv()
        dwkv_all[0] = dwkv_own[...]
        for d in (1, 2, 3):
            dwkv_all[d] = came_kv[d - 1]
        for copy in copies:
            copy.wait_send()

    drive(
        gain_sums(me, gains, gains_out, came, mine, came_z),
        z_reduce_scatter(me, part, below, above, sums_up, sums_down, own, 11.3),
        weights(),
        plane_scatter(me, dwo, dwo_own, scratch[6:], 6.0, 9.0),
    )


def sixth(part, dwqkv, dwo, gains):
    rows, cols = dwqkv.shape[0] // 8, dwqkv.shape[1]
    wide = dwo.shape[1]
    whole = pltpu.VMEM(part.shape, bf16)
    return pl.pallas_call(
        sixth_kernel,
        out_shape=(
            shape((part.shape[0] // 4, part.shape[1]), f32),
            shape((rows, wide), f32),
            shape((4, rows, cols - wide)),
            shape((rows, wide), f32),
            shape((8, gains.shape[1]), f32),
        ),
        in_specs=[VM, HB, HB, VM],
        out_specs=[VM] * 5,
        scratch_shapes=[
            whole, whole, whole, whole,
            pltpu.VMEM((rows, cols), f32),
            pltpu.VMEM((rows, cols - wide), bf16),
            pltpu.VMEM((3, rows, cols - wide), bf16),
            pltpu.VMEM((7, 8, gains.shape[1]), f32),
            pltpu.VMEM((8, gains.shape[1]), f32),
            pltpu.VMEM((3, 8, gains.shape[1]), f32),
        ]
        + plane_scatter_scratch(rows, cols)
        + plane_scatter_scratch(rows, wide)
        + dma_sems(64),
        compiler_params=params(6),
        name="scatter_last",
    )(part, dwqkv, dwo, gains)


def local_fast(
    tokens, w_query, w_key, w_value, w_out, w_gate, w_up, w_down, gain_attn, gain_mlp, stretch_order, cotangent
):
    row_count, width = tokens.shape
    groups = 4
    heads = H // groups
    head_rows = row_count * groups
    stretch_rows = head_rows // 2
    cols = width // 8
    contract_last = (((1,), (1,)), ((), ()))
    contract_first = (((0,), (0,)), ((), ()))
    z = lax.axis_index("head")
    b = lax.axis_index("blk")
    place = lax.axis_index("fsdp") * 4 + b
    own_first = z * row_count

    def turn(values):
        return jnp.concatenate(
            [
                lax.dynamic_slice_in_dim(values, jnp.bitwise_xor(place, i) * cols, cols, values.ndim - 1)
                for i in range(8)
            ],
            axis=-1,
        )

    def own_rows(values):
        return lax.dynamic_slice_in_dim(values, own_first, row_count, 0)

    query_positions = stretch_positions(stretch_order, b * head_rows, head_rows, stretch_rows)
    key_positions = jnp.concatenate(
        [
            stretch_positions(stretch_order, jnp.bitwise_xor(b, i) * head_rows, head_rows, stretch_rows)
            for i in range(4)
        ]
    )
    key_pos = jnp.broadcast_to(key_positions[:, None], (key_positions.shape[0], 128))
    query_pos = jnp.broadcast_to(query_positions[None, :], (8, head_rows))
    cos_rows, sin_rows = rope_tables(query_positions, HD)
    cos_t, sin_t = cos_rows.T, sin_rows.T

    def rotate_t(values):
        a, c = values[..., : HD // 2, :], values[..., HD // 2 :, :]
        return jnp.concatenate([a * cos_t - c * sin_t, c * cos_t + a * sin_t], axis=-2)

    def unrotate_t(values):
        a, c = values[..., : HD // 2, :], values[..., HD // 2 :, :]
        return jnp.concatenate([a * cos_t + c * sin_t, c * cos_t - a * sin_t], axis=-2)

    slot_first = z * HD
    w_qkv = jnp.concatenate(
        [
            w_query,
            lax.dynamic_slice_in_dim(w_key, slot_first, HD, 1),
            lax.dynamic_slice_in_dim(w_value, slot_first, HD, 1),
        ],
        axis=1,
    )
    gains = jnp.concatenate([gain_attn[None], gain_mlp[None], jnp.zeros((30, cols), bf16)])
    tok_all, wqkv_all, gains_all, wo_all, wg_all = first(tokens, w_qkv, gains, w_out, w_gate)
    gains_all = gains_all.reshape(8, 32, cols)
    gain_one = gains_all[:, 0].reshape(width).astype(f32)
    gain_two = gains_all[:, 1].reshape(width).astype(f32)

    x_rows = turn(tok_all).astype(f32)
    inv_attn = lax.rsqrt(jnp.mean(x_rows * x_rows, axis=-1, keepdims=True) + norm_epsilon)
    normed = (x_rows * inv_attn * gain_one).astype(bf16)
    qkv_t = lax.dot_general(wqkv_all, normed, (((0,), (1,)), ((), ())), preferred_element_type=f32)
    wide = heads * HD
    q_t = rotate_t(qkv_t[:wide].reshape(heads, HD, head_rows)).astype(bf16) * bf16(1.0 / math.sqrt(HD))
    k_t = rotate_t(qkv_t[wide : wide + HD]).astype(bf16)
    v_t = qkv_t[wide + HD :].astype(bf16)
    kv_own = jnp.concatenate([k_t, v_t], axis=0).T
    out_t, log_sum, kv_all, cot_all, wu_all = second(q_t, kv_own, key_pos, query_pos, cotangent, w_up)
    attended_t = out_t.astype(bf16).reshape(wide, head_rows)
    branch_part = lax.dot_general(
        attended_t, wo_all, (((0,), (1,)), ((), ())), preferred_element_type=f32
    ).astype(bf16)
    branch, wd_all = third(branch_part, w_down)

    hidden_rows = x_rows + branch.astype(f32)
    inv_mlp = lax.rsqrt(jnp.mean(hidden_rows * hidden_rows, axis=-1, keepdims=True) + norm_epsilon)
    normed_two = (hidden_rows * inv_mlp * gain_two).astype(bf16)
    gate = jnp.dot(normed_two, wg_all, preferred_element_type=f32)
    up = jnp.dot(normed_two, wu_all, preferred_element_type=f32)
    gate_sigmoid = jax.nn.sigmoid(gate)
    gate_silu = gate * gate_sigmoid
    hidden = (gate_silu * up).astype(bf16)
    out_part = lax.dot_general(hidden, wd_all, contract_last, preferred_element_type=f32).astype(bf16)

    cot_rows = turn(cot_all)
    grad_hidden = jnp.dot(cot_rows, wd_all, preferred_element_type=f32)
    d_gate = (grad_hidden * up * gate_sigmoid * (1.0 + gate * (1.0 - gate_sigmoid))).astype(bf16)
    d_up = (grad_hidden * gate_silu).astype(bf16)
    two_part = lax.dot_general(d_gate, wg_all, contract_last, preferred_element_type=f32)
    two_part = two_part + lax.dot_general(d_up, wu_all, contract_last, preferred_element_type=f32)
    dwd = lax.dot_general(cot_rows, hidden, contract_first, preferred_element_type=f32).astype(bf16)
    dwg = lax.dot_general(normed_two, d_gate, contract_first, preferred_element_type=f32).astype(bf16)
    dwu = lax.dot_general(normed_two, d_up, contract_first, preferred_element_type=f32).astype(bf16)
    grad_two, dwd_own = fourth(two_part.astype(bf16), dwd)

    grad_two = grad_two.astype(f32)
    grad_hidden_rows = cot_rows.astype(f32) + norm_input_grad(hidden_rows, inv_mlp, gain_two, grad_two)
    grad_low = grad_hidden_rows.astype(bf16)
    g_t = lax.dot_general(wo_all, grad_low, (((0,), (1,)), ((), ())), preferred_element_type=f32)
    g_t = g_t.astype(bf16).reshape(heads, HD, head_rows)
    dwo = lax.dot_general(
        grad_low, attended_t, (((0,), (1,)), ((), ())), preferred_element_type=f32
    ).astype(bf16)
    delta = jnp.sum(g_t.astype(f32) * out_t, axis=1, keepdims=True)
    q_n = q_t.transpose(0, 2, 1)
    g_n = g_t.transpose(0, 2, 1)
    dq_t, dkv, out_own, dwg_own, dwu_own = fifth(
        q_t, q_n, g_t, g_n, kv_all, log_sum, delta, key_pos, query_pos, out_part, dwg, dwu
    )

    dkv_t = dkv.T.astype(bf16).astype(f32)
    dqkv_t = jnp.concatenate(
        [
            unrotate_t(dq_t.astype(f32)).reshape(wide, head_rows).astype(bf16),
            unrotate_t(dkv_t[:HD]).astype(bf16),
            dkv_t[HD:].astype(bf16),
        ]
    )
    one_part = lax.dot_general(dqkv_t, wqkv_all, (((0,), (1,)), ((), ())), preferred_element_type=f32)
    dwqkv = lax.dot_general(
        normed, dqkv_t, (((0,), (1,)), ((), ())), preferred_element_type=f32
    ).astype(bf16)
    gain_one_part = jnp.sum(one_part * (x_rows * inv_attn), axis=0).reshape(8, 1, cols)
    gain_two_part = jnp.sum(
        own_rows(grad_two) * own_rows(hidden_rows) * own_rows(inv_mlp), axis=0
    ).reshape(8, 1, cols)
    gain_parts = jnp.concatenate(
        [gain_one_part, gain_two_part, jnp.zeros((8, 6, cols), f32)], axis=1
    ).reshape(64, cols)
    grad_one, dwq_own, dwkv_all, dwo_own, gain_grads = sixth(one_part.astype(bf16), dwqkv, dwo, gain_parts)

    layer_low = turn((own_rows(hidden_rows) + out_own).astype(bf16))
    x_own = own_rows(x_rows)
    grad_tokens = own_rows(grad_hidden_rows) + norm_input_grad(x_own, own_rows(inv_attn), gain_one, grad_one)
    grad_tokens = turn(grad_tokens.astype(bf16))
    slots = jnp.concatenate(
        [lax.dynamic_slice_in_dim(dwkv_all, (z - j) % 4, 1, 0) for j in range(4)], axis=0
    ).astype(f32)
    grad_key = slots[:, :, :HD].transpose(1, 0, 2).reshape(cols, groups * HD)
    grad_value = slots[:, :, HD:].transpose(1, 0, 2).reshape(cols, groups * HD)
    return (
        layer_low,
        grad_tokens,
        dwq_own,
        grad_key,
        grad_value,
        dwo_own,
        dwg_own,
        dwu_own,
        dwd_own,
        gain_grads[0],
        gain_grads[1],
    )


def solution(mesh):
    sizes = (mesh.shape["fsdp"], mesh.shape["blk"], mesh.shape["head"])
    return jax.shard_map(
        local_fast if sizes == (2, 4, 4) else local,
        mesh=mesh,
        in_specs=(
            P(("fsdp", "blk", "head"), None),
            P(("fsdp", "blk"), "head"),
            P(("fsdp", "blk"), None),
            P(("fsdp", "blk"), None),
            P(("fsdp", "blk"), "head"),
            P(("fsdp", "blk"), "head"),
            P(("fsdp", "blk"), "head"),
            P(("fsdp", "blk"), "head"),
            P(("fsdp", "blk")),
            P(("fsdp", "blk")),
            P(),
            P(("fsdp", "blk", "head"), None),
        ),
        out_specs=(
            P(("fsdp", "blk", "head"), None),
            P(("fsdp", "blk", "head"), None),
            P(("fsdp", "blk"), "head"),
            P(("fsdp", "blk"), None),
            P(("fsdp", "blk"), None),
            P(("fsdp", "blk"), "head"),
            P(("fsdp", "blk"), "head"),
            P(("fsdp", "blk"), "head"),
            P(("fsdp", "blk"), "head"),
            P(("fsdp", "blk")),
            P(("fsdp", "blk")),
        ),
        check_vma=False,
    )
```

```python
import math

import jax
import jax.numpy as jnp
from jax import lax
from jax.experimental import pallas as pl
from jax.experimental.pallas import tpu as pltpu
from jax.sharding import PartitionSpec as P

H = 32
KV = 4
HD = 64


norm_epsilon = 1e-05
rope_base = 10000.0
masked_value = -1e30


def rope_tables(positions, head_dim):
    half_dim = head_dim // 2
    frequency = rope_base ** (-(jnp.arange(half_dim, dtype=jnp.float32) * (2.0 / head_dim)))
    angles = positions.astype(jnp.float32)[:, None] * frequency[None, :]
    return (jnp.cos(angles), jnp.sin(angles))


def rotate(values, cosine, sine_table):
    half_dim = values.shape[-1] // 2
    first_half = values[..., :half_dim]
    second_half = values[..., half_dim:]
    cos_rows = cosine[:, None, :]
    sin_rows = sine_table[:, None, :]
    return jnp.concatenate(
        [
            first_half * cos_rows - second_half * sin_rows,
            second_half * cos_rows + first_half * sin_rows,
        ],
        axis=-1,
    )


def unrotate(values, cosine, sine_table):
    half_dim = values.shape[-1] // 2
    first_half = values[..., :half_dim]
    second_half = values[..., half_dim:]
    cos_rows = cosine[:, None, :]
    sin_rows = sine_table[:, None, :]
    return jnp.concatenate(
        [
            first_half * cos_rows + second_half * sin_rows,
            second_half * cos_rows - first_half * sin_rows,
        ],
        axis=-1,
    )


def stretch_positions(stretch_order, first_row, row_span, stretch_rows):
    storage = first_row + jnp.arange(row_span, dtype=jnp.int32)
    stretch_index = storage // stretch_rows
    match_table = (
        stretch_index[:, None] == jnp.arange(stretch_order.shape[0], dtype=jnp.int32)[None, :]
    )
    stretch_base = jnp.sum(jnp.where(match_table, stretch_order[None, :], 0), axis=1)
    return stretch_base * stretch_rows + storage % stretch_rows


def norm_input_grad(values, inverse, gain_vector, grad_normed):
    scaled = grad_normed * gain_vector
    inner = jnp.mean(scaled * values, axis=-1, keepdims=True)
    return inverse * scaled - values * inverse * inverse * inverse * inner


def gain_grad(values, inverse, grad_normed):
    return jnp.sum(grad_normed * values * inverse, axis=0)


def fold_block(
    state_now, keys_block, values_block, key_positions, query_heads, query_positions, score_scale
):
    running_max, running_sum, running_out = state_now
    scores = (
        jnp.einsum("qhd,kd->hqk", query_heads, keys_block, preferred_element_type=jnp.float32)
        * score_scale
    )
    allowed = (query_positions[:, None] >= key_positions[None, :])[None]
    scores = jnp.where(allowed, scores, masked_value)
    new_max = jnp.maximum(running_max, jnp.max(scores, axis=-1))
    weights = jnp.where(allowed, jnp.exp(scores - new_max[..., None]), 0.0)
    factor = jnp.exp(running_max - new_max)
    running_sum = running_sum * factor + jnp.sum(weights, axis=-1)
    running_out = running_out * factor[..., None] + jnp.einsum(
        "hqk,kd->hqd",
        weights.astype(jnp.bfloat16),
        values_block,
        preferred_element_type=jnp.float32,
    )
    return (new_max, running_sum, running_out)


def local(
    tokens,
    w_query,
    w_key,
    w_value,
    w_out,
    w_gate,
    w_up,
    w_down,
    gain_attn,
    gain_mlp,
    stretch_order,
    cotangent,
):
    row_count = tokens.shape[0]
    groups = lax.axis_size("head")
    blocks = lax.axis_size("blk")
    local_heads = H // groups
    repeats = groups // KV
    head_rows = row_count * groups
    stretch_rows = head_rows // 2
    score_scale = 1.0 / math.sqrt(HD)
    contract_last = (((1,), (1,)), ((), ()))
    contract_first = (((0,), (0,)), ((), ()))
    head_index = lax.axis_index("head")
    own_first = head_index * row_count
    block_first = lax.axis_index("blk") * head_rows
    positions = stretch_positions(stretch_order, block_first + own_first, row_count, stretch_rows)
    query_positions = stretch_positions(stretch_order, block_first, head_rows, stretch_rows)
    cos_own, sin_own = rope_tables(positions, HD)
    cos_block, sin_block = rope_tables(query_positions, HD)

    def layer_weights():
        return (
            lax.all_gather(w_query, ("fsdp", "blk"), axis=0, tiled=True),
            lax.all_gather(w_key, ("fsdp", "blk"), axis=0, tiled=True),
            lax.all_gather(w_value, ("fsdp", "blk"), axis=0, tiled=True),
            lax.all_gather(w_out, ("fsdp", "blk"), axis=0, tiled=True),
            lax.all_gather(w_gate, ("fsdp", "blk"), axis=0, tiled=True),
            lax.all_gather(w_up, ("fsdp", "blk"), axis=0, tiled=True),
            lax.all_gather(w_down, ("fsdp", "blk"), axis=0, tiled=True),
            lax.all_gather(gain_attn, ("fsdp", "blk"), axis=0, tiled=True),
            lax.all_gather(gain_mlp, ("fsdp", "blk"), axis=0, tiled=True),
        )

    def gather_query(columns):
        return lax.all_gather(columns, "head", axis=1, tiled=True)

    (
        query_cols,
        key_full,
        value_full,
        out_cols,
        gate_cols,
        up_cols,
        down_cols,
        gain_one,
        gain_two,
    ) = layer_weights()
    tokens_float = tokens.astype(jnp.float32)
    inv_attn = lax.rsqrt(
        jnp.mean(tokens_float * tokens_float, axis=-1, keepdims=True) + norm_epsilon
    )
    normed = (tokens_float * inv_attn * gain_one.astype(jnp.float32)).astype(jnp.bfloat16)
    normed_rows, cotangent_rows = (
        lax.all_gather(normed, "head", axis=0, tiled=True),
        lax.all_gather(cotangent, "head", axis=0, tiled=True),
    )
    query_all = gather_query(query_cols)
    query_lin = jnp.dot(normed, query_all, preferred_element_type=jnp.float32).reshape(
        row_count, H, HD
    )
    key_lin = jnp.dot(normed, key_full, preferred_element_type=jnp.float32).reshape(
        row_count, KV, HD
    )
    value_lin = jnp.dot(normed, value_full, preferred_element_type=jnp.float32).reshape(
        row_count, KV, HD
    )
    query_rot = rotate(query_lin, cos_own, sin_own).astype(jnp.bfloat16).reshape(row_count, H * HD)
    key_rot = rotate(key_lin, cos_own, sin_own).astype(jnp.bfloat16)
    key_slots = jnp.repeat(key_rot, repeats, axis=1).reshape(row_count, groups * HD)
    value_slots = jnp.repeat(value_lin.astype(jnp.bfloat16), repeats, axis=1).reshape(
        row_count, groups * HD
    )
    query_recv, key_own, value_own = (
        lax.all_to_all(query_rot, "head", split_axis=1, concat_axis=0, tiled=True),
        lax.all_to_all(key_slots, "head", split_axis=1, concat_axis=0, tiled=True),
        lax.all_to_all(value_slots, "head", split_axis=1, concat_axis=0, tiled=True),
    )
    query_heads = query_recv.reshape(head_rows, local_heads, HD)
    initial = (
        jnp.full((local_heads, head_rows), masked_value, jnp.float32),
        jnp.zeros((local_heads, head_rows), jnp.float32),
        jnp.zeros((local_heads, head_rows, HD), jnp.float32),
    )
    state_now = initial
    keys_piece = lax.all_gather(key_own, "blk", axis=0, tiled=True)
    values_piece = lax.all_gather(value_own, "blk", axis=0, tiled=True)
    piece_rows = keys_piece.shape[0]

    def scan_step(state_inner, step_index):
        offset = step_index * head_rows
        keys_block = lax.dynamic_slice_in_dim(keys_piece, offset, head_rows, 0)
        values_block = lax.dynamic_slice_in_dim(values_piece, offset, head_rows, 0)
        key_positions = stretch_positions(stretch_order, offset, head_rows, stretch_rows)
        return (
            fold_block(
                state_inner,
                keys_block,
                values_block,
                key_positions,
                query_heads,
                query_positions,
                score_scale,
            ),
            None,
        )

    state_now, unused = lax.scan(
        scan_step, state_now, jnp.arange(piece_rows // head_rows, dtype=jnp.int32)
    )
    running_max, running_sum, running_out = state_now
    attended_float = running_out / running_sum[..., None]
    log_sum = running_max + jnp.log(running_sum)
    attended_heads = (
        attended_float.astype(jnp.bfloat16).transpose(1, 0, 2).reshape(head_rows, local_heads * HD)
    )
    branch = lax.dot_general(
        attended_heads, out_cols, contract_last, preferred_element_type=jnp.float32
    )
    own_branch = lax.dynamic_slice_in_dim(branch, own_first, row_count, 0)
    partial_value = lax.dynamic_update_slice_in_dim(branch, own_branch + tokens_float, own_first, 0)
    hidden_rows = lax.psum(partial_value.astype(jnp.bfloat16), "head").astype(jnp.float32)
    inv_mlp = lax.rsqrt(jnp.mean(hidden_rows * hidden_rows, axis=-1, keepdims=True) + norm_epsilon)
    normed_two_rows = (hidden_rows * inv_mlp * gain_two.astype(jnp.float32)).astype(jnp.bfloat16)
    gate_proj = jnp.dot(normed_two_rows, gate_cols, preferred_element_type=jnp.float32)
    up_proj = jnp.dot(normed_two_rows, up_cols, preferred_element_type=jnp.float32)
    gate_sigmoid = jax.nn.sigmoid(gate_proj)
    gate_silu = gate_proj * gate_sigmoid
    hidden = (gate_silu * up_proj).astype(jnp.bfloat16)
    hidden_own = lax.dynamic_slice_in_dim(hidden_rows, own_first, row_count, 0)
    output_float = hidden_own + lax.psum_scatter(
        lax.dot_general(
            hidden, down_cols, contract_last, preferred_element_type=jnp.float32
        ).astype(jnp.bfloat16),
        "head",
        scatter_dimension=0,
        tiled=True,
    ).astype(jnp.float32)
    layer_low = output_float.astype(jnp.bfloat16)
    (
        query_cols,
        key_full,
        value_full,
        out_cols,
        gate_cols,
        up_cols,
        down_cols,
        gain_one,
        gain_two,
    ) = layer_weights()
    query_all = gather_query(query_cols)
    grad_hidden = jnp.dot(cotangent_rows, down_cols, preferred_element_type=jnp.float32)
    grad_gate_rows = (
        grad_hidden * up_proj * gate_sigmoid * (1.0 + gate_proj * (1.0 - gate_sigmoid))
    ).astype(jnp.bfloat16)
    grad_up_rows = (grad_hidden * gate_silu).astype(jnp.bfloat16)
    grad_w_down = lax.dot_general(
        cotangent_rows, hidden, contract_first, preferred_element_type=jnp.float32
    )
    grad_w_gate = lax.dot_general(
        normed_two_rows, grad_gate_rows, contract_first, preferred_element_type=jnp.float32
    )
    grad_w_up = lax.dot_general(
        normed_two_rows, grad_up_rows, contract_first, preferred_element_type=jnp.float32
    )
    normed_two_part = lax.dot_general(
        grad_gate_rows, gate_cols, contract_last, preferred_element_type=jnp.float32
    )
    normed_two_part = normed_two_part + lax.dot_general(
        grad_up_rows, up_cols, contract_last, preferred_element_type=jnp.float32
    )
    grad_normed_two = lax.psum(normed_two_part.astype(jnp.bfloat16), "head").astype(jnp.float32)
    gain_two_float = gain_two.astype(jnp.float32)
    grad_hidden_rows = cotangent_rows.astype(jnp.float32) + norm_input_grad(
        hidden_rows, inv_mlp, gain_two_float, grad_normed_two
    )
    own_grad_two = lax.dynamic_slice_in_dim(grad_normed_two, own_first, row_count, 0)
    own_inv_mlp = lax.dynamic_slice_in_dim(inv_mlp, own_first, row_count, 0)
    grad_gain_two = gain_grad(hidden_own, own_inv_mlp, own_grad_two)
    grad_low_rows = grad_hidden_rows.astype(jnp.bfloat16)
    grad_w_out = lax.dot_general(
        grad_low_rows, attended_heads, contract_first, preferred_element_type=jnp.float32
    )
    grad_heads = (
        jnp.dot(grad_low_rows, out_cols, preferred_element_type=jnp.float32)
        .astype(jnp.bfloat16)
        .reshape(head_rows, local_heads, HD)
    )
    keys_all, values_all = (
        lax.all_gather(key_own, "blk", axis=0, tiled=True),
        lax.all_gather(value_own, "blk", axis=0, tiled=True),
    )
    row_delta = jnp.sum(grad_heads.astype(jnp.float32).transpose(1, 0, 2) * attended_float, axis=-1)

    def back_block(grad_query_acc, block_index):
        offset = block_index * head_rows
        keys_block = lax.dynamic_slice_in_dim(keys_all, offset, head_rows, 0)
        values_block = lax.dynamic_slice_in_dim(values_all, offset, head_rows, 0)
        key_positions = stretch_positions(stretch_order, offset, head_rows, stretch_rows)
        scores = (
            jnp.einsum("qhd,kd->hqk", query_heads, keys_block, preferred_element_type=jnp.float32)
            * score_scale
        )
        allowed = (query_positions[:, None] >= key_positions[None, :])[None]
        probs_block = jnp.where(allowed, jnp.exp(scores - log_sum[..., None]), 0.0)
        grad_probs = jnp.einsum(
            "qhd,kd->hqk", grad_heads, values_block, preferred_element_type=jnp.float32
        )
        grad_scores = (probs_block * (grad_probs - row_delta[..., None])).astype(jnp.bfloat16)
        grad_query_acc = grad_query_acc + jnp.einsum(
            "hqk,kd->qhd", grad_scores, keys_block, preferred_element_type=jnp.float32
        )
        grad_key_part = (
            jnp.einsum("hqk,qhd->kd", grad_scores, query_heads, preferred_element_type=jnp.float32)
            * score_scale
        )
        grad_value_part = jnp.einsum(
            "hqk,qhd->kd",
            probs_block.astype(jnp.bfloat16),
            grad_heads,
            preferred_element_type=jnp.float32,
        )
        return (grad_query_acc, (grad_key_part, grad_value_part))

    grad_query_acc, (key_terms, value_terms) = lax.scan(
        back_block,
        jnp.zeros((head_rows, local_heads, HD), jnp.float32),
        jnp.arange(blocks, dtype=jnp.int32),
    )
    grad_key_sum, grad_value_sum = (
        lax.psum_scatter(
            key_terms.reshape(blocks * head_rows, HD).astype(jnp.bfloat16),
            "blk",
            scatter_dimension=0,
            tiled=True,
        ).astype(jnp.float32),
        lax.psum_scatter(
            value_terms.reshape(blocks * head_rows, HD).astype(jnp.bfloat16),
            "blk",
            scatter_dimension=0,
            tiled=True,
        ).astype(jnp.float32),
    )
    grad_query_rot = (grad_query_acc * score_scale).astype(jnp.bfloat16)
    grad_query_lin_heads = (
        unrotate(grad_query_rot.astype(jnp.float32), cos_block, sin_block)
        .astype(jnp.bfloat16)
        .reshape(head_rows, local_heads * HD)
    )
    key_slot_grad = grad_key_sum.astype(jnp.bfloat16)
    value_slot_grad = grad_value_sum.astype(jnp.bfloat16)
    grad_w_query = lax.dot_general(
        normed_rows, grad_query_lin_heads, contract_first, preferred_element_type=jnp.float32
    )
    query_back, key_back, value_back = (
        lax.all_to_all(grad_query_lin_heads, "head", split_axis=0, concat_axis=1, tiled=True),
        lax.all_to_all(key_slot_grad, "head", split_axis=0, concat_axis=1, tiled=True),
        lax.all_to_all(value_slot_grad, "head", split_axis=0, concat_axis=1, tiled=True),
    )
    key_slot_lin = (
        unrotate(key_back.astype(jnp.float32).reshape(row_count, groups, HD), cos_own, sin_own)
        .astype(jnp.bfloat16)
        .reshape(row_count, KV, repeats, HD)
    )
    value_slot_lin = value_back.reshape(row_count, KV, repeats, HD)
    grad_w_key = jnp.einsum(
        "td,tjrc->djc", normed, key_slot_lin, preferred_element_type=jnp.float32
    ).reshape(-1, KV * HD)
    grad_w_value = jnp.einsum(
        "td,tjrc->djc", normed, value_slot_lin, preferred_element_type=jnp.float32
    ).reshape(-1, KV * HD)
    grad_normed = lax.dot_general(
        query_back, query_all, contract_last, preferred_element_type=jnp.float32
    )
    grad_normed = grad_normed + jnp.einsum(
        "tjrc,djc->td",
        key_slot_lin,
        key_full.reshape(-1, KV, HD),
        preferred_element_type=jnp.float32,
    )
    grad_normed = grad_normed + jnp.einsum(
        "tjrc,djc->td",
        value_slot_lin,
        value_full.reshape(-1, KV, HD),
        preferred_element_type=jnp.float32,
    )
    gain_one_float = gain_one.astype(jnp.float32)
    grad_input_norm = norm_input_grad(tokens_float, inv_attn, gain_one_float, grad_normed)
    grad_gain_one = gain_grad(tokens_float, inv_attn, grad_normed)
    grad_hidden_own = lax.dynamic_slice_in_dim(grad_hidden_rows, own_first, row_count, 0)
    grad_tokens = (grad_hidden_own + grad_input_norm).astype(jnp.bfloat16)
    head_sums = (
        lax.psum(grad_w_key.astype(jnp.bfloat16), "head").astype(jnp.float32),
        lax.psum(grad_w_value.astype(jnp.bfloat16), "head").astype(jnp.float32),
        lax.psum(grad_gain_one.astype(jnp.bfloat16), "head").astype(jnp.float32),
        lax.psum(grad_gain_two.astype(jnp.bfloat16), "head").astype(jnp.float32),
    )
    reduced = (
        lax.psum_scatter(
            grad_w_query.astype(jnp.bfloat16), ("fsdp", "blk"), scatter_dimension=0, tiled=True
        ).astype(jnp.float32),
        lax.psum_scatter(
            head_sums[0].astype(jnp.bfloat16), ("fsdp", "blk"), scatter_dimension=0, tiled=True
        ).astype(jnp.float32),
        lax.psum_scatter(
            head_sums[1].astype(jnp.bfloat16), ("fsdp", "blk"), scatter_dimension=0, tiled=True
        ).astype(jnp.float32),
        lax.psum_scatter(
            grad_w_out.astype(jnp.bfloat16), ("fsdp", "blk"), scatter_dimension=0, tiled=True
        ).astype(jnp.float32),
        lax.psum_scatter(
            grad_w_gate.astype(jnp.bfloat16), ("fsdp", "blk"), scatter_dimension=0, tiled=True
        ).astype(jnp.float32),
        lax.psum_scatter(
            grad_w_up.astype(jnp.bfloat16), ("fsdp", "blk"), scatter_dimension=0, tiled=True
        ).astype(jnp.float32),
        lax.psum_scatter(
            grad_w_down.astype(jnp.bfloat16), ("fsdp", "blk"), scatter_dimension=0, tiled=True
        ).astype(jnp.float32),
        lax.psum_scatter(
            head_sums[2].astype(jnp.bfloat16), ("fsdp", "blk"), scatter_dimension=0, tiled=True
        ).astype(jnp.float32),
        lax.psum_scatter(
            head_sums[3].astype(jnp.bfloat16), ("fsdp", "blk"), scatter_dimension=0, tiled=True
        ).astype(jnp.float32),
    )
    return (
        layer_low,
        grad_tokens,
        reduced[0],
        reduced[1],
        reduced[2],
        reduced[3],
        reduced[4],
        reduced[5],
        reduced[6],
        reduced[7],
        reduced[8],
    )


MESH = pl.DeviceIdType.MESH
f32, bf16 = jnp.float32, jnp.bfloat16
VM = pl.BlockSpec(memory_space=pltpu.VMEM)
HB = pl.BlockSpec(memory_space=pl.ANY)


def dma_sems(n):
    return [pltpu.SemaphoreType.DMA((n,)), pltpu.SemaphoreType.DMA((n,))]


class Here:
    def __init__(self, send_sem, recv_sem):
        self.y = lax.axis_index("fsdp")
        blk = lax.axis_index("blk")
        self.x, self.c = blk // 2, blk % 2
        self.z = lax.axis_index("head")
        self.send_sem, self.recv_sem, self.used = send_sem, recv_sem, 0

    def plane(self, i):
        y = 1 - self.y if i & 4 else self.y
        x = 1 - self.x if i & 2 else self.x
        c = 1 - self.c if i & 1 else self.c
        return {"fsdp": y, "blk": x * 2 + c}

    def number(self, i):
        at = self.plane(i)
        return at["fsdp"] * 4 + at["blk"]

    def up(self):
        return {"head": self.z + 1}

    def down(self):
        return {"head": self.z - 1}

    def copy(self, src, dst, device):
        k = self.used
        self.used += 1
        return self.again(k, src, dst, device)

    def slot(self):
        self.used += 1
        return self.used - 1

    def again(self, k, src, dst, device):
        return pltpu.make_async_remote_copy(
            src_ref=src,
            dst_ref=dst,
            send_sem=self.send_sem.at[k],
            recv_sem=self.recv_sem.at[k],
            device_id=device,
            device_id_type=MESH,
        )

    def local(self, src, dst):
        k = self.used
        self.used += 1
        return pltpu.make_async_copy(src, dst, self.send_sem.at[k])

    def enter(self, offsets, along_z=True, all_z=False):
        bar = pltpu.get_barrier_semaphore()
        for i in offsets:
            pl.semaphore_signal(bar, inc=1, device_id=self.plane(i), device_id_type=MESH)
        if all_z:
            for d in (1, 2, 3):
                pl.semaphore_signal(
                    bar, inc=1, device_id={"head": (self.z + d) % 4}, device_id_type=MESH
                )
            pl.semaphore_wait(bar, len(offsets) + 3)
            return
        if along_z:

            @pl.when(self.z > 0)
            def _():
                pl.semaphore_signal(bar, inc=1, device_id=self.down(), device_id_type=MESH)

            @pl.when(self.z < 3)
            def _():
                pl.semaphore_signal(bar, inc=1, device_id=self.up(), device_id_type=MESH)

        peers = len(offsets)
        if along_z:
            peers = peers + jnp.where(self.z > 0, 1, 0) + jnp.where(self.z < 3, 1, 0)
        pl.semaphore_wait(bar, peers)


def drive(*tasks):
    waiting = [(0.0, i, task) for i, task in enumerate(tasks)]
    while waiting:
        waiting.sort(key=lambda item: item[:2])
        _, i, task = waiting.pop(0)
        at = next(task, None)
        if at is not None:
            waiting.append((at, i, task))


def z_gather(me, src, dst, unit, begin=0.0):
    rows = src.shape[0]
    z = me.z

    def block(j):
        return dst.at[pl.ds(pl.multiple_of(j * rows, rows), rows)]

    ups = [me.slot() for _ in range(3)]
    downs = [me.slot() for _ in range(3)]
    if begin:
        yield begin

    @pl.when(z < 3)
    def _():
        me.again(ups[0], src, block(z), me.up()).start()

    @pl.when(z > 0)
    def _():
        me.again(downs[0], src, block(z), me.down()).start()

    own = me.local(src, block(z))
    own.start()
    for j in (1, 2, 3):
        yield begin + unit * j

        @pl.when(z >= j)
        def _():
            me.again(ups[j - 1], block(z - j), block(z - j), me.up()).wait_recv()

        if j < 3:

            @pl.when((z >= j) & (z < 3))
            def _():
                me.again(ups[j], block(z - j), block(z - j), me.up()).start()

        @pl.when(z <= 3 - j)
        def _():
            me.again(downs[j - 1], block(z + j), block(z + j), me.down()).wait_recv()

        if j < 3:

            @pl.when((z <= 3 - j) & (z > 0))
            def _():
                me.again(downs[j], block(z + j), block(z + j), me.down()).start()

    yield begin + unit * 3.2
    own.wait()
    for j in (0, 1, 2):

        @pl.when((z >= j) & (z < 3))
        def _():
            me.again(ups[j], block(z - j), block(z - j), me.up()).wait_send()

        @pl.when((z <= 3 - j) & (z > 0))
        def _():
            me.again(downs[j], block(z + j), block(z + j), me.down()).wait_send()


def plane_gather(me, src, dst, unit, begin=0.0):
    rows = src.shape[0]
    half = rows // 2

    def block(i):
        return dst.at[pl.ds(pl.multiple_of(me.number(i) * rows, rows), rows)]

    def part(i, h):
        return dst.at[pl.ds(pl.multiple_of(me.number(i) * rows + h * half, half), half)]

    if begin:
        yield begin
    heads = src.at[pl.ds(0, half)], src.at[pl.ds(half, half)]
    x_in, y_in = [], []
    for h in (0, 1):
        x_in.append(me.copy(heads[h], part(0, h), me.plane(2)))
        x_in[h].start()
        y_in.append(me.copy(heads[1 - h], part(0, 1 - h), me.plane(4)))
        y_in[h].start()
    to_c = me.copy(src, block(0), me.plane(1))
    own = me.local(src, block(0))
    to_c.start()
    own.start()
    yield begin + unit * 0.5
    x_in[0].wait_recv()
    x_on = me.copy(part(2, 0), part(2, 0), me.plane(4))
    x_on.start()
    y_in[0].wait_recv()
    y_on = me.copy(part(4, 1), part(4, 1), me.plane(2))
    y_on.start()
    yield begin + unit
    x_in[1].wait_recv()
    x_core = me.copy(block(2), block(2), me.plane(1))
    x_core.start()
    y_in[1].wait_recv()
    y_core = me.copy(block(4), block(4), me.plane(1))
    y_core.start()
    yield begin + unit * 1.5
    x_on.wait_recv()
    d0_core = me.copy(part(6, 0), part(6, 0), me.plane(1))
    d0_core.start()
    y_on.wait_recv()
    d1_core = me.copy(part(6, 1), part(6, 1), me.plane(1))
    d1_core.start()
    yield begin + unit * 1.5 + 2.0
    own.wait()
    for copy in (to_c, x_core, y_core, d0_core, d1_core):
        copy.wait_recv()
    for copy in (*x_in, *y_in, to_c, x_on, x_core, y_on, y_core, d0_core, d1_core):
        copy.wait_send()


def add_rows(dst, a, b, step=32):
    rows = a.shape[0]

    def body(i, _):
        at = pl.ds(pl.multiple_of(i * step, step), step)
        dst[at, :] = (a[at, :].astype(f32) + b[at, :].astype(f32)).astype(dst.dtype)
        return 0

    lax.fori_loop(0, rows // step, body, 0)


def z_reduce_all(me, part, total, inbox, across, partial, out, unit, chunks=8, begin=0.0):
    rows = part.shape[0] // chunks
    z = me.z
    end = (z == 0) | (z == 3)
    middle = (z == 1) | (z == 2)
    inward = {"head": jnp.where(z < 2, z + 1, z - 1)}
    outward = {"head": jnp.where(z < 2, z - 1, z + 1)}
    first = [me.slot() for _ in range(chunks)]
    second = [me.slot() for _ in range(chunks)]
    third = [me.slot() for _ in range(chunks)]
    store = [me.slot() for _ in range(chunks)]

    def at(ref, k):
        return ref.at[pl.ds(k * rows, rows)]

    def put(k):
        return pltpu.make_async_copy(at(total, k), at(out, k), me.send_sem.at[store[k]])

    if begin:
        yield begin

    @pl.when(end)
    def _():
        for k in range(chunks):
            me.again(first[k], at(part, k), at(inbox, k), inward).start()

    hop = unit / chunks
    for k in range(chunks + 2):
        yield begin + hop * (k + 1) + 2.0

        @pl.when(middle)
        def _():
            if k < chunks:
                me.again(first[k], at(part, k), at(inbox, k), inward).wait_recv()
                add_rows(at(partial, k), at(part, k), at(inbox, k))
                me.again(second[k], at(partial, k), at(across, k), inward).start()
            if 1 <= k <= chunks:
                j = k - 1
                me.again(second[j], at(partial, j), at(across, j), inward).wait_recv()
                add_rows(at(total, j), at(partial, j), at(across, j))
                me.again(third[j], at(total, j), at(total, j), outward).start()
                put(j).start()

        @pl.when(end)
        def _():
            if k >= 2:
                j = k - 2
                me.again(third[j], at(total, j), at(total, j), outward).wait_recv()
                put(j).start()

    yield begin + unit + hop * 3

    @pl.when(end)
    def _():
        for k in range(chunks):
            me.again(first[k], at(part, k), at(inbox, k), inward).wait_send()

    @pl.when(middle)
    def _():
        for k in range(chunks):
            me.again(second[k], at(partial, k), at(across, k), inward).wait_send()
            me.again(third[k], at(total, k), at(total, k), outward).wait_send()

    for k in range(chunks):
        put(k).wait()


def z_reduce_scatter(me, part, from_below, from_above, sums_up, sums_down, own, unit, begin=0.0):
    rows = part.shape[0] // 4
    z = me.z
    ups = [me.slot() for _ in range(4)]
    downs = [me.slot() for _ in range(4)]

    def at(ref, j):
        return ref.at[pl.ds(j * rows, rows)]

    def up(j, source):
        return me.again(ups[j], at(source, j), at(from_below, j), me.up())

    def down(j, source):
        return me.again(downs[j], at(source, j), at(from_above, j), me.down())

    def start(j):
        @pl.when(z == 0)
        def _():
            up(j, part).start()

        @pl.when(z == 3)
        def _():
            down(3 - j, part).start()

    def relay(j, stop):
        @pl.when(z == stop)
        def _():
            up(j, part).wait_recv()
            add_rows(at(sums_up, j), at(part, j), at(from_below, j))
            up(j, sums_up).start()

        @pl.when(z == 3 - stop)
        def _():
            i = 3 - j
            down(i, part).wait_recv()
            add_rows(at(sums_down, i), at(part, i), at(from_above, i))
            down(i, sums_down).start()

    yield begin
    start(3)
    yield begin + unit * 0.6
    start(2)
    yield begin + unit + 1.0
    relay(3, 1)
    yield begin + unit * 1.6
    start(1)
    yield begin + unit * 2 + 1.0
    relay(3, 2)
    relay(2, 1)
    yield begin + unit * 3 + 1.5
    for j in range(4):

        @pl.when(z == j)
        def _():
            if j > 0:
                up(j, part).wait_recv()
            if j < 3:
                down(j, part).wait_recv()

            def body(i, _):
                span = pl.ds(pl.multiple_of(i * 32, 32), 32)
                there = pl.ds(pl.multiple_of(j * rows + i * 32, 32), 32)
                value = part[there, :].astype(f32)
                if j > 0:
                    value = value + from_below[there, :].astype(f32)
                if j < 3:
                    value = value + from_above[there, :].astype(f32)
                own[span, :] = value
                return 0

            lax.fori_loop(0, rows // 32, body, 0)
            for i in range(4):
                if i > j:
                    up(i, part).wait_send()
                if i < j:
                    down(i, part).wait_send()


def plane_scatter_scratch(rows, cols):
    half = rows // 2
    return [
        pltpu.VMEM((4, rows, cols), bf16),
        pltpu.VMEM((4, rows, cols), bf16),
        pltpu.VMEM((2, half, cols), bf16),
        pltpu.VMEM((2, half, cols), bf16),
        pltpu.VMEM((half, cols), bf16),
        pltpu.VMEM((half, cols), bf16),
    ]


def plane_scatter(me, src, out, scratch, unit, begin=0.0):
    held, other, over_x, over_y, last_y, last_x = scratch
    rows = out.shape[0]
    half = rows // 2

    def block(i):
        return src.at[pl.ds(pl.multiple_of(me.number(i) * rows, rows), rows)]

    first, second = pl.ds(0, half), pl.ds(half, half)
    if begin:
        yield begin
    loads, cores = {}, {}
    for i in (6, 2, 4, 0):
        cores[i] = me.copy(block(i + 1), other.at[i // 2], me.plane(1))
        cores[i].start()
        loads[i] = me.local(block(i), held.at[i // 2])
        loads[i].start()
    yield begin + 3.0
    for i in (6, 2, 4, 0):
        loads[i].wait()
        cores[i].wait_recv()
        add_rows(held.at[i // 2], held.at[i // 2], other.at[i // 2])
        if i == 6:
            six_x = me.copy(held.at[3, first], over_x.at[1], me.plane(2))
            six_y = me.copy(held.at[3, second], over_y.at[1], me.plane(4))
            six_x.start()
            six_y.start()
        if i == 2:
            two_x = me.copy(held.at[1, first], over_x.at[0], me.plane(2))
            two_x.start()
        if i == 4:
            four_y = me.copy(held.at[2, second], over_y.at[0], me.plane(4))
            four_y.start()
    yield begin + 4.0 + unit * 0.5
    six_x.wait_recv()
    add_rows(held.at[2, first], held.at[2, first], over_x.at[1])
    to_y = me.copy(held.at[2, first], last_y, me.plane(4))
    to_y.start()
    six_y.wait_recv()
    add_rows(held.at[1, second], held.at[1, second], over_y.at[1])
    to_x = me.copy(held.at[1, second], last_x, me.plane(2))
    to_x.start()
    yield begin + 5.0 + unit * 1.5
    two_x.wait_recv()
    four_y.wait_recv()
    to_y.wait_recv()
    to_x.wait_recv()

    def body(i, _):
        at = pl.ds(pl.multiple_of(i * 32, 32), 32)
        low = pl.ds(pl.multiple_of(half + i * 32, 32), 32)
        out[at, :] = (
            held[0, at, :].astype(f32) + over_x[0, at, :].astype(f32) + last_y[at, :].astype(f32)
        ).astype(out.dtype)
        out[low, :] = (
            held[0, low, :].astype(f32) + over_y[0, at, :].astype(f32) + last_x[at, :].astype(f32)
        ).astype(out.dtype)
        return 0

    lax.fori_loop(0, half // 32, body, 0)
    for i in (6, 2, 4, 0):
        cores[i].wait_send()
    for copy in (six_x, six_y, two_x, four_y, to_y, to_x):
        copy.wait_send()


def params(number, vmem=60 * 2**20):
    return pltpu.CompilerParams(
        collective_id=number, has_side_effects=True, vmem_limit_bytes=vmem
    )


def shape(dims, kind=bf16):
    return jax.ShapeDtypeStruct(dims, kind)


def first_kernel(tok, wqkv, gains, tok_all, wqkv_all, gains_all, ss, rs):
    me = Here(ss, rs)
    me.enter((1, 2, 4))
    drive(
        z_gather(me, tok, tok_all, 11.3),
        plane_gather(me, gains, gains_all, 2.0),
        plane_gather(me, wqkv, wqkv_all, 7.0),
    )


def first(tok, wqkv, gains):
    def grown(a, n):
        return shape((a.shape[0] * n,) + a.shape[1:])

    return pl.pallas_call(
        first_kernel,
        out_shape=(grown(tok, 4), grown(wqkv, 8), grown(gains, 8)),
        in_specs=[VM] * 3,
        out_specs=[HB] * 3,
        scratch_shapes=dma_sems(64),
        compiler_params=params(1),
        name="gather_first",
    )(tok, wqkv, gains)


def alone(flops, vmem=60 * 2**20):
    return dict(
        compiler_params=pltpu.CompilerParams(vmem_limit_bytes=vmem),
        cost_estimate=pl.CostEstimate(flops=int(flops), bytes_accessed=2**23, transcendentals=0),
    )


def gain_row(gains, which):
    return jnp.concatenate(
        [gains[i * 32 : i * 32 + 16, :].astype(f32)[which : which + 1] for i in range(8)], axis=1
    )


def rotate_heads(values, cos, sin, inverse=False):
    out = []
    for h in range(values.shape[0] // HD):
        a = values[h * HD : h * HD + HD // 2]
        b = values[h * HD + HD // 2 : (h + 1) * HD]
        if inverse:
            out += [a * cos + b * sin, b * cos - a * sin]
        else:
            out += [a * cos - b * sin, b * cos + a * sin]
    return jnp.concatenate(out, axis=0)


def project_kernel(tok, wqkv, gains, cos_t, sin_t, normed, q_t, q_n, kv_own):
    heads = q_t.shape[0]
    wide = heads * HD
    gain = gain_row(gains, 0)

    def body(i, _):
        at = pl.ds(pl.multiple_of(i * 128, 128), 128)
        x = tok[at, :].astype(f32)
        inv = lax.rsqrt(jnp.mean(x * x, axis=1, keepdims=True) + norm_epsilon)
        low = (x * inv * gain).astype(bf16)
        normed[at, :] = low
        lin = jnp.dot(low, wqkv[...], preferred_element_type=f32).T
        cos, sin = cos_t[:, at], sin_t[:, at]
        turned = rotate_heads(lin[: wide + HD], cos, sin)
        query = turned[:wide].astype(bf16) * bf16(1.0 / math.sqrt(HD))
        for h in range(heads):
            q_t[h, :, at] = query[h * HD : (h + 1) * HD]
        natural = query.astype(f32).T
        for h in range(heads):
            q_n[h, at, :] = natural[:, h * HD : (h + 1) * HD].astype(bf16)
        kv_own[at, :] = jnp.concatenate([turned[wide:], lin[wide + HD :]], axis=0).T.astype(bf16)
        return 0

    lax.fori_loop(0, tok.shape[0] // 128, body, 0)


def project(tok, wqkv, gains, cos_t, sin_t):
    rows = tok.shape[0]
    heads = (wqkv.shape[1] - 2 * HD) // HD
    return pl.pallas_call(
        project_kernel,
        out_shape=(
            shape(tok.shape),
            shape((heads, HD, rows)),
            shape((heads, rows, HD)),
            shape((rows, 2 * HD)),
        ),
        in_specs=[VM] * 5,
        out_specs=[VM] * 4,
        name="project",
        **alone(2 * rows * wqkv.shape[0] * wqkv.shape[1]),
    )(tok, wqkv, gains, cos_t, sin_t)


def attention_forward(me, q_t, kv_own, kv, v_t, key_pos, query_pos, out_t, attended, log_sum, kv_all, per):
    heads, hd, rows = q_t.shape
    blocks = kv.shape[0] // rows

    def block(i):
        return kv.at[pl.ds(i * rows, rows)]

    copies = [me.copy(kv_own, block(i), me.plane(i)) for i in (1, 2, 3)]
    for copy in copies:
        copy.start()
    own = me.local(kv_own, block(0))
    own.start()
    yield 0.2
    own.wait()
    for copy in copies:
        copy.wait_recv()
    save = me.local(kv, kv_all)
    save.start()
    for i in range(blocks):
        v_t[:, i * rows : (i + 1) * rows] = kv[i * rows : (i + 1) * rows, :].astype(f32).T[hd:, :].astype(bf16)

    def one_head(h):
        q = q_t[h]
        limit = query_pos[0:1, :]

        def step(i, state):
            top, total, acc = state
            at = pl.ds(pl.multiple_of(i * rows, rows), rows)
            s = jnp.dot(kv[at, 0:hd], q, preferred_element_type=f32)
            pos = key_pos[at, :]
            pos = jnp.concatenate([pos] * (rows // 128), axis=1)
            s = jnp.where(pos <= limit, s, masked_value)
            new = jnp.maximum(top, jnp.max(s, axis=0, keepdims=True))
            p = jnp.exp(s - new)
            factor = jnp.exp(top - new)
            total = total * factor + jnp.sum(p, axis=0, keepdims=True)
            acc = acc * factor + jnp.dot(v_t[:, at], p.astype(bf16), preferred_element_type=f32)
            return new, total, acc

        top, total, acc = lax.fori_loop(
            0,
            blocks,
            step,
            (
                jnp.full((1, rows), masked_value, f32),
                jnp.zeros((1, rows), f32),
                jnp.zeros((hd, rows), f32),
            ),
        )
        acc = acc / total
        out_t[h] = acc
        log_sum[h] = top + jnp.log(total)
        return acc

    for h in range(0, heads, 2):
        yield 6.0 + per * h
        pair = jnp.concatenate([one_head(h), one_head(h + 1)], axis=0)
        attended[:, h * hd : (h + 2) * hd] = pair.T.astype(bf16)
    yield 6.0 + per * heads
    save.wait()
    for copy in copies:
        copy.wait_send()


def second_kernel(
    q_t, kv_own, key_pos, query_pos, cot, wo, wu,
    out_t, attended, log_sum, kv_all, cot_all, wo_all, wu_all, kv, v_t, ss, rs
):
    me = Here(ss, rs)
    me.enter((1, 2, 3, 4))
    drive(
        attention_forward(
            me, q_t, kv_own, kv, v_t, key_pos, query_pos, out_t, attended, log_sum, kv_all, 4.0
        ),
        z_gather(me, cot, cot_all, 11.3, 0.1),
        plane_gather(me, wo, wo_all, 6.0, 0.3),
        plane_gather(me, wu, wu_all, 15.5, 6.0),
    )


def second(q_t, kv_own, key_pos, query_pos, cot, wo, wu):
    heads, hd, rows = q_t.shape
    keys = key_pos.shape[0]
    return pl.pallas_call(
        second_kernel,
        out_shape=(
            shape((heads, hd, rows), f32),
            shape((rows, heads * hd)),
            shape((heads, 1, rows), f32),
            shape((keys, 2 * hd)),
            shape((cot.shape[0] * 4, cot.shape[1])),
            shape((wo.shape[0] * 8, wo.shape[1])),
            shape((wu.shape[0] * 8, wu.shape[1])),
        ),
        in_specs=[VM] * 7,
        out_specs=[VM] * 3 + [HB] * 4,
        scratch_shapes=[pltpu.VMEM((keys, 2 * hd), bf16), pltpu.VMEM((hd, keys), bf16)] + dma_sems(64),
        compiler_params=params(2),
        name="attention_forward",
    )(q_t, kv_own, key_pos, query_pos, cot, wo, wu)


def third_kernel(part, wg, wd, total_out, wg_all, wd_all, total, inbox, across, partial, ss, rs):
    me = Here(ss, rs)
    me.enter((1, 2, 4))
    drive(
        z_reduce_all(me, part, total, inbox, across, partial, total_out, 45.0, 16),
        plane_gather(me, wg, wg_all, 15.5, 0.1),
        plane_gather(me, wd, wd_all, 15.5, 15.0),
    )


def third(part, wg, wd):
    rows = pltpu.VMEM(part.shape, bf16)

    def grown(a):
        return shape((a.shape[0] * 8, a.shape[1]))

    return pl.pallas_call(
        third_kernel,
        out_shape=(shape(part.shape), grown(wg), grown(wd)),
        in_specs=[VM] * 3,
        out_specs=[HB] * 3,
        scratch_shapes=[rows] * 4 + dma_sems(96),
        compiler_params=params(3),
        name="sum_branch",
    )(part, wg, wd)


def contract_rows(left, right):
    return lax.dot_general(left, right, (((0,), (0,)), ((), ())), preferred_element_type=f32)


def contract_last_dims(left, right):
    return lax.dot_general(left, right, (((1,), (1,)), ((), ())), preferred_element_type=f32)


def fourth_kernel(
    part, cot_all, hidden, normed_two, d_gate, d_up, wd_all,
    total_out, dwd_own, dwg, dwu, out_part,
    total, inbox, across, partial, left_a, left_b, right_a, right_b, right_c, wd, dwd, stage, *rest
):
    *scratch, ss, rs = rest
    me = Here(ss, rs)
    me.enter((1, 2, 4))
    blocks = left_a.shape[1] // 256
    pairs = ((cot_all, left_a), (hidden, right_a), (normed_two, left_b), (d_gate, right_b), (d_up, right_c), (wd_all, wd))
    loads = [me.local(src, dst) for src, dst in pairs]

    def block(ref, i):
        return ref[:, i * 256 : (i + 1) * 256]

    def down():
        yield 0.2
        for load in loads:
            load.start()
        loads[0].wait()
        loads[1].wait()
        for i in range(blocks):
            yield 2.5 + i
            dwd[i * 256 : (i + 1) * 256, :] = contract_rows(block(left_a, i), right_a[...]).astype(bf16)
        yield from plane_scatter(me, dwd, dwd_own, scratch, 15.5, 2.6 + blocks)

    puts = [me.slot(), me.slot()]
    busy = [None, None]

    def put(n, value, dst):
        k = n % 2
        if busy[k] is not None:
            busy[k].wait()
        view = stage.at[k, pl.ds(0, value.shape[0]), pl.ds(0, value.shape[1])]
        stage[k, : value.shape[0], : value.shape[1]] = value.astype(bf16)
        busy[k] = pltpu.make_async_copy(view, dst, me.send_sem.at[puts[k]])
        busy[k].start()

    def others():
        n = 0
        yield 11.0
        loads[2].wait()
        for load, right, dst in ((loads[3], right_b, dwg), (loads[4], right_c, dwu)):
            load.wait()
            for i in range(blocks):
                yield 12.0 + n
                value = contract_rows(block(left_b, i), right[...])
                put(n, value, dst.at[pl.ds(i * 256, 256)])
                n += 1
        loads[5].wait()
        for i in range(hidden.shape[0] // 128):
            for h in (0, 1):
                yield 12.0 + n
                at = slice(i * 128, (i + 1) * 128)
                half = wd.shape[0] // 2
                value = contract_last_dims(right_a[at, :], wd[h * half : (h + 1) * half, :])
                put(n, value, out_part.at[pl.ds(i * 128, 128), pl.ds(h * half, half)])
                n += 1
        for copy in busy:
            copy.wait()

    drive(
        z_reduce_all(me, part, total, inbox, across, partial, total_out, 45.0, 16),
        down(),
        others(),
    )


def fourth(part, cot_all, hidden, normed_two, d_gate, d_up, wd_all):
    rows = pltpu.VMEM(part.shape, bf16)
    units = pltpu.VMEM(hidden.shape, bf16)
    weight = pltpu.VMEM(wd_all.shape, bf16)
    own = (wd_all.shape[0] // 8, wd_all.shape[1])
    return pl.pallas_call(
        fourth_kernel,
        out_shape=(
            shape(part.shape), shape(own, f32), shape(wd_all.shape), shape(wd_all.shape), shape(part.shape)
        ),
        in_specs=[VM] + [HB] * 6,
        out_specs=[HB, VM, HB, HB, HB],
        scratch_shapes=[rows] * 6 + [units] * 3 + [weight] * 2
        + [pltpu.VMEM((2, 256, max(own[1], wd_all.shape[0] // 2)), bf16)]
        + plane_scatter_scratch(*own) + dma_sems(128),
        compiler_params=params(4, 63 * 2**20),
        name="sum_grad_normed_two",
    )(part, cot_all, hidden, normed_two, d_gate, d_up, wd_all)


def prepare_kernel(cot, tok, branch, grad_two, gains, wo, out_t, attended, g_t, g_n, delta, own, gain_part, dwo, low):
    heads = g_t.shape[0]
    gain = gain_row(gains, 1)
    z = lax.axis_index("head")

    def body(i, _):
        at = pl.ds(pl.multiple_of(i * 128, 128), 128)
        h = tok[at, :].astype(f32) + branch[at, :].astype(f32)
        e = grad_two[at, :].astype(f32)
        inv = lax.rsqrt(jnp.mean(h * h, axis=1, keepdims=True) + norm_epsilon)
        u = e * gain
        inner = jnp.mean(u * h, axis=1, keepdims=True)
        grad = cot[at, :].astype(f32) + (inv * u - h * (inv * inv * inv * inner))

        @pl.when(i == z)
        def _():
            own[...] = grad
            gain_part[...] = jnp.broadcast_to(
                jnp.sum(e * h * inv, axis=0, keepdims=True), gain_part.shape
            )

        small = grad.astype(bf16)
        low[at, :] = small
        g = jnp.dot(small, wo[...], preferred_element_type=f32).astype(bf16)
        turned = g.astype(f32).T
        for head in range(heads):
            g_n[head, at, :] = g[:, head * HD : (head + 1) * HD]
            mine = turned[head * HD : (head + 1) * HD]
            g_t[head, :, at] = mine.astype(bf16)
            delta[head, :, at] = jnp.sum(mine * out_t[head, :, at], axis=0, keepdims=True)
        return 0

    lax.fori_loop(0, tok.shape[0] // 128, body, 0)
    for i in range(dwo.shape[0] // 256):
        span = slice(i * 256, (i + 1) * 256)
        dwo[span, :] = contract_rows(low[:, span], attended[...]).astype(bf16)


def prepare(cot, tok, branch, grad_two, gains, wo, out_t, attended):
    heads, hd, rows = out_t.shape
    width = tok.shape[1]
    return pl.pallas_call(
        prepare_kernel,
        out_shape=(
            shape((heads, hd, rows)),
            shape((heads, rows, hd)),
            shape((heads, 1, rows), f32),
            shape((rows // 4, width), f32),
            shape((8, width), f32),
            shape(wo.shape),
        ),
        in_specs=[VM] * 8,
        out_specs=[VM] * 6,
        scratch_shapes=[pltpu.VMEM(tok.shape, bf16)],
        name="prepare_backward",
        **alone(4 * rows * width * heads * hd),
    )(cot, tok, branch, grad_two, gains, wo, out_t, attended)


def attention_backward(me, q_t, q_n, g_t, g_n, kv_all, log_sum, delta, key_pos, query_pos, dq_t, dkv_own, kv, k_t, dk, dv, dkv, came, per):
    heads, hd, rows = q_t.shape
    blocks = kv.shape[0] // rows
    load = me.local(kv_all, kv)
    load.start()
    dk[...] = jnp.zeros_like(dk)
    dv[...] = jnp.zeros_like(dv)
    load.wait()
    for i in range(blocks):
        k_t[:, i * rows : (i + 1) * rows] = kv[i * rows : (i + 1) * rows, :].astype(f32).T[:hd, :].astype(bf16)

    def head(h, _):
        q, g = q_t[h], g_t[h]
        limit = query_pos[0:1, :]

        def step(i, acc):
            at = pl.ds(pl.multiple_of(i * rows, rows), rows)
            both = kv[at, :]
            s = jnp.dot(both[:, 0:hd], q, preferred_element_type=f32)
            pos = key_pos[at, :]
            pos = jnp.concatenate([pos] * (rows // 128), axis=1)
            s = jnp.where(pos <= limit, s, masked_value)
            p = jnp.exp(s - log_sum[h])
            dp = jnp.dot(both[:, hd:], g, preferred_element_type=f32)
            ds = (p * (dp - delta[h])).astype(bf16)
            dv[at, :] += jnp.dot(p.astype(bf16), g_n[h], preferred_element_type=f32)
            dk[at, :] += jnp.dot(ds, q_n[h], preferred_element_type=f32)
            return acc + jnp.dot(k_t[:, at], ds, preferred_element_type=f32)

        acc = lax.fori_loop(0, blocks, step, jnp.zeros((hd, rows), f32))
        dq_t[h] = (acc * (1.0 / math.sqrt(hd))).astype(bf16)
        return 0

    for h in range(0, heads, 2):
        yield 0.3 + per * h
        lax.fori_loop(h, h + 2, head, 0)
    for i in range(blocks):
        at = slice(i * rows, (i + 1) * rows)
        dkv[at, :] = jnp.concatenate([dk[at, :], dv[at, :]], axis=1).astype(bf16)
    copies = [
        me.copy(dkv.at[pl.ds(i * rows, rows)], came.at[i - 1], me.plane(i)) for i in (1, 2, 3)
    ]
    for copy in copies:
        copy.start()
    yield 0.3 + per * heads + 8.0
    for copy in copies:
        copy.wait_recv()
    value = dkv[0:rows, :].astype(f32)
    for i in range(blocks - 1):
        value = value + came[i].astype(f32)
    dkv_own[...] = value
    for copy in copies:
        copy.wait_send()


def fifth_kernel(
    q_t, q_n, g_t, g_n, kv_all, log_sum, delta, key_pos, query_pos, out_part, dwg, dwu,
    dq_t, dkv_own, out_own, dwg_own, dwu_own,
    kv, k_t, dk, dv, dkv, came, below, above, sums_up, sums_down, *rest
):
    *scratch, ss, rs = rest
    me = Here(ss, rs)
    me.enter((1, 2, 3, 4))
    drive(
        plane_scatter(me, dwg, dwg_own, scratch[:6], 15.5),
        plane_scatter(me, dwu, dwu_own, scratch[6:], 15.5, 18.0),
        z_reduce_scatter(me, out_part, below, above, sums_up, sums_down, out_own, 11.3),
        attention_backward(
            me, q_t, q_n, g_t, g_n, kv_all, log_sum, delta, key_pos, query_pos,
            dq_t, dkv_own, kv, k_t, dk, dv, dkv, came, 6.0,
        ),
    )


def fifth(q_t, q_n, g_t, g_n, kv_all, log_sum, delta, key_pos, query_pos, out_part, dwg, dwu):
    heads, hd, rows = q_t.shape
    keys = key_pos.shape[0]
    own = (dwg.shape[0] // 8, dwg.shape[1])
    part = pltpu.VMEM(out_part.shape, bf16)
    return pl.pallas_call(
        fifth_kernel,
        out_shape=(
            shape((heads, hd, rows)),
            shape((rows, 2 * hd), f32),
            shape((out_part.shape[0] // 4, out_part.shape[1]), f32),
            shape(own, f32),
            shape(own, f32),
        ),
        in_specs=[VM] * 4 + [HB] + [VM] * 5 + [HB] * 2,
        out_specs=[VM] * 5,
        scratch_shapes=[
            pltpu.VMEM((keys, 2 * hd), bf16),
            pltpu.VMEM((hd, keys), bf16),
            pltpu.VMEM((keys, hd), f32),
            pltpu.VMEM((keys, hd), f32),
            pltpu.VMEM((keys, 2 * hd), bf16),
            pltpu.VMEM((keys // rows - 1, rows, 2 * hd), bf16),
            part, part, part, part,
        ]
        + plane_scatter_scratch(*own) * 2
        + dma_sems(64),
        compiler_params=params(5),
        name="attention_backward",
    )(q_t, q_n, g_t, g_n, kv_all, log_sum, delta, key_pos, query_pos, out_part, dwg, dwu)


def finish_kernel(dq_t, dkv, cos_t, sin_t, wqkv, normed, tok, gain_two, one_part, dwqkv, gain_parts, lin):
    heads = dq_t.shape[0]
    wide = heads * HD
    width = tok.shape[1]
    cols = width // 8

    def body(i, total):
        at = pl.ds(pl.multiple_of(i * 128, 128), 128)
        cos, sin = cos_t[:, at], sin_t[:, at]
        kv = dkv[at, :].astype(bf16).astype(f32).T
        grads = jnp.concatenate([dq_t[h, :, at].astype(f32) for h in range(heads)] + [kv[:HD]], axis=0)
        grads = rotate_heads(grads, cos, sin, inverse=True)
        natural = jnp.concatenate([grads, kv[HD:]], axis=0).T.astype(bf16)
        lin[at, :] = natural
        one = contract_last_dims(natural, wqkv[...])
        one_part[at, :] = one.astype(bf16)
        x = tok[at, :].astype(f32)
        inv = lax.rsqrt(jnp.mean(x * x, axis=1, keepdims=True) + norm_epsilon)
        return total + jnp.sum(one * x * inv, axis=0, keepdims=True)

    total = lax.fori_loop(0, tok.shape[0] // 128, body, jnp.zeros((1, width), f32))
    for i in range(8):
        span = slice(i * cols, (i + 1) * cols)
        gain_parts[i * 8 : (i + 1) * 8, :] = jnp.concatenate(
            [total[:, span], gain_two[0:1, span], jnp.zeros((6, cols), f32)], axis=0
        )
        dwqkv[span, :] = contract_rows(normed[:, span], lin[...]).astype(bf16)


def finish(dq_t, dkv, cos_t, sin_t, wqkv, normed, tok, gain_two):
    width = tok.shape[1]
    return pl.pallas_call(
        finish_kernel,
        out_shape=(shape(tok.shape), shape(wqkv.shape), shape((64, width // 8), f32)),
        in_specs=[VM] * 8,
        out_specs=[VM] * 3,
        scratch_shapes=[pltpu.VMEM((tok.shape[0], wqkv.shape[1]), bf16)],
        name="finish_attention",
        **alone(4 * tok.shape[0] * width * wqkv.shape[1]),
    )(dq_t, dkv, cos_t, sin_t, wqkv, normed, tok, gain_two)


def gain_sums(me, src, out, came, mine, came_z):
    def block(i):
        return pl.ds(pl.multiple_of(me.number(i) * 8, 8), 8)

    copies = [me.copy(src.at[block(i)], came.at[i - 1], me.plane(i)) for i in range(1, 8)]
    for copy in copies:
        copy.start()
    yield 4.0
    value = src[block(0), :]
    for i, copy in enumerate(copies):
        copy.wait_recv()
        value = value + came[i]
    mine[...] = value
    again = [
        me.copy(mine, came_z.at[d - 1], {"head": (me.z + d) % 4}) for d in (1, 2, 3)
    ]
    for copy in again:
        copy.start()
    yield 20.0
    for d, copy in enumerate(again):
        copy.wait_recv()
        value = value + came_z[d]
    out[...] = value
    for copy in copies + again:
        copy.wait_send()


def sixth_kernel(
    part, dwqkv, dwo, gains,
    own, dwq_own, dwkv_all, dwo_own, gains_out,
    below, above, sums_up, sums_down, dwqkv_own, dwkv_own, came_kv, came, mine, came_z, *rest
):
    *scratch, ss, rs = rest
    me = Here(ss, rs)
    me.enter(tuple(range(1, 8)), all_z=True)
    wide = dwq_own.shape[1]

    def weights():
        yield from plane_scatter(me, dwqkv, dwqkv_own, scratch[:6], 7.0, 0.1)
        dwq_own[...] = dwqkv_own[:, :wide]
        dwkv_own[...] = dwqkv_own[:, wide:].astype(bf16)
        copies = [
            me.copy(dwkv_own, came_kv.at[d - 1], {"head": (me.z + d) % 4}) for d in (1, 2, 3)
        ]
        for copy in copies:
            copy.start()
        yield 37.0
        for copy in copies:
            copy.wait_recv()
        dwkv_all[0] = dwkv_own[...]
        for d in (1, 2, 3):
            dwkv_all[d] = came_kv[d - 1]
        for copy in copies:
            copy.wait_send()

    drive(
        gain_sums(me, gains, gains_out, came, mine, came_z),
        z_reduce_scatter(me, part, below, above, sums_up, sums_down, own, 11.3),
        weights(),
        plane_scatter(me, dwo, dwo_own, scratch[6:], 6.0, 9.0),
    )


def sixth(part, dwqkv, dwo, gains):
    rows, cols = dwqkv.shape[0] // 8, dwqkv.shape[1]
    wide = dwo.shape[1]
    whole = pltpu.VMEM(part.shape, bf16)
    return pl.pallas_call(
        sixth_kernel,
        out_shape=(
            shape((part.shape[0] // 4, part.shape[1]), f32),
            shape((rows, wide), f32),
            shape((4, rows, cols - wide)),
            shape((rows, wide), f32),
            shape((8, gains.shape[1]), f32),
        ),
        in_specs=[VM, HB, HB, VM],
        out_specs=[VM] * 5,
        scratch_shapes=[
            whole, whole, whole, whole,
            pltpu.VMEM((rows, cols), f32),
            pltpu.VMEM((rows, cols - wide), bf16),
            pltpu.VMEM((3, rows, cols - wide), bf16),
            pltpu.VMEM((7, 8, gains.shape[1]), f32),
            pltpu.VMEM((8, gains.shape[1]), f32),
            pltpu.VMEM((3, 8, gains.shape[1]), f32),
        ]
        + plane_scatter_scratch(rows, cols)
        + plane_scatter_scratch(rows, wide)
        + dma_sems(64),
        compiler_params=params(6),
        name="scatter_last",
    )(part, dwqkv, dwo, gains)


def local_fast(
    tokens, w_query, w_key, w_value, w_out, w_gate, w_up, w_down, gain_attn, gain_mlp, stretch_order, cotangent
):
    row_count, width = tokens.shape
    groups = 4
    head_rows = row_count * groups
    stretch_rows = head_rows // 2
    cols = width // 8
    contract_last = (((1,), (1,)), ((), ()))
    z = lax.axis_index("head")
    b = lax.axis_index("blk")
    own_first = z * row_count

    def own_rows(values):
        return lax.dynamic_slice_in_dim(values, own_first, row_count, 0)

    query_positions = stretch_positions(stretch_order, b * head_rows, head_rows, stretch_rows)
    key_positions = jnp.concatenate(
        [
            stretch_positions(stretch_order, jnp.bitwise_xor(b, i) * head_rows, head_rows, stretch_rows)
            for i in range(4)
        ]
    )
    key_pos = jnp.broadcast_to(key_positions[:, None], (key_positions.shape[0], 128))
    query_pos = jnp.broadcast_to(query_positions[None, :], (8, head_rows))
    half = HD // 2
    frequency = rope_base ** (-(jnp.arange(half, dtype=f32) * (2.0 / HD)))
    angles = frequency[:, None] * query_positions.astype(f32)[None, :]
    cos_t, sin_t = jnp.cos(angles), jnp.sin(angles)

    slot_first = z * HD
    w_qkv = jnp.concatenate(
        [
            w_query,
            lax.dynamic_slice_in_dim(w_key, slot_first, HD, 1),
            lax.dynamic_slice_in_dim(w_value, slot_first, HD, 1),
        ],
        axis=1,
    )
    gains = jnp.concatenate([gain_attn[None], gain_mlp[None], jnp.zeros((30, cols), bf16)])
    tok_all, wqkv_all, gains_all = first(tokens, w_qkv, gains)
    normed, q_t, q_n, kv_own = project(tok_all, wqkv_all, gains_all, cos_t, sin_t)
    out_t, attended, log_sum, kv_all, cot_all, wo_all, wu_all = second(
        q_t, kv_own, key_pos, query_pos, cotangent, w_out, w_up
    )
    branch_part = lax.dot_general(attended, wo_all, contract_last, preferred_element_type=f32).astype(bf16)
    branch, wg_all, wd_all = third(branch_part, w_gate, w_down)

    gain_rows = gains_all.reshape(8, 32, cols)
    gain_one = gain_rows[:, 0].reshape(width).astype(f32)
    gain_two = gain_rows[:, 1].reshape(width).astype(f32)
    hidden_rows = tok_all.astype(f32) + branch.astype(f32)
    inv_mlp = lax.rsqrt(jnp.mean(hidden_rows * hidden_rows, axis=-1, keepdims=True) + norm_epsilon)
    normed_two = (hidden_rows * inv_mlp * gain_two).astype(bf16)
    gate = jnp.dot(normed_two, wg_all, preferred_element_type=f32)
    up = jnp.dot(normed_two, wu_all, preferred_element_type=f32)
    gate_sigmoid = jax.nn.sigmoid(gate)
    gate_silu = gate * gate_sigmoid
    hidden = (gate_silu * up).astype(bf16)
    grad_hidden = jnp.dot(cot_all, wd_all, preferred_element_type=f32)
    d_gate = (grad_hidden * up * gate_sigmoid * (1.0 + gate * (1.0 - gate_sigmoid))).astype(bf16)
    d_up = (grad_hidden * gate_silu).astype(bf16)
    two_part = lax.dot_general(d_gate, wg_all, contract_last, preferred_element_type=f32)
    two_part = two_part + lax.dot_general(d_up, wu_all, contract_last, preferred_element_type=f32)
    grad_two, dwd_own, dwg, dwu, out_part = fourth(
        two_part.astype(bf16), cot_all, hidden, normed_two, d_gate, d_up, wd_all
    )

    g_t, g_n, delta, grad_hidden_own, gain_two_part, dwo = prepare(
        cot_all, tok_all, branch, grad_two, gains_all, wo_all, out_t, attended
    )
    dq_t, dkv, out_own, dwg_own, dwu_own = fifth(
        q_t, q_n, g_t, g_n, kv_all, log_sum, delta, key_pos, query_pos, out_part, dwg, dwu
    )
    one_part, dwqkv, gain_parts = finish(
        dq_t, dkv, cos_t, sin_t, wqkv_all, normed, tok_all, gain_two_part
    )
    grad_one, dwq_own, dwkv_all, dwo_own, gain_grads = sixth(one_part, dwqkv, dwo, gain_parts)

    x_own = tokens.astype(f32)
    layer_low = (x_own + own_rows(branch).astype(f32) + out_own).astype(bf16)
    inv_own = lax.rsqrt(jnp.mean(x_own * x_own, axis=-1, keepdims=True) + norm_epsilon)
    grad_tokens = (grad_hidden_own + norm_input_grad(x_own, inv_own, gain_one, grad_one)).astype(bf16)
    slots = jnp.concatenate(
        [lax.dynamic_slice_in_dim(dwkv_all, (z - j) % 4, 1, 0) for j in range(4)], axis=0
    ).astype(f32)
    grad_key = slots[:, :, :HD].transpose(1, 0, 2).reshape(cols, groups * HD)
    grad_value = slots[:, :, HD:].transpose(1, 0, 2).reshape(cols, groups * HD)
    return (
        layer_low,
        grad_tokens,
        dwq_own,
        grad_key,
        grad_value,
        dwo_own,
        dwg_own,
        dwu_own,
        dwd_own,
        gain_grads[0],
        gain_grads[1],
    )


def solution(mesh):
    sizes = (mesh.shape["fsdp"], mesh.shape["blk"], mesh.shape["head"])
    return jax.shard_map(
        local_fast if sizes == (2, 4, 4) else local,
        mesh=mesh,
        in_specs=(
            P(("fsdp", "blk", "head"), None),
            P(("fsdp", "blk"), "head"),
            P(("fsdp", "blk"), None),
            P(("fsdp", "blk"), None),
            P(("fsdp", "blk"), "head"),
            P(("fsdp", "blk"), "head"),
            P(("fsdp", "blk"), "head"),
            P(("fsdp", "blk"), "head"),
            P(("fsdp", "blk")),
            P(("fsdp", "blk")),
            P(),
            P(("fsdp", "blk", "head"), None),
        ),
        out_specs=(
            P(("fsdp", "blk", "head"), None),
            P(("fsdp", "blk", "head"), None),
            P(("fsdp", "blk"), "head"),
            P(("fsdp", "blk"), None),
            P(("fsdp", "blk"), None),
            P(("fsdp", "blk"), "head"),
            P(("fsdp", "blk"), "head"),
            P(("fsdp", "blk"), "head"),
            P(("fsdp", "blk"), "head"),
            P(("fsdp", "blk")),
            P(("fsdp", "blk")),
        ),
        check_vma=False,
    )
```

```python
import math

import jax
import jax.numpy as jnp
from jax import lax
from jax.experimental import pallas as pl
from jax.experimental.pallas import tpu as pltpu
from jax.sharding import PartitionSpec as P

H = 32
KV = 4
HD = 64


norm_epsilon = 1e-05
rope_base = 10000.0
masked_value = -1e30


def rope_tables(positions, head_dim):
    half_dim = head_dim // 2
    frequency = rope_base ** (-(jnp.arange(half_dim, dtype=jnp.float32) * (2.0 / head_dim)))
    angles = positions.astype(jnp.float32)[:, None] * frequency[None, :]
    return (jnp.cos(angles), jnp.sin(angles))


def rotate(values, cosine, sine_table):
    half_dim = values.shape[-1] // 2
    first_half = values[..., :half_dim]
    second_half = values[..., half_dim:]
    cos_rows = cosine[:, None, :]
    sin_rows = sine_table[:, None, :]
    return jnp.concatenate(
        [
            first_half * cos_rows - second_half * sin_rows,
            second_half * cos_rows + first_half * sin_rows,
        ],
        axis=-1,
    )


def unrotate(values, cosine, sine_table):
    half_dim = values.shape[-1] // 2
    first_half = values[..., :half_dim]
    second_half = values[..., half_dim:]
    cos_rows = cosine[:, None, :]
    sin_rows = sine_table[:, None, :]
    return jnp.concatenate(
        [
            first_half * cos_rows + second_half * sin_rows,
            second_half * cos_rows - first_half * sin_rows,
        ],
        axis=-1,
    )


def stretch_positions(stretch_order, first_row, row_span, stretch_rows):
    storage = first_row + jnp.arange(row_span, dtype=jnp.int32)
    stretch_index = storage // stretch_rows
    match_table = (
        stretch_index[:, None] == jnp.arange(stretch_order.shape[0], dtype=jnp.int32)[None, :]
    )
    stretch_base = jnp.sum(jnp.where(match_table, stretch_order[None, :], 0), axis=1)
    return stretch_base * stretch_rows + storage % stretch_rows


def norm_input_grad(values, inverse, gain_vector, grad_normed):
    scaled = grad_normed * gain_vector
    inner = jnp.mean(scaled * values, axis=-1, keepdims=True)
    return inverse * scaled - values * inverse * inverse * inverse * inner


def gain_grad(values, inverse, grad_normed):
    return jnp.sum(grad_normed * values * inverse, axis=0)


def fold_block(
    state_now, keys_block, values_block, key_positions, query_heads, query_positions, score_scale
):
    running_max, running_sum, running_out = state_now
    scores = (
        jnp.einsum("qhd,kd->hqk", query_heads, keys_block, preferred_element_type=jnp.float32)
        * score_scale
    )
    allowed = (query_positions[:, None] >= key_positions[None, :])[None]
    scores = jnp.where(allowed, scores, masked_value)
    new_max = jnp.maximum(running_max, jnp.max(scores, axis=-1))
    weights = jnp.where(allowed, jnp.exp(scores - new_max[..., None]), 0.0)
    factor = jnp.exp(running_max - new_max)
    running_sum = running_sum * factor + jnp.sum(weights, axis=-1)
    running_out = running_out * factor[..., None] + jnp.einsum(
        "hqk,kd->hqd",
        weights.astype(jnp.bfloat16),
        values_block,
        preferred_element_type=jnp.float32,
    )
    return (new_max, running_sum, running_out)


def local(
    tokens,
    w_query,
    w_key,
    w_value,
    w_out,
    w_gate,
    w_up,
    w_down,
    gain_attn,
    gain_mlp,
    stretch_order,
    cotangent,
):
    row_count = tokens.shape[0]
    groups = lax.axis_size("head")
    blocks = lax.axis_size("blk")
    local_heads = H // groups
    repeats = groups // KV
    head_rows = row_count * groups
    stretch_rows = head_rows // 2
    score_scale = 1.0 / math.sqrt(HD)
    contract_last = (((1,), (1,)), ((), ()))
    contract_first = (((0,), (0,)), ((), ()))
    head_index = lax.axis_index("head")
    own_first = head_index * row_count
    block_first = lax.axis_index("blk") * head_rows
    positions = stretch_positions(stretch_order, block_first + own_first, row_count, stretch_rows)
    query_positions = stretch_positions(stretch_order, block_first, head_rows, stretch_rows)
    cos_own, sin_own = rope_tables(positions, HD)
    cos_block, sin_block = rope_tables(query_positions, HD)

    def layer_weights():
        return (
            lax.all_gather(w_query, ("fsdp", "blk"), axis=0, tiled=True),
            lax.all_gather(w_key, ("fsdp", "blk"), axis=0, tiled=True),
            lax.all_gather(w_value, ("fsdp", "blk"), axis=0, tiled=True),
            lax.all_gather(w_out, ("fsdp", "blk"), axis=0, tiled=True),
            lax.all_gather(w_gate, ("fsdp", "blk"), axis=0, tiled=True),
            lax.all_gather(w_up, ("fsdp", "blk"), axis=0, tiled=True),
            lax.all_gather(w_down, ("fsdp", "blk"), axis=0, tiled=True),
            lax.all_gather(gain_attn, ("fsdp", "blk"), axis=0, tiled=True),
            lax.all_gather(gain_mlp, ("fsdp", "blk"), axis=0, tiled=True),
        )

    def gather_query(columns):
        return lax.all_gather(columns, "head", axis=1, tiled=True)

    (
        query_cols,
        key_full,
        value_full,
        out_cols,
        gate_cols,
        up_cols,
        down_cols,
        gain_one,
        gain_two,
    ) = layer_weights()
    tokens_float = tokens.astype(jnp.float32)
    inv_attn = lax.rsqrt(
        jnp.mean(tokens_float * tokens_float, axis=-1, keepdims=True) + norm_epsilon
    )
    normed = (tokens_float * inv_attn * gain_one.astype(jnp.float32)).astype(jnp.bfloat16)
    normed_rows, cotangent_rows = (
        lax.all_gather(normed, "head", axis=0, tiled=True),
        lax.all_gather(cotangent, "head", axis=0, tiled=True),
    )
    query_all = gather_query(query_cols)
    query_lin = jnp.dot(normed, query_all, preferred_element_type=jnp.float32).reshape(
        row_count, H, HD
    )
    key_lin = jnp.dot(normed, key_full, preferred_element_type=jnp.float32).reshape(
        row_count, KV, HD
    )
    value_lin = jnp.dot(normed, value_full, preferred_element_type=jnp.float32).reshape(
        row_count, KV, HD
    )
    query_rot = rotate(query_lin, cos_own, sin_own).astype(jnp.bfloat16).reshape(row_count, H * HD)
    key_rot = rotate(key_lin, cos_own, sin_own).astype(jnp.bfloat16)
    key_slots = jnp.repeat(key_rot, repeats, axis=1).reshape(row_count, groups * HD)
    value_slots = jnp.repeat(value_lin.astype(jnp.bfloat16), repeats, axis=1).reshape(
        row_count, groups * HD
    )
    query_recv, key_own, value_own = (
        lax.all_to_all(query_rot, "head", split_axis=1, concat_axis=0, tiled=True),
        lax.all_to_all(key_slots, "head", split_axis=1, concat_axis=0, tiled=True),
        lax.all_to_all(value_slots, "head", split_axis=1, concat_axis=0, tiled=True),
    )
    query_heads = query_recv.reshape(head_rows, local_heads, HD)
    initial = (
        jnp.full((local_heads, head_rows), masked_value, jnp.float32),
        jnp.zeros((local_heads, head_rows), jnp.float32),
        jnp.zeros((local_heads, head_rows, HD), jnp.float32),
    )
    state_now = initial
    keys_piece = lax.all_gather(key_own, "blk", axis=0, tiled=True)
    values_piece = lax.all_gather(value_own, "blk", axis=0, tiled=True)
    piece_rows = keys_piece.shape[0]

    def scan_step(state_inner, step_index):
        offset = step_index * head_rows
        keys_block = lax.dynamic_slice_in_dim(keys_piece, offset, head_rows, 0)
        values_block = lax.dynamic_slice_in_dim(values_piece, offset, head_rows, 0)
        key_positions = stretch_positions(stretch_order, offset, head_rows, stretch_rows)
        return (
            fold_block(
                state_inner,
                keys_block,
                values_block,
                key_positions,
                query_heads,
                query_positions,
                score_scale,
            ),
            None,
        )

    state_now, unused = lax.scan(
        scan_step, state_now, jnp.arange(piece_rows // head_rows, dtype=jnp.int32)
    )
    running_max, running_sum, running_out = state_now
    attended_float = running_out / running_sum[..., None]
    log_sum = running_max + jnp.log(running_sum)
    attended_heads = (
        attended_float.astype(jnp.bfloat16).transpose(1, 0, 2).reshape(head_rows, local_heads * HD)
    )
    branch = lax.dot_general(
        attended_heads, out_cols, contract_last, preferred_element_type=jnp.float32
    )
    own_branch = lax.dynamic_slice_in_dim(branch, own_first, row_count, 0)
    partial_value = lax.dynamic_update_slice_in_dim(branch, own_branch + tokens_float, own_first, 0)
    hidden_rows = lax.psum(partial_value.astype(jnp.bfloat16), "head").astype(jnp.float32)
    inv_mlp = lax.rsqrt(jnp.mean(hidden_rows * hidden_rows, axis=-1, keepdims=True) + norm_epsilon)
    normed_two_rows = (hidden_rows * inv_mlp * gain_two.astype(jnp.float32)).astype(jnp.bfloat16)
    gate_proj = jnp.dot(normed_two_rows, gate_cols, preferred_element_type=jnp.float32)
    up_proj = jnp.dot(normed_two_rows, up_cols, preferred_element_type=jnp.float32)
    gate_sigmoid = jax.nn.sigmoid(gate_proj)
    gate_silu = gate_proj * gate_sigmoid
    hidden = (gate_silu * up_proj).astype(jnp.bfloat16)
    hidden_own = lax.dynamic_slice_in_dim(hidden_rows, own_first, row_count, 0)
    output_float = hidden_own + lax.psum_scatter(
        lax.dot_general(
            hidden, down_cols, contract_last, preferred_element_type=jnp.float32
        ).astype(jnp.bfloat16),
        "head",
        scatter_dimension=0,
        tiled=True,
    ).astype(jnp.float32)
    layer_low = output_float.astype(jnp.bfloat16)
    (
        query_cols,
        key_full,
        value_full,
        out_cols,
        gate_cols,
        up_cols,
        down_cols,
        gain_one,
        gain_two,
    ) = layer_weights()
    query_all = gather_query(query_cols)
    grad_hidden = jnp.dot(cotangent_rows, down_cols, preferred_element_type=jnp.float32)
    grad_gate_rows = (
        grad_hidden * up_proj * gate_sigmoid * (1.0 + gate_proj * (1.0 - gate_sigmoid))
    ).astype(jnp.bfloat16)
    grad_up_rows = (grad_hidden * gate_silu).astype(jnp.bfloat16)
    grad_w_down = lax.dot_general(
        cotangent_rows, hidden, contract_first, preferred_element_type=jnp.float32
    )
    grad_w_gate = lax.dot_general(
        normed_two_rows, grad_gate_rows, contract_first, preferred_element_type=jnp.float32
    )
    grad_w_up = lax.dot_general(
        normed_two_rows, grad_up_rows, contract_first, preferred_element_type=jnp.float32
    )
    normed_two_part = lax.dot_general(
        grad_gate_rows, gate_cols, contract_last, preferred_element_type=jnp.float32
    )
    normed_two_part = normed_two_part + lax.dot_general(
        grad_up_rows, up_cols, contract_last, preferred_element_type=jnp.float32
    )
    grad_normed_two = lax.psum(normed_two_part.astype(jnp.bfloat16), "head").astype(jnp.float32)
    gain_two_float = gain_two.astype(jnp.float32)
    grad_hidden_rows = cotangent_rows.astype(jnp.float32) + norm_input_grad(
        hidden_rows, inv_mlp, gain_two_float, grad_normed_two
    )
    own_grad_two = lax.dynamic_slice_in_dim(grad_normed_two, own_first, row_count, 0)
    own_inv_mlp = lax.dynamic_slice_in_dim(inv_mlp, own_first, row_count, 0)
    grad_gain_two = gain_grad(hidden_own, own_inv_mlp, own_grad_two)
    grad_low_rows = grad_hidden_rows.astype(jnp.bfloat16)
    grad_w_out = lax.dot_general(
        grad_low_rows, attended_heads, contract_first, preferred_element_type=jnp.float32
    )
    grad_heads = (
        jnp.dot(grad_low_rows, out_cols, preferred_element_type=jnp.float32)
        .astype(jnp.bfloat16)
        .reshape(head_rows, local_heads, HD)
    )
    keys_all, values_all = (
        lax.all_gather(key_own, "blk", axis=0, tiled=True),
        lax.all_gather(value_own, "blk", axis=0, tiled=True),
    )
    row_delta = jnp.sum(grad_heads.astype(jnp.float32).transpose(1, 0, 2) * attended_float, axis=-1)

    def back_block(grad_query_acc, block_index):
        offset = block_index * head_rows
        keys_block = lax.dynamic_slice_in_dim(keys_all, offset, head_rows, 0)
        values_block = lax.dynamic_slice_in_dim(values_all, offset, head_rows, 0)
        key_positions = stretch_positions(stretch_order, offset, head_rows, stretch_rows)
        scores = (
            jnp.einsum("qhd,kd->hqk", query_heads, keys_block, preferred_element_type=jnp.float32)
            * score_scale
        )
        allowed = (query_positions[:, None] >= key_positions[None, :])[None]
        probs_block = jnp.where(allowed, jnp.exp(scores - log_sum[..., None]), 0.0)
        grad_probs = jnp.einsum(
            "qhd,kd->hqk", grad_heads, values_block, preferred_element_type=jnp.float32
        )
        grad_scores = (probs_block * (grad_probs - row_delta[..., None])).astype(jnp.bfloat16)
        grad_query_acc = grad_query_acc + jnp.einsum(
            "hqk,kd->qhd", grad_scores, keys_block, preferred_element_type=jnp.float32
        )
        grad_key_part = (
            jnp.einsum("hqk,qhd->kd", grad_scores, query_heads, preferred_element_type=jnp.float32)
            * score_scale
        )
        grad_value_part = jnp.einsum(
            "hqk,qhd->kd",
            probs_block.astype(jnp.bfloat16),
            grad_heads,
            preferred_element_type=jnp.float32,
        )
        return (grad_query_acc, (grad_key_part, grad_value_part))

    grad_query_acc, (key_terms, value_terms) = lax.scan(
        back_block,
        jnp.zeros((head_rows, local_heads, HD), jnp.float32),
        jnp.arange(blocks, dtype=jnp.int32),
    )
    grad_key_sum, grad_value_sum = (
        lax.psum_scatter(
            key_terms.reshape(blocks * head_rows, HD).astype(jnp.bfloat16),
            "blk",
            scatter_dimension=0,
            tiled=True,
        ).astype(jnp.float32),
        lax.psum_scatter(
            value_terms.reshape(blocks * head_rows, HD).astype(jnp.bfloat16),
            "blk",
            scatter_dimension=0,
            tiled=True,
        ).astype(jnp.float32),
    )
    grad_query_rot = (grad_query_acc * score_scale).astype(jnp.bfloat16)
    grad_query_lin_heads = (
        unrotate(grad_query_rot.astype(jnp.float32), cos_block, sin_block)
        .astype(jnp.bfloat16)
        .reshape(head_rows, local_heads * HD)
    )
    key_slot_grad = grad_key_sum.astype(jnp.bfloat16)
    value_slot_grad = grad_value_sum.astype(jnp.bfloat16)
    grad_w_query = lax.dot_general(
        normed_rows, grad_query_lin_heads, contract_first, preferred_element_type=jnp.float32
    )
    query_back, key_back, value_back = (
        lax.all_to_all(grad_query_lin_heads, "head", split_axis=0, concat_axis=1, tiled=True),
        lax.all_to_all(key_slot_grad, "head", split_axis=0, concat_axis=1, tiled=True),
        lax.all_to_all(value_slot_grad, "head", split_axis=0, concat_axis=1, tiled=True),
    )
    key_slot_lin = (
        unrotate(key_back.astype(jnp.float32).reshape(row_count, groups, HD), cos_own, sin_own)
        .astype(jnp.bfloat16)
        .reshape(row_count, KV, repeats, HD)
    )
    value_slot_lin = value_back.reshape(row_count, KV, repeats, HD)
    grad_w_key = jnp.einsum(
        "td,tjrc->djc", normed, key_slot_lin, preferred_element_type=jnp.float32
    ).reshape(-1, KV * HD)
    grad_w_value = jnp.einsum(
        "td,tjrc->djc", normed, value_slot_lin, preferred_element_type=jnp.float32
    ).reshape(-1, KV * HD)
    grad_normed = lax.dot_general(
        query_back, query_all, contract_last, preferred_element_type=jnp.float32
    )
    grad_normed = grad_normed + jnp.einsum(
        "tjrc,djc->td",
        key_slot_lin,
        key_full.reshape(-1, KV, HD),
        preferred_element_type=jnp.float32,
    )
    grad_normed = grad_normed + jnp.einsum(
        "tjrc,djc->td",
        value_slot_lin,
        value_full.reshape(-1, KV, HD),
        preferred_element_type=jnp.float32,
    )
    gain_one_float = gain_one.astype(jnp.float32)
    grad_input_norm = norm_input_grad(tokens_float, inv_attn, gain_one_float, grad_normed)
    grad_gain_one = gain_grad(tokens_float, inv_attn, grad_normed)
    grad_hidden_own = lax.dynamic_slice_in_dim(grad_hidden_rows, own_first, row_count, 0)
    grad_tokens = (grad_hidden_own + grad_input_norm).astype(jnp.bfloat16)
    head_sums = (
        lax.psum(grad_w_key.astype(jnp.bfloat16), "head").astype(jnp.float32),
        lax.psum(grad_w_value.astype(jnp.bfloat16), "head").astype(jnp.float32),
        lax.psum(grad_gain_one.astype(jnp.bfloat16), "head").astype(jnp.float32),
        lax.psum(grad_gain_two.astype(jnp.bfloat16), "head").astype(jnp.float32),
    )
    reduced = (
        lax.psum_scatter(
            grad_w_query.astype(jnp.bfloat16), ("fsdp", "blk"), scatter_dimension=0, tiled=True
        ).astype(jnp.float32),
        lax.psum_scatter(
            head_sums[0].astype(jnp.bfloat16), ("fsdp", "blk"), scatter_dimension=0, tiled=True
        ).astype(jnp.float32),
        lax.psum_scatter(
            head_sums[1].astype(jnp.bfloat16), ("fsdp", "blk"), scatter_dimension=0, tiled=True
        ).astype(jnp.float32),
        lax.psum_scatter(
            grad_w_out.astype(jnp.bfloat16), ("fsdp", "blk"), scatter_dimension=0, tiled=True
        ).astype(jnp.float32),
        lax.psum_scatter(
            grad_w_gate.astype(jnp.bfloat16), ("fsdp", "blk"), scatter_dimension=0, tiled=True
        ).astype(jnp.float32),
        lax.psum_scatter(
            grad_w_up.astype(jnp.bfloat16), ("fsdp", "blk"), scatter_dimension=0, tiled=True
        ).astype(jnp.float32),
        lax.psum_scatter(
            grad_w_down.astype(jnp.bfloat16), ("fsdp", "blk"), scatter_dimension=0, tiled=True
        ).astype(jnp.float32),
        lax.psum_scatter(
            head_sums[2].astype(jnp.bfloat16), ("fsdp", "blk"), scatter_dimension=0, tiled=True
        ).astype(jnp.float32),
        lax.psum_scatter(
            head_sums[3].astype(jnp.bfloat16), ("fsdp", "blk"), scatter_dimension=0, tiled=True
        ).astype(jnp.float32),
    )
    return (
        layer_low,
        grad_tokens,
        reduced[0],
        reduced[1],
        reduced[2],
        reduced[3],
        reduced[4],
        reduced[5],
        reduced[6],
        reduced[7],
        reduced[8],
    )


MESH = pl.DeviceIdType.MESH
f32, bf16 = jnp.float32, jnp.bfloat16
VM = pl.BlockSpec(memory_space=pltpu.VMEM)
HB = pl.BlockSpec(memory_space=pl.ANY)


def dma_sems(n):
    return [pltpu.SemaphoreType.DMA((n,)), pltpu.SemaphoreType.DMA((n,))]


class Here:
    def __init__(self, send_sem, recv_sem):
        self.y = lax.axis_index("fsdp")
        blk = lax.axis_index("blk")
        self.x, self.c = blk // 2, blk % 2
        self.z = lax.axis_index("head")
        self.end = (self.z == 0) | (self.z == 3)
        self.middle = (self.z == 1) | (self.z == 2)
        self.inward = {"head": jnp.where(self.z < 2, self.z + 1, self.z - 1)}
        self.outward = {"head": jnp.where(self.z < 2, self.z - 1, self.z + 1)}
        self.send_sem, self.recv_sem, self.used = send_sem, recv_sem, 0

    def plane(self, i):
        y = 1 - self.y if i & 4 else self.y
        x = 1 - self.x if i & 2 else self.x
        c = 1 - self.c if i & 1 else self.c
        return {"fsdp": y, "blk": x * 2 + c}

    def number(self, i):
        at = self.plane(i)
        return at["fsdp"] * 4 + at["blk"]

    def up(self):
        return {"head": self.z + 1}

    def down(self):
        return {"head": self.z - 1}

    def copy(self, src, dst, device):
        k = self.used
        self.used += 1
        return self.again(k, src, dst, device)

    def slot(self):
        self.used += 1
        return self.used - 1

    def again(self, k, src, dst, device):
        return pltpu.make_async_remote_copy(
            src_ref=src,
            dst_ref=dst,
            send_sem=self.send_sem.at[k],
            recv_sem=self.recv_sem.at[k],
            device_id=device,
            device_id_type=MESH,
        )

    def local(self, src, dst):
        k = self.used
        self.used += 1
        return pltpu.make_async_copy(src, dst, self.send_sem.at[k])

    def enter(self, offsets, along_z=True, all_z=False):
        bar = pltpu.get_barrier_semaphore()
        for i in offsets:
            pl.semaphore_signal(bar, inc=1, device_id=self.plane(i), device_id_type=MESH)
        if all_z:
            for d in (1, 2, 3):
                pl.semaphore_signal(
                    bar, inc=1, device_id={"head": (self.z + d) % 4}, device_id_type=MESH
                )
            pl.semaphore_wait(bar, len(offsets) + 3)
            return
        if along_z:

            @pl.when(self.z > 0)
            def _():
                pl.semaphore_signal(bar, inc=1, device_id=self.down(), device_id_type=MESH)

            @pl.when(self.z < 3)
            def _():
                pl.semaphore_signal(bar, inc=1, device_id=self.up(), device_id_type=MESH)

        peers = len(offsets)
        if along_z:
            peers = peers + jnp.where(self.z > 0, 1, 0) + jnp.where(self.z < 3, 1, 0)
        pl.semaphore_wait(bar, peers)


class Order:
    def __init__(self, *tasks):
        self.now, self.count, self.waiting = 0.0, 0, []
        for task in tasks:
            self.add(task)

    def add(self, task, at=None):
        self.waiting.append((self.now if at is None else at, self.count, task))
        self.count += 1

    def next_at(self):
        return min(self.waiting, default=(math.inf,))[0]

    def step(self):
        item = min(self.waiting, key=lambda entry: entry[:2])
        self.waiting.remove(item)
        at = next(item[2], None)
        if at is not None:
            self.waiting.append((max(at, item[0]), item[1], item[2]))

    def pump(self, until):
        while self.next_at() <= until:
            self.step()
        self.now = max(self.now, until)

    def finish(self):
        while self.waiting:
            self.step()

    def loop(self, n, each, item, before=None):
        start = self.now

        def body(i, _):
            for k in range(n):
                while self.waiting and (
                    self.next_at() <= start + k * each or (before is not None and before(k))
                ):

                    @pl.when(i == k)
                    def _():
                        self.step()

            item(i)
            return 0

        lax.fori_loop(0, n, body, 0)
        self.now = start + n * each


def drive(*tasks):
    Order(*tasks).finish()


def z_gather(me, src, dst, unit, begin=0.0):
    rows = src.shape[0]
    z = me.z

    def block(j):
        return dst.at[pl.ds(pl.multiple_of(j * rows, rows), rows)]

    ups = [me.slot() for _ in range(3)]
    downs = [me.slot() for _ in range(3)]
    if begin:
        yield begin

    @pl.when(z < 3)
    def _():
        me.again(ups[0], src, block(z), me.up()).start()

    @pl.when(z > 0)
    def _():
        me.again(downs[0], src, block(z), me.down()).start()

    own = me.local(src, block(z))
    own.start()
    for j in (1, 2, 3):
        yield begin + unit * j

        @pl.when(z >= j)
        def _():
            me.again(ups[j - 1], block(z - j), block(z - j), me.up()).wait_recv()

        if j < 3:

            @pl.when((z >= j) & (z < 3))
            def _():
                me.again(ups[j], block(z - j), block(z - j), me.up()).start()

        @pl.when(z <= 3 - j)
        def _():
            me.again(downs[j - 1], block(z + j), block(z + j), me.down()).wait_recv()

        if j < 3:

            @pl.when((z <= 3 - j) & (z > 0))
            def _():
                me.again(downs[j], block(z + j), block(z + j), me.down()).start()

    yield begin + unit * 3.2
    own.wait()
    for j in (0, 1, 2):

        @pl.when((z >= j) & (z < 3))
        def _():
            me.again(ups[j], block(z - j), block(z - j), me.up()).wait_send()

        @pl.when((z <= 3 - j) & (z > 0))
        def _():
            me.again(downs[j], block(z + j), block(z + j), me.down()).wait_send()


def plane_gather(me, src, dst, unit, begin=0.0):
    rows = src.shape[0]
    half = rows // 2

    def block(i):
        return dst.at[pl.ds(pl.multiple_of(me.number(i) * rows, rows), rows)]

    def part(i, h):
        return dst.at[pl.ds(pl.multiple_of(me.number(i) * rows + h * half, half), half)]

    if begin:
        yield begin
    heads = src.at[pl.ds(0, half)], src.at[pl.ds(half, half)]
    x_in, y_in = [], []
    for h in (0, 1):
        x_in.append(me.copy(heads[h], part(0, h), me.plane(2)))
        x_in[h].start()
        y_in.append(me.copy(heads[1 - h], part(0, 1 - h), me.plane(4)))
        y_in[h].start()
    to_c = me.copy(src, block(0), me.plane(1))
    own = me.local(src, block(0))
    to_c.start()
    own.start()
    yield begin + unit * 0.5
    x_in[0].wait_recv()
    x_on = me.copy(part(2, 0), part(2, 0), me.plane(4))
    x_on.start()
    y_in[0].wait_recv()
    y_on = me.copy(part(4, 1), part(4, 1), me.plane(2))
    y_on.start()
    yield begin + unit
    x_in[1].wait_recv()
    x_core = me.copy(block(2), block(2), me.plane(1))
    x_core.start()
    y_in[1].wait_recv()
    y_core = me.copy(block(4), block(4), me.plane(1))
    y_core.start()
    yield begin + unit * 1.5
    x_on.wait_recv()
    d0_core = me.copy(part(6, 0), part(6, 0), me.plane(1))
    d0_core.start()
    y_on.wait_recv()
    d1_core = me.copy(part(6, 1), part(6, 1), me.plane(1))
    d1_core.start()
    yield begin + unit * 1.5 + 2.0
    own.wait()
    for copy in (to_c, x_core, y_core, d0_core, d1_core):
        copy.wait_recv()
    for copy in (*x_in, *y_in, to_c, x_on, x_core, y_on, y_core, d0_core, d1_core):
        copy.wait_send()


def add_rows(dst, a, b, step=32):
    rows = a.shape[0]

    def body(i, _):
        at = pl.ds(pl.multiple_of(i * step, step), step)
        dst[at, :] = (a[at, :].astype(f32) + b[at, :].astype(f32)).astype(dst.dtype)
        return 0

    lax.fori_loop(0, rows // step, body, 0)


class Progress:
    def __init__(self, parts):
        self.parts, self.whole = parts, 0


def z_reduce_all(me, part, total, inbox, across, out, unit, chunks, progress, begin=0.0):
    rows = part.shape[0] // chunks
    end, middle = me.end, me.middle
    first = [me.slot() for _ in range(chunks)]
    second = [me.slot() for _ in range(chunks)]
    third = [me.slot() for _ in range(chunks)]
    store = [me.slot() for _ in range(chunks)]

    def at(ref, k):
        return ref.at[pl.ds(k * rows, rows)]

    def send_in(k):
        return me.again(first[k], at(part, k), at(inbox, k), me.inward)

    def send_across(k):
        return me.again(second[k], at(inbox, k), at(across, k), me.inward)

    def send_out(k):
        return me.again(third[k], at(total, k), at(total, k), me.outward)

    def put(k):
        if out is not None:
            return pltpu.make_async_copy(at(total, k), at(out, k), me.send_sem.at[store[k]])

    yield begin
    hop = unit / chunks
    time, sent = begin, 0
    for k in range(chunks + 2):
        while min(k, chunks - 1) >= progress.parts:
            time += 1.0
            yield time
        new = range(sent, min(progress.parts, chunks))
        sent = max(sent, min(progress.parts, chunks))
        if len(new):

            @pl.when(end)
            def _():
                for j in new:
                    send_in(j).start()

        time = max(time + hop, begin + hop * (k + 1) + 2.0)
        yield time

        @pl.when(middle)
        def _():
            if k < chunks:
                send_in(k).wait_recv()
                add_rows(at(inbox, k), at(part, k), at(inbox, k))
                send_across(k).start()
            if 1 <= k <= chunks:
                send_across(k - 1).wait_recv()
                add_rows(at(total, k - 1), at(inbox, k - 1), at(across, k - 1))
                send_out(k - 1).start()
                if out is not None:
                    put(k - 1).start()

        @pl.when(end)
        def _():
            if k >= 2:
                send_out(k - 2).wait_recv()
                if out is not None:
                    put(k - 2).start()

        progress.whole = max(0, k - 1)
    yield time + 1.0

    @pl.when(end)
    def _():
        for k in range(chunks):
            send_in(k).wait_send()

    @pl.when(middle)
    def _():
        for k in range(chunks):
            send_across(k).wait_send()
            send_out(k).wait_send()

    if out is not None:
        for k in range(chunks):
            put(k).wait()


def z_reduce_scatter(me, part, from_below, from_above, own, unit, begin=0.0):
    rows = part.shape[0] // 4
    z = me.z
    ups = [me.slot() for _ in range(4)]
    downs = [me.slot() for _ in range(4)]

    def at(ref, j):
        return ref.at[pl.ds(j * rows, rows)]

    def up(j, source):
        return me.again(ups[j], at(source, j), at(from_below, j), me.up())

    def down(j, source):
        return me.again(downs[j], at(source, j), at(from_above, j), me.down())

    def start(j):
        @pl.when(z == 0)
        def _():
            up(j, part).start()

        @pl.when(z == 3)
        def _():
            down(3 - j, part).start()

    def relay(j, stop):
        @pl.when(z == stop)
        def _():
            up(j, part).wait_recv()
            add_rows(at(from_below, j), at(part, j), at(from_below, j))
            up(j, from_below).start()

        @pl.when(z == 3 - stop)
        def _():
            i = 3 - j
            down(i, part).wait_recv()
            add_rows(at(from_above, i), at(part, i), at(from_above, i))
            down(i, from_above).start()

    yield begin
    start(3)
    yield begin + unit * 0.6
    start(2)
    yield begin + unit + 1.0
    relay(3, 1)
    yield begin + unit * 1.6
    start(1)
    yield begin + unit * 2 + 1.0
    relay(3, 2)
    relay(2, 1)
    yield begin + unit * 3 + 1.5
    for j in range(4):

        @pl.when(z == j)
        def _():
            if j > 0:
                up(j, part).wait_recv()
            if j < 3:
                down(j, part).wait_recv()

            def body(i, _):
                span = pl.ds(pl.multiple_of(i * 32, 32), 32)
                there = pl.ds(pl.multiple_of(j * rows + i * 32, 32), 32)
                value = part[there, :].astype(f32)
                if j > 0:
                    value = value + from_below[there, :].astype(f32)
                if j < 3:
                    value = value + from_above[there, :].astype(f32)
                own[span, :] = value
                return 0

            lax.fori_loop(0, rows // 32, body, 0)
            for i in range(4):
                if i > j:
                    up(i, part).wait_send()
                if i < j:
                    down(i, part).wait_send()


def offsets_of(me, j):
    dx, dy, dc = 1 - (j % 4) // 2, 1 - j % 2, 1 - j // 4
    y = me.y + dy - 2 * me.y * dy
    x = me.x + dx - 2 * me.x * dx
    c = me.c + dc - 2 * me.c * dc
    return y * 4 + x * 2 + c


def plane_scatter_scratch(rows, cols):
    half = rows // 2
    return [
        pltpu.VMEM((8, rows, cols), bf16),
        pltpu.VMEM((4, rows, cols), bf16),
        pltpu.VMEM((2, half, cols), bf16),
        pltpu.VMEM((2, half, cols), bf16),
        pltpu.VMEM((half, cols), bf16),
        pltpu.VMEM((half, cols), bf16),
    ]


class PlaneScatter:
    def __init__(self, me, scratch):
        self.blocks, self.other, self.over_x, self.over_y, self.last_y, self.last_x = scratch
        blocks, rows = self.blocks, self.blocks.shape[1]
        half = rows // 2
        self.half, self.first, self.second = half, pl.ds(0, half), pl.ds(half, half)
        first, second = self.first, self.second
        self.core = [me.copy(blocks.at[j], self.other.at[j], me.plane(1)) for j in range(4)]
        self.far_x = me.copy(blocks.at[4, first], self.over_x.at[1], me.plane(2))
        self.far_y = me.copy(blocks.at[4, second], self.over_y.at[1], me.plane(4))
        self.near_x = me.copy(blocks.at[5, first], self.over_x.at[0], me.plane(2))
        self.near_y = me.copy(blocks.at[6, second], self.over_y.at[0], me.plane(4))
        self.to_y = me.copy(blocks.at[6, first], self.last_y, me.plane(4))
        self.to_x = me.copy(blocks.at[5, second], self.last_x, me.plane(2))

    def steps(self, out, unit, begin):
        blocks, half, first, second = self.blocks, self.half, self.first, self.second
        for j in range(4):
            yield begin + 0.3 * j
            self.core[j].wait_recv()
            add_rows(blocks.at[4 + j], blocks.at[4 + j], self.other.at[j])
            if j == 0:
                self.far_x.start()
                self.far_y.start()
            if j == 1:
                self.near_x.start()
            if j == 2:
                self.near_y.start()
        yield begin + 3.0 + unit * 0.5
        self.far_x.wait_recv()
        add_rows(blocks.at[6, first], blocks.at[6, first], self.over_x.at[1])
        self.to_y.start()
        self.far_y.wait_recv()
        add_rows(blocks.at[5, second], blocks.at[5, second], self.over_y.at[1])
        self.to_x.start()
        yield begin + 4.0 + unit * 1.5
        for copy in (self.near_x, self.near_y, self.to_y, self.to_x):
            copy.wait_recv()

        def body(i, _):
            at = pl.ds(pl.multiple_of(i * 32, 32), 32)
            low = pl.ds(pl.multiple_of(half + i * 32, 32), 32)
            for rows, near, last in ((at, self.over_x, self.last_y), (low, self.over_y, self.last_x)):
                value = blocks[7, rows, :].astype(f32) + near[0, at, :].astype(f32)
                out[rows, :] = (value + last[at, :].astype(f32)).astype(out.dtype)
            return 0

        lax.fori_loop(0, half // 32, body, 0)
        for copy in (*self.core, self.far_x, self.far_y, self.near_x, self.near_y, self.to_y, self.to_x):
            copy.wait_send()


def plane_scatter(me, src, out, scratch, unit, begin=0.0):
    scatter = PlaneScatter(me, scratch)
    rows = out.shape[0]
    loads = [
        me.local(
            src.at[pl.ds(pl.multiple_of(offsets_of(me, j) * rows, rows), rows)], scatter.blocks.at[j]
        )
        for j in range(8)
    ]
    yield begin
    for load in loads:
        load.start()
    for j in range(4):
        loads[j].wait()
        scatter.core[j].start()
    yield begin + 1.0
    for j in range(4, 8):
        loads[j].wait()
    yield from scatter.steps(out, unit, begin + 2.5)


def params(number, vmem=60 * 2**20):
    return pltpu.CompilerParams(
        collective_id=number, has_side_effects=True, vmem_limit_bytes=vmem
    )


def shape(dims, kind=bf16):
    return jax.ShapeDtypeStruct(dims, kind)


def first_kernel(tok, wqkv, gains, tok_all, wqkv_all, gains_all, ss, rs):
    me = Here(ss, rs)
    me.enter((1, 2, 4))
    drive(
        z_gather(me, tok, tok_all, 11.3),
        plane_gather(me, gains, gains_all, 2.0),
        plane_gather(me, wqkv, wqkv_all, 7.0),
    )


def first(tok, wqkv, gains):
    def grown(a, n):
        return shape((a.shape[0] * n,) + a.shape[1:])

    return pl.pallas_call(
        first_kernel,
        out_shape=(grown(tok, 4), grown(wqkv, 8), grown(gains, 8)),
        in_specs=[VM] * 3,
        out_specs=[HB] * 3,
        scratch_shapes=dma_sems(64),
        compiler_params=params(1),
        name="gather_first",
    )(tok, wqkv, gains)


def alone(flops, vmem=60 * 2**20):
    return dict(
        compiler_params=pltpu.CompilerParams(vmem_limit_bytes=vmem),
        cost_estimate=pl.CostEstimate(flops=int(flops), bytes_accessed=2**23, transcendentals=0),
    )


def gain_row(gains, which):
    return jnp.concatenate(
        [gains[i * 32 : i * 32 + 16, :].astype(f32)[which : which + 1] for i in range(8)], axis=1
    )


def rotate_heads(values, cos, sin, inverse=False):
    out = []
    for h in range(values.shape[0] // HD):
        a = values[h * HD : h * HD + HD // 2]
        b = values[h * HD + HD // 2 : (h + 1) * HD]
        if inverse:
            out += [a * cos + b * sin, b * cos - a * sin]
        else:
            out += [a * cos - b * sin, b * cos + a * sin]
    return jnp.concatenate(out, axis=0)


def project_kernel(tok, wqkv, gains, cos_t, sin_t, normed, q_t, q_n, kv_own):
    heads = q_t.shape[0]
    wide = heads * HD
    gain = gain_row(gains, 0)

    def body(i, _):
        at = pl.ds(pl.multiple_of(i * 128, 128), 128)
        x = tok[at, :].astype(f32)
        inv = lax.rsqrt(jnp.mean(x * x, axis=1, keepdims=True) + norm_epsilon)
        low = (x * inv * gain).astype(bf16)
        normed[at, :] = low
        lin = jnp.dot(low, wqkv[...], preferred_element_type=f32).T
        cos, sin = cos_t[:, at], sin_t[:, at]
        turned = rotate_heads(lin[: wide + HD], cos, sin)
        query = turned[:wide].astype(bf16) * bf16(1.0 / math.sqrt(HD))
        for h in range(heads):
            q_t[h, :, at] = query[h * HD : (h + 1) * HD]
        natural = query.astype(f32).T
        for h in range(heads):
            q_n[h, at, :] = natural[:, h * HD : (h + 1) * HD].astype(bf16)
        kv_own[at, :] = jnp.concatenate([turned[wide:], lin[wide + HD :]], axis=0).T.astype(bf16)
        return 0

    lax.fori_loop(0, tok.shape[0] // 128, body, 0)


def project(tok, wqkv, gains, cos_t, sin_t):
    rows = tok.shape[0]
    heads = (wqkv.shape[1] - 2 * HD) // HD
    return pl.pallas_call(
        project_kernel,
        out_shape=(
            shape(tok.shape),
            shape((heads, HD, rows)),
            shape((heads, rows, HD)),
            shape((rows, 2 * HD)),
        ),
        in_specs=[VM] * 5,
        out_specs=[VM] * 4,
        name="project",
        **alone(2 * rows * wqkv.shape[0] * wqkv.shape[1]),
    )(tok, wqkv, gains, cos_t, sin_t)


def attention_forward(me, q_t, kv_own, kv, v_t, key_pos, query_pos, out_t, attended, log_sum, kv_all, per):
    heads, hd, rows = q_t.shape
    blocks = kv.shape[0] // rows

    def block(i):
        return kv.at[pl.ds(i * rows, rows)]

    copies = [me.copy(kv_own, block(i), me.plane(i)) for i in (1, 2, 3)]
    for copy in copies:
        copy.start()
    own = me.local(kv_own, block(0))
    own.start()
    yield 0.2
    own.wait()
    for copy in copies:
        copy.wait_recv()
    save = me.local(kv, kv_all)
    save.start()
    for i in range(blocks):
        v_t[:, i * rows : (i + 1) * rows] = kv[i * rows : (i + 1) * rows, :].astype(f32).T[hd:, :].astype(bf16)

    def one_head(h):
        q = q_t[h]
        limit = query_pos[0:1, :]

        def step(i, state):
            top, total, acc = state
            at = pl.ds(pl.multiple_of(i * rows, rows), rows)
            s = jnp.dot(kv[at, 0:hd], q, preferred_element_type=f32)
            pos = key_pos[at, :]
            pos = jnp.concatenate([pos] * (rows // 128), axis=1)
            s = jnp.where(pos <= limit, s, masked_value)
            new = jnp.maximum(top, jnp.max(s, axis=0, keepdims=True))
            p = jnp.exp(s - new)
            factor = jnp.exp(top - new)
            total = total * factor + jnp.sum(p, axis=0, keepdims=True)
            acc = acc * factor + jnp.dot(v_t[:, at], p.astype(bf16), preferred_element_type=f32)
            return new, total, acc

        top, total, acc = lax.fori_loop(
            0,
            blocks,
            step,
            (
                jnp.full((1, rows), masked_value, f32),
                jnp.zeros((1, rows), f32),
                jnp.zeros((hd, rows), f32),
            ),
        )
        acc = acc / total
        out_t[h] = acc
        log_sum[h] = top + jnp.log(total)
        return acc

    for h in range(0, heads, 2):
        yield 6.0 + per * h
        pair = jnp.concatenate([one_head(h), one_head(h + 1)], axis=0)
        attended[:, h * hd : (h + 2) * hd] = pair.T.astype(bf16)
    yield 6.0 + per * heads
    save.wait()
    for copy in copies:
        copy.wait_send()


def second_kernel(
    q_t, kv_own, key_pos, query_pos, cot, wo, wu,
    out_t, attended, log_sum, kv_all, cot_all, wo_all, wu_all, kv, v_t, ss, rs
):
    me = Here(ss, rs)
    me.enter((1, 2, 3, 4))
    drive(
        attention_forward(
            me, q_t, kv_own, kv, v_t, key_pos, query_pos, out_t, attended, log_sum, kv_all, 4.0
        ),
        z_gather(me, cot, cot_all, 11.3, 0.1),
        plane_gather(me, wo, wo_all, 6.0, 0.3),
        plane_gather(me, wu, wu_all, 15.5, 6.0),
    )


def second(q_t, kv_own, key_pos, query_pos, cot, wo, wu):
    heads, hd, rows = q_t.shape
    keys = key_pos.shape[0]
    return pl.pallas_call(
        second_kernel,
        out_shape=(
            shape((heads, hd, rows), f32),
            shape((rows, heads * hd)),
            shape((heads, 1, rows), f32),
            shape((keys, 2 * hd)),
            shape((cot.shape[0] * 4, cot.shape[1])),
            shape((wo.shape[0] * 8, wo.shape[1])),
            shape((wu.shape[0] * 8, wu.shape[1])),
        ),
        in_specs=[VM] * 7,
        out_specs=[VM] * 3 + [HB] * 4,
        scratch_shapes=[pltpu.VMEM((keys, 2 * hd), bf16), pltpu.VMEM((hd, keys), bf16)] + dma_sems(64),
        compiler_params=params(2),
        name="attention_forward",
    )(q_t, kv_own, key_pos, query_pos, cot, wo, wu)


def third_kernel(part, wg, wd, total_out, wg_all, wd_all, total, inbox, across, ss, rs):
    me = Here(ss, rs)
    me.enter((1, 2, 4))
    drive(
        z_reduce_all(me, part, total, inbox, across, total_out, 45.0, 16, Progress(16)),
        plane_gather(me, wg, wg_all, 15.5, 0.1),
        plane_gather(me, wd, wd_all, 15.5, 15.0),
    )


def third(part, wg, wd):
    rows = pltpu.VMEM(part.shape, bf16)

    def grown(a):
        return shape((a.shape[0] * 8, a.shape[1]))

    return pl.pallas_call(
        third_kernel,
        out_shape=(shape(part.shape), grown(wg), grown(wd)),
        in_specs=[VM] * 3,
        out_specs=[HB] * 3,
        scratch_shapes=[rows] * 3 + dma_sems(96),
        compiler_params=params(3),
        name="sum_branch",
    )(part, wg, wd)


def contract_rows(left, right):
    return lax.dot_general(left, right, (((0,), (0,)), ((), ())), preferred_element_type=f32)


def contract_last_dims(left, right):
    return lax.dot_general(left, right, (((1,), (1,)), ((), ())), preferred_element_type=f32)


def backward_kernel(
    part, cot_all, hidden, normed_two, d_gate, d_up, wd_all, tok_all, branch, gains, wo_all,
    out_t_all, attended_all, q_t_all, q_n_all, kv_all, log_sum, key_pos, query_pos,
    dwd_own, dwg_own, dwu, out_own, dwo, own, gain_part, dq_t, dkv_own,
    total, inbox, across, cot, out_part, below, above, q_t, q_n, kv, k_t, came, *rest
):
    scratch_d, scratch_g, (ss, rs) = rest[:6], rest[6:12], rest[12:]
    me = Here(ss, rs)
    me.enter((1, 2, 3, 4))
    z = me.z
    rows, width = part.shape
    heads, hd, _ = q_t.shape
    keys = kv.shape[0]
    cols = width // 8
    progress = Progress(16)
    order = Order(z_reduce_all(me, part, total, inbox, across, None, 45.0, 16, progress))
    down, gate = PlaneScatter(me, scratch_d), PlaneScatter(me, scratch_g)
    cot_load = me.local(cot_all, cot)
    cot_load.start()
    later = [me.local(src, dst) for src, dst in ((kv_all, kv), (q_t_all, q_t), (q_n_all, q_n))]
    stores = [me.slot() for _ in range(4)]

    def weights(left, right_h, right_g, right_u, stage, wd):
        pairs = ((hidden, right_h), (normed_two, left), (d_gate, right_g), (d_up, right_u))
        loads = [me.local(src, dst) for src, dst in pairs]
        for load in loads:
            load.start()
        for load in later:
            load.start()
        cot_load.wait()
        loads[0].wait()
        order.pump(2.0)

        def columns(j):
            return pl.ds(pl.multiple_of(offsets_of(me, j) * cols, cols), cols)

        def send(scatter, j):
            for k in range(4):

                @pl.when(j == k)
                def _():
                    scatter.core[k].start()

        def down_item(j):
            down.blocks[j] = contract_rows(cot[:, columns(j)], right_h[...]).astype(bf16)
            send(down, j)

        order.loop(8, 0.9, down_item)
        order.add(down.steps(dwd_own, 15.5, order.now + 0.1))
        loads[1].wait()
        loads[2].wait()

        def gate_item(j):
            gate.blocks[j] = contract_rows(left[:, columns(j)], right_g[...]).astype(bf16)
            send(gate, j)

        order.loop(8, 0.9, gate_item)
        order.add(gate.steps(dwg_own, 15.5, order.now + 15.0))
        loads[3].wait()

        def put(j):
            at = pl.ds(pl.multiple_of(j * cols, cols), cols)
            return pltpu.make_async_copy(stage.at[j % 2], dwu.at[at], ss.at[stores[0]])

        def up_item(j):
            @pl.when(j >= 1)
            def _():
                put(j - 1).wait()

            at = pl.ds(pl.multiple_of(j * cols, cols), cols)
            stage[j % 2] = contract_rows(left[:, at], right_u[...]).astype(bf16)
            put(j).start()

        order.loop(8, 0.9, up_item)
        put(7).wait()

        def fetch(j):
            at = pl.ds(pl.multiple_of(j * cols, cols), cols)
            return pltpu.make_async_copy(wd_all.at[at], wd.at[j % 2], ss.at[stores[1]])

        fetch(0).start()

        def out_item(j):
            fetch(j).wait()

            @pl.when(j < 7)
            def _():
                fetch(j + 1).start()

            at = pl.ds(pl.multiple_of(j * cols, cols), cols)
            out_part[:, at] = contract_last_dims(right_h[...], wd[j % 2]).astype(bf16)

        order.loop(8, 0.7, out_item)

    units = pltpu.VMEM(hidden.shape, bf16)
    weight = pltpu.VMEM((2, cols, hidden.shape[1]), bf16)
    pl.run_scoped(weights, pltpu.VMEM(part.shape, bf16), units, units, units, weight, weight)

    def attention(tok, summed, wo, out_t, attended, g_t, g_n, delta, dk, dv):
        gain = gain_row(gains, 1)

        def fetch(r):
            at = pl.ds(pl.multiple_of(r * 128, 128), 128)
            return (
                pltpu.make_async_copy(tok_all.at[at], tok, ss.at[stores[2]]),
                pltpu.make_async_copy(branch.at[at], summed, ss.at[stores[3]]),
            )

        for copy in fetch(0):
            copy.start()
        loads = [
            me.local(src, dst)
            for src, dst in ((wo_all, wo), (out_t_all, out_t), (attended_all, attended))
        ]
        for load in loads:
            load.start()
        dk[...] = jnp.zeros_like(dk)
        dv[...] = jnp.zeros_like(dv)
        for load in later:
            load.wait()
        for i in range(keys // rows):
            span = slice(i * rows, (i + 1) * rows)
            k_t[:, span] = kv[span, :].astype(f32).T[:hd, :].astype(bf16)
        for load in loads:
            load.wait()
        order.add(z_reduce_scatter(me, out_part, below, above, out_own, 11.3, 47.0), 47.0)

        def prepare(r):
            for copy in fetch(r):
                copy.wait()
            at = pl.ds(pl.multiple_of(r * 128, 128), 128)
            h = tok[...].astype(f32) + summed[...].astype(f32)
            e = total[at, :].astype(f32)
            inv = lax.rsqrt(jnp.mean(h * h, axis=1, keepdims=True) + norm_epsilon)
            u = e * gain
            inner = jnp.mean(u * h, axis=1, keepdims=True)
            grad = cot[at, :].astype(f32) + (inv * u - h * (inv * inv * inv * inner))

            @pl.when(r == z)
            def _():
                own[...] = grad
                gain_part[...] = jnp.broadcast_to(
                    jnp.sum(e * h * inv, axis=0, keepdims=True), gain_part.shape
                )

            small = grad.astype(bf16)
            cot[at, :] = small
            g = jnp.dot(small, wo[...], preferred_element_type=f32).astype(bf16)
            turned = g.astype(f32).T
            for head in range(heads):
                g_n[head] = g[:, head * hd : (head + 1) * hd]
                mine = turned[head * hd : (head + 1) * hd]
                g_t[head] = mine.astype(bf16)
                delta[head] = jnp.sum(mine * out_t[head, :, at], axis=0, keepdims=True)

            @pl.when(r < rows // 128 - 1)
            def _():
                for copy in fetch(r + 1):
                    copy.start()

        def item(i):
            r, h = i // heads, i % heads

            @pl.when(h == 0)
            def _():
                prepare(r)

            at = pl.ds(pl.multiple_of(r * 128, 128), 128)
            s = jnp.dot(kv[:, 0:hd], q_t[h, :, at], preferred_element_type=f32)
            s = jnp.where(key_pos[...] <= query_pos[0:1, at], s, masked_value)
            p = jnp.exp(s - log_sum[h, :, at])
            dp = jnp.dot(kv[:, hd:], g_t[h], preferred_element_type=f32)
            ds = (p * (dp - delta[h])).astype(bf16)
            dv[...] += jnp.dot(p.astype(bf16), g_n[h], preferred_element_type=f32)
            dk[...] += jnp.dot(ds, q_n[h, at, :], preferred_element_type=f32)
            grad = jnp.dot(k_t[...], ds, preferred_element_type=f32)
            dq_t[h, :, at] = (grad * (1.0 / math.sqrt(hd))).astype(bf16)

        def before(k):
            return progress.whole < (k // heads + 1) * 4

        order.loop(heads * rows // 128, 1.2, item, before)
        for i in range(keys // rows):
            span = slice(i * rows, (i + 1) * rows)
            kv[span, :] = jnp.concatenate([dk[span, :], dv[span, :]], axis=1).astype(bf16)
        copies = [
            me.copy(kv.at[pl.ds(i * rows, rows)], came.at[i - 1], me.plane(i)) for i in (1, 2, 3)
        ]
        for copy in copies:
            copy.start()

        def out_item(i):
            span = pl.ds(pl.multiple_of(i * cols, cols), cols)
            dwo[span, :] = contract_rows(cot[:, span], attended[...]).astype(bf16)

        order.loop(8, 0.4, out_item)
        order.pump(order.now + 2.0)
        value = kv[0:rows, :].astype(f32)
        for i, copy in enumerate(copies):
            copy.wait_recv()
            value = value + came[i].astype(f32)
        dkv_own[...] = value
        for copy in copies:
            copy.wait_send()

    slots = pltpu.VMEM((128, width), bf16)
    pl.run_scoped(
        attention,
        slots,
        slots,
        pltpu.VMEM(wo_all.shape, bf16),
        pltpu.VMEM(out_t_all.shape, f32),
        pltpu.VMEM(attended_all.shape, bf16),
        pltpu.VMEM((heads, hd, 128), bf16),
        pltpu.VMEM((heads, 128, hd), bf16),
        pltpu.VMEM((heads, 1, 128), f32),
        pltpu.VMEM((keys, hd), f32),
        pltpu.VMEM((keys, hd), f32),
    )
    order.finish()


def backward(
    part, cot_all, hidden, normed_two, d_gate, d_up, wd_all, tok_all, branch, gains, wo_all,
    out_t, attended, q_t, q_n, kv_all, log_sum, key_pos, query_pos
):
    heads, hd, rows = q_t.shape
    keys = key_pos.shape[0]
    width = part.shape[1]
    whole = pltpu.VMEM(part.shape, bf16)
    own = (wd_all.shape[0] // 8, wd_all.shape[1])
    return pl.pallas_call(
        backward_kernel,
        out_shape=(
            shape(own, f32),
            shape(own, f32),
            shape(wd_all.shape),
            shape((rows // 4, width), f32),
            shape(wo_all.shape),
            shape((rows // 4, width), f32),
            shape((8, width), f32),
            shape((heads, hd, rows)),
            shape((rows, 2 * hd), f32),
        ),
        in_specs=[VM] + [HB] * 8 + [VM] + [HB] * 6 + [VM] * 3,
        out_specs=[VM, VM, HB] + [VM] * 6,
        scratch_shapes=[whole] * 7
        + [
            pltpu.VMEM(q_t.shape, bf16),
            pltpu.VMEM(q_n.shape, bf16),
            pltpu.VMEM((keys, 2 * hd), bf16),
            pltpu.VMEM((hd, keys), bf16),
            pltpu.VMEM((keys // rows - 1, rows, 2 * hd), bf16),
        ]
        + plane_scatter_scratch(*own) * 2
        + dma_sems(160),
        compiler_params=params(4, 67043328),
        name="backward",
    )(
        part, cot_all, hidden, normed_two, d_gate, d_up, wd_all, tok_all, branch, gains, wo_all,
        out_t, attended, q_t, q_n, kv_all, log_sum, key_pos, query_pos
    )


def finish_kernel(dq_t, dkv, cos_t, sin_t, wqkv, normed, tok, gain_two, one_part, dwqkv, gain_parts, lin):
    heads = dq_t.shape[0]
    wide = heads * HD
    width = tok.shape[1]
    cols = width // 8

    def body(i, total):
        at = pl.ds(pl.multiple_of(i * 128, 128), 128)
        cos, sin = cos_t[:, at], sin_t[:, at]
        kv = dkv[at, :].astype(bf16).astype(f32).T
        grads = jnp.concatenate([dq_t[h, :, at].astype(f32) for h in range(heads)] + [kv[:HD]], axis=0)
        grads = rotate_heads(grads, cos, sin, inverse=True)
        natural = jnp.concatenate([grads, kv[HD:]], axis=0).T.astype(bf16)
        lin[at, :] = natural
        one = contract_last_dims(natural, wqkv[...])
        one_part[at, :] = one.astype(bf16)
        x = tok[at, :].astype(f32)
        inv = lax.rsqrt(jnp.mean(x * x, axis=1, keepdims=True) + norm_epsilon)
        return total + jnp.sum(one * x * inv, axis=0, keepdims=True)

    total = lax.fori_loop(0, tok.shape[0] // 128, body, jnp.zeros((1, width), f32))
    for i in range(8):
        span = slice(i * cols, (i + 1) * cols)
        gain_parts[i * 8 : (i + 1) * 8, :] = jnp.concatenate(
            [total[:, span], gain_two[0:1, span], jnp.zeros((6, cols), f32)], axis=0
        )
        dwqkv[span, :] = contract_rows(normed[:, span], lin[...]).astype(bf16)


def finish(dq_t, dkv, cos_t, sin_t, wqkv, normed, tok, gain_two):
    width = tok.shape[1]
    return pl.pallas_call(
        finish_kernel,
        out_shape=(shape(tok.shape), shape(wqkv.shape), shape((64, width // 8), f32)),
        in_specs=[VM] * 8,
        out_specs=[VM] * 3,
        scratch_shapes=[pltpu.VMEM((tok.shape[0], wqkv.shape[1]), bf16)],
        name="finish_attention",
        **alone(4 * tok.shape[0] * width * wqkv.shape[1]),
    )(dq_t, dkv, cos_t, sin_t, wqkv, normed, tok, gain_two)


def gain_sums(me, src, out, came, mine, came_z):
    def block(i):
        return pl.ds(pl.multiple_of(me.number(i) * 8, 8), 8)

    copies = [me.copy(src.at[block(i)], came.at[i - 1], me.plane(i)) for i in range(1, 8)]
    for copy in copies:
        copy.start()
    yield 4.0
    value = src[block(0), :]
    for i, copy in enumerate(copies):
        copy.wait_recv()
        value = value + came[i]
    mine[...] = value
    again = [
        me.copy(mine, came_z.at[d - 1], {"head": (me.z + d) % 4}) for d in (1, 2, 3)
    ]
    for copy in again:
        copy.start()
    yield 20.0
    for d, copy in enumerate(again):
        copy.wait_recv()
        value = value + came_z[d]
    out[...] = value
    for copy in copies + again:
        copy.wait_send()


def sixth_kernel(
    part, dwqkv, dwo, dwu, gains,
    own, dwq_own, dwkv_all, dwo_own, dwu_own, gains_out,
    below, above, dwqkv_own, dwkv_own, came_kv, came, mine, came_z, *rest
):
    *scratch, ss, rs = rest
    me = Here(ss, rs)
    me.enter(tuple(range(1, 8)), all_z=True)
    wide = dwq_own.shape[1]

    def weights():
        yield from plane_scatter(me, dwqkv, dwqkv_own, scratch[:6], 7.0, 18.0)
        dwq_own[...] = dwqkv_own[:, :wide]
        dwkv_own[...] = dwqkv_own[:, wide:].astype(bf16)
        copies = [
            me.copy(dwkv_own, came_kv.at[d - 1], {"head": (me.z + d) % 4}) for d in (1, 2, 3)
        ]
        for copy in copies:
            copy.start()
        yield 45.0
        for copy in copies:
            copy.wait_recv()
        dwkv_all[0] = dwkv_own[...]
        for d in (1, 2, 3):
            dwkv_all[d] = came_kv[d - 1]
        for copy in copies:
            copy.wait_send()

    drive(
        gain_sums(me, gains, gains_out, came, mine, came_z),
        z_reduce_scatter(me, part, below, above, own, 11.3),
        plane_scatter(me, dwu, dwu_own, scratch[12:], 15.5, 0.1),
        plane_scatter(me, dwo, dwo_own, scratch[6:12], 8.0, 9.0),
        weights(),
    )


def sixth(part, dwqkv, dwo, dwu, gains):
    rows, cols = dwqkv.shape[0] // 8, dwqkv.shape[1]
    wide = dwo.shape[1]
    whole = pltpu.VMEM(part.shape, bf16)
    return pl.pallas_call(
        sixth_kernel,
        out_shape=(
            shape((part.shape[0] // 4, part.shape[1]), f32),
            shape((rows, wide), f32),
            shape((4, rows, cols - wide)),
            shape((rows, wide), f32),
            shape((rows, dwu.shape[1]), f32),
            shape((8, gains.shape[1]), f32),
        ),
        in_specs=[VM, HB, HB, HB, VM],
        out_specs=[VM] * 6,
        scratch_shapes=[
            whole, whole,
            pltpu.VMEM((rows, cols), f32),
            pltpu.VMEM((rows, cols - wide), bf16),
            pltpu.VMEM((3, rows, cols - wide), bf16),
            pltpu.VMEM((7, 8, gains.shape[1]), f32),
            pltpu.VMEM((8, gains.shape[1]), f32),
            pltpu.VMEM((3, 8, gains.shape[1]), f32),
        ]
        + plane_scatter_scratch(rows, cols)
        + plane_scatter_scratch(rows, wide)
        + plane_scatter_scratch(rows, dwu.shape[1])
        + dma_sems(96),
        compiler_params=params(6),
        name="scatter_last",
    )(part, dwqkv, dwo, dwu, gains)


def local_fast(
    tokens, w_query, w_key, w_value, w_out, w_gate, w_up, w_down, gain_attn, gain_mlp, stretch_order, cotangent
):
    row_count, width = tokens.shape
    groups = 4
    head_rows = row_count * groups
    stretch_rows = head_rows // 2
    cols = width // 8
    contract_last = (((1,), (1,)), ((), ()))
    z = lax.axis_index("head")
    b = lax.axis_index("blk")
    own_first = z * row_count

    def own_rows(values):
        return lax.dynamic_slice_in_dim(values, own_first, row_count, 0)

    query_positions = stretch_positions(stretch_order, b * head_rows, head_rows, stretch_rows)
    key_positions = jnp.concatenate(
        [
            stretch_positions(stretch_order, jnp.bitwise_xor(b, i) * head_rows, head_rows, stretch_rows)
            for i in range(4)
        ]
    )
    key_pos = jnp.broadcast_to(key_positions[:, None], (key_positions.shape[0], 128))
    query_pos = jnp.broadcast_to(query_positions[None, :], (8, head_rows))
    half = HD // 2
    frequency = rope_base ** (-(jnp.arange(half, dtype=f32) * (2.0 / HD)))
    angles = frequency[:, None] * query_positions.astype(f32)[None, :]
    cos_t, sin_t = jnp.cos(angles), jnp.sin(angles)

    slot_first = z * HD
    w_qkv = jnp.concatenate(
        [
            w_query,
            lax.dynamic_slice_in_dim(w_key, slot_first, HD, 1),
            lax.dynamic_slice_in_dim(w_value, slot_first, HD, 1),
        ],
        axis=1,
    )
    gains = jnp.concatenate([gain_attn[None], gain_mlp[None], jnp.zeros((30, cols), bf16)])
    tok_all, wqkv_all, gains_all = first(tokens, w_qkv, gains)
    normed, q_t, q_n, kv_own = project(tok_all, wqkv_all, gains_all, cos_t, sin_t)
    out_t, attended, log_sum, kv_all, cot_all, wo_all, wu_all = second(
        q_t, kv_own, key_pos, query_pos, cotangent, w_out, w_up
    )
    branch_part = lax.dot_general(attended, wo_all, contract_last, preferred_element_type=f32).astype(bf16)
    branch, wg_all, wd_all = third(branch_part, w_gate, w_down)

    gain_rows = gains_all.reshape(8, 32, cols)
    gain_one = gain_rows[:, 0].reshape(width).astype(f32)
    gain_two = gain_rows[:, 1].reshape(width).astype(f32)
    hidden_rows = tok_all.astype(f32) + branch.astype(f32)
    inv_mlp = lax.rsqrt(jnp.mean(hidden_rows * hidden_rows, axis=-1, keepdims=True) + norm_epsilon)
    normed_two = (hidden_rows * inv_mlp * gain_two).astype(bf16)
    gate = jnp.dot(normed_two, wg_all, preferred_element_type=f32)
    up = jnp.dot(normed_two, wu_all, preferred_element_type=f32)
    gate_sigmoid = jax.nn.sigmoid(gate)
    gate_silu = gate * gate_sigmoid
    hidden = (gate_silu * up).astype(bf16)
    grad_hidden = jnp.dot(cot_all, wd_all, preferred_element_type=f32)
    d_gate = (grad_hidden * up * gate_sigmoid * (1.0 + gate * (1.0 - gate_sigmoid))).astype(bf16)
    d_up = (grad_hidden * gate_silu).astype(bf16)
    two_part = lax.dot_general(d_gate, wg_all, contract_last, preferred_element_type=f32)
    two_part = two_part + lax.dot_general(d_up, wu_all, contract_last, preferred_element_type=f32)
    dwd_own, dwg_own, dwu, out_own, dwo, grad_hidden_own, gain_two_part, dq_t, dkv = backward(
        two_part.astype(bf16), cot_all, hidden, normed_two, d_gate, d_up, wd_all, tok_all, branch,
        gains_all, wo_all, out_t, attended, q_t, q_n, kv_all, log_sum, key_pos, query_pos,
    )
    one_part, dwqkv, gain_parts = finish(
        dq_t, dkv, cos_t, sin_t, wqkv_all, normed, tok_all, gain_two_part
    )
    grad_one, dwq_own, dwkv_all, dwo_own, dwu_own, gain_grads = sixth(
        one_part, dwqkv, dwo, dwu, gain_parts
    )

    x_own = tokens.astype(f32)
    layer_low = (x_own + own_rows(branch).astype(f32) + out_own).astype(bf16)
    inv_own = lax.rsqrt(jnp.mean(x_own * x_own, axis=-1, keepdims=True) + norm_epsilon)
    grad_tokens = (grad_hidden_own + norm_input_grad(x_own, inv_own, gain_one, grad_one)).astype(bf16)
    slots = jnp.concatenate(
        [lax.dynamic_slice_in_dim(dwkv_all, (z - j) % 4, 1, 0) for j in range(4)], axis=0
    ).astype(f32)
    grad_key = slots[:, :, :HD].transpose(1, 0, 2).reshape(cols, groups * HD)
    grad_value = slots[:, :, HD:].transpose(1, 0, 2).reshape(cols, groups * HD)
    return (
        layer_low,
        grad_tokens,
        dwq_own,
        grad_key,
        grad_value,
        dwo_own,
        dwg_own,
        dwu_own,
        dwd_own,
        gain_grads[0],
        gain_grads[1],
    )


def solution(mesh):
    sizes = (mesh.shape["fsdp"], mesh.shape["blk"], mesh.shape["head"])
    return jax.shard_map(
        local_fast if sizes == (2, 4, 4) else local,
        mesh=mesh,
        in_specs=(
            P(("fsdp", "blk", "head"), None),
            P(("fsdp", "blk"), "head"),
            P(("fsdp", "blk"), None),
            P(("fsdp", "blk"), None),
            P(("fsdp", "blk"), "head"),
            P(("fsdp", "blk"), "head"),
            P(("fsdp", "blk"), "head"),
            P(("fsdp", "blk"), "head"),
            P(("fsdp", "blk")),
            P(("fsdp", "blk")),
            P(),
            P(("fsdp", "blk", "head"), None),
        ),
        out_specs=(
            P(("fsdp", "blk", "head"), None),
            P(("fsdp", "blk", "head"), None),
            P(("fsdp", "blk"), "head"),
            P(("fsdp", "blk"), None),
            P(("fsdp", "blk"), None),
            P(("fsdp", "blk"), "head"),
            P(("fsdp", "blk"), "head"),
            P(("fsdp", "blk"), "head"),
            P(("fsdp", "blk"), "head"),
            P(("fsdp", "blk")),
            P(("fsdp", "blk")),
        ),
        check_vma=False,
    )
```

```python
import math

import jax
import jax.numpy as jnp
import numpy as np
from jax import lax
from jax.experimental import pallas as pl
from jax.experimental.pallas import tpu as pltpu
from jax.sharding import PartitionSpec as P

H = 32
KV = 4
HD = 64


norm_epsilon = 1e-05
rope_base = 10000.0
masked_value = -1e30


def rope_tables(positions, head_dim):
    half_dim = head_dim // 2
    frequency = rope_base ** (-(jnp.arange(half_dim, dtype=jnp.float32) * (2.0 / head_dim)))
    angles = positions.astype(jnp.float32)[:, None] * frequency[None, :]
    return (jnp.cos(angles), jnp.sin(angles))


def rotate(values, cosine, sine_table):
    half_dim = values.shape[-1] // 2
    first_half = values[..., :half_dim]
    second_half = values[..., half_dim:]
    cos_rows = cosine[:, None, :]
    sin_rows = sine_table[:, None, :]
    return jnp.concatenate(
        [
            first_half * cos_rows - second_half * sin_rows,
            second_half * cos_rows + first_half * sin_rows,
        ],
        axis=-1,
    )


def unrotate(values, cosine, sine_table):
    half_dim = values.shape[-1] // 2
    first_half = values[..., :half_dim]
    second_half = values[..., half_dim:]
    cos_rows = cosine[:, None, :]
    sin_rows = sine_table[:, None, :]
    return jnp.concatenate(
        [
            first_half * cos_rows + second_half * sin_rows,
            second_half * cos_rows - first_half * sin_rows,
        ],
        axis=-1,
    )


def stretch_positions(stretch_order, first_row, row_span, stretch_rows):
    storage = first_row + jnp.arange(row_span, dtype=jnp.int32)
    stretch_index = storage // stretch_rows
    match_table = (
        stretch_index[:, None] == jnp.arange(stretch_order.shape[0], dtype=jnp.int32)[None, :]
    )
    stretch_base = jnp.sum(jnp.where(match_table, stretch_order[None, :], 0), axis=1)
    return stretch_base * stretch_rows + storage % stretch_rows


def norm_input_grad(values, inverse, gain_vector, grad_normed):
    scaled = grad_normed * gain_vector
    inner = jnp.mean(scaled * values, axis=-1, keepdims=True)
    return inverse * scaled - values * inverse * inverse * inverse * inner


def gain_grad(values, inverse, grad_normed):
    return jnp.sum(grad_normed * values * inverse, axis=0)


def fold_block(
    state_now, keys_block, values_block, key_positions, query_heads, query_positions, score_scale
):
    running_max, running_sum, running_out = state_now
    scores = (
        jnp.einsum("qhd,kd->hqk", query_heads, keys_block, preferred_element_type=jnp.float32)
        * score_scale
    )
    allowed = (query_positions[:, None] >= key_positions[None, :])[None]
    scores = jnp.where(allowed, scores, masked_value)
    new_max = jnp.maximum(running_max, jnp.max(scores, axis=-1))
    weights = jnp.where(allowed, jnp.exp(scores - new_max[..., None]), 0.0)
    factor = jnp.exp(running_max - new_max)
    running_sum = running_sum * factor + jnp.sum(weights, axis=-1)
    running_out = running_out * factor[..., None] + jnp.einsum(
        "hqk,kd->hqd",
        weights.astype(jnp.bfloat16),
        values_block,
        preferred_element_type=jnp.float32,
    )
    return (new_max, running_sum, running_out)


def local(
    tokens,
    w_query,
    w_key,
    w_value,
    w_out,
    w_gate,
    w_up,
    w_down,
    gain_attn,
    gain_mlp,
    stretch_order,
    cotangent,
):
    row_count = tokens.shape[0]
    groups = lax.axis_size("head")
    blocks = lax.axis_size("blk")
    local_heads = H // groups
    repeats = groups // KV
    head_rows = row_count * groups
    stretch_rows = head_rows // 2
    score_scale = 1.0 / math.sqrt(HD)
    contract_last = (((1,), (1,)), ((), ()))
    contract_first = (((0,), (0,)), ((), ()))
    head_index = lax.axis_index("head")
    own_first = head_index * row_count
    block_first = lax.axis_index("blk") * head_rows
    positions = stretch_positions(stretch_order, block_first + own_first, row_count, stretch_rows)
    query_positions = stretch_positions(stretch_order, block_first, head_rows, stretch_rows)
    cos_own, sin_own = rope_tables(positions, HD)
    cos_block, sin_block = rope_tables(query_positions, HD)

    def layer_weights():
        return (
            lax.all_gather(w_query, ("fsdp", "blk"), axis=0, tiled=True),
            lax.all_gather(w_key, ("fsdp", "blk"), axis=0, tiled=True),
            lax.all_gather(w_value, ("fsdp", "blk"), axis=0, tiled=True),
            lax.all_gather(w_out, ("fsdp", "blk"), axis=0, tiled=True),
            lax.all_gather(w_gate, ("fsdp", "blk"), axis=0, tiled=True),
            lax.all_gather(w_up, ("fsdp", "blk"), axis=0, tiled=True),
            lax.all_gather(w_down, ("fsdp", "blk"), axis=0, tiled=True),
            lax.all_gather(gain_attn, ("fsdp", "blk"), axis=0, tiled=True),
            lax.all_gather(gain_mlp, ("fsdp", "blk"), axis=0, tiled=True),
        )

    def gather_query(columns):
        return lax.all_gather(columns, "head", axis=1, tiled=True)

    (
        query_cols,
        key_full,
        value_full,
        out_cols,
        gate_cols,
        up_cols,
        down_cols,
        gain_one,
        gain_two,
    ) = layer_weights()
    tokens_float = tokens.astype(jnp.float32)
    inv_attn = lax.rsqrt(
        jnp.mean(tokens_float * tokens_float, axis=-1, keepdims=True) + norm_epsilon
    )
    normed = (tokens_float * inv_attn * gain_one.astype(jnp.float32)).astype(jnp.bfloat16)
    normed_rows, cotangent_rows = (
        lax.all_gather(normed, "head", axis=0, tiled=True),
        lax.all_gather(cotangent, "head", axis=0, tiled=True),
    )
    query_all = gather_query(query_cols)
    query_lin = jnp.dot(normed, query_all, preferred_element_type=jnp.float32).reshape(
        row_count, H, HD
    )
    key_lin = jnp.dot(normed, key_full, preferred_element_type=jnp.float32).reshape(
        row_count, KV, HD
    )
    value_lin = jnp.dot(normed, value_full, preferred_element_type=jnp.float32).reshape(
        row_count, KV, HD
    )
    query_rot = rotate(query_lin, cos_own, sin_own).astype(jnp.bfloat16).reshape(row_count, H * HD)
    key_rot = rotate(key_lin, cos_own, sin_own).astype(jnp.bfloat16)
    key_slots = jnp.repeat(key_rot, repeats, axis=1).reshape(row_count, groups * HD)
    value_slots = jnp.repeat(value_lin.astype(jnp.bfloat16), repeats, axis=1).reshape(
        row_count, groups * HD
    )
    query_recv, key_own, value_own = (
        lax.all_to_all(query_rot, "head", split_axis=1, concat_axis=0, tiled=True),
        lax.all_to_all(key_slots, "head", split_axis=1, concat_axis=0, tiled=True),
        lax.all_to_all(value_slots, "head", split_axis=1, concat_axis=0, tiled=True),
    )
    query_heads = query_recv.reshape(head_rows, local_heads, HD)
    initial = (
        jnp.full((local_heads, head_rows), masked_value, jnp.float32),
        jnp.zeros((local_heads, head_rows), jnp.float32),
        jnp.zeros((local_heads, head_rows, HD), jnp.float32),
    )
    state_now = initial
    keys_piece = lax.all_gather(key_own, "blk", axis=0, tiled=True)
    values_piece = lax.all_gather(value_own, "blk", axis=0, tiled=True)
    piece_rows = keys_piece.shape[0]

    def scan_step(state_inner, step_index):
        offset = step_index * head_rows
        keys_block = lax.dynamic_slice_in_dim(keys_piece, offset, head_rows, 0)
        values_block = lax.dynamic_slice_in_dim(values_piece, offset, head_rows, 0)
        key_positions = stretch_positions(stretch_order, offset, head_rows, stretch_rows)
        return (
            fold_block(
                state_inner,
                keys_block,
                values_block,
                key_positions,
                query_heads,
                query_positions,
                score_scale,
            ),
            None,
        )

    state_now, unused = lax.scan(
        scan_step, state_now, jnp.arange(piece_rows // head_rows, dtype=jnp.int32)
    )
    running_max, running_sum, running_out = state_now
    attended_float = running_out / running_sum[..., None]
    log_sum = running_max + jnp.log(running_sum)
    attended_heads = (
        attended_float.astype(jnp.bfloat16).transpose(1, 0, 2).reshape(head_rows, local_heads * HD)
    )
    branch = lax.dot_general(
        attended_heads, out_cols, contract_last, preferred_element_type=jnp.float32
    )
    own_branch = lax.dynamic_slice_in_dim(branch, own_first, row_count, 0)
    partial_value = lax.dynamic_update_slice_in_dim(branch, own_branch + tokens_float, own_first, 0)
    hidden_rows = lax.psum(partial_value.astype(jnp.bfloat16), "head").astype(jnp.float32)
    inv_mlp = lax.rsqrt(jnp.mean(hidden_rows * hidden_rows, axis=-1, keepdims=True) + norm_epsilon)
    normed_two_rows = (hidden_rows * inv_mlp * gain_two.astype(jnp.float32)).astype(jnp.bfloat16)
    gate_proj = jnp.dot(normed_two_rows, gate_cols, preferred_element_type=jnp.float32)
    up_proj = jnp.dot(normed_two_rows, up_cols, preferred_element_type=jnp.float32)
    gate_sigmoid = jax.nn.sigmoid(gate_proj)
    gate_silu = gate_proj * gate_sigmoid
    hidden = (gate_silu * up_proj).astype(jnp.bfloat16)
    hidden_own = lax.dynamic_slice_in_dim(hidden_rows, own_first, row_count, 0)
    output_float = hidden_own + lax.psum_scatter(
        lax.dot_general(
            hidden, down_cols, contract_last, preferred_element_type=jnp.float32
        ).astype(jnp.bfloat16),
        "head",
        scatter_dimension=0,
        tiled=True,
    ).astype(jnp.float32)
    layer_low = output_float.astype(jnp.bfloat16)
    (
        query_cols,
        key_full,
        value_full,
        out_cols,
        gate_cols,
        up_cols,
        down_cols,
        gain_one,
        gain_two,
    ) = layer_weights()
    query_all = gather_query(query_cols)
    grad_hidden = jnp.dot(cotangent_rows, down_cols, preferred_element_type=jnp.float32)
    grad_gate_rows = (
        grad_hidden * up_proj * gate_sigmoid * (1.0 + gate_proj * (1.0 - gate_sigmoid))
    ).astype(jnp.bfloat16)
    grad_up_rows = (grad_hidden * gate_silu).astype(jnp.bfloat16)
    grad_w_down = lax.dot_general(
        cotangent_rows, hidden, contract_first, preferred_element_type=jnp.float32
    )
    grad_w_gate = lax.dot_general(
        normed_two_rows, grad_gate_rows, contract_first, preferred_element_type=jnp.float32
    )
    grad_w_up = lax.dot_general(
        normed_two_rows, grad_up_rows, contract_first, preferred_element_type=jnp.float32
    )
    normed_two_part = lax.dot_general(
        grad_gate_rows, gate_cols, contract_last, preferred_element_type=jnp.float32
    )
    normed_two_part = normed_two_part + lax.dot_general(
        grad_up_rows, up_cols, contract_last, preferred_element_type=jnp.float32
    )
    grad_normed_two = lax.psum(normed_two_part.astype(jnp.bfloat16), "head").astype(jnp.float32)
    gain_two_float = gain_two.astype(jnp.float32)
    grad_hidden_rows = cotangent_rows.astype(jnp.float32) + norm_input_grad(
        hidden_rows, inv_mlp, gain_two_float, grad_normed_two
    )
    own_grad_two = lax.dynamic_slice_in_dim(grad_normed_two, own_first, row_count, 0)
    own_inv_mlp = lax.dynamic_slice_in_dim(inv_mlp, own_first, row_count, 0)
    grad_gain_two = gain_grad(hidden_own, own_inv_mlp, own_grad_two)
    grad_low_rows = grad_hidden_rows.astype(jnp.bfloat16)
    grad_w_out = lax.dot_general(
        grad_low_rows, attended_heads, contract_first, preferred_element_type=jnp.float32
    )
    grad_heads = (
        jnp.dot(grad_low_rows, out_cols, preferred_element_type=jnp.float32)
        .astype(jnp.bfloat16)
        .reshape(head_rows, local_heads, HD)
    )
    keys_all, values_all = (
        lax.all_gather(key_own, "blk", axis=0, tiled=True),
        lax.all_gather(value_own, "blk", axis=0, tiled=True),
    )
    row_delta = jnp.sum(grad_heads.astype(jnp.float32).transpose(1, 0, 2) * attended_float, axis=-1)

    def back_block(grad_query_acc, block_index):
        offset = block_index * head_rows
        keys_block = lax.dynamic_slice_in_dim(keys_all, offset, head_rows, 0)
        values_block = lax.dynamic_slice_in_dim(values_all, offset, head_rows, 0)
        key_positions = stretch_positions(stretch_order, offset, head_rows, stretch_rows)
        scores = (
            jnp.einsum("qhd,kd->hqk", query_heads, keys_block, preferred_element_type=jnp.float32)
            * score_scale
        )
        allowed = (query_positions[:, None] >= key_positions[None, :])[None]
        probs_block = jnp.where(allowed, jnp.exp(scores - log_sum[..., None]), 0.0)
        grad_probs = jnp.einsum(
            "qhd,kd->hqk", grad_heads, values_block, preferred_element_type=jnp.float32
        )
        grad_scores = (probs_block * (grad_probs - row_delta[..., None])).astype(jnp.bfloat16)
        grad_query_acc = grad_query_acc + jnp.einsum(
            "hqk,kd->qhd", grad_scores, keys_block, preferred_element_type=jnp.float32
        )
        grad_key_part = (
            jnp.einsum("hqk,qhd->kd", grad_scores, query_heads, preferred_element_type=jnp.float32)
            * score_scale
        )
        grad_value_part = jnp.einsum(
            "hqk,qhd->kd",
            probs_block.astype(jnp.bfloat16),
            grad_heads,
            preferred_element_type=jnp.float32,
        )
        return (grad_query_acc, (grad_key_part, grad_value_part))

    grad_query_acc, (key_terms, value_terms) = lax.scan(
        back_block,
        jnp.zeros((head_rows, local_heads, HD), jnp.float32),
        jnp.arange(blocks, dtype=jnp.int32),
    )
    grad_key_sum, grad_value_sum = (
        lax.psum_scatter(
            key_terms.reshape(blocks * head_rows, HD).astype(jnp.bfloat16),
            "blk",
            scatter_dimension=0,
            tiled=True,
        ).astype(jnp.float32),
        lax.psum_scatter(
            value_terms.reshape(blocks * head_rows, HD).astype(jnp.bfloat16),
            "blk",
            scatter_dimension=0,
            tiled=True,
        ).astype(jnp.float32),
    )
    grad_query_rot = (grad_query_acc * score_scale).astype(jnp.bfloat16)
    grad_query_lin_heads = (
        unrotate(grad_query_rot.astype(jnp.float32), cos_block, sin_block)
        .astype(jnp.bfloat16)
        .reshape(head_rows, local_heads * HD)
    )
    key_slot_grad = grad_key_sum.astype(jnp.bfloat16)
    value_slot_grad = grad_value_sum.astype(jnp.bfloat16)
    grad_w_query = lax.dot_general(
        normed_rows, grad_query_lin_heads, contract_first, preferred_element_type=jnp.float32
    )
    query_back, key_back, value_back = (
        lax.all_to_all(grad_query_lin_heads, "head", split_axis=0, concat_axis=1, tiled=True),
        lax.all_to_all(key_slot_grad, "head", split_axis=0, concat_axis=1, tiled=True),
        lax.all_to_all(value_slot_grad, "head", split_axis=0, concat_axis=1, tiled=True),
    )
    key_slot_lin = (
        unrotate(key_back.astype(jnp.float32).reshape(row_count, groups, HD), cos_own, sin_own)
        .astype(jnp.bfloat16)
        .reshape(row_count, KV, repeats, HD)
    )
    value_slot_lin = value_back.reshape(row_count, KV, repeats, HD)
    grad_w_key = jnp.einsum(
        "td,tjrc->djc", normed, key_slot_lin, preferred_element_type=jnp.float32
    ).reshape(-1, KV * HD)
    grad_w_value = jnp.einsum(
        "td,tjrc->djc", normed, value_slot_lin, preferred_element_type=jnp.float32
    ).reshape(-1, KV * HD)
    grad_normed = lax.dot_general(
        query_back, query_all, contract_last, preferred_element_type=jnp.float32
    )
    grad_normed = grad_normed + jnp.einsum(
        "tjrc,djc->td",
        key_slot_lin,
        key_full.reshape(-1, KV, HD),
        preferred_element_type=jnp.float32,
    )
    grad_normed = grad_normed + jnp.einsum(
        "tjrc,djc->td",
        value_slot_lin,
        value_full.reshape(-1, KV, HD),
        preferred_element_type=jnp.float32,
    )
    gain_one_float = gain_one.astype(jnp.float32)
    grad_input_norm = norm_input_grad(tokens_float, inv_attn, gain_one_float, grad_normed)
    grad_gain_one = gain_grad(tokens_float, inv_attn, grad_normed)
    grad_hidden_own = lax.dynamic_slice_in_dim(grad_hidden_rows, own_first, row_count, 0)
    grad_tokens = (grad_hidden_own + grad_input_norm).astype(jnp.bfloat16)
    head_sums = (
        lax.psum(grad_w_key.astype(jnp.bfloat16), "head").astype(jnp.float32),
        lax.psum(grad_w_value.astype(jnp.bfloat16), "head").astype(jnp.float32),
        lax.psum(grad_gain_one.astype(jnp.bfloat16), "head").astype(jnp.float32),
        lax.psum(grad_gain_two.astype(jnp.bfloat16), "head").astype(jnp.float32),
    )
    reduced = (
        lax.psum_scatter(
            grad_w_query.astype(jnp.bfloat16), ("fsdp", "blk"), scatter_dimension=0, tiled=True
        ).astype(jnp.float32),
        lax.psum_scatter(
            head_sums[0].astype(jnp.bfloat16), ("fsdp", "blk"), scatter_dimension=0, tiled=True
        ).astype(jnp.float32),
        lax.psum_scatter(
            head_sums[1].astype(jnp.bfloat16), ("fsdp", "blk"), scatter_dimension=0, tiled=True
        ).astype(jnp.float32),
        lax.psum_scatter(
            grad_w_out.astype(jnp.bfloat16), ("fsdp", "blk"), scatter_dimension=0, tiled=True
        ).astype(jnp.float32),
        lax.psum_scatter(
            grad_w_gate.astype(jnp.bfloat16), ("fsdp", "blk"), scatter_dimension=0, tiled=True
        ).astype(jnp.float32),
        lax.psum_scatter(
            grad_w_up.astype(jnp.bfloat16), ("fsdp", "blk"), scatter_dimension=0, tiled=True
        ).astype(jnp.float32),
        lax.psum_scatter(
            grad_w_down.astype(jnp.bfloat16), ("fsdp", "blk"), scatter_dimension=0, tiled=True
        ).astype(jnp.float32),
        lax.psum_scatter(
            head_sums[2].astype(jnp.bfloat16), ("fsdp", "blk"), scatter_dimension=0, tiled=True
        ).astype(jnp.float32),
        lax.psum_scatter(
            head_sums[3].astype(jnp.bfloat16), ("fsdp", "blk"), scatter_dimension=0, tiled=True
        ).astype(jnp.float32),
    )
    return (
        layer_low,
        grad_tokens,
        reduced[0],
        reduced[1],
        reduced[2],
        reduced[3],
        reduced[4],
        reduced[5],
        reduced[6],
        reduced[7],
        reduced[8],
    )


MESH = pl.DeviceIdType.MESH
f32, bf16 = jnp.float32, jnp.bfloat16
VM = pl.BlockSpec(memory_space=pltpu.VMEM)
HB = pl.BlockSpec(memory_space=pl.ANY)


def dma_sems(n):
    return [pltpu.SemaphoreType.DMA((n,)), pltpu.SemaphoreType.DMA((n,))]


class Here:
    def __init__(self, send_sem, recv_sem):
        self.y = lax.axis_index("fsdp")
        blk = lax.axis_index("blk")
        self.x, self.c = blk // 2, blk % 2
        self.z = lax.axis_index("head")
        self.end = (self.z == 0) | (self.z == 3)
        self.middle = (self.z == 1) | (self.z == 2)
        self.inward = {"head": jnp.where(self.z < 2, self.z + 1, self.z - 1)}
        self.outward = {"head": jnp.where(self.z < 2, self.z - 1, self.z + 1)}
        self.send_sem, self.recv_sem, self.used = send_sem, recv_sem, 0

    def plane(self, i):
        y = 1 - self.y if i & 4 else self.y
        x = 1 - self.x if i & 2 else self.x
        c = 1 - self.c if i & 1 else self.c
        return {"fsdp": y, "blk": x * 2 + c}

    def number(self, i):
        at = self.plane(i)
        return at["fsdp"] * 4 + at["blk"]

    def up(self):
        return {"head": self.z + 1}

    def down(self):
        return {"head": self.z - 1}

    def copy(self, src, dst, device):
        k = self.used
        self.used += 1
        return self.again(k, src, dst, device)

    def slot(self):
        self.used += 1
        return self.used - 1

    def again(self, k, src, dst, device):
        return pltpu.make_async_remote_copy(
            src_ref=src,
            dst_ref=dst,
            send_sem=self.send_sem.at[k],
            recv_sem=self.recv_sem.at[k],
            device_id=device,
            device_id_type=MESH,
        )

    def local(self, src, dst):
        k = self.used
        self.used += 1
        return pltpu.make_async_copy(src, dst, self.send_sem.at[k])

    def enter(self, offsets, along_z=True, all_z=False):
        bar = pltpu.get_barrier_semaphore()
        for i in offsets:
            pl.semaphore_signal(bar, inc=1, device_id=self.plane(i), device_id_type=MESH)
        if all_z:
            for d in (1, 2, 3):
                pl.semaphore_signal(
                    bar, inc=1, device_id={"head": (self.z + d) % 4}, device_id_type=MESH
                )
            pl.semaphore_wait(bar, len(offsets) + 3)
            return
        if along_z:

            @pl.when(self.z > 0)
            def _():
                pl.semaphore_signal(bar, inc=1, device_id=self.down(), device_id_type=MESH)

            @pl.when(self.z < 3)
            def _():
                pl.semaphore_signal(bar, inc=1, device_id=self.up(), device_id_type=MESH)

        peers = len(offsets)
        if along_z:
            peers = peers + jnp.where(self.z > 0, 1, 0) + jnp.where(self.z < 3, 1, 0)
        pl.semaphore_wait(bar, peers)


class Order:
    def __init__(self, *tasks):
        self.now, self.count, self.waiting = 0.0, 0, []
        for task in tasks:
            self.add(task)

    def add(self, task, at=None):
        self.waiting.append((self.now if at is None else at, self.count, task))
        self.count += 1

    def next_at(self):
        return min(self.waiting, default=(math.inf,))[0]

    def step(self):
        item = min(self.waiting, key=lambda entry: entry[:2])
        self.waiting.remove(item)
        at = next(item[2], None)
        if at is not None:
            self.waiting.append((max(at, item[0]), item[1], item[2]))

    def pump(self, until):
        while self.next_at() <= until:
            self.step()
        self.now = max(self.now, until)

    def until(self, *flags):
        while not all(flag.up for flag in flags):
            self.now = max(self.now, self.next_at())
            self.step()

    def finish(self):
        while self.waiting:
            self.step()

    def loop(self, n, each, item, before=None):
        start = self.now

        def body(i, _):
            for k in range(n):
                while self.waiting and (
                    self.next_at() <= start + k * each or (before is not None and before(k))
                ):

                    @pl.when(i == k)
                    def _():
                        self.step()

            item(i)
            return 0

        lax.fori_loop(0, n, body, 0)
        self.now = start + n * each


def drive(*tasks):
    Order(*tasks).finish()


class Flag:
    def __init__(self):
        self.up = False


def z_gather(me, src, dst, unit, begin=0.0, done=None):
    rows = src.shape[0]
    z = me.z

    def block(j):
        return dst.at[pl.ds(pl.multiple_of(j * rows, rows), rows)]

    ups = [me.slot() for _ in range(3)]
    downs = [me.slot() for _ in range(3)]
    own = me.local(src, block(z))

    def up(j):
        return me.again(ups[j], src if j == 0 else block(z - j), block(z - j), me.up())

    def down(j):
        return me.again(downs[j], src if j == 0 else block(z + j), block(z + j), me.down())

    def steps():
        yield begin

        @pl.when(z < 3)
        def _():
            up(0).start()

        @pl.when(z > 0)
        def _():
            down(0).start()

        own.start()
        for j in (1, 2, 3):
            yield begin + unit * j

            @pl.when(z >= j)
            def _():
                up(j - 1).wait_recv()

            if j < 3:

                @pl.when((z >= j) & (z < 3))
                def _():
                    up(j).start()

            @pl.when(z <= 3 - j)
            def _():
                down(j - 1).wait_recv()

            if j < 3:

                @pl.when((z <= 3 - j) & (z > 0))
                def _():
                    down(j).start()

        own.wait()
        if done is not None:
            done.up = True
        yield begin + unit * 3 + 1.0
        for j in (0, 1, 2):

            @pl.when((z >= j) & (z < 3))
            def _():
                up(j).wait_send()

            @pl.when((z <= 3 - j) & (z > 0))
            def _():
                down(j).wait_send()

    return steps()


def plane_gather(me, src, dst, unit, begin=0.0, done=None):
    rows = src.shape[0]
    half = rows // 2

    def part(i, h):
        return dst.at[pl.ds(pl.multiple_of(me.number(i) * rows + h * half, half), half)]

    def block(i):
        return dst.at[pl.ds(pl.multiple_of(me.number(i) * rows, rows), rows)]

    halves = src.at[pl.ds(0, half)], src.at[pl.ds(half, half)]
    x_in = [me.copy(halves[h], part(0, h), me.plane(2)) for h in (0, 1)]
    y_in = [me.copy(halves[h], part(0, h), me.plane(4)) for h in (1, 0)]
    to_c = me.copy(src, block(0), me.plane(1))
    own = me.local(src, block(0))
    x_on = me.copy(part(2, 0), part(2, 0), me.plane(4))
    y_on = me.copy(part(4, 1), part(4, 1), me.plane(2))
    x_core = me.copy(block(2), block(2), me.plane(1))
    y_core = me.copy(block(4), block(4), me.plane(1))
    far = [me.copy(part(6, h), part(6, h), me.plane(1)) for h in (0, 1)]

    def steps():
        yield begin
        for copy in (x_in[0], y_in[0], x_in[1], y_in[1], to_c, own):
            copy.start()
        yield begin + unit * 0.5
        x_in[0].wait_recv()
        x_on.start()
        y_in[0].wait_recv()
        y_on.start()
        yield begin + unit
        x_in[1].wait_recv()
        x_core.start()
        y_in[1].wait_recv()
        y_core.start()
        yield begin + unit * 1.5
        x_on.wait_recv()
        far[0].start()
        y_on.wait_recv()
        far[1].start()
        yield begin + unit * 1.5 + 2.0
        own.wait()
        for copy in (to_c, x_core, y_core, *far):
            copy.wait_recv()
        if done is not None:
            done.up = True
        yield begin + unit * 1.5 + 2.5
        for copy in (*x_in, *y_in, to_c, x_on, x_core, y_on, y_core, *far):
            copy.wait_send()

    return steps()


def add_rows(dst, a, b, step=32):
    rows = a.shape[0]

    def body(i, _):
        at = pl.ds(pl.multiple_of(i * step, step), step)
        dst[at, :] = (a[at, :].astype(f32) + b[at, :].astype(f32)).astype(dst.dtype)
        return 0

    lax.fori_loop(0, rows // step, body, 0)


class Progress:
    def __init__(self, parts):
        self.parts, self.whole = parts, 0


def z_reduce_all(me, part, total, inbox, across, out, unit, chunks, progress, begin=0.0):
    rows = part.shape[0] // chunks
    end, middle = me.end, me.middle
    first = [me.slot() for _ in range(chunks)]
    second = [me.slot() for _ in range(chunks)]
    third = [me.slot() for _ in range(chunks)]
    store = [me.slot() for _ in range(chunks)]

    def at(ref, k):
        return ref.at[pl.ds(k * rows, rows)]

    def send_in(k):
        return me.again(first[k], at(part, k), at(inbox, k), me.inward)

    def send_across(k):
        return me.again(second[k], at(inbox, k), at(across, k), me.inward)

    def send_out(k):
        return me.again(third[k], at(total, k), at(total, k), me.outward)

    def put(k):
        if out is not None:
            return pltpu.make_async_copy(at(total, k), at(out, k), me.send_sem.at[store[k]])

    yield begin
    hop = unit / chunks
    time, sent = begin, 0
    for k in range(chunks + 2):
        while min(k, chunks - 1) >= progress.parts:
            time += 1.0
            yield time
        new = range(sent, min(progress.parts, chunks))
        sent = max(sent, min(progress.parts, chunks))
        if len(new):

            @pl.when(end)
            def _():
                for j in new:
                    send_in(j).start()

        time = max(time + hop, begin + hop * (k + 1) + 2.0)
        yield time

        @pl.when(middle)
        def _():
            if k < chunks:
                send_in(k).wait_recv()
                add_rows(at(inbox, k), at(part, k), at(inbox, k))
                send_across(k).start()
            if 1 <= k <= chunks:
                send_across(k - 1).wait_recv()
                add_rows(at(total, k - 1), at(inbox, k - 1), at(across, k - 1))
                send_out(k - 1).start()
                if out is not None:
                    put(k - 1).start()

        @pl.when(end)
        def _():
            if k >= 2:
                send_out(k - 2).wait_recv()
                if out is not None:
                    put(k - 2).start()

        progress.whole = max(0, k - 1)
    yield time + 1.0

    @pl.when(end)
    def _():
        for k in range(chunks):
            send_in(k).wait_send()

    @pl.when(middle)
    def _():
        for k in range(chunks):
            send_across(k).wait_send()
            send_out(k).wait_send()

    if out is not None:
        for k in range(chunks):
            put(k).wait()


def z_reduce_scatter(me, part, from_below, from_above, own, unit, begin=0.0):
    rows = part.shape[0] // 4
    z = me.z
    ups = [me.slot() for _ in range(4)]
    downs = [me.slot() for _ in range(4)]

    def at(ref, j):
        return ref.at[pl.ds(j * rows, rows)]

    def up(j, source):
        return me.again(ups[j], at(source, j), at(from_below, j), me.up())

    def down(j, source):
        return me.again(downs[j], at(source, j), at(from_above, j), me.down())

    def start(j):
        @pl.when(z == 0)
        def _():
            up(j, part).start()

        @pl.when(z == 3)
        def _():
            down(3 - j, part).start()

    def relay(j, stop):
        @pl.when(z == stop)
        def _():
            up(j, part).wait_recv()
            add_rows(at(from_below, j), at(part, j), at(from_below, j))
            up(j, from_below).start()

        @pl.when(z == 3 - stop)
        def _():
            i = 3 - j
            down(i, part).wait_recv()
            add_rows(at(from_above, i), at(part, i), at(from_above, i))
            down(i, from_above).start()

    yield begin
    start(3)
    yield begin + unit * 0.6
    start(2)
    yield begin + unit + 1.0
    relay(3, 1)
    yield begin + unit * 1.6
    start(1)
    yield begin + unit * 2 + 1.0
    relay(3, 2)
    relay(2, 1)
    yield begin + unit * 3 + 1.5
    for j in range(4):

        @pl.when(z == j)
        def _():
            if j > 0:
                up(j, part).wait_recv()
            if j < 3:
                down(j, part).wait_recv()

            def body(i, _):
                span = pl.ds(pl.multiple_of(i * 32, 32), 32)
                there = pl.ds(pl.multiple_of(j * rows + i * 32, 32), 32)
                value = part[there, :].astype(f32)
                if j > 0:
                    value = value + from_below[there, :].astype(f32)
                if j < 3:
                    value = value + from_above[there, :].astype(f32)
                own[span, :] = value
                return 0

            lax.fori_loop(0, rows // 32, body, 0)
            for i in range(4):
                if i > j:
                    up(i, part).wait_send()
                if i < j:
                    down(i, part).wait_send()


def offsets_of(me, j):
    dx, dy, dc = 1 - (j % 4) // 2, 1 - j % 2, 1 - j // 4
    y = me.y + dy - 2 * me.y * dy
    x = me.x + dx - 2 * me.x * dx
    c = me.c + dc - 2 * me.c * dc
    return y * 4 + x * 2 + c


def plane_scatter_scratch(rows, cols):
    half = rows // 2
    return [
        pltpu.VMEM((8, rows, cols), bf16),
        pltpu.VMEM((4, rows, cols), bf16),
        pltpu.VMEM((2, half, cols), bf16),
        pltpu.VMEM((2, half, cols), bf16),
        pltpu.VMEM((half, cols), bf16),
        pltpu.VMEM((half, cols), bf16),
    ]


class PlaneScatter:
    def __init__(self, me, scratch):
        self.blocks, self.other, self.over_x, self.over_y, self.last_y, self.last_x = scratch
        blocks, rows = self.blocks, self.blocks.shape[1]
        half = rows // 2
        self.half, self.first, self.second = half, pl.ds(0, half), pl.ds(half, half)
        first, second = self.first, self.second
        self.core = [me.copy(blocks.at[j], self.other.at[j], me.plane(1)) for j in range(4)]
        self.far_x = me.copy(blocks.at[4, first], self.over_x.at[1], me.plane(2))
        self.far_y = me.copy(blocks.at[4, second], self.over_y.at[1], me.plane(4))
        self.near_x = me.copy(blocks.at[5, first], self.over_x.at[0], me.plane(2))
        self.near_y = me.copy(blocks.at[6, second], self.over_y.at[0], me.plane(4))
        self.to_y = me.copy(blocks.at[6, first], self.last_y, me.plane(4))
        self.to_x = me.copy(blocks.at[5, second], self.last_x, me.plane(2))

    def steps(self, out, unit, begin):
        blocks, half, first, second = self.blocks, self.half, self.first, self.second
        for j in range(4):
            yield begin + 0.3 * j
            self.core[j].wait_recv()
            add_rows(blocks.at[4 + j], blocks.at[4 + j], self.other.at[j])
            if j == 0:
                self.far_x.start()
                self.far_y.start()
            if j == 1:
                self.near_x.start()
            if j == 2:
                self.near_y.start()
        yield begin + 3.0 + unit * 0.5
        self.far_x.wait_recv()
        add_rows(blocks.at[6, first], blocks.at[6, first], self.over_x.at[1])
        self.to_y.start()
        self.far_y.wait_recv()
        add_rows(blocks.at[5, second], blocks.at[5, second], self.over_y.at[1])
        self.to_x.start()
        yield begin + 4.0 + unit * 1.5
        for copy in (self.near_x, self.near_y, self.to_y, self.to_x):
            copy.wait_recv()

        def body(i, _):
            at = pl.ds(pl.multiple_of(i * 32, 32), 32)
            low = pl.ds(pl.multiple_of(half + i * 32, 32), 32)
            for rows, near, last in ((at, self.over_x, self.last_y), (low, self.over_y, self.last_x)):
                value = blocks[7, rows, :].astype(f32) + near[0, at, :].astype(f32)
                out[rows, :] = (value + last[at, :].astype(f32)).astype(out.dtype)
            return 0

        lax.fori_loop(0, half // 32, body, 0)
        for copy in (*self.core, self.far_x, self.far_y, self.near_x, self.near_y, self.to_y, self.to_x):
            copy.wait_send()


def plane_scatter(me, src, out, scratch, unit, begin=0.0):
    scatter = PlaneScatter(me, scratch)
    rows = out.shape[0]
    loads = [
        me.local(
            src.at[pl.ds(pl.multiple_of(offsets_of(me, j) * rows, rows), rows)], scatter.blocks.at[j]
        )
        for j in range(8)
    ]
    yield begin
    for load in loads:
        load.start()
    for j in range(4):
        loads[j].wait()
        scatter.core[j].start()
    yield begin + 1.0
    for j in range(4, 8):
        loads[j].wait()
    yield from scatter.steps(out, unit, begin + 2.5)


def params(number, vmem=60 * 2**20):
    return pltpu.CompilerParams(
        collective_id=number, has_side_effects=True, vmem_limit_bytes=vmem
    )


def shape(dims, kind=bf16):
    return jax.ShapeDtypeStruct(dims, kind)


def alone(flops, vmem=60 * 2**20):
    return dict(
        compiler_params=pltpu.CompilerParams(vmem_limit_bytes=vmem),
        cost_estimate=pl.CostEstimate(flops=int(flops), bytes_accessed=2**23, transcendentals=0),
    )


def gain_row(gains, which):
    return jnp.concatenate([gains[i * 16 + which : i * 16 + which + 1, :] for i in range(8)], axis=1)


def rotate_heads(values, cos, sin, inverse=False):
    out = []
    for h in range(values.shape[0] // HD):
        a = values[h * HD : h * HD + HD // 2]
        b = values[h * HD + HD // 2 : (h + 1) * HD]
        if inverse:
            out += [a * cos + b * sin, b * cos - a * sin]
        else:
            out += [a * cos - b * sin, b * cos + a * sin]
    return jnp.concatenate(out, axis=0)


def block_positions(order_ref, number, stretch_rows):
    row = lax.broadcasted_iota(jnp.int32, (stretch_rows, 128), 0)
    return jnp.concatenate(
        [row + order_ref[number * 2 + i] * stretch_rows for i in range(2)], axis=0
    )


def forward_kernel(
    order_ref, tok, w_query, w_key, w_value, gains, frequency, wo, cot, wg, wu, wd,
    tok_all, wqkv_all, gains_all, wo_all, wg_all, wu_all, wd_all, cot_all, kv_all, branch,
    normed, q_t, q_n, out_t, attended, log_sum, key_pos, query_pos, cos_t, sin_t,
    wqkv, gain_src, toks, wqkvs, wos, kv_own, kv, v_t, att_t, part, total, inbox, across, ss, rs
):
    me = Here(ss, rs)
    z = me.z
    heads, hd, rows = q_t.shape
    wide = heads * hd
    keys = kv.shape[0]
    wqkv[:, :wide] = w_query[...]
    for j in range(4):

        @pl.when(z == j)
        def _():
            wqkv[:, wide : wide + hd] = w_key[:, j * hd : (j + 1) * hd]
            wqkv[:, wide + hd :] = w_value[:, j * hd : (j + 1) * hd]

    gain_src[...] = jnp.concatenate([gains[...], jnp.zeros((14, gains.shape[1]), f32)], axis=0)
    me.enter((1, 2, 3, 4))
    have_tok, have_gains, have_wqkv, have_wo = Flag(), Flag(), Flag(), Flag()
    progress = Progress(0)
    order = Order(
        z_gather(me, tok, toks, 11.3, 0.0, have_tok),
        plane_gather(me, gain_src, gains_all, 2.0, 0.0, have_gains),
        plane_gather(me, wqkv, wqkvs, 7.0, 0.1, have_wqkv),
        plane_gather(me, wo, wos, 6.0, 8.0, have_wo),
        plane_gather(me, wg, wg_all, 15.5, 17.0),
        z_gather(me, cot, cot_all, 11.3, 23.5),
    )
    c_number = me.x * 2 + me.c
    for i in range(4):
        x = 1 - me.x if i & 2 else me.x
        c = 1 - me.c if i & 1 else me.c
        key_pos[i * rows : (i + 1) * rows, :] = block_positions(order_ref, x * 2 + c, rows // 2)
    lane = lax.broadcasted_iota(jnp.int32, (hd // 2, rows // 2), 1)
    for i in range(2):
        span = slice(i * rows // 2, (i + 1) * rows // 2)
        position = lane + order_ref[c_number * 2 + i] * (rows // 2)
        query_pos[:, span] = position[:8]
        freq = jnp.concatenate([frequency[...]] * (rows // 256), axis=1)
        angle = position.astype(f32) * freq
        cos_t[:, span] = jnp.cos(angle)
        sin_t[:, span] = jnp.sin(angle)
    order.until(have_tok, have_gains, have_wqkv)
    saves = [me.local(toks, tok_all), me.local(wqkvs, wqkv_all)]
    for save in saves:
        save.start()
    gain = gain_row(gains_all, 0)

    def project(i):
        at = pl.ds(pl.multiple_of(i * 128, 128), 128)
        x = toks[at, :].astype(f32)
        inv = lax.rsqrt(jnp.mean(x * x, axis=1, keepdims=True) + norm_epsilon)
        low = (x * inv * gain).astype(bf16)
        normed[at, :] = low
        lin = jnp.dot(low, wqkvs[...], preferred_element_type=f32).T
        cos, sin = cos_t[:, at], sin_t[:, at]
        turned = rotate_heads(lin[: wide + hd], cos, sin)
        query = turned[:wide].astype(bf16) * bf16(1.0 / math.sqrt(hd))
        natural = query.astype(f32).T
        for h in range(heads):
            q_t[h, :, at] = query[h * hd : (h + 1) * hd]
            q_n[h, at, :] = natural[:, h * hd : (h + 1) * hd].astype(bf16)
        kv_own[at, :] = jnp.concatenate([turned[wide:], lin[wide + hd :]], axis=0).T.astype(bf16)

    order.loop(rows // 128, 1.9, project)

    def block(i):
        return kv.at[pl.ds(i * rows, rows)]

    copies = [me.copy(kv_own, block(i), me.plane(i)) for i in (1, 2, 3)]
    own = me.local(kv_own, block(0))
    for copy in (*copies, own):
        copy.start()
    order.pump(order.now + 4.0)
    order.add(plane_gather(me, wu, wu_all, 15.5, order.now))
    order.add(plane_gather(me, wd, wd_all, 15.5, order.now + 16.0))
    own.wait()
    for copy in copies:
        copy.wait_recv()
    save = me.local(kv, kv_all)
    save.start()
    for i in range(keys // rows):
        span = slice(i * rows, (i + 1) * rows)
        v_t[:, span] = kv[span, :].astype(f32).T[hd:, :].astype(bf16)
    order.until(have_wo)
    save_wo = me.local(wos, wo_all)
    save_wo.start()
    order.add(
        z_reduce_all(me, part, total, inbox, across, branch, 45.0, 16, progress, order.now)
    )

    def item(i):
        r, h = i // heads, i % heads
        at = pl.ds(pl.multiple_of(r * 128, 128), 128)
        s = jnp.dot(kv[:, 0:hd], q_t[h, :, at], preferred_element_type=f32)
        s = jnp.where(key_pos[...] <= query_pos[0:1, at], s, masked_value)
        top = jnp.max(s, axis=0, keepdims=True)
        p = jnp.exp(s - top)
        norm = jnp.sum(p, axis=0, keepdims=True)
        o = jnp.dot(v_t[...], p.astype(bf16), preferred_element_type=f32) / norm
        out_t[h, :, at] = o
        log_sum[h, :, at] = top + jnp.log(norm)
        att_t[pl.ds(pl.multiple_of(h * hd, hd), hd), :] = o

        @pl.when(h == heads - 1)
        def _():
            natural = att_t[...].T.astype(bf16)
            attended[at, :] = natural
            part[at, :] = contract_last_dims(natural, wos[...]).astype(bf16)

    def before(k):
        progress.parts = k // heads * 4
        return False

    order.loop(heads * rows // 128, 0.75, item, before)
    progress.parts = 16
    order.finish()
    for copy in copies:
        copy.wait_send()
    for copy in (save, save_wo, *saves):
        copy.wait()


def forward(stretch_order, tok, w_query, w_key, w_value, gains, frequency, wo, cot, wg, wu, wd):
    rows = tok.shape[0] * 4
    width = tok.shape[1]
    heads = w_query.shape[1] // HD
    keys = rows * 4
    qkv = (w_query.shape[0], w_query.shape[1] + 2 * HD)

    def grown(a, n=8):
        return shape((a.shape[0] * n,) + a.shape[1:], a.dtype)

    def room(a):
        return pltpu.VMEM(a.shape, a.dtype)

    gain_block = shape((16, gains.shape[1]), f32)
    wqkv = shape(qkv)
    block = shape((rows, width))
    return pl.pallas_call(
        forward_kernel,
        out_shape=(
            block, grown(wqkv), grown(gain_block), grown(wo), grown(wg), grown(wu), grown(wd), block,
            shape((keys, 2 * HD)), block,
            block,
            shape((heads, HD, rows)),
            shape((heads, rows, HD)),
            shape((heads, HD, rows), f32),
            shape((rows, heads * HD)),
            shape((heads, 1, rows), f32),
            shape((keys, 128), jnp.int32),
            shape((8, rows), jnp.int32),
            shape((HD // 2, rows), f32),
            shape((HD // 2, rows), f32),
        ),
        in_specs=[pl.BlockSpec(memory_space=pltpu.SMEM)] + [VM] * 7 + [HB] * 4,
        out_specs=[HB, HB, VM] + [HB] * 7 + [VM] * 10,
        scratch_shapes=[
            room(wqkv), room(gain_block), room(block), room(grown(wqkv)), room(grown(wo)),
            pltpu.VMEM((rows, 2 * HD), bf16),
            pltpu.VMEM((keys, 2 * HD), bf16),
            pltpu.VMEM((HD, keys), bf16),
            pltpu.VMEM((heads * HD, 128), f32),
            room(block), room(block), room(block), room(block),
        ] + dma_sems(192),
        compiler_params=params(1),
        name="forward",
    )(stretch_order, tok, w_query, w_key, w_value, gains, frequency, wo, cot, wg, wu, wd)


def contract_rows(left, right):
    return lax.dot_general(left, right, (((0,), (0,)), ((), ())), preferred_element_type=f32)


def contract_last_dims(left, right):
    return lax.dot_general(left, right, (((1,), (1,)), ((), ())), preferred_element_type=f32)


def backward_kernel(
    part, cot_all, hidden, normed_two, d_gate, d_up, wd_all, tok_all, branch, gains, wo_all,
    out_t_all, attended_all, q_t_all, q_n_all, kv_all, log_sum, key_pos, query_pos,
    dwd_own, dwg_own, dwu, out_own, dwo, own, gain_part, dq_t, dkv_own,
    total, inbox, across, cot, out_part, below, above, q_t, q_n, kv, k_t, came, *rest
):
    scratch_d, scratch_g, (ss, rs) = rest[:6], rest[6:12], rest[12:]
    me = Here(ss, rs)
    me.enter((1, 2, 3, 4))
    z = me.z
    rows, width = part.shape
    heads, hd, _ = q_t.shape
    keys = kv.shape[0]
    cols = width // 8
    progress = Progress(16)
    order = Order(z_reduce_all(me, part, total, inbox, across, None, 45.0, 16, progress))
    down, gate = PlaneScatter(me, scratch_d), PlaneScatter(me, scratch_g)
    cot_load = me.local(cot_all, cot)
    cot_load.start()
    later = [me.local(src, dst) for src, dst in ((kv_all, kv), (q_t_all, q_t), (q_n_all, q_n))]
    stores = [me.slot() for _ in range(4)]

    def weights(left, right_h, right_g, right_u, stage, wd):
        pairs = ((hidden, right_h), (normed_two, left), (d_gate, right_g), (d_up, right_u))
        loads = [me.local(src, dst) for src, dst in pairs]
        for load in loads:
            load.start()
        for load in later:
            load.start()
        cot_load.wait()
        loads[0].wait()
        order.pump(2.0)

        def columns(j):
            return pl.ds(pl.multiple_of(offsets_of(me, j) * cols, cols), cols)

        def send(scatter, j):
            for k in range(4):

                @pl.when(j == k)
                def _():
                    scatter.core[k].start()

        def down_item(j):
            down.blocks[j] = contract_rows(cot[:, columns(j)], right_h[...]).astype(bf16)
            send(down, j)

        order.loop(8, 0.9, down_item)
        order.add(down.steps(dwd_own, 15.5, order.now + 0.1))
        loads[1].wait()
        loads[2].wait()

        def gate_item(j):
            gate.blocks[j] = contract_rows(left[:, columns(j)], right_g[...]).astype(bf16)
            send(gate, j)

        order.loop(8, 0.9, gate_item)
        order.add(gate.steps(dwg_own, 15.5, order.now + 15.0))
        loads[3].wait()

        def put(j):
            at = pl.ds(pl.multiple_of(j * cols, cols), cols)
            return pltpu.make_async_copy(stage.at[j % 2], dwu.at[at], ss.at[stores[0]])

        def up_item(j):
            @pl.when(j >= 1)
            def _():
                put(j - 1).wait()

            at = pl.ds(pl.multiple_of(j * cols, cols), cols)
            stage[j % 2] = contract_rows(left[:, at], right_u[...]).astype(bf16)
            put(j).start()

        order.loop(8, 0.9, up_item)
        put(7).wait()

        def fetch(j):
            at = pl.ds(pl.multiple_of(j * cols, cols), cols)
            return pltpu.make_async_copy(wd_all.at[at], wd.at[j % 2], ss.at[stores[1]])

        fetch(0).start()

        def out_item(j):
            fetch(j).wait()

            @pl.when(j < 7)
            def _():
                fetch(j + 1).start()

            at = pl.ds(pl.multiple_of(j * cols, cols), cols)
            out_part[:, at] = contract_last_dims(right_h[...], wd[j % 2]).astype(bf16)

        order.loop(8, 0.7, out_item)

    units = pltpu.VMEM(hidden.shape, bf16)
    weight = pltpu.VMEM((2, cols, hidden.shape[1]), bf16)
    pl.run_scoped(weights, pltpu.VMEM(part.shape, bf16), units, units, units, weight, weight)

    def attention(tok, summed, wo, out_t, attended, g_t, g_n, delta, dk, dv):
        gain = gain_row(gains, 1)

        def fetch(r):
            at = pl.ds(pl.multiple_of(r * 128, 128), 128)
            return (
                pltpu.make_async_copy(tok_all.at[at], tok, ss.at[stores[2]]),
                pltpu.make_async_copy(branch.at[at], summed, ss.at[stores[3]]),
            )

        for copy in fetch(0):
            copy.start()
        loads = [
            me.local(src, dst)
            for src, dst in ((wo_all, wo), (out_t_all, out_t), (attended_all, attended))
        ]
        for load in loads:
            load.start()
        dk[...] = jnp.zeros_like(dk)
        dv[...] = jnp.zeros_like(dv)
        for load in later:
            load.wait()
        for i in range(keys // rows):
            span = slice(i * rows, (i + 1) * rows)
            k_t[:, span] = kv[span, :].astype(f32).T[:hd, :].astype(bf16)
        for load in loads:
            load.wait()
        order.add(z_reduce_scatter(me, out_part, below, above, out_own, 11.3, 47.0), 47.0)

        def prepare(r):
            for copy in fetch(r):
                copy.wait()
            at = pl.ds(pl.multiple_of(r * 128, 128), 128)
            h = tok[...].astype(f32) + summed[...].astype(f32)
            e = total[at, :].astype(f32)
            inv = lax.rsqrt(jnp.mean(h * h, axis=1, keepdims=True) + norm_epsilon)
            u = e * gain
            inner = jnp.mean(u * h, axis=1, keepdims=True)
            grad = cot[at, :].astype(f32) + (inv * u - h * (inv * inv * inv * inner))

            @pl.when(r == z)
            def _():
                own[...] = grad
                gain_part[...] = jnp.broadcast_to(
                    jnp.sum(e * h * inv, axis=0, keepdims=True), gain_part.shape
                )

            small = grad.astype(bf16)
            cot[at, :] = small
            g = jnp.dot(small, wo[...], preferred_element_type=f32).astype(bf16)
            turned = g.astype(f32).T
            for head in range(heads):
                g_n[head] = g[:, head * hd : (head + 1) * hd]
                mine = turned[head * hd : (head + 1) * hd]
                g_t[head] = mine.astype(bf16)
                delta[head] = jnp.sum(mine * out_t[head, :, at], axis=0, keepdims=True)

            @pl.when(r < rows // 128 - 1)
            def _():
                for copy in fetch(r + 1):
                    copy.start()

        def item(i):
            r, h = i // heads, i % heads

            @pl.when(h == 0)
            def _():
                prepare(r)

            at = pl.ds(pl.multiple_of(r * 128, 128), 128)
            s = jnp.dot(kv[:, 0:hd], q_t[h, :, at], preferred_element_type=f32)
            s = jnp.where(key_pos[...] <= query_pos[0:1, at], s, masked_value)
            p = jnp.exp(s - log_sum[h, :, at])
            dp = jnp.dot(kv[:, hd:], g_t[h], preferred_element_type=f32)
            ds = (p * (dp - delta[h])).astype(bf16)
            dv[...] += jnp.dot(p.astype(bf16), g_n[h], preferred_element_type=f32)
            dk[...] += jnp.dot(ds, q_n[h, at, :], preferred_element_type=f32)
            grad = jnp.dot(k_t[...], ds, preferred_element_type=f32)
            dq_t[h, :, at] = (grad * (1.0 / math.sqrt(hd))).astype(bf16)

        def before(k):
            return progress.whole < (k // heads + 1) * 4

        order.loop(heads * rows // 128, 1.2, item, before)
        for i in range(keys // rows):
            span = slice(i * rows, (i + 1) * rows)
            kv[span, :] = jnp.concatenate([dk[span, :], dv[span, :]], axis=1).astype(bf16)
        copies = [
            me.copy(kv.at[pl.ds(i * rows, rows)], came.at[i - 1], me.plane(i)) for i in (1, 2, 3)
        ]
        for copy in copies:
            copy.start()

        def out_item(i):
            span = pl.ds(pl.multiple_of(i * cols, cols), cols)
            dwo[span, :] = contract_rows(cot[:, span], attended[...]).astype(bf16)

        order.loop(8, 0.4, out_item)
        order.pump(order.now + 2.0)
        value = kv[0:rows, :].astype(f32)
        for i, copy in enumerate(copies):
            copy.wait_recv()
            value = value + came[i].astype(f32)
        dkv_own[...] = value
        for copy in copies:
            copy.wait_send()

    slots = pltpu.VMEM((128, width), bf16)
    pl.run_scoped(
        attention,
        slots,
        slots,
        pltpu.VMEM(wo_all.shape, bf16),
        pltpu.VMEM(out_t_all.shape, f32),
        pltpu.VMEM(attended_all.shape, bf16),
        pltpu.VMEM((heads, hd, 128), bf16),
        pltpu.VMEM((heads, 128, hd), bf16),
        pltpu.VMEM((heads, 1, 128), f32),
        pltpu.VMEM((keys, hd), f32),
        pltpu.VMEM((keys, hd), f32),
    )
    order.finish()


def backward(
    part, cot_all, hidden, normed_two, d_gate, d_up, wd_all, tok_all, branch, gains, wo_all,
    out_t, attended, q_t, q_n, kv_all, log_sum, key_pos, query_pos
):
    heads, hd, rows = q_t.shape
    keys = key_pos.shape[0]
    width = part.shape[1]
    whole = pltpu.VMEM(part.shape, bf16)
    own = (wd_all.shape[0] // 8, wd_all.shape[1])
    return pl.pallas_call(
        backward_kernel,
        out_shape=(
            shape(own, f32),
            shape(own, f32),
            shape(wd_all.shape),
            shape((rows // 4, width), f32),
            shape(wo_all.shape),
            shape((rows // 4, width), f32),
            shape((8, width), f32),
            shape((heads, hd, rows)),
            shape((rows, 2 * hd), f32),
        ),
        in_specs=[VM] + [HB] * 8 + [VM] + [HB] * 6 + [VM] * 3,
        out_specs=[VM, VM, HB] + [VM] * 6,
        scratch_shapes=[whole] * 7
        + [
            pltpu.VMEM(q_t.shape, bf16),
            pltpu.VMEM(q_n.shape, bf16),
            pltpu.VMEM((keys, 2 * hd), bf16),
            pltpu.VMEM((hd, keys), bf16),
            pltpu.VMEM((keys // rows - 1, rows, 2 * hd), bf16),
        ]
        + plane_scatter_scratch(*own) * 2
        + dma_sems(160),
        compiler_params=params(4, 67043328),
        name="backward",
    )(
        part, cot_all, hidden, normed_two, d_gate, d_up, wd_all, tok_all, branch, gains, wo_all,
        out_t, attended, q_t, q_n, kv_all, log_sum, key_pos, query_pos
    )


def finish_kernel(dq_t, dkv, cos_t, sin_t, wqkv, normed, tok, gain_two, one_part, dwqkv, gain_parts, lin):
    heads = dq_t.shape[0]
    wide = heads * HD
    width = tok.shape[1]
    cols = width // 8

    def body(i, total):
        at = pl.ds(pl.multiple_of(i * 128, 128), 128)
        cos, sin = cos_t[:, at], sin_t[:, at]
        kv = dkv[at, :].astype(bf16).astype(f32).T
        grads = jnp.concatenate([dq_t[h, :, at].astype(f32) for h in range(heads)] + [kv[:HD]], axis=0)
        grads = rotate_heads(grads, cos, sin, inverse=True)
        natural = jnp.concatenate([grads, kv[HD:]], axis=0).T.astype(bf16)
        lin[at, :] = natural
        one = contract_last_dims(natural, wqkv[...])
        one_part[at, :] = one.astype(bf16)
        x = tok[at, :].astype(f32)
        inv = lax.rsqrt(jnp.mean(x * x, axis=1, keepdims=True) + norm_epsilon)
        return total + jnp.sum(one * x * inv, axis=0, keepdims=True)

    total = lax.fori_loop(0, tok.shape[0] // 128, body, jnp.zeros((1, width), f32))
    for i in range(8):
        span = slice(i * cols, (i + 1) * cols)
        gain_parts[i * 8 : (i + 1) * 8, :] = jnp.concatenate(
            [total[:, span], gain_two[0:1, span], jnp.zeros((6, cols), f32)], axis=0
        )
        dwqkv[span, :] = contract_rows(normed[:, span], lin[...]).astype(bf16)


def finish(dq_t, dkv, cos_t, sin_t, wqkv, normed, tok, gain_two):
    width = tok.shape[1]
    return pl.pallas_call(
        finish_kernel,
        out_shape=(shape(tok.shape), shape(wqkv.shape), shape((64, width // 8), f32)),
        in_specs=[VM] * 8,
        out_specs=[VM] * 3,
        scratch_shapes=[pltpu.VMEM((tok.shape[0], wqkv.shape[1]), bf16)],
        name="finish_attention",
        **alone(4 * tok.shape[0] * width * wqkv.shape[1]),
    )(dq_t, dkv, cos_t, sin_t, wqkv, normed, tok, gain_two)


def gain_sums(me, src, out, came, mine, came_z):
    def block(i):
        return pl.ds(pl.multiple_of(me.number(i) * 8, 8), 8)

    copies = [me.copy(src.at[block(i)], came.at[i - 1], me.plane(i)) for i in range(1, 8)]
    for copy in copies:
        copy.start()
    yield 4.0
    value = src[block(0), :]
    for i, copy in enumerate(copies):
        copy.wait_recv()
        value = value + came[i]
    mine[...] = value
    again = [
        me.copy(mine, came_z.at[d - 1], {"head": (me.z + d) % 4}) for d in (1, 2, 3)
    ]
    for copy in again:
        copy.start()
    yield 20.0
    for d, copy in enumerate(again):
        copy.wait_recv()
        value = value + came_z[d]
    out[...] = value
    for copy in copies + again:
        copy.wait_send()


def sixth_kernel(
    part, dwqkv, dwo, dwu, gains,
    own, dwq_own, dwkv_all, dwo_own, dwu_own, gains_out,
    below, above, dwqkv_own, dwkv_own, came_kv, came, mine, came_z, *rest
):
    *scratch, ss, rs = rest
    me = Here(ss, rs)
    me.enter(tuple(range(1, 8)), all_z=True)
    wide = dwq_own.shape[1]

    def weights():
        yield from plane_scatter(me, dwqkv, dwqkv_own, scratch[:6], 7.0, 18.0)
        dwq_own[...] = dwqkv_own[:, :wide]
        dwkv_own[...] = dwqkv_own[:, wide:].astype(bf16)
        copies = [
            me.copy(dwkv_own, came_kv.at[d - 1], {"head": (me.z + d) % 4}) for d in (1, 2, 3)
        ]
        for copy in copies:
            copy.start()
        yield 45.0
        for copy in copies:
            copy.wait_recv()
        dwkv_all[0] = dwkv_own[...]
        for d in (1, 2, 3):
            dwkv_all[d] = came_kv[d - 1]
        for copy in copies:
            copy.wait_send()

    drive(
        gain_sums(me, gains, gains_out, came, mine, came_z),
        z_reduce_scatter(me, part, below, above, own, 11.3),
        plane_scatter(me, dwu, dwu_own, scratch[12:], 15.5, 0.1),
        plane_scatter(me, dwo, dwo_own, scratch[6:12], 8.0, 9.0),
        weights(),
    )


def sixth(part, dwqkv, dwo, dwu, gains):
    rows, cols = dwqkv.shape[0] // 8, dwqkv.shape[1]
    wide = dwo.shape[1]
    whole = pltpu.VMEM(part.shape, bf16)
    return pl.pallas_call(
        sixth_kernel,
        out_shape=(
            shape((part.shape[0] // 4, part.shape[1]), f32),
            shape((rows, wide), f32),
            shape((4, rows, cols - wide)),
            shape((rows, wide), f32),
            shape((rows, dwu.shape[1]), f32),
            shape((8, gains.shape[1]), f32),
        ),
        in_specs=[VM, HB, HB, HB, VM],
        out_specs=[VM] * 6,
        scratch_shapes=[
            whole, whole,
            pltpu.VMEM((rows, cols), f32),
            pltpu.VMEM((rows, cols - wide), bf16),
            pltpu.VMEM((3, rows, cols - wide), bf16),
            pltpu.VMEM((7, 8, gains.shape[1]), f32),
            pltpu.VMEM((8, gains.shape[1]), f32),
            pltpu.VMEM((3, 8, gains.shape[1]), f32),
        ]
        + plane_scatter_scratch(rows, cols)
        + plane_scatter_scratch(rows, wide)
        + plane_scatter_scratch(rows, dwu.shape[1])
        + dma_sems(96),
        compiler_params=params(6),
        name="scatter_last",
    )(part, dwqkv, dwo, dwu, gains)


def local_fast(
    tokens, w_query, w_key, w_value, w_out, w_gate, w_up, w_down, gain_attn, gain_mlp, stretch_order, cotangent
):
    row_count, width = tokens.shape
    groups = 4
    cols = width // 8
    contract_last = (((1,), (1,)), ((), ()))
    z = lax.axis_index("head")
    own_first = z * row_count

    def own_rows(values):
        return lax.dynamic_slice_in_dim(values, own_first, row_count, 0)

    frequency = rope_base ** (-(np.arange(HD // 2, dtype=np.float32) * np.float32(2.0 / HD)))
    frequency = jnp.asarray(np.broadcast_to(frequency.astype(np.float32)[:, None], (HD // 2, 128)))
    gains = jnp.concatenate([gain_attn[None], gain_mlp[None]]).astype(f32)
    (
        tok_all, wqkv_all, gains_all, wo_all, wg_all, wu_all, wd_all, cot_all, kv_all, branch,
        normed, q_t, q_n, out_t, attended, log_sum, key_pos, query_pos, cos_t, sin_t,
    ) = forward(
        stretch_order, tokens, w_query, w_key, w_value, gains, frequency, w_out, cotangent, w_gate, w_up, w_down
    )
    gain_rows = gains_all.reshape(8, 16, cols)
    gain_one = gain_rows[:, 0].reshape(width)
    gain_two = gain_rows[:, 1].reshape(width)
    hidden_rows = tok_all.astype(f32) + branch.astype(f32)
    inv_mlp = lax.rsqrt(jnp.mean(hidden_rows * hidden_rows, axis=-1, keepdims=True) + norm_epsilon)
    normed_two = (hidden_rows * inv_mlp * gain_two).astype(bf16)
    gate = jnp.dot(normed_two, wg_all, preferred_element_type=f32)
    up = jnp.dot(normed_two, wu_all, preferred_element_type=f32)
    gate_sigmoid = jax.nn.sigmoid(gate)
    gate_silu = gate * gate_sigmoid
    hidden = (gate_silu * up).astype(bf16)
    grad_hidden = jnp.dot(cot_all, wd_all, preferred_element_type=f32)
    d_gate = (grad_hidden * up * gate_sigmoid * (1.0 + gate * (1.0 - gate_sigmoid))).astype(bf16)
    d_up = (grad_hidden * gate_silu).astype(bf16)
    two_part = lax.dot_general(d_gate, wg_all, contract_last, preferred_element_type=f32)
    two_part = two_part + lax.dot_general(d_up, wu_all, contract_last, preferred_element_type=f32)
    dwd_own, dwg_own, dwu, out_own, dwo, grad_hidden_own, gain_two_part, dq_t, dkv = backward(
        two_part.astype(bf16), cot_all, hidden, normed_two, d_gate, d_up, wd_all, tok_all, branch,
        gains_all, wo_all, out_t, attended, q_t, q_n, kv_all, log_sum, key_pos, query_pos,
    )
    one_part, dwqkv, gain_parts = finish(
        dq_t, dkv, cos_t, sin_t, wqkv_all, normed, tok_all, gain_two_part
    )
    grad_one, dwq_own, dwkv_all, dwo_own, dwu_own, gain_grads = sixth(
        one_part, dwqkv, dwo, dwu, gain_parts
    )

    x_own = tokens.astype(f32)
    layer_low = (x_own + own_rows(branch).astype(f32) + out_own).astype(bf16)
    inv_own = lax.rsqrt(jnp.mean(x_own * x_own, axis=-1, keepdims=True) + norm_epsilon)
    grad_tokens = (grad_hidden_own + norm_input_grad(x_own, inv_own, gain_one, grad_one)).astype(bf16)
    slots = jnp.concatenate(
        [lax.dynamic_slice_in_dim(dwkv_all, (z - j) % 4, 1, 0) for j in range(4)], axis=0
    ).astype(f32)
    grad_key = slots[:, :, :HD].transpose(1, 0, 2).reshape(cols, groups * HD)
    grad_value = slots[:, :, HD:].transpose(1, 0, 2).reshape(cols, groups * HD)
    return (
        layer_low,
        grad_tokens,
        dwq_own,
        grad_key,
        grad_value,
        dwo_own,
        dwg_own,
        dwu_own,
        dwd_own,
        gain_grads[0],
        gain_grads[1],
    )


def solution(mesh):
    sizes = (mesh.shape["fsdp"], mesh.shape["blk"], mesh.shape["head"])
    return jax.shard_map(
        local_fast if sizes == (2, 4, 4) else local,
        mesh=mesh,
        in_specs=(
            P(("fsdp", "blk", "head"), None),
            P(("fsdp", "blk"), "head"),
            P(("fsdp", "blk"), None),
            P(("fsdp", "blk"), None),
            P(("fsdp", "blk"), "head"),
            P(("fsdp", "blk"), "head"),
            P(("fsdp", "blk"), "head"),
            P(("fsdp", "blk"), "head"),
            P(("fsdp", "blk")),
            P(("fsdp", "blk")),
            P(),
            P(("fsdp", "blk", "head"), None),
        ),
        out_specs=(
            P(("fsdp", "blk", "head"), None),
            P(("fsdp", "blk", "head"), None),
            P(("fsdp", "blk"), "head"),
            P(("fsdp", "blk"), None),
            P(("fsdp", "blk"), None),
            P(("fsdp", "blk"), "head"),
            P(("fsdp", "blk"), "head"),
            P(("fsdp", "blk"), "head"),
            P(("fsdp", "blk"), "head"),
            P(("fsdp", "blk")),
            P(("fsdp", "blk")),
        ),
        check_vma=False,
    )
```

```python
import math

import jax
import jax.numpy as jnp
import numpy as np
from jax import lax
from jax.experimental import pallas as pl
from jax.experimental.pallas import tpu as pltpu
from jax.sharding import PartitionSpec as P

H = 32
KV = 4
HD = 64


norm_epsilon = 1e-05
rope_base = 10000.0
masked_value = -1e30


def rope_tables(positions, head_dim):
    half_dim = head_dim // 2
    frequency = rope_base ** (-(jnp.arange(half_dim, dtype=jnp.float32) * (2.0 / head_dim)))
    angles = positions.astype(jnp.float32)[:, None] * frequency[None, :]
    return (jnp.cos(angles), jnp.sin(angles))


def rotate(values, cosine, sine_table):
    half_dim = values.shape[-1] // 2
    first_half = values[..., :half_dim]
    second_half = values[..., half_dim:]
    cos_rows = cosine[:, None, :]
    sin_rows = sine_table[:, None, :]
    return jnp.concatenate(
        [
            first_half * cos_rows - second_half * sin_rows,
            second_half * cos_rows + first_half * sin_rows,
        ],
        axis=-1,
    )


def unrotate(values, cosine, sine_table):
    half_dim = values.shape[-1] // 2
    first_half = values[..., :half_dim]
    second_half = values[..., half_dim:]
    cos_rows = cosine[:, None, :]
    sin_rows = sine_table[:, None, :]
    return jnp.concatenate(
        [
            first_half * cos_rows + second_half * sin_rows,
            second_half * cos_rows - first_half * sin_rows,
        ],
        axis=-1,
    )


def stretch_positions(stretch_order, first_row, row_span, stretch_rows):
    storage = first_row + jnp.arange(row_span, dtype=jnp.int32)
    stretch_index = storage // stretch_rows
    match_table = (
        stretch_index[:, None] == jnp.arange(stretch_order.shape[0], dtype=jnp.int32)[None, :]
    )
    stretch_base = jnp.sum(jnp.where(match_table, stretch_order[None, :], 0), axis=1)
    return stretch_base * stretch_rows + storage % stretch_rows


def norm_input_grad(values, inverse, gain_vector, grad_normed):
    scaled = grad_normed * gain_vector
    inner = jnp.mean(scaled * values, axis=-1, keepdims=True)
    return inverse * scaled - values * inverse * inverse * inverse * inner


def gain_grad(values, inverse, grad_normed):
    return jnp.sum(grad_normed * values * inverse, axis=0)


def fold_block(
    state_now, keys_block, values_block, key_positions, query_heads, query_positions, score_scale
):
    running_max, running_sum, running_out = state_now
    scores = (
        jnp.einsum("qhd,kd->hqk", query_heads, keys_block, preferred_element_type=jnp.float32)
        * score_scale
    )
    allowed = (query_positions[:, None] >= key_positions[None, :])[None]
    scores = jnp.where(allowed, scores, masked_value)
    new_max = jnp.maximum(running_max, jnp.max(scores, axis=-1))
    weights = jnp.where(allowed, jnp.exp(scores - new_max[..., None]), 0.0)
    factor = jnp.exp(running_max - new_max)
    running_sum = running_sum * factor + jnp.sum(weights, axis=-1)
    running_out = running_out * factor[..., None] + jnp.einsum(
        "hqk,kd->hqd",
        weights.astype(jnp.bfloat16),
        values_block,
        preferred_element_type=jnp.float32,
    )
    return (new_max, running_sum, running_out)


def local(
    tokens,
    w_query,
    w_key,
    w_value,
    w_out,
    w_gate,
    w_up,
    w_down,
    gain_attn,
    gain_mlp,
    stretch_order,
    cotangent,
):
    row_count = tokens.shape[0]
    groups = lax.axis_size("head")
    blocks = lax.axis_size("blk")
    local_heads = H // groups
    repeats = groups // KV
    head_rows = row_count * groups
    stretch_rows = head_rows // 2
    score_scale = 1.0 / math.sqrt(HD)
    contract_last = (((1,), (1,)), ((), ()))
    contract_first = (((0,), (0,)), ((), ()))
    head_index = lax.axis_index("head")
    own_first = head_index * row_count
    block_first = lax.axis_index("blk") * head_rows
    positions = stretch_positions(stretch_order, block_first + own_first, row_count, stretch_rows)
    query_positions = stretch_positions(stretch_order, block_first, head_rows, stretch_rows)
    cos_own, sin_own = rope_tables(positions, HD)
    cos_block, sin_block = rope_tables(query_positions, HD)

    def layer_weights():
        return (
            lax.all_gather(w_query, ("fsdp", "blk"), axis=0, tiled=True),
            lax.all_gather(w_key, ("fsdp", "blk"), axis=0, tiled=True),
            lax.all_gather(w_value, ("fsdp", "blk"), axis=0, tiled=True),
            lax.all_gather(w_out, ("fsdp", "blk"), axis=0, tiled=True),
            lax.all_gather(w_gate, ("fsdp", "blk"), axis=0, tiled=True),
            lax.all_gather(w_up, ("fsdp", "blk"), axis=0, tiled=True),
            lax.all_gather(w_down, ("fsdp", "blk"), axis=0, tiled=True),
            lax.all_gather(gain_attn, ("fsdp", "blk"), axis=0, tiled=True),
            lax.all_gather(gain_mlp, ("fsdp", "blk"), axis=0, tiled=True),
        )

    def gather_query(columns):
        return lax.all_gather(columns, "head", axis=1, tiled=True)

    (
        query_cols,
        key_full,
        value_full,
        out_cols,
        gate_cols,
        up_cols,
        down_cols,
        gain_one,
        gain_two,
    ) = layer_weights()
    tokens_float = tokens.astype(jnp.float32)
    inv_attn = lax.rsqrt(
        jnp.mean(tokens_float * tokens_float, axis=-1, keepdims=True) + norm_epsilon
    )
    normed = (tokens_float * inv_attn * gain_one.astype(jnp.float32)).astype(jnp.bfloat16)
    normed_rows, cotangent_rows = (
        lax.all_gather(normed, "head", axis=0, tiled=True),
        lax.all_gather(cotangent, "head", axis=0, tiled=True),
    )
    query_all = gather_query(query_cols)
    query_lin = jnp.dot(normed, query_all, preferred_element_type=jnp.float32).reshape(
        row_count, H, HD
    )
    key_lin = jnp.dot(normed, key_full, preferred_element_type=jnp.float32).reshape(
        row_count, KV, HD
    )
    value_lin = jnp.dot(normed, value_full, preferred_element_type=jnp.float32).reshape(
        row_count, KV, HD
    )
    query_rot = rotate(query_lin, cos_own, sin_own).astype(jnp.bfloat16).reshape(row_count, H * HD)
    key_rot = rotate(key_lin, cos_own, sin_own).astype(jnp.bfloat16)
    key_slots = jnp.repeat(key_rot, repeats, axis=1).reshape(row_count, groups * HD)
    value_slots = jnp.repeat(value_lin.astype(jnp.bfloat16), repeats, axis=1).reshape(
        row_count, groups * HD
    )
    query_recv, key_own, value_own = (
        lax.all_to_all(query_rot, "head", split_axis=1, concat_axis=0, tiled=True),
        lax.all_to_all(key_slots, "head", split_axis=1, concat_axis=0, tiled=True),
        lax.all_to_all(value_slots, "head", split_axis=1, concat_axis=0, tiled=True),
    )
    query_heads = query_recv.reshape(head_rows, local_heads, HD)
    initial = (
        jnp.full((local_heads, head_rows), masked_value, jnp.float32),
        jnp.zeros((local_heads, head_rows), jnp.float32),
        jnp.zeros((local_heads, head_rows, HD), jnp.float32),
    )
    state_now = initial
    keys_piece = lax.all_gather(key_own, "blk", axis=0, tiled=True)
    values_piece = lax.all_gather(value_own, "blk", axis=0, tiled=True)
    piece_rows = keys_piece.shape[0]

    def scan_step(state_inner, step_index):
        offset = step_index * head_rows
        keys_block = lax.dynamic_slice_in_dim(keys_piece, offset, head_rows, 0)
        values_block = lax.dynamic_slice_in_dim(values_piece, offset, head_rows, 0)
        key_positions = stretch_positions(stretch_order, offset, head_rows, stretch_rows)
        return (
            fold_block(
                state_inner,
                keys_block,
                values_block,
                key_positions,
                query_heads,
                query_positions,
                score_scale,
            ),
            None,
        )

    state_now, unused = lax.scan(
        scan_step, state_now, jnp.arange(piece_rows // head_rows, dtype=jnp.int32)
    )
    running_max, running_sum, running_out = state_now
    attended_float = running_out / running_sum[..., None]
    log_sum = running_max + jnp.log(running_sum)
    attended_heads = (
        attended_float.astype(jnp.bfloat16).transpose(1, 0, 2).reshape(head_rows, local_heads * HD)
    )
    branch = lax.dot_general(
        attended_heads, out_cols, contract_last, preferred_element_type=jnp.float32
    )
    own_branch = lax.dynamic_slice_in_dim(branch, own_first, row_count, 0)
    partial_value = lax.dynamic_update_slice_in_dim(branch, own_branch + tokens_float, own_first, 0)
    hidden_rows = lax.psum(partial_value.astype(jnp.bfloat16), "head").astype(jnp.float32)
    inv_mlp = lax.rsqrt(jnp.mean(hidden_rows * hidden_rows, axis=-1, keepdims=True) + norm_epsilon)
    normed_two_rows = (hidden_rows * inv_mlp * gain_two.astype(jnp.float32)).astype(jnp.bfloat16)
    gate_proj = jnp.dot(normed_two_rows, gate_cols, preferred_element_type=jnp.float32)
    up_proj = jnp.dot(normed_two_rows, up_cols, preferred_element_type=jnp.float32)
    gate_sigmoid = jax.nn.sigmoid(gate_proj)
    gate_silu = gate_proj * gate_sigmoid
    hidden = (gate_silu * up_proj).astype(jnp.bfloat16)
    hidden_own = lax.dynamic_slice_in_dim(hidden_rows, own_first, row_count, 0)
    output_float = hidden_own + lax.psum_scatter(
        lax.dot_general(
            hidden, down_cols, contract_last, preferred_element_type=jnp.float32
        ).astype(jnp.bfloat16),
        "head",
        scatter_dimension=0,
        tiled=True,
    ).astype(jnp.float32)
    layer_low = output_float.astype(jnp.bfloat16)
    (
        query_cols,
        key_full,
        value_full,
        out_cols,
        gate_cols,
        up_cols,
        down_cols,
        gain_one,
        gain_two,
    ) = layer_weights()
    query_all = gather_query(query_cols)
    grad_hidden = jnp.dot(cotangent_rows, down_cols, preferred_element_type=jnp.float32)
    grad_gate_rows = (
        grad_hidden * up_proj * gate_sigmoid * (1.0 + gate_proj * (1.0 - gate_sigmoid))
    ).astype(jnp.bfloat16)
    grad_up_rows = (grad_hidden * gate_silu).astype(jnp.bfloat16)
    grad_w_down = lax.dot_general(
        cotangent_rows, hidden, contract_first, preferred_element_type=jnp.float32
    )
    grad_w_gate = lax.dot_general(
        normed_two_rows, grad_gate_rows, contract_first, preferred_element_type=jnp.float32
    )
    grad_w_up = lax.dot_general(
        normed_two_rows, grad_up_rows, contract_first, preferred_element_type=jnp.float32
    )
    normed_two_part = lax.dot_general(
        grad_gate_rows, gate_cols, contract_last, preferred_element_type=jnp.float32
    )
    normed_two_part = normed_two_part + lax.dot_general(
        grad_up_rows, up_cols, contract_last, preferred_element_type=jnp.float32
    )
    grad_normed_two = lax.psum(normed_two_part.astype(jnp.bfloat16), "head").astype(jnp.float32)
    gain_two_float = gain_two.astype(jnp.float32)
    grad_hidden_rows = cotangent_rows.astype(jnp.float32) + norm_input_grad(
        hidden_rows, inv_mlp, gain_two_float, grad_normed_two
    )
    own_grad_two = lax.dynamic_slice_in_dim(grad_normed_two, own_first, row_count, 0)
    own_inv_mlp = lax.dynamic_slice_in_dim(inv_mlp, own_first, row_count, 0)
    grad_gain_two = gain_grad(hidden_own, own_inv_mlp, own_grad_two)
    grad_low_rows = grad_hidden_rows.astype(jnp.bfloat16)
    grad_w_out = lax.dot_general(
        grad_low_rows, attended_heads, contract_first, preferred_element_type=jnp.float32
    )
    grad_heads = (
        jnp.dot(grad_low_rows, out_cols, preferred_element_type=jnp.float32)
        .astype(jnp.bfloat16)
        .reshape(head_rows, local_heads, HD)
    )
    keys_all, values_all = (
        lax.all_gather(key_own, "blk", axis=0, tiled=True),
        lax.all_gather(value_own, "blk", axis=0, tiled=True),
    )
    row_delta = jnp.sum(grad_heads.astype(jnp.float32).transpose(1, 0, 2) * attended_float, axis=-1)

    def back_block(grad_query_acc, block_index):
        offset = block_index * head_rows
        keys_block = lax.dynamic_slice_in_dim(keys_all, offset, head_rows, 0)
        values_block = lax.dynamic_slice_in_dim(values_all, offset, head_rows, 0)
        key_positions = stretch_positions(stretch_order, offset, head_rows, stretch_rows)
        scores = (
            jnp.einsum("qhd,kd->hqk", query_heads, keys_block, preferred_element_type=jnp.float32)
            * score_scale
        )
        allowed = (query_positions[:, None] >= key_positions[None, :])[None]
        probs_block = jnp.where(allowed, jnp.exp(scores - log_sum[..., None]), 0.0)
        grad_probs = jnp.einsum(
            "qhd,kd->hqk", grad_heads, values_block, preferred_element_type=jnp.float32
        )
        grad_scores = (probs_block * (grad_probs - row_delta[..., None])).astype(jnp.bfloat16)
        grad_query_acc = grad_query_acc + jnp.einsum(
            "hqk,kd->qhd", grad_scores, keys_block, preferred_element_type=jnp.float32
        )
        grad_key_part = (
            jnp.einsum("hqk,qhd->kd", grad_scores, query_heads, preferred_element_type=jnp.float32)
            * score_scale
        )
        grad_value_part = jnp.einsum(
            "hqk,qhd->kd",
            probs_block.astype(jnp.bfloat16),
            grad_heads,
            preferred_element_type=jnp.float32,
        )
        return (grad_query_acc, (grad_key_part, grad_value_part))

    grad_query_acc, (key_terms, value_terms) = lax.scan(
        back_block,
        jnp.zeros((head_rows, local_heads, HD), jnp.float32),
        jnp.arange(blocks, dtype=jnp.int32),
    )
    grad_key_sum, grad_value_sum = (
        lax.psum_scatter(
            key_terms.reshape(blocks * head_rows, HD).astype(jnp.bfloat16),
            "blk",
            scatter_dimension=0,
            tiled=True,
        ).astype(jnp.float32),
        lax.psum_scatter(
            value_terms.reshape(blocks * head_rows, HD).astype(jnp.bfloat16),
            "blk",
            scatter_dimension=0,
            tiled=True,
        ).astype(jnp.float32),
    )
    grad_query_rot = (grad_query_acc * score_scale).astype(jnp.bfloat16)
    grad_query_lin_heads = (
        unrotate(grad_query_rot.astype(jnp.float32), cos_block, sin_block)
        .astype(jnp.bfloat16)
        .reshape(head_rows, local_heads * HD)
    )
    key_slot_grad = grad_key_sum.astype(jnp.bfloat16)
    value_slot_grad = grad_value_sum.astype(jnp.bfloat16)
    grad_w_query = lax.dot_general(
        normed_rows, grad_query_lin_heads, contract_first, preferred_element_type=jnp.float32
    )
    query_back, key_back, value_back = (
        lax.all_to_all(grad_query_lin_heads, "head", split_axis=0, concat_axis=1, tiled=True),
        lax.all_to_all(key_slot_grad, "head", split_axis=0, concat_axis=1, tiled=True),
        lax.all_to_all(value_slot_grad, "head", split_axis=0, concat_axis=1, tiled=True),
    )
    key_slot_lin = (
        unrotate(key_back.astype(jnp.float32).reshape(row_count, groups, HD), cos_own, sin_own)
        .astype(jnp.bfloat16)
        .reshape(row_count, KV, repeats, HD)
    )
    value_slot_lin = value_back.reshape(row_count, KV, repeats, HD)
    grad_w_key = jnp.einsum(
        "td,tjrc->djc", normed, key_slot_lin, preferred_element_type=jnp.float32
    ).reshape(-1, KV * HD)
    grad_w_value = jnp.einsum(
        "td,tjrc->djc", normed, value_slot_lin, preferred_element_type=jnp.float32
    ).reshape(-1, KV * HD)
    grad_normed = lax.dot_general(
        query_back, query_all, contract_last, preferred_element_type=jnp.float32
    )
    grad_normed = grad_normed + jnp.einsum(
        "tjrc,djc->td",
        key_slot_lin,
        key_full.reshape(-1, KV, HD),
        preferred_element_type=jnp.float32,
    )
    grad_normed = grad_normed + jnp.einsum(
        "tjrc,djc->td",
        value_slot_lin,
        value_full.reshape(-1, KV, HD),
        preferred_element_type=jnp.float32,
    )
    gain_one_float = gain_one.astype(jnp.float32)
    grad_input_norm = norm_input_grad(tokens_float, inv_attn, gain_one_float, grad_normed)
    grad_gain_one = gain_grad(tokens_float, inv_attn, grad_normed)
    grad_hidden_own = lax.dynamic_slice_in_dim(grad_hidden_rows, own_first, row_count, 0)
    grad_tokens = (grad_hidden_own + grad_input_norm).astype(jnp.bfloat16)
    head_sums = (
        lax.psum(grad_w_key.astype(jnp.bfloat16), "head").astype(jnp.float32),
        lax.psum(grad_w_value.astype(jnp.bfloat16), "head").astype(jnp.float32),
        lax.psum(grad_gain_one.astype(jnp.bfloat16), "head").astype(jnp.float32),
        lax.psum(grad_gain_two.astype(jnp.bfloat16), "head").astype(jnp.float32),
    )
    reduced = (
        lax.psum_scatter(
            grad_w_query.astype(jnp.bfloat16), ("fsdp", "blk"), scatter_dimension=0, tiled=True
        ).astype(jnp.float32),
        lax.psum_scatter(
            head_sums[0].astype(jnp.bfloat16), ("fsdp", "blk"), scatter_dimension=0, tiled=True
        ).astype(jnp.float32),
        lax.psum_scatter(
            head_sums[1].astype(jnp.bfloat16), ("fsdp", "blk"), scatter_dimension=0, tiled=True
        ).astype(jnp.float32),
        lax.psum_scatter(
            grad_w_out.astype(jnp.bfloat16), ("fsdp", "blk"), scatter_dimension=0, tiled=True
        ).astype(jnp.float32),
        lax.psum_scatter(
            grad_w_gate.astype(jnp.bfloat16), ("fsdp", "blk"), scatter_dimension=0, tiled=True
        ).astype(jnp.float32),
        lax.psum_scatter(
            grad_w_up.astype(jnp.bfloat16), ("fsdp", "blk"), scatter_dimension=0, tiled=True
        ).astype(jnp.float32),
        lax.psum_scatter(
            grad_w_down.astype(jnp.bfloat16), ("fsdp", "blk"), scatter_dimension=0, tiled=True
        ).astype(jnp.float32),
        lax.psum_scatter(
            head_sums[2].astype(jnp.bfloat16), ("fsdp", "blk"), scatter_dimension=0, tiled=True
        ).astype(jnp.float32),
        lax.psum_scatter(
            head_sums[3].astype(jnp.bfloat16), ("fsdp", "blk"), scatter_dimension=0, tiled=True
        ).astype(jnp.float32),
    )
    return (
        layer_low,
        grad_tokens,
        reduced[0],
        reduced[1],
        reduced[2],
        reduced[3],
        reduced[4],
        reduced[5],
        reduced[6],
        reduced[7],
        reduced[8],
    )


MESH = pl.DeviceIdType.MESH
f32, bf16 = jnp.float32, jnp.bfloat16
VM = pl.BlockSpec(memory_space=pltpu.VMEM)
HB = pl.BlockSpec(memory_space=pl.ANY)


def dma_sems(n):
    return [pltpu.SemaphoreType.DMA((n,)), pltpu.SemaphoreType.DMA((n,))]


class Here:
    def __init__(self, send_sem, recv_sem):
        self.y = lax.axis_index("fsdp")
        blk = lax.axis_index("blk")
        self.x, self.c = blk // 2, blk % 2
        self.z = lax.axis_index("head")
        self.end = (self.z == 0) | (self.z == 3)
        self.middle = (self.z == 1) | (self.z == 2)
        self.inward = {"head": jnp.where(self.z < 2, self.z + 1, self.z - 1)}
        self.outward = {"head": jnp.where(self.z < 2, self.z - 1, self.z + 1)}
        self.send_sem, self.recv_sem, self.used = send_sem, recv_sem, 0

    def plane(self, i):
        y = 1 - self.y if i & 4 else self.y
        x = 1 - self.x if i & 2 else self.x
        c = 1 - self.c if i & 1 else self.c
        return {"fsdp": y, "blk": x * 2 + c}

    def number(self, i):
        at = self.plane(i)
        return at["fsdp"] * 4 + at["blk"]

    def up(self):
        return {"head": self.z + 1}

    def down(self):
        return {"head": self.z - 1}

    def copy(self, src, dst, device):
        k = self.used
        self.used += 1
        return self.again(k, src, dst, device)

    def slot(self):
        self.used += 1
        return self.used - 1

    def again(self, k, src, dst, device):
        return pltpu.make_async_remote_copy(
            src_ref=src,
            dst_ref=dst,
            send_sem=self.send_sem.at[k],
            recv_sem=self.recv_sem.at[k],
            device_id=device,
            device_id_type=MESH,
        )

    def local(self, src, dst):
        k = self.used
        self.used += 1
        return pltpu.make_async_copy(src, dst, self.send_sem.at[k])

    def free_in_plane(self, sem):
        for i in (1, 2, 4):
            pl.semaphore_signal(sem, inc=1, device_id=self.plane(i), device_id_type=MESH)

    def free_along_z(self, sem):
        @pl.when(self.z > 0)
        def _():
            pl.semaphore_signal(sem, inc=1, device_id=self.down(), device_id_type=MESH)

        @pl.when(self.z < 3)
        def _():
            pl.semaphore_signal(sem, inc=1, device_id=self.up(), device_id_type=MESH)

    def wait_along_z(self, sem):
        pl.semaphore_wait(sem, jnp.where(self.z > 0, 1, 0) + jnp.where(self.z < 3, 1, 0))

    def enter(self, offsets, along_z=True, all_z=False):
        bar = pltpu.get_barrier_semaphore()
        for i in offsets:
            pl.semaphore_signal(bar, inc=1, device_id=self.plane(i), device_id_type=MESH)
        if all_z:
            for d in (1, 2, 3):
                pl.semaphore_signal(
                    bar, inc=1, device_id={"head": (self.z + d) % 4}, device_id_type=MESH
                )
            pl.semaphore_wait(bar, len(offsets) + 3)
            return
        if along_z:

            @pl.when(self.z > 0)
            def _():
                pl.semaphore_signal(bar, inc=1, device_id=self.down(), device_id_type=MESH)

            @pl.when(self.z < 3)
            def _():
                pl.semaphore_signal(bar, inc=1, device_id=self.up(), device_id_type=MESH)

        peers = len(offsets)
        if along_z:
            peers = peers + jnp.where(self.z > 0, 1, 0) + jnp.where(self.z < 3, 1, 0)
        pl.semaphore_wait(bar, peers)


class Order:
    def __init__(self, *tasks):
        self.now, self.count, self.waiting = 0.0, 0, []
        for task in tasks:
            self.add(task)

    def add(self, task, at=None):
        self.waiting.append((self.now if at is None else at, self.count, task))
        self.count += 1

    def next_at(self):
        return min(self.waiting, default=(math.inf,))[0]

    def step(self):
        item = min(self.waiting, key=lambda entry: entry[:2])
        self.waiting.remove(item)
        at = next(item[2], None)
        if at is not None:
            self.waiting.append((max(at, item[0]), item[1], item[2]))

    def pump(self, until):
        while self.next_at() <= until:
            self.step()
        self.now = max(self.now, until)

    def until(self, *flags):
        while not all(flag.up for flag in flags):
            self.now = max(self.now, self.next_at())
            self.step()

    def finish(self):
        while self.waiting:
            self.step()

    def loop(self, n, each, item, before=None):
        start = self.now

        def body(i, _):
            for k in range(n):
                while self.waiting and (
                    self.next_at() <= start + k * each or (before is not None and before(k))
                ):

                    @pl.when(i == k)
                    def _():
                        self.step()

            item(i)
            return 0

        lax.fori_loop(0, n, body, 0)
        self.now = start + n * each


def drive(*tasks):
    Order(*tasks).finish()


class Flag:
    def __init__(self):
        self.up = False


def z_gather(me, src, dst, unit, begin=0.0, done=None, issue=None):
    rows = src.shape[0]
    half = rows // 2
    z = me.z

    def block(j, h):
        return dst.at[pl.ds(pl.multiple_of(j * rows + h * half, half), half)]

    ups = [me.slot() for _ in range(6)]
    downs = [me.slot() for _ in range(6)]
    own = me.local(src, dst.at[pl.ds(pl.multiple_of(z * rows, rows), rows)])

    def up(j, h):
        mine = src.at[pl.ds(h * half, half)] if j == 0 else block(z - j, h)
        return me.again(ups[2 * j + h], mine, block(z - j, h), me.up())

    def down(j, h):
        mine = src.at[pl.ds(h * half, half)] if j == 0 else block(z + j, h)
        return me.again(downs[2 * j + h], mine, block(z + j, h), me.down())

    def steps():
        yield begin if issue is None else issue

        @pl.when(z < 3)
        def _():
            up(0, 0).start()
            up(0, 1).start()

        @pl.when(z > 0)
        def _():
            down(0, 0).start()
            down(0, 1).start()

        own.start()
        for j in (1, 2, 3):
            for h in (0, 1):
                yield begin + unit * (j - 0.5 + h * 0.5) + 1.8 + 0.4 * j

                @pl.when(z >= j)
                def _():
                    up(j - 1, h).wait_recv()

                if j < 3:

                    @pl.when((z >= j) & (z < 3))
                    def _():
                        up(j, h).start()

                @pl.when(z <= 3 - j)
                def _():
                    down(j - 1, h).wait_recv()

                if j < 3:

                    @pl.when((z <= 3 - j) & (z > 0))
                    def _():
                        down(j, h).start()

        own.wait()
        if done is not None:
            done.up = True
        yield begin + unit * 3 + 15.0
        for j in (0, 1, 2):

            @pl.when((z >= j) & (z < 3))
            def _():
                up(j, 0).wait_send()
                up(j, 1).wait_send()

            @pl.when((z <= 3 - j) & (z > 0))
            def _():
                down(j, 0).wait_send()
                down(j, 1).wait_send()

    return steps()


def plane_gather(me, src, dst, unit, begin=0.0, done=None, issue=None):
    rows = src.shape[0]
    half = rows // 2

    def part(i, h):
        return dst.at[pl.ds(pl.multiple_of(me.number(i) * rows + h * half, half), half)]

    def block(i):
        return dst.at[pl.ds(pl.multiple_of(me.number(i) * rows, rows), rows)]

    halves = src.at[pl.ds(0, half)], src.at[pl.ds(half, half)]
    x_in = [me.copy(halves[h], part(0, h), me.plane(2)) for h in (0, 1)]
    y_in = [me.copy(halves[h], part(0, h), me.plane(4)) for h in (1, 0)]
    to_c = me.copy(src, block(0), me.plane(1))
    own = me.local(src, block(0))
    x_on = me.copy(part(2, 0), part(2, 0), me.plane(4))
    y_on = me.copy(part(4, 1), part(4, 1), me.plane(2))
    x_core = me.copy(block(2), block(2), me.plane(1))
    y_core = me.copy(block(4), block(4), me.plane(1))
    far = [me.copy(part(6, h), part(6, h), me.plane(1)) for h in (0, 1)]

    def steps():
        yield begin if issue is None else issue
        for copy in (x_in[0], y_in[0], x_in[1], y_in[1], to_c, own):
            copy.start()
        yield begin + unit * 0.5 + 2.0
        x_in[0].wait_recv()
        x_on.start()
        y_in[0].wait_recv()
        y_on.start()
        yield begin + unit + 2.5
        x_in[1].wait_recv()
        x_core.start()
        y_in[1].wait_recv()
        y_core.start()
        yield begin + unit * 1.5 + 4.5
        x_on.wait_recv()
        far[0].start()
        y_on.wait_recv()
        far[1].start()
        yield begin + unit * 1.5 + 6.5
        own.wait()
        for copy in (to_c, x_core, y_core, *far):
            copy.wait_recv()
        if done is not None:
            done.up = True
        yield begin + unit * 1.5 + 15.0
        for copy in (*x_in, *y_in, to_c, x_on, x_core, y_on, y_core, *far):
            copy.wait_send()

    return steps()


def plane_direct(me, src, dst, done):
    rows = src.shape[0]
    place = dst.at[pl.ds(pl.multiple_of(me.number(0) * rows, rows), rows)]
    copies = [me.copy(src, place, me.plane(i)) for i in range(1, 8)]
    own = me.local(src, place)

    def steps():
        for copy in (*copies, own):
            copy.start()
        yield 5.0
        own.wait()
        for copy in copies:
            copy.wait_recv()
        done.up = True
        yield 15.0
        for copy in copies:
            copy.wait_send()

    return steps()


def add_rows(dst, a, b, step=32):
    rows = a.shape[0]

    def body(i, _):
        at = pl.ds(pl.multiple_of(i * step, step), step)
        dst[at, :] = (a[at, :].astype(f32) + b[at, :].astype(f32)).astype(dst.dtype)
        return 0

    lax.fori_loop(0, rows // step, body, 0)


class Progress:
    def __init__(self, parts):
        self.parts, self.entered, self.crossed, self.left = parts, 0, 0, 0
        self.sent_in, self.sent_out = Flag(), Flag()

    def whole(self):
        return min(self.crossed, self.left)


def z_reduce_all(me, part, total, inbox, across, out, unit, chunks, progress, begin=0.0):
    rows = part.shape[0] // chunks
    first = [me.slot() for _ in range(chunks)]
    second = [me.slot() for _ in range(chunks)]
    third = [me.slot() for _ in range(chunks)]
    store = [me.slot() for _ in range(chunks)]
    hop = unit / chunks

    def at(ref, k):
        return ref.at[pl.ds(k * rows, rows)]

    def send_in(k):
        return me.again(first[k], at(part, k), at(inbox, k), me.inward)

    def send_across(k):
        return me.again(second[k], at(inbox, k), at(across, k), me.inward)

    def send_out(k):
        return me.again(third[k], at(total, k), at(total, k), me.outward)

    def put(k):
        return pltpu.make_async_copy(at(total, k), at(out, k), me.send_sem.at[store[k]])

    def entering():
        yield begin
        time, sent = begin, 0
        for k in range(chunks):
            while k >= progress.parts:
                time += 0.5
                yield time
            new, sent = range(sent, progress.parts), progress.parts
            if len(new):

                @pl.when(me.end)
                def _():
                    for j in new:
                        send_in(j).start()

            time = max(time, begin + 2.0) + hop
            yield time

            @pl.when(me.middle)
            def _():
                send_in(k).wait_recv()
                add_rows(at(inbox, k), at(part, k), at(inbox, k))
                send_across(k).start()

            progress.entered = k + 1
        yield time + 20.0

        @pl.when(me.end)
        def _():
            for k in range(chunks):
                send_in(k).wait_send()

        progress.sent_in.up = True

    def crossing():
        yield begin
        time = begin
        for k in range(chunks):
            while k >= progress.entered:
                time += 0.5
                yield time
            time = max(time, begin + 4.0 + hop) + hop
            yield time

            @pl.when(me.middle)
            def _():
                send_across(k).wait_recv()
                add_rows(at(total, k), at(inbox, k), at(across, k))
                send_out(k).start()
                if out is not None:
                    put(k).start()

            progress.crossed = k + 1
        yield time + 10.0

        @pl.when(me.middle)
        def _():
            for k in range(chunks):
                send_across(k).wait_send()
                send_out(k).wait_send()

        progress.sent_out.up = True

    def leaving():
        yield begin
        time = begin
        for k in range(chunks):
            while k >= progress.crossed:
                time += 0.5
                yield time
            time = max(time, begin + 6.0 + 2 * hop) + hop
            yield time

            @pl.when(me.end)
            def _():
                send_out(k).wait_recv()
                if out is not None:
                    put(k).start()

            progress.left = k + 1
        if out is not None:
            yield time + 2.0
            for k in range(chunks):
                put(k).wait()

    return entering(), crossing(), leaving()


def z_reduce_scatter(me, part, from_below, from_above, own, unit, begin=0.0, done=None):
    rows = part.shape[0] // 4
    z = me.z
    ups = [me.slot() for _ in range(4)]
    downs = [me.slot() for _ in range(4)]

    def at(ref, j):
        return ref.at[pl.ds(j * rows, rows)]

    def up(j, source):
        return me.again(ups[j], at(source, j), at(from_below, j), me.up())

    def down(j, source):
        return me.again(downs[j], at(source, j), at(from_above, j), me.down())

    def start(j):
        @pl.when(z == 0)
        def _():
            up(j, part).start()

        @pl.when(z == 3)
        def _():
            down(3 - j, part).start()

    def relay(j, stop):
        @pl.when(z == stop)
        def _():
            up(j, part).wait_recv()
            add_rows(at(from_below, j), at(part, j), at(from_below, j))
            up(j, from_below).start()

        @pl.when(z == 3 - stop)
        def _():
            i = 3 - j
            down(i, part).wait_recv()
            add_rows(at(from_above, i), at(part, i), at(from_above, i))
            down(i, from_above).start()

    yield begin
    start(3)
    yield begin + unit * 0.6
    start(2)
    yield begin + unit + 1.0
    relay(3, 1)
    yield begin + unit * 1.6
    start(1)
    yield begin + unit * 2 + 1.0
    relay(3, 2)
    relay(2, 1)
    yield begin + unit * 3 + 1.5
    for j in range(4):

        @pl.when(z == j)
        def _():
            if j > 0:
                up(j, part).wait_recv()
            if j < 3:
                down(j, part).wait_recv()

            def body(i, _):
                span = pl.ds(pl.multiple_of(i * 32, 32), 32)
                there = pl.ds(pl.multiple_of(j * rows + i * 32, 32), 32)
                value = part[there, :].astype(f32)
                if j > 0:
                    value = value + from_below[there, :].astype(f32)
                if j < 3:
                    value = value + from_above[there, :].astype(f32)
                own[span, :] = value
                return 0

            lax.fori_loop(0, rows // 32, body, 0)
            for i in range(4):
                if i > j:
                    up(i, part).wait_send()
                if i < j:
                    down(i, part).wait_send()

    if done is not None:
        done.up = True


def offsets_of(me, j):
    dx, dy, dc = 1 - (j % 4) // 2, 1 - j % 2, 1 - j // 4
    y = me.y + dy - 2 * me.y * dy
    x = me.x + dx - 2 * me.x * dx
    c = me.c + dc - 2 * me.c * dc
    return y * 4 + x * 2 + c


def plane_scatter_scratch(rows, cols):
    half = rows // 2
    return [
        pltpu.VMEM((8, rows, cols), bf16),
        pltpu.VMEM((4, rows, cols), bf16),
        pltpu.VMEM((2, half, cols), bf16),
        pltpu.VMEM((2, half, cols), bf16),
        pltpu.VMEM((half, cols), bf16),
        pltpu.VMEM((half, cols), bf16),
    ]


class PlaneScatter:
    def __init__(self, me, scratch):
        self.me = me
        self.blocks, self.other, self.over_x, self.over_y, self.last_y, self.last_x = scratch
        blocks, rows = self.blocks, self.blocks.shape[1]
        half = rows // 2
        self.half, self.first, self.second = half, pl.ds(0, half), pl.ds(half, half)
        first, second = self.first, self.second
        self.core = [me.copy(blocks.at[j], self.other.at[j], me.plane(1)) for j in range(4)]
        self.far_x = me.copy(blocks.at[4, first], self.over_x.at[1], me.plane(2))
        self.far_y = me.copy(blocks.at[4, second], self.over_y.at[1], me.plane(4))
        self.near_x = me.copy(blocks.at[5, first], self.over_x.at[0], me.plane(2))
        self.near_y = me.copy(blocks.at[6, second], self.over_y.at[0], me.plane(4))
        self.to_y = me.copy(blocks.at[6, first], self.last_y, me.plane(4))
        self.to_x = me.copy(blocks.at[5, second], self.last_x, me.plane(2))

    def steps(self, out, unit, begin, done, free=None):
        blocks, half, first, second = self.blocks, self.half, self.first, self.second
        for j in range(4):
            yield begin + 0.3 * j
            self.core[j].wait_recv()
            add_rows(blocks.at[4 + j], blocks.at[4 + j], self.other.at[j])
            if j == 0:
                self.far_x.start()
                self.far_y.start()
            if j == 1:
                self.near_x.start()
            if j == 2:
                self.near_y.start()
        yield begin + 3.0 + unit * 0.5
        self.far_x.wait_recv()
        add_rows(blocks.at[6, first], blocks.at[6, first], self.over_x.at[1])
        self.to_y.start()
        self.far_y.wait_recv()
        add_rows(blocks.at[5, second], blocks.at[5, second], self.over_y.at[1])
        self.to_x.start()
        yield begin + 4.0 + unit * 1.5
        for copy in (self.near_x, self.near_y, self.to_y, self.to_x):
            copy.wait_recv()

        def body(i, _):
            at = pl.ds(pl.multiple_of(i * 32, 32), 32)
            low = pl.ds(pl.multiple_of(half + i * 32, 32), 32)
            for rows, near, last in ((at, self.over_x, self.last_y), (low, self.over_y, self.last_x)):
                value = blocks[7, rows, :].astype(f32) + near[0, at, :].astype(f32)
                out[rows, :] = (value + last[at, :].astype(f32)).astype(out.dtype)
            return 0

        lax.fori_loop(0, half // 32, body, 0)
        for copy in (*self.core, self.far_x, self.far_y, self.near_x, self.near_y, self.to_y, self.to_x):
            copy.wait_send()
        done.up = True
        if free is not None:
            self.me.free_in_plane(free)


def params(number, vmem=60 * 2**20):
    return pltpu.CompilerParams(
        collective_id=number, has_side_effects=True, vmem_limit_bytes=vmem
    )


def shape(dims, kind=bf16):
    return jax.ShapeDtypeStruct(dims, kind)


def alone(flops, vmem=60 * 2**20):
    return dict(
        compiler_params=pltpu.CompilerParams(vmem_limit_bytes=vmem),
        cost_estimate=pl.CostEstimate(flops=int(flops), bytes_accessed=2**23, transcendentals=0),
    )


def gain_row(gains, which):
    return jnp.concatenate([gains[i * 8 + which : i * 8 + which + 1, :] for i in range(8)], axis=1)


def rotate_heads(values, cos, sin, inverse=False):
    out = []
    for h in range(values.shape[0] // HD):
        a = values[h * HD : h * HD + HD // 2]
        b = values[h * HD + HD // 2 : (h + 1) * HD]
        if inverse:
            out += [a * cos + b * sin, b * cos - a * sin]
        else:
            out += [a * cos - b * sin, b * cos + a * sin]
    return jnp.concatenate(out, axis=0)


def block_positions(order_ref, number, stretch_rows):
    row = lax.broadcasted_iota(jnp.int32, (stretch_rows, 128), 0)
    return jnp.concatenate(
        [row + order_ref[number * 2 + i] * stretch_rows for i in range(2)], axis=0
    )


def forward_kernel(
    order_ref, tok, w_query, w_key, w_value, gains, frequency, wo, cot, wg, wu, wd,
    tok_all, wqkv_all, gains_all, wo_all, wg_all, wu_all, wd_all, cot_all, kv_all, branch,
    normed, q_t, q_n, out_t, attended, log_sum, key_pos, query_pos, cos_t, sin_t,
    wqkv, gain_src, toks, wqkvs, wos, kv_own, kv, v_t, att_t, part, total, inbox, across, ss, rs
):
    me = Here(ss, rs)
    z = me.z
    heads, hd, rows = q_t.shape
    wide = heads * hd
    keys = kv.shape[0]
    wqkv[:, :wide] = w_query[...]
    for j in range(4):

        @pl.when(z == j)
        def _():
            wqkv[:, wide : wide + hd] = w_key[:, j * hd : (j + 1) * hd]
            wqkv[:, wide + hd :] = w_value[:, j * hd : (j + 1) * hd]

    gain_src[...] = jnp.concatenate([gains[...], jnp.zeros((6, gains.shape[1]), f32)], axis=0)
    me.enter(tuple(range(1, 8)))
    lanes = att_t.shape[1]
    have_tok, have_gains, have_wqkv, have_wo = Flag(), Flag(), Flag(), Flag()
    progress = Progress(0)
    order = Order(
        z_gather(me, tok, toks, 11.3, 0.0, have_tok),
        plane_direct(me, gain_src, gains_all, have_gains),
        plane_gather(me, wqkv, wqkvs, 7.0, 0.5, have_wqkv, 0.0),
        plane_gather(me, wo, wos, 6.0, 11.0, have_wo, 7.5),
        plane_gather(me, wg, wg_all, 15.5, 20.0, None, 17.0),
        z_gather(me, cot, cot_all, 11.3, 37.0, None, 27.0),
    )
    c_number = me.x * 2 + me.c
    for i in range(4):
        x = 1 - me.x if i & 2 else me.x
        c = 1 - me.c if i & 1 else me.c
        key_pos[i * rows : (i + 1) * rows, :] = block_positions(order_ref, x * 2 + c, rows // 2)
    lane = lax.broadcasted_iota(jnp.int32, (hd // 2, rows // 2), 1)
    for i in range(2):
        span = slice(i * rows // 2, (i + 1) * rows // 2)
        position = lane + order_ref[c_number * 2 + i] * (rows // 2)
        query_pos[:, span] = position[:8]
        freq = jnp.concatenate([frequency[...]] * (rows // 256), axis=1)
        angle = position.astype(f32) * freq
        cos_t[:, span] = jnp.cos(angle)
        sin_t[:, span] = jnp.sin(angle)
    order.until(have_tok, have_gains, have_wqkv)
    saves = [me.local(toks, tok_all), me.local(wqkvs, wqkv_all)]
    for save in saves:
        save.start()
    gain = gain_row(gains_all, 0)

    def project(i):
        at = pl.ds(pl.multiple_of(i * 128, 128), 128)
        x = toks[at, :].astype(f32)
        inv = lax.rsqrt(jnp.mean(x * x, axis=1, keepdims=True) + norm_epsilon)
        low = (x * inv * gain).astype(bf16)
        normed[at, :] = low
        lin = jnp.dot(low, wqkvs[...], preferred_element_type=f32).T
        cos, sin = cos_t[:, at], sin_t[:, at]
        turned = rotate_heads(lin[: wide + hd], cos, sin)
        query = turned[:wide].astype(bf16) * bf16(1.0 / math.sqrt(hd))
        natural = query.astype(f32).T
        for h in range(heads):
            q_t[h, :, at] = query[h * hd : (h + 1) * hd]
            q_n[h, at, :] = natural[:, h * hd : (h + 1) * hd].astype(bf16)
        kv_own[at, :] = jnp.concatenate([turned[wide:], lin[wide + hd :]], axis=0).T.astype(bf16)

    order.loop(rows // 128, 1.0, project)

    def block(i):
        return kv.at[pl.ds(i * rows, rows)]

    copies = [me.copy(kv_own, block(i), me.plane(i)) for i in (1, 2, 3)]
    own = me.local(kv_own, block(0))
    for copy in (*copies, own):
        copy.start()
    order.pump(order.now + 4.0)
    order.add(plane_gather(me, wu, wu_all, 15.5, order.now))
    order.add(plane_gather(me, wd, wd_all, 15.5, order.now + 24.0, None, order.now + 14.0))
    own.wait()
    for copy in copies:
        copy.wait_recv()
    save = me.local(kv, kv_all)
    save.start()
    for i in range(keys // rows):
        span = slice(i * rows, (i + 1) * rows)
        v_t[:, span] = kv[span, :].astype(f32).T[hd:, :].astype(bf16)
    order.until(have_wo)
    save_wo = me.local(wos, wo_all)
    save_wo.start()
    for task in z_reduce_all(me, part, total, inbox, across, branch, 45.0, 16, progress, order.now):
        order.add(task)

    def item(i):
        r, h = i // heads, i % heads
        at = pl.ds(pl.multiple_of(r * lanes, lanes), lanes)
        s = jnp.dot(kv[:, 0:hd], q_t[h, :, at], preferred_element_type=f32)
        pos = jnp.concatenate([key_pos[...]] * (lanes // 128), axis=1)
        s = jnp.where(pos <= query_pos[0:1, at], s, masked_value)
        top = jnp.max(s, axis=0, keepdims=True)
        p = jnp.exp(s - top)
        norm = jnp.sum(p, axis=0, keepdims=True)
        o = jnp.dot(v_t[...], p.astype(bf16), preferred_element_type=f32) / norm
        out_t[h, :, at] = o
        log_sum[h, :, at] = top + jnp.log(norm)
        att_t[pl.ds(pl.multiple_of(h * hd, hd), hd), :] = o

        @pl.when(h == heads - 1)
        def _():
            natural = att_t[...].T.astype(bf16)
            attended[at, :] = natural
            part[at, :] = contract_last_dims(natural, wos[...]).astype(bf16)

    def before(k):
        progress.parts = k // heads * (lanes // 32)
        return False

    order.loop(heads * rows // lanes, 1.2, item, before)
    progress.parts = 16
    order.finish()
    for copy in copies:
        copy.wait_send()
    for copy in (save, save_wo, *saves):
        copy.wait()


def forward(stretch_order, tok, w_query, w_key, w_value, gains, frequency, wo, cot, wg, wu, wd):
    rows = tok.shape[0] * 4
    width = tok.shape[1]
    heads = w_query.shape[1] // HD
    keys = rows * 4
    qkv = (w_query.shape[0], w_query.shape[1] + 2 * HD)

    def grown(a, n=8):
        return shape((a.shape[0] * n,) + a.shape[1:], a.dtype)

    def room(a):
        return pltpu.VMEM(a.shape, a.dtype)

    gain_block = shape((8, gains.shape[1]), f32)
    wqkv = shape(qkv)
    block = shape((rows, width))
    return pl.pallas_call(
        forward_kernel,
        out_shape=(
            block, grown(wqkv), grown(gain_block), grown(wo), grown(wg), grown(wu), grown(wd), block,
            shape((keys, 2 * HD)), block,
            block,
            shape((heads, HD, rows)),
            shape((heads, rows, HD)),
            shape((heads, HD, rows), f32),
            shape((rows, heads * HD)),
            shape((heads, 1, rows), f32),
            shape((keys, 128), jnp.int32),
            shape((8, rows), jnp.int32),
            shape((HD // 2, rows), f32),
            shape((HD // 2, rows), f32),
        ),
        in_specs=[pl.BlockSpec(memory_space=pltpu.SMEM)] + [VM] * 7 + [HB] * 4,
        out_specs=[HB, HB, VM] + [HB] * 7 + [VM] * 10,
        scratch_shapes=[
            room(wqkv), room(gain_block), room(block), room(grown(wqkv)), room(grown(wo)),
            pltpu.VMEM((rows, 2 * HD), bf16),
            pltpu.VMEM((keys, 2 * HD), bf16),
            pltpu.VMEM((HD, keys), bf16),
            pltpu.VMEM((heads * HD, 256), f32),
            room(block), room(block), room(block), room(block),
        ] + dma_sems(224),
        compiler_params=params(1),
        name="forward",
    )(stretch_order, tok, w_query, w_key, w_value, gains, frequency, wo, cot, wg, wu, wd)


def contract_rows(left, right):
    return lax.dot_general(left, right, (((0,), (0,)), ((), ())), preferred_element_type=f32)


def contract_last_dims(left, right):
    return lax.dot_general(left, right, (((1,), (1,)), ((), ())), preferred_element_type=f32)


def gain_sums(me, src, out, came, mine, came_z):
    def block(i):
        return pl.ds(pl.multiple_of(me.number(i) * 8, 8), 8)

    own = block(0)
    copies = [me.copy(src.at[block(i)], came.at[i - 1], me.plane(i)) for i in range(1, 8)]
    again = [
        me.copy(mine, came_z.at[d - 1], {"head": (me.z + d) % 4}) for d in (1, 2, 3)
    ]

    def steps(begin):
        for copy in copies:
            copy.start()
        yield begin + 6.0
        value = src[own, :]
        for i, copy in enumerate(copies):
            copy.wait_recv()
            value = value + came[i]
        mine[...] = value
        for copy in again:
            copy.start()
        yield begin + 35.0
        value = mine[...]
        for d, copy in enumerate(again):
            copy.wait_recv()
            value = value + came_z[d]
        out[...] = value
        for copy in copies + again:
            copy.wait_send()

    return steps


def backward_kernel(
    part, cot_all, hidden, normed_two, d_gate, d_up, wd_all, tok_all, branch, gains, wo_all,
    out_t_all, attended_all, q_t_all, q_n_all, kv_all, wqkv_all, normed_all, log_sum, key_pos, query_pos, cos_t, sin_t,
    dwd_own, dwg_own, dwu_own, dw_own, dwkv_all, out_own, own, grad_one, gains_out,
    total, inbox, across, cot, out_part, below, above, q_t, q_n, kv, k_t, came, dq_t,
    gain_two, gain_parts, came_gain, gain_mine, gain_z, dwkv_own, came_kv, *rest
):
    scratch_d, scratch_g = rest[:6], rest[6:12]
    free_d, free_g, free_z, ss, rs = rest[12:]
    me = Here(ss, rs)
    me.enter(tuple(range(1, 8)), all_z=True)
    z = me.z
    rows, width = part.shape
    heads, hd, _ = q_t.shape
    wide = heads * hd
    lin_cols = wide + 2 * hd
    keys = kv.shape[0]
    cols = width // 8
    progress = Progress(16)
    order = Order(*z_reduce_all(me, part, total, inbox, across, None, 45.0, 16, progress))
    down, gate = PlaneScatter(me, scratch_d), PlaneScatter(me, scratch_g)
    up = PlaneScatter(me, scratch_d)
    narrow = [ref.at[(slice(None),) * (len(ref.shape) - 1) + (pl.ds(0, lin_cols + wide),)] for ref in scratch_g]
    both = PlaneScatter(me, narrow)
    down_done, gate_done, up_done, both_done, out_done, one_done = (Flag() for _ in range(6))
    cot_load = me.local(cot_all, cot)
    cot_load.start()
    later = [me.local(src, dst) for src, dst in ((kv_all, kv), (q_t_all, q_t), (q_n_all, q_n))]
    stores = [me.slot() for _ in range(5)]
    back = [
        me.copy(kv.at[pl.ds(i * rows, rows)], came.at[i - 1], me.plane(i)) for i in (1, 2, 3)
    ]
    kv_sends = [
        me.copy(dwkv_own, came_kv.at[d - 1], {"head": (z + d) % 4}) for d in (1, 2, 3)
    ]

    gains_steps = gain_sums(me, gain_parts, gains_out, came_gain, gain_mine, gain_z)

    def columns(j):
        return pl.ds(pl.multiple_of(offsets_of(me, j) * cols, cols), cols)

    def send(scatter, j):
        for k in range(4):

            @pl.when(j == k)
            def _():
                scatter.core[k].start()

    def weights(left, right_h, right_g, wd):
        pairs = ((hidden, right_h), (normed_two, left), (d_gate, right_g))
        loads = [me.local(src, dst) for src, dst in pairs]
        for load in loads:
            load.start()
        for load in later:
            load.start()
        cot_load.wait()
        loads[0].wait()
        order.pump(2.0)

        def down_item(j):
            down.blocks[j] = contract_rows(cot[:, columns(j)], right_h[...]).astype(bf16)
            send(down, j)

        order.loop(8, 0.65, down_item)
        order.add(down.steps(dwd_own, 16.5, order.now + 0.1, down_done, free_d))
        loads[1].wait()
        loads[2].wait()

        def gate_item(j):
            gate.blocks[j] = contract_rows(left[:, columns(j)], right_g[...]).astype(bf16)
            send(gate, j)

        order.loop(8, 0.75, gate_item)
        order.add(gate.steps(dwg_own, 16.5, order.now + 19.0, gate_done, free_g))

        def fetch(j):
            at = pl.ds(pl.multiple_of(j * cols, cols), cols)
            return pltpu.make_async_copy(wd_all.at[at], wd.at[j % 2], ss.at[stores[1]])

        fetch(0).start()

        def out_item(j):
            fetch(j).wait()

            @pl.when(j < 7)
            def _():
                fetch(j + 1).start()

            at = pl.ds(pl.multiple_of(j * cols, cols), cols)
            out_part[:, at] = contract_last_dims(right_h[...], wd[j % 2]).astype(bf16)

        order.loop(8, 1.2, out_item)

    units = pltpu.VMEM(hidden.shape, bf16)
    weight = pltpu.VMEM((2, cols, hidden.shape[1]), bf16)
    pl.run_scoped(weights, pltpu.VMEM(part.shape, bf16), units, units, weight)

    def attention(tok, summed, wo, out_t, attended, g_t, g_n, delta, dk, dv):
        gain = gain_row(gains, 1)

        def fetch(r):
            at = pl.ds(pl.multiple_of(r * 128, 128), 128)
            return (
                pltpu.make_async_copy(tok_all.at[at], tok, ss.at[stores[2]]),
                pltpu.make_async_copy(branch.at[at], summed, ss.at[stores[3]]),
            )

        for copy in fetch(0):
            copy.start()
        loads = [
            me.local(src, dst)
            for src, dst in ((wo_all, wo), (out_t_all, out_t), (attended_all, attended))
        ]
        for load in loads:
            load.start()
        dk[...] = jnp.zeros_like(dk)
        dv[...] = jnp.zeros_like(dv)
        for load in later:
            load.wait()
        for i in range(keys // rows):
            span = slice(i * rows, (i + 1) * rows)
            k_t[:, span] = kv[span, :].astype(f32).T[:hd, :].astype(bf16)
        for load in loads:
            load.wait()
        order.add(z_reduce_scatter(me, out_part, below, above, out_own, 12.0, 42.0, out_done), 42.0)

        def prepare(r):
            for copy in fetch(r):
                copy.wait()
            at = pl.ds(pl.multiple_of(r * 128, 128), 128)
            h = tok[...].astype(f32) + summed[...].astype(f32)
            e = total[at, :].astype(f32)
            inv = lax.rsqrt(jnp.mean(h * h, axis=1, keepdims=True) + norm_epsilon)
            u = e * gain
            inner = jnp.mean(u * h, axis=1, keepdims=True)
            grad = cot[at, :].astype(f32) + (inv * u - h * (inv * inv * inv * inner))

            @pl.when(r == z)
            def _():
                own[...] = grad
                gain_two[...] = jnp.broadcast_to(jnp.sum(e * h * inv, axis=0, keepdims=True), gain_two.shape)

            small = grad.astype(bf16)
            cot[at, :] = small
            g = jnp.dot(small, wo[...], preferred_element_type=f32).astype(bf16)
            turned = g.astype(f32).T
            for head in range(heads):
                g_n[head] = g[:, head * hd : (head + 1) * hd]
                mine = turned[head * hd : (head + 1) * hd]
                g_t[head] = mine.astype(bf16)
                delta[head] = jnp.sum(mine * out_t[head, :, at], axis=0, keepdims=True)

            @pl.when(r < rows // 128 - 1)
            def _():
                for copy in fetch(r + 1):
                    copy.start()

        def item(i):
            r, h = i // heads, i % heads

            @pl.when(h == 0)
            def _():
                prepare(r)

            at = pl.ds(pl.multiple_of(r * 128, 128), 128)
            s = jnp.dot(kv[:, 0:hd], q_t[h, :, at], preferred_element_type=f32)
            s = jnp.where(key_pos[...] <= query_pos[0:1, at], s, masked_value)
            p = jnp.exp(s - log_sum[h, :, at])
            dp = jnp.dot(kv[:, hd:], g_t[h], preferred_element_type=f32)
            ds = (p * (dp - delta[h])).astype(bf16)
            dv[...] += jnp.dot(p.astype(bf16), g_n[h], preferred_element_type=f32)
            dk[...] += jnp.dot(ds, q_n[h, at, :], preferred_element_type=f32)
            grad = jnp.dot(k_t[...], ds, preferred_element_type=f32)
            dq_t[h, :, at] = (grad * (1.0 / math.sqrt(hd))).astype(bf16)

        def before(k):
            return progress.whole() < (k // heads + 1) * 4

        order.loop(heads * rows // 128, 1.25, item, before)
        for i in range(keys // rows):
            span = slice(i * rows, (i + 1) * rows)
            kv[span, :] = jnp.concatenate([dk[span, :], dv[span, :]], axis=1).astype(bf16)
        for copy in back:
            copy.start()
        order.until(gate_done)
        pl.semaphore_wait(free_g, 3)

        def low_item(j):
            both.blocks[j, :, lin_cols:] = contract_rows(cot[:, columns(j)], attended[...]).astype(bf16)

        order.loop(8, 0.4, low_item)

    slots = pltpu.VMEM((128, width), bf16)
    pl.run_scoped(
        attention,
        slots,
        slots,
        pltpu.VMEM(wo_all.shape, bf16),
        pltpu.VMEM(out_t_all.shape, f32),
        pltpu.VMEM(attended_all.shape, bf16),
        pltpu.VMEM((heads, hd, 128), bf16),
        pltpu.VMEM((heads, 128, hd), bf16),
        pltpu.VMEM((heads, 1, 128), f32),
        pltpu.VMEM((keys, hd), f32),
        pltpu.VMEM((keys, hd), f32),
    )

    def last(left, right_u, wqkv, normed, lin, gain_one):
        tok = cot
        pairs = ((wqkv_all, wqkv), (normed_two, left), (d_up, right_u), (normed_all, normed), (tok_all, tok))
        loads = [me.local(src, dst) for src, dst in pairs]
        for load in loads:
            load.start()
        gain_one[...] = jnp.zeros_like(gain_one)
        order.until(progress.sent_in, progress.sent_out, down_done)
        pl.semaphore_wait(free_d, 3)
        loads[1].wait()
        loads[2].wait()

        def up_item(j):
            up.blocks[j] = contract_rows(left[:, columns(j)], right_u[...]).astype(bf16)
            send(up, j)

        order.loop(8, 0.75, up_item)
        order.add(up.steps(dwu_own, 16.5, order.now + 0.1, up_done))
        for copy in back:
            copy.wait_recv()
        mine = kv[0:rows, :].astype(f32)
        for i in range(keys // rows - 1):
            mine = mine + came[i].astype(f32)
        for copy in back:
            copy.wait_send()
        kv[0:rows, :] = mine.astype(bf16)
        for load in (loads[0], loads[3], loads[4]):
            load.wait()

        def finish_item(i):
            at = pl.ds(pl.multiple_of(i * 128, 128), 128)
            grads_kv = kv[at, :].astype(f32).T
            grads = jnp.concatenate(
                [dq_t[h, :, at].astype(f32) for h in range(heads)] + [grads_kv[:hd]], axis=0
            )
            grads = rotate_heads(grads, cos_t[:, at], sin_t[:, at], inverse=True)
            natural = jnp.concatenate([grads, grads_kv[hd:]], axis=0).T.astype(bf16)
            lin[at, :] = natural
            one = contract_last_dims(natural, wqkv[...])
            total[at, :] = one.astype(bf16)
            x = tok[at, :].astype(f32)
            inv = lax.rsqrt(jnp.mean(x * x, axis=1, keepdims=True) + norm_epsilon)
            gain_one[0:1, :] += jnp.sum(one * x * inv, axis=0, keepdims=True)

        order.loop(rows // 128, 2.0, finish_item)
        for i in range(8):
            span = slice(i * cols, (i + 1) * cols)
            gain_parts[i * 8 : (i + 1) * 8, :] = jnp.concatenate(
                [gain_one[0:1, span], gain_two[0:1, span], jnp.zeros((6, cols), f32)], axis=0
            )
        order.until(out_done)
        me.free_along_z(free_z)
        order.add(gains_steps(order.now))
        order.step()
        me.wait_along_z(free_z)
        order.add(z_reduce_scatter(me, total, below, above, grad_one, 12.0, order.now, one_done), order.now)

        def both_item(j):
            both.blocks[j, :, :lin_cols] = contract_rows(normed[:, columns(j)], lin[...]).astype(bf16)
            send(both, j)

        order.loop(8, 0.5, both_item)
        order.add(both.steps(dw_own, 13.0, order.now + 0.1, both_done))

    pl.run_scoped(
        last,
        pltpu.VMEM(part.shape, bf16),
        units,
        pltpu.VMEM(wqkv_all.shape, bf16),
        pltpu.VMEM(part.shape, bf16),
        pltpu.VMEM((rows, lin_cols), bf16),
        pltpu.VMEM((8, width), f32),
    )
    order.until(both_done)
    dwkv_own[...] = dw_own[:, wide:lin_cols].astype(bf16)
    for copy in kv_sends:
        copy.start()
    order.finish()
    for copy in kv_sends:
        copy.wait_recv()
    dwkv_all[0] = dwkv_own[...]
    for d in (1, 2, 3):
        dwkv_all[d] = came_kv[d - 1]
    for copy in kv_sends:
        copy.wait_send()


def backward(
    part, cot_all, hidden, normed_two, d_gate, d_up, wd_all, tok_all, branch, gains, wo_all,
    out_t, attended, q_t, q_n, kv_all, wqkv_all, normed, log_sum, key_pos, query_pos, cos_t, sin_t
):
    heads, hd, rows = q_t.shape
    keys = key_pos.shape[0]
    width = part.shape[1]
    cols = width // 8
    whole = pltpu.VMEM(part.shape, bf16)
    own = (wd_all.shape[0] // 8, wd_all.shape[1])
    narrow = wqkv_all.shape[1] + wo_all.shape[1]
    return pl.pallas_call(
        backward_kernel,
        out_shape=(
            shape(own),
            shape(own),
            shape(own),
            shape((own[0], narrow), f32),
            shape((4, own[0], 2 * hd)),
            shape((rows // 4, width), f32),
            shape((rows // 4, width), f32),
            shape((rows // 4, width), f32),
            shape((8, cols), f32),
        ),
        in_specs=[VM] + [HB] * 8 + [VM] + [HB] * 8 + [VM] * 5,
        out_specs=[VM] * 9,
        scratch_shapes=[whole] * 7
        + [
            pltpu.VMEM(q_t.shape, bf16),
            pltpu.VMEM(q_n.shape, bf16),
            pltpu.VMEM((keys, 2 * hd), bf16),
            pltpu.VMEM((hd, keys), bf16),
            pltpu.VMEM((keys // rows - 1, rows, 2 * hd), bf16),
            pltpu.VMEM(q_t.shape, bf16),
            pltpu.VMEM((8, width), f32),
            pltpu.VMEM((64, cols), f32),
            pltpu.VMEM((7, 8, cols), f32),
            pltpu.VMEM((8, cols), f32),
            pltpu.VMEM((3, 8, cols), f32),
            pltpu.VMEM((own[0], 2 * hd), bf16),
            pltpu.VMEM((3, own[0], 2 * hd), bf16),
        ]
        + plane_scatter_scratch(*own) * 2
        + [pltpu.SemaphoreType.REGULAR] * 3
        + dma_sems(224),
        compiler_params=params(4, 67043328),
        name="backward",
    )(
        part, cot_all, hidden, normed_two, d_gate, d_up, wd_all, tok_all, branch, gains, wo_all,
        out_t, attended, q_t, q_n, kv_all, wqkv_all, normed, log_sum, key_pos, query_pos, cos_t, sin_t
    )


def local_fast(
    tokens, w_query, w_key, w_value, w_out, w_gate, w_up, w_down, gain_attn, gain_mlp, stretch_order, cotangent
):
    row_count, width = tokens.shape
    groups = 4
    cols = width // 8
    contract_last = (((1,), (1,)), ((), ()))
    z = lax.axis_index("head")
    own_first = z * row_count

    def own_rows(values):
        return lax.dynamic_slice_in_dim(values, own_first, row_count, 0)

    frequency = rope_base ** (-(np.arange(HD // 2, dtype=np.float32) * np.float32(2.0 / HD)))
    frequency = jnp.asarray(np.broadcast_to(frequency.astype(np.float32)[:, None], (HD // 2, 128)))
    gains = jnp.concatenate([gain_attn[None], gain_mlp[None]]).astype(f32)
    (
        tok_all, wqkv_all, gains_all, wo_all, wg_all, wu_all, wd_all, cot_all, kv_all, branch,
        normed, q_t, q_n, out_t, attended, log_sum, key_pos, query_pos, cos_t, sin_t,
    ) = forward(
        stretch_order, tokens, w_query, w_key, w_value, gains, frequency, w_out, cotangent, w_gate, w_up, w_down
    )
    gain_rows = gains_all.reshape(8, 8, cols)
    gain_one = gain_rows[:, 0].reshape(width)
    gain_two = gain_rows[:, 1].reshape(width)
    hidden_rows = tok_all.astype(f32) + branch.astype(f32)
    inv_mlp = lax.rsqrt(jnp.mean(hidden_rows * hidden_rows, axis=-1, keepdims=True) + norm_epsilon)
    normed_two = (hidden_rows * inv_mlp * gain_two).astype(bf16)
    gate = jnp.dot(normed_two, wg_all, preferred_element_type=f32)
    up = jnp.dot(normed_two, wu_all, preferred_element_type=f32)
    gate_sigmoid = jax.nn.sigmoid(gate)
    gate_silu = gate * gate_sigmoid
    hidden = (gate_silu * up).astype(bf16)
    grad_hidden = jnp.dot(cot_all, wd_all, preferred_element_type=f32)
    d_gate = (grad_hidden * up * gate_sigmoid * (1.0 + gate * (1.0 - gate_sigmoid))).astype(bf16)
    d_up = (grad_hidden * gate_silu).astype(bf16)
    two_part = lax.dot_general(d_gate, wg_all, contract_last, preferred_element_type=f32)
    two_part = two_part + lax.dot_general(d_up, wu_all, contract_last, preferred_element_type=f32)
    dwd_own, dwg_own, dwu_own, dw_own, dwkv_all, out_own, grad_hidden_own, grad_one, gain_grads = backward(
        two_part.astype(bf16), cot_all, hidden, normed_two, d_gate, d_up, wd_all, tok_all, branch,
        gains_all, wo_all, out_t, attended, q_t, q_n, kv_all, wqkv_all, normed, log_sum, key_pos, query_pos,
        cos_t, sin_t,
    )

    x_own = tokens.astype(f32)
    layer_low = (x_own + own_rows(branch).astype(f32) + out_own).astype(bf16)
    inv_own = lax.rsqrt(jnp.mean(x_own * x_own, axis=-1, keepdims=True) + norm_epsilon)
    grad_tokens = (grad_hidden_own + norm_input_grad(x_own, inv_own, gain_one, grad_one)).astype(bf16)
    slots = jnp.concatenate(
        [lax.dynamic_slice_in_dim(dwkv_all, (z - j) % 4, 1, 0) for j in range(4)], axis=0
    ).astype(f32)
    grad_key = slots[:, :, :HD].transpose(1, 0, 2).reshape(cols, groups * HD)
    grad_value = slots[:, :, HD:].transpose(1, 0, 2).reshape(cols, groups * HD)
    return (
        layer_low,
        grad_tokens,
        dw_own[:, : w_query.shape[1]],
        grad_key,
        grad_value,
        dw_own[:, w_query.shape[1] + 2 * HD :],
        dwg_own.astype(f32),
        dwu_own.astype(f32),
        dwd_own.astype(f32),
        gain_grads[0],
        gain_grads[1],
    )


def solution(mesh):
    sizes = (mesh.shape["fsdp"], mesh.shape["blk"], mesh.shape["head"])
    return jax.shard_map(
        local_fast if sizes == (2, 4, 4) else local,
        mesh=mesh,
        in_specs=(
            P(("fsdp", "blk", "head"), None),
            P(("fsdp", "blk"), "head"),
            P(("fsdp", "blk"), None),
            P(("fsdp", "blk"), None),
            P(("fsdp", "blk"), "head"),
            P(("fsdp", "blk"), "head"),
            P(("fsdp", "blk"), "head"),
            P(("fsdp", "blk"), "head"),
            P(("fsdp", "blk")),
            P(("fsdp", "blk")),
            P(),
            P(("fsdp", "blk", "head"), None),
        ),
        out_specs=(
            P(("fsdp", "blk", "head"), None),
            P(("fsdp", "blk", "head"), None),
            P(("fsdp", "blk"), "head"),
            P(("fsdp", "blk"), None),
            P(("fsdp", "blk"), None),
            P(("fsdp", "blk"), "head"),
            P(("fsdp", "blk"), "head"),
            P(("fsdp", "blk"), "head"),
            P(("fsdp", "blk"), "head"),
            P(("fsdp", "blk")),
            P(("fsdp", "blk")),
        ),
        check_vma=False,
    )
```

```python
import math

import jax
import jax.numpy as jnp
import numpy as np
from jax import lax
from jax.experimental import pallas as pl
from jax.experimental.pallas import tpu as pltpu
from jax.sharding import PartitionSpec as P

H = 32
KV = 4
HD = 64


norm_epsilon = 1e-05
rope_base = 10000.0
masked_value = -1e30


def rope_tables(positions, head_dim):
    half_dim = head_dim // 2
    frequency = rope_base ** (-(jnp.arange(half_dim, dtype=jnp.float32) * (2.0 / head_dim)))
    angles = positions.astype(jnp.float32)[:, None] * frequency[None, :]
    return (jnp.cos(angles), jnp.sin(angles))


def rotate(values, cosine, sine_table):
    half_dim = values.shape[-1] // 2
    first_half = values[..., :half_dim]
    second_half = values[..., half_dim:]
    cos_rows = cosine[:, None, :]
    sin_rows = sine_table[:, None, :]
    return jnp.concatenate(
        [
            first_half * cos_rows - second_half * sin_rows,
            second_half * cos_rows + first_half * sin_rows,
        ],
        axis=-1,
    )


def unrotate(values, cosine, sine_table):
    half_dim = values.shape[-1] // 2
    first_half = values[..., :half_dim]
    second_half = values[..., half_dim:]
    cos_rows = cosine[:, None, :]
    sin_rows = sine_table[:, None, :]
    return jnp.concatenate(
        [
            first_half * cos_rows + second_half * sin_rows,
            second_half * cos_rows - first_half * sin_rows,
        ],
        axis=-1,
    )


def stretch_positions(stretch_order, first_row, row_span, stretch_rows):
    storage = first_row + jnp.arange(row_span, dtype=jnp.int32)
    stretch_index = storage // stretch_rows
    match_table = (
        stretch_index[:, None] == jnp.arange(stretch_order.shape[0], dtype=jnp.int32)[None, :]
    )
    stretch_base = jnp.sum(jnp.where(match_table, stretch_order[None, :], 0), axis=1)
    return stretch_base * stretch_rows + storage % stretch_rows


def norm_input_grad(values, inverse, gain_vector, grad_normed):
    scaled = grad_normed * gain_vector
    inner = jnp.mean(scaled * values, axis=-1, keepdims=True)
    return inverse * scaled - values * inverse * inverse * inverse * inner


def gain_grad(values, inverse, grad_normed):
    return jnp.sum(grad_normed * values * inverse, axis=0)


def fold_block(
    state_now, keys_block, values_block, key_positions, query_heads, query_positions, score_scale
):
    running_max, running_sum, running_out = state_now
    scores = (
        jnp.einsum("qhd,kd->hqk", query_heads, keys_block, preferred_element_type=jnp.float32)
        * score_scale
    )
    allowed = (query_positions[:, None] >= key_positions[None, :])[None]
    scores = jnp.where(allowed, scores, masked_value)
    new_max = jnp.maximum(running_max, jnp.max(scores, axis=-1))
    weights = jnp.where(allowed, jnp.exp(scores - new_max[..., None]), 0.0)
    factor = jnp.exp(running_max - new_max)
    running_sum = running_sum * factor + jnp.sum(weights, axis=-1)
    running_out = running_out * factor[..., None] + jnp.einsum(
        "hqk,kd->hqd",
        weights.astype(jnp.bfloat16),
        values_block,
        preferred_element_type=jnp.float32,
    )
    return (new_max, running_sum, running_out)


def local(
    tokens,
    w_query,
    w_key,
    w_value,
    w_out,
    w_gate,
    w_up,
    w_down,
    gain_attn,
    gain_mlp,
    stretch_order,
    cotangent,
):
    row_count = tokens.shape[0]
    groups = lax.axis_size("head")
    blocks = lax.axis_size("blk")
    local_heads = H // groups
    repeats = groups // KV
    head_rows = row_count * groups
    stretch_rows = head_rows // 2
    score_scale = 1.0 / math.sqrt(HD)
    contract_last = (((1,), (1,)), ((), ()))
    contract_first = (((0,), (0,)), ((), ()))
    head_index = lax.axis_index("head")
    own_first = head_index * row_count
    block_first = lax.axis_index("blk") * head_rows
    positions = stretch_positions(stretch_order, block_first + own_first, row_count, stretch_rows)
    query_positions = stretch_positions(stretch_order, block_first, head_rows, stretch_rows)
    cos_own, sin_own = rope_tables(positions, HD)
    cos_block, sin_block = rope_tables(query_positions, HD)

    def layer_weights():
        return (
            lax.all_gather(w_query, ("fsdp", "blk"), axis=0, tiled=True),
            lax.all_gather(w_key, ("fsdp", "blk"), axis=0, tiled=True),
            lax.all_gather(w_value, ("fsdp", "blk"), axis=0, tiled=True),
            lax.all_gather(w_out, ("fsdp", "blk"), axis=0, tiled=True),
            lax.all_gather(w_gate, ("fsdp", "blk"), axis=0, tiled=True),
            lax.all_gather(w_up, ("fsdp", "blk"), axis=0, tiled=True),
            lax.all_gather(w_down, ("fsdp", "blk"), axis=0, tiled=True),
            lax.all_gather(gain_attn, ("fsdp", "blk"), axis=0, tiled=True),
            lax.all_gather(gain_mlp, ("fsdp", "blk"), axis=0, tiled=True),
        )

    def gather_query(columns):
        return lax.all_gather(columns, "head", axis=1, tiled=True)

    (
        query_cols,
        key_full,
        value_full,
        out_cols,
        gate_cols,
        up_cols,
        down_cols,
        gain_one,
        gain_two,
    ) = layer_weights()
    tokens_float = tokens.astype(jnp.float32)
    inv_attn = lax.rsqrt(
        jnp.mean(tokens_float * tokens_float, axis=-1, keepdims=True) + norm_epsilon
    )
    normed = (tokens_float * inv_attn * gain_one.astype(jnp.float32)).astype(jnp.bfloat16)
    normed_rows, cotangent_rows = (
        lax.all_gather(normed, "head", axis=0, tiled=True),
        lax.all_gather(cotangent, "head", axis=0, tiled=True),
    )
    query_all = gather_query(query_cols)
    query_lin = jnp.dot(normed, query_all, preferred_element_type=jnp.float32).reshape(
        row_count, H, HD
    )
    key_lin = jnp.dot(normed, key_full, preferred_element_type=jnp.float32).reshape(
        row_count, KV, HD
    )
    value_lin = jnp.dot(normed, value_full, preferred_element_type=jnp.float32).reshape(
        row_count, KV, HD
    )
    query_rot = rotate(query_lin, cos_own, sin_own).astype(jnp.bfloat16).reshape(row_count, H * HD)
    key_rot = rotate(key_lin, cos_own, sin_own).astype(jnp.bfloat16)
    key_slots = jnp.repeat(key_rot, repeats, axis=1).reshape(row_count, groups * HD)
    value_slots = jnp.repeat(value_lin.astype(jnp.bfloat16), repeats, axis=1).reshape(
        row_count, groups * HD
    )
    query_recv, key_own, value_own = (
        lax.all_to_all(query_rot, "head", split_axis=1, concat_axis=0, tiled=True),
        lax.all_to_all(key_slots, "head", split_axis=1, concat_axis=0, tiled=True),
        lax.all_to_all(value_slots, "head", split_axis=1, concat_axis=0, tiled=True),
    )
    query_heads = query_recv.reshape(head_rows, local_heads, HD)
    initial = (
        jnp.full((local_heads, head_rows), masked_value, jnp.float32),
        jnp.zeros((local_heads, head_rows), jnp.float32),
        jnp.zeros((local_heads, head_rows, HD), jnp.float32),
    )
    state_now = initial
    keys_piece = lax.all_gather(key_own, "blk", axis=0, tiled=True)
    values_piece = lax.all_gather(value_own, "blk", axis=0, tiled=True)
    piece_rows = keys_piece.shape[0]

    def scan_step(state_inner, step_index):
        offset = step_index * head_rows
        keys_block = lax.dynamic_slice_in_dim(keys_piece, offset, head_rows, 0)
        values_block = lax.dynamic_slice_in_dim(values_piece, offset, head_rows, 0)
        key_positions = stretch_positions(stretch_order, offset, head_rows, stretch_rows)
        return (
            fold_block(
                state_inner,
                keys_block,
                values_block,
                key_positions,
                query_heads,
                query_positions,
                score_scale,
            ),
            None,
        )

    state_now, unused = lax.scan(
        scan_step, state_now, jnp.arange(piece_rows // head_rows, dtype=jnp.int32)
    )
    running_max, running_sum, running_out = state_now
    attended_float = running_out / running_sum[..., None]
    log_sum = running_max + jnp.log(running_sum)
    attended_heads = (
        attended_float.astype(jnp.bfloat16).transpose(1, 0, 2).reshape(head_rows, local_heads * HD)
    )
    branch = lax.dot_general(
        attended_heads, out_cols, contract_last, preferred_element_type=jnp.float32
    )
    own_branch = lax.dynamic_slice_in_dim(branch, own_first, row_count, 0)
    partial_value = lax.dynamic_update_slice_in_dim(branch, own_branch + tokens_float, own_first, 0)
    hidden_rows = lax.psum(partial_value.astype(jnp.bfloat16), "head").astype(jnp.float32)
    inv_mlp = lax.rsqrt(jnp.mean(hidden_rows * hidden_rows, axis=-1, keepdims=True) + norm_epsilon)
    normed_two_rows = (hidden_rows * inv_mlp * gain_two.astype(jnp.float32)).astype(jnp.bfloat16)
    gate_proj = jnp.dot(normed_two_rows, gate_cols, preferred_element_type=jnp.float32)
    up_proj = jnp.dot(normed_two_rows, up_cols, preferred_element_type=jnp.float32)
    gate_sigmoid = jax.nn.sigmoid(gate_proj)
    gate_silu = gate_proj * gate_sigmoid
    hidden = (gate_silu * up_proj).astype(jnp.bfloat16)
    hidden_own = lax.dynamic_slice_in_dim(hidden_rows, own_first, row_count, 0)
    output_float = hidden_own + lax.psum_scatter(
        lax.dot_general(
            hidden, down_cols, contract_last, preferred_element_type=jnp.float32
        ).astype(jnp.bfloat16),
        "head",
        scatter_dimension=0,
        tiled=True,
    ).astype(jnp.float32)
    layer_low = output_float.astype(jnp.bfloat16)
    (
        query_cols,
        key_full,
        value_full,
        out_cols,
        gate_cols,
        up_cols,
        down_cols,
        gain_one,
        gain_two,
    ) = layer_weights()
    query_all = gather_query(query_cols)
    grad_hidden = jnp.dot(cotangent_rows, down_cols, preferred_element_type=jnp.float32)
    grad_gate_rows = (
        grad_hidden * up_proj * gate_sigmoid * (1.0 + gate_proj * (1.0 - gate_sigmoid))
    ).astype(jnp.bfloat16)
    grad_up_rows = (grad_hidden * gate_silu).astype(jnp.bfloat16)
    grad_w_down = lax.dot_general(
        cotangent_rows, hidden, contract_first, preferred_element_type=jnp.float32
    )
    grad_w_gate = lax.dot_general(
        normed_two_rows, grad_gate_rows, contract_first, preferred_element_type=jnp.float32
    )
    grad_w_up = lax.dot_general(
        normed_two_rows, grad_up_rows, contract_first, preferred_element_type=jnp.float32
    )
    normed_two_part = lax.dot_general(
        grad_gate_rows, gate_cols, contract_last, preferred_element_type=jnp.float32
    )
    normed_two_part = normed_two_part + lax.dot_general(
        grad_up_rows, up_cols, contract_last, preferred_element_type=jnp.float32
    )
    grad_normed_two = lax.psum(normed_two_part.astype(jnp.bfloat16), "head").astype(jnp.float32)
    gain_two_float = gain_two.astype(jnp.float32)
    grad_hidden_rows = cotangent_rows.astype(jnp.float32) + norm_input_grad(
        hidden_rows, inv_mlp, gain_two_float, grad_normed_two
    )
    own_grad_two = lax.dynamic_slice_in_dim(grad_normed_two, own_first, row_count, 0)
    own_inv_mlp = lax.dynamic_slice_in_dim(inv_mlp, own_first, row_count, 0)
    grad_gain_two = gain_grad(hidden_own, own_inv_mlp, own_grad_two)
    grad_low_rows = grad_hidden_rows.astype(jnp.bfloat16)
    grad_w_out = lax.dot_general(
        grad_low_rows, attended_heads, contract_first, preferred_element_type=jnp.float32
    )
    grad_heads = (
        jnp.dot(grad_low_rows, out_cols, preferred_element_type=jnp.float32)
        .astype(jnp.bfloat16)
        .reshape(head_rows, local_heads, HD)
    )
    keys_all, values_all = (
        lax.all_gather(key_own, "blk", axis=0, tiled=True),
        lax.all_gather(value_own, "blk", axis=0, tiled=True),
    )
    row_delta = jnp.sum(grad_heads.astype(jnp.float32).transpose(1, 0, 2) * attended_float, axis=-1)

    def back_block(grad_query_acc, block_index):
        offset = block_index * head_rows
        keys_block = lax.dynamic_slice_in_dim(keys_all, offset, head_rows, 0)
        values_block = lax.dynamic_slice_in_dim(values_all, offset, head_rows, 0)
        key_positions = stretch_positions(stretch_order, offset, head_rows, stretch_rows)
        scores = (
            jnp.einsum("qhd,kd->hqk", query_heads, keys_block, preferred_element_type=jnp.float32)
            * score_scale
        )
        allowed = (query_positions[:, None] >= key_positions[None, :])[None]
        probs_block = jnp.where(allowed, jnp.exp(scores - log_sum[..., None]), 0.0)
        grad_probs = jnp.einsum(
            "qhd,kd->hqk", grad_heads, values_block, preferred_element_type=jnp.float32
        )
        grad_scores = (probs_block * (grad_probs - row_delta[..., None])).astype(jnp.bfloat16)
        grad_query_acc = grad_query_acc + jnp.einsum(
            "hqk,kd->qhd", grad_scores, keys_block, preferred_element_type=jnp.float32
        )
        grad_key_part = (
            jnp.einsum("hqk,qhd->kd", grad_scores, query_heads, preferred_element_type=jnp.float32)
            * score_scale
        )
        grad_value_part = jnp.einsum(
            "hqk,qhd->kd",
            probs_block.astype(jnp.bfloat16),
            grad_heads,
            preferred_element_type=jnp.float32,
        )
        return (grad_query_acc, (grad_key_part, grad_value_part))

    grad_query_acc, (key_terms, value_terms) = lax.scan(
        back_block,
        jnp.zeros((head_rows, local_heads, HD), jnp.float32),
        jnp.arange(blocks, dtype=jnp.int32),
    )
    grad_key_sum, grad_value_sum = (
        lax.psum_scatter(
            key_terms.reshape(blocks * head_rows, HD).astype(jnp.bfloat16),
            "blk",
            scatter_dimension=0,
            tiled=True,
        ).astype(jnp.float32),
        lax.psum_scatter(
            value_terms.reshape(blocks * head_rows, HD).astype(jnp.bfloat16),
            "blk",
            scatter_dimension=0,
            tiled=True,
        ).astype(jnp.float32),
    )
    grad_query_rot = (grad_query_acc * score_scale).astype(jnp.bfloat16)
    grad_query_lin_heads = (
        unrotate(grad_query_rot.astype(jnp.float32), cos_block, sin_block)
        .astype(jnp.bfloat16)
        .reshape(head_rows, local_heads * HD)
    )
    key_slot_grad = grad_key_sum.astype(jnp.bfloat16)
    value_slot_grad = grad_value_sum.astype(jnp.bfloat16)
    grad_w_query = lax.dot_general(
        normed_rows, grad_query_lin_heads, contract_first, preferred_element_type=jnp.float32
    )
    query_back, key_back, value_back = (
        lax.all_to_all(grad_query_lin_heads, "head", split_axis=0, concat_axis=1, tiled=True),
        lax.all_to_all(key_slot_grad, "head", split_axis=0, concat_axis=1, tiled=True),
        lax.all_to_all(value_slot_grad, "head", split_axis=0, concat_axis=1, tiled=True),
    )
    key_slot_lin = (
        unrotate(key_back.astype(jnp.float32).reshape(row_count, groups, HD), cos_own, sin_own)
        .astype(jnp.bfloat16)
        .reshape(row_count, KV, repeats, HD)
    )
    value_slot_lin = value_back.reshape(row_count, KV, repeats, HD)
    grad_w_key = jnp.einsum(
        "td,tjrc->djc", normed, key_slot_lin, preferred_element_type=jnp.float32
    ).reshape(-1, KV * HD)
    grad_w_value = jnp.einsum(
        "td,tjrc->djc", normed, value_slot_lin, preferred_element_type=jnp.float32
    ).reshape(-1, KV * HD)
    grad_normed = lax.dot_general(
        query_back, query_all, contract_last, preferred_element_type=jnp.float32
    )
    grad_normed = grad_normed + jnp.einsum(
        "tjrc,djc->td",
        key_slot_lin,
        key_full.reshape(-1, KV, HD),
        preferred_element_type=jnp.float32,
    )
    grad_normed = grad_normed + jnp.einsum(
        "tjrc,djc->td",
        value_slot_lin,
        value_full.reshape(-1, KV, HD),
        preferred_element_type=jnp.float32,
    )
    gain_one_float = gain_one.astype(jnp.float32)
    grad_input_norm = norm_input_grad(tokens_float, inv_attn, gain_one_float, grad_normed)
    grad_gain_one = gain_grad(tokens_float, inv_attn, grad_normed)
    grad_hidden_own = lax.dynamic_slice_in_dim(grad_hidden_rows, own_first, row_count, 0)
    grad_tokens = (grad_hidden_own + grad_input_norm).astype(jnp.bfloat16)
    head_sums = (
        lax.psum(grad_w_key.astype(jnp.bfloat16), "head").astype(jnp.float32),
        lax.psum(grad_w_value.astype(jnp.bfloat16), "head").astype(jnp.float32),
        lax.psum(grad_gain_one.astype(jnp.bfloat16), "head").astype(jnp.float32),
        lax.psum(grad_gain_two.astype(jnp.bfloat16), "head").astype(jnp.float32),
    )
    reduced = (
        lax.psum_scatter(
            grad_w_query.astype(jnp.bfloat16), ("fsdp", "blk"), scatter_dimension=0, tiled=True
        ).astype(jnp.float32),
        lax.psum_scatter(
            head_sums[0].astype(jnp.bfloat16), ("fsdp", "blk"), scatter_dimension=0, tiled=True
        ).astype(jnp.float32),
        lax.psum_scatter(
            head_sums[1].astype(jnp.bfloat16), ("fsdp", "blk"), scatter_dimension=0, tiled=True
        ).astype(jnp.float32),
        lax.psum_scatter(
            grad_w_out.astype(jnp.bfloat16), ("fsdp", "blk"), scatter_dimension=0, tiled=True
        ).astype(jnp.float32),
        lax.psum_scatter(
            grad_w_gate.astype(jnp.bfloat16), ("fsdp", "blk"), scatter_dimension=0, tiled=True
        ).astype(jnp.float32),
        lax.psum_scatter(
            grad_w_up.astype(jnp.bfloat16), ("fsdp", "blk"), scatter_dimension=0, tiled=True
        ).astype(jnp.float32),
        lax.psum_scatter(
            grad_w_down.astype(jnp.bfloat16), ("fsdp", "blk"), scatter_dimension=0, tiled=True
        ).astype(jnp.float32),
        lax.psum_scatter(
            head_sums[2].astype(jnp.bfloat16), ("fsdp", "blk"), scatter_dimension=0, tiled=True
        ).astype(jnp.float32),
        lax.psum_scatter(
            head_sums[3].astype(jnp.bfloat16), ("fsdp", "blk"), scatter_dimension=0, tiled=True
        ).astype(jnp.float32),
    )
    return (
        layer_low,
        grad_tokens,
        reduced[0],
        reduced[1],
        reduced[2],
        reduced[3],
        reduced[4],
        reduced[5],
        reduced[6],
        reduced[7],
        reduced[8],
    )


MESH = pl.DeviceIdType.MESH
f32, bf16 = jnp.float32, jnp.bfloat16
VM = pl.BlockSpec(memory_space=pltpu.VMEM)
HB = pl.BlockSpec(memory_space=pl.ANY)


def dma_sems(n):
    return [pltpu.SemaphoreType.DMA((n,)), pltpu.SemaphoreType.DMA((n,))]


class Here:
    def __init__(self, send_sem, recv_sem):
        self.y = lax.axis_index("fsdp")
        blk = lax.axis_index("blk")
        self.x, self.c = blk // 2, blk % 2
        self.z = lax.axis_index("head")
        self.end = (self.z == 0) | (self.z == 3)
        self.middle = (self.z == 1) | (self.z == 2)
        self.inward = {"head": jnp.where(self.z < 2, self.z + 1, self.z - 1)}
        self.outward = {"head": jnp.where(self.z < 2, self.z - 1, self.z + 1)}
        self.send_sem, self.recv_sem, self.used = send_sem, recv_sem, 0

    def plane(self, i):
        y = 1 - self.y if i & 4 else self.y
        x = 1 - self.x if i & 2 else self.x
        c = 1 - self.c if i & 1 else self.c
        return {"fsdp": y, "blk": x * 2 + c}

    def number(self, i):
        at = self.plane(i)
        return at["fsdp"] * 4 + at["blk"]

    def up(self):
        return {"head": self.z + 1}

    def down(self):
        return {"head": self.z - 1}

    def copy(self, src, dst, device):
        k = self.used
        self.used += 1
        return self.again(k, src, dst, device)

    def slot(self):
        self.used += 1
        return self.used - 1

    def again(self, k, src, dst, device):
        return pltpu.make_async_remote_copy(
            src_ref=src,
            dst_ref=dst,
            send_sem=self.send_sem.at[k],
            recv_sem=self.recv_sem.at[k],
            device_id=device,
            device_id_type=MESH,
        )

    def local(self, src, dst):
        k = self.used
        self.used += 1
        return pltpu.make_async_copy(src, dst, self.send_sem.at[k])

    def free_in_plane(self, sem):
        for i in (1, 2, 4):
            pl.semaphore_signal(sem, inc=1, device_id=self.plane(i), device_id_type=MESH)

    def free_along_z(self, sem):
        @pl.when(self.z > 0)
        def _():
            pl.semaphore_signal(sem, inc=1, device_id=self.down(), device_id_type=MESH)

        @pl.when(self.z < 3)
        def _():
            pl.semaphore_signal(sem, inc=1, device_id=self.up(), device_id_type=MESH)

    def wait_along_z(self, sem):
        pl.semaphore_wait(sem, jnp.where(self.z > 0, 1, 0) + jnp.where(self.z < 3, 1, 0))

    def enter(self, offsets, along_z=True, all_z=False):
        bar = pltpu.get_barrier_semaphore()
        for i in offsets:
            pl.semaphore_signal(bar, inc=1, device_id=self.plane(i), device_id_type=MESH)
        if all_z:
            for d in (1, 2, 3):
                pl.semaphore_signal(
                    bar, inc=1, device_id={"head": (self.z + d) % 4}, device_id_type=MESH
                )
            pl.semaphore_wait(bar, len(offsets) + 3)
            return
        if along_z:

            @pl.when(self.z > 0)
            def _():
                pl.semaphore_signal(bar, inc=1, device_id=self.down(), device_id_type=MESH)

            @pl.when(self.z < 3)
            def _():
                pl.semaphore_signal(bar, inc=1, device_id=self.up(), device_id_type=MESH)

        peers = len(offsets)
        if along_z:
            peers = peers + jnp.where(self.z > 0, 1, 0) + jnp.where(self.z < 3, 1, 0)
        pl.semaphore_wait(bar, peers)


class Order:
    def __init__(self, *tasks):
        self.now, self.count, self.waiting = 0.0, 0, []
        for task in tasks:
            self.add(task)

    def add(self, task, at=None):
        self.waiting.append((self.now if at is None else at, self.count, task))
        self.count += 1

    def next_at(self):
        return min(self.waiting, default=(math.inf,))[0]

    def step(self):
        item = min(self.waiting, key=lambda entry: entry[:2])
        self.waiting.remove(item)
        at = next(item[2], None)
        if at is not None:
            self.waiting.append((max(at, item[0]), item[1], item[2]))

    def pump(self, until):
        while self.next_at() <= until:
            self.step()
        self.now = max(self.now, until)

    def until(self, *flags):
        while not all(flag.up for flag in flags):
            self.now = max(self.now, self.next_at())
            self.step()

    def finish(self):
        while self.waiting:
            self.step()

    def loop(self, n, each, item, before=None):
        start = self.now

        def body(i, _):
            for k in range(n):
                while self.waiting and (
                    self.next_at() <= start + k * each or (before is not None and before(k))
                ):

                    @pl.when(i == k)
                    def _():
                        self.step()

            item(i)
            return 0

        lax.fori_loop(0, n, body, 0)
        self.now = start + n * each


def drive(*tasks):
    Order(*tasks).finish()


class Flag:
    def __init__(self):
        self.up = False


def z_gather(me, src, dst, unit, begin=0.0, done=None, issue=None):
    rows = src.shape[0]
    half = rows // 2
    z = me.z

    def block(j, h):
        return dst.at[pl.ds(pl.multiple_of(j * rows + h * half, half), half)]

    ups = [me.slot() for _ in range(6)]
    downs = [me.slot() for _ in range(6)]
    own = me.local(src, dst.at[pl.ds(pl.multiple_of(z * rows, rows), rows)])

    def up(j, h):
        mine = src.at[pl.ds(h * half, half)] if j == 0 else block(z - j, h)
        return me.again(ups[2 * j + h], mine, block(z - j, h), me.up())

    def down(j, h):
        mine = src.at[pl.ds(h * half, half)] if j == 0 else block(z + j, h)
        return me.again(downs[2 * j + h], mine, block(z + j, h), me.down())

    def steps():
        yield begin if issue is None else issue

        @pl.when(z < 3)
        def _():
            up(0, 0).start()
            up(0, 1).start()

        @pl.when(z > 0)
        def _():
            down(0, 0).start()
            down(0, 1).start()

        own.start()
        for j in (1, 2, 3):
            for h in (0, 1):
                yield begin + unit * (j - 0.5 + h * 0.5) + 1.8 + 0.4 * j

                @pl.when(z >= j)
                def _():
                    up(j - 1, h).wait_recv()

                if j < 3:

                    @pl.when((z >= j) & (z < 3))
                    def _():
                        up(j, h).start()

                @pl.when(z <= 3 - j)
                def _():
                    down(j - 1, h).wait_recv()

                if j < 3:

                    @pl.when((z <= 3 - j) & (z > 0))
                    def _():
                        down(j, h).start()

        own.wait()
        if done is not None:
            done.up = True
        yield begin + unit * 3 + 15.0
        for j in (0, 1, 2):

            @pl.when((z >= j) & (z < 3))
            def _():
                up(j, 0).wait_send()
                up(j, 1).wait_send()

            @pl.when((z <= 3 - j) & (z > 0))
            def _():
                down(j, 0).wait_send()
                down(j, 1).wait_send()

    return steps()


def plane_gather(me, src, dst, unit, begin=0.0, done=None, issue=None):
    rows = src.shape[0]
    half = rows // 2

    def part(i, h):
        return dst.at[pl.ds(pl.multiple_of(me.number(i) * rows + h * half, half), half)]

    def block(i):
        return dst.at[pl.ds(pl.multiple_of(me.number(i) * rows, rows), rows)]

    halves = src.at[pl.ds(0, half)], src.at[pl.ds(half, half)]
    x_in = [me.copy(halves[h], part(0, h), me.plane(2)) for h in (0, 1)]
    y_in = [me.copy(halves[h], part(0, h), me.plane(4)) for h in (1, 0)]
    to_c = me.copy(src, block(0), me.plane(1))
    own = me.local(src, block(0))
    x_on = me.copy(part(2, 0), part(2, 0), me.plane(4))
    y_on = me.copy(part(4, 1), part(4, 1), me.plane(2))
    x_core = me.copy(block(2), block(2), me.plane(1))
    y_core = me.copy(block(4), block(4), me.plane(1))
    far = [me.copy(part(6, h), part(6, h), me.plane(1)) for h in (0, 1)]

    def steps():
        yield begin if issue is None else issue
        for copy in (x_in[0], y_in[0], x_in[1], y_in[1], to_c, own):
            copy.start()
        yield begin + unit * 0.5 + 2.0
        x_in[0].wait_recv()
        x_on.start()
        y_in[0].wait_recv()
        y_on.start()
        yield begin + unit + 2.5
        x_in[1].wait_recv()
        x_core.start()
        y_in[1].wait_recv()
        y_core.start()
        yield begin + unit * 1.5 + 4.5
        x_on.wait_recv()
        far[0].start()
        y_on.wait_recv()
        far[1].start()
        yield begin + unit * 1.5 + 6.5
        own.wait()
        for copy in (to_c, x_core, y_core, *far):
            copy.wait_recv()
        if done is not None:
            done.up = True
        yield begin + unit * 1.5 + 15.0
        for copy in (*x_in, *y_in, to_c, x_on, x_core, y_on, y_core, *far):
            copy.wait_send()

    return steps()


def plane_direct(me, src, dst, done):
    rows = src.shape[0]
    place = dst.at[pl.ds(pl.multiple_of(me.number(0) * rows, rows), rows)]
    copies = [me.copy(src, place, me.plane(i)) for i in range(1, 8)]
    own = me.local(src, place)

    def steps():
        for copy in (*copies, own):
            copy.start()
        yield 5.0
        own.wait()
        for copy in copies:
            copy.wait_recv()
        done.up = True
        yield 15.0
        for copy in copies:
            copy.wait_send()

    return steps()


def add_rows(dst, a, b, step=32):
    rows = a.shape[0]

    def body(i, _):
        at = pl.ds(pl.multiple_of(i * step, step), step)
        dst[at, :] = (a[at, :].astype(f32) + b[at, :].astype(f32)).astype(dst.dtype)
        return 0

    lax.fori_loop(0, rows // step, body, 0)


class Progress:
    def __init__(self, parts):
        self.parts, self.entered, self.crossed, self.left = parts, 0, 0, 0
        self.sent_in, self.sent_out = Flag(), Flag()

    def whole(self):
        return min(self.crossed, self.left)


def z_reduce_all(me, part, total, inbox, across, out, unit, chunks, progress, begin=0.0, lag=0.0):
    rows = part.shape[0] // chunks
    first = [me.slot() for _ in range(chunks)]
    second = [me.slot() for _ in range(chunks)]
    third = [me.slot() for _ in range(chunks)]
    store = [me.slot() for _ in range(chunks)]
    hop = unit / chunks

    def at(ref, k):
        return ref.at[pl.ds(k * rows, rows)]

    def send_in(k):
        return me.again(first[k], at(part, k), at(inbox, k), me.inward)

    def send_across(k):
        return me.again(second[k], at(inbox, k), at(across, k), me.inward)

    def send_out(k):
        return me.again(third[k], at(total, k), at(total, k), me.outward)

    def put(k):
        return pltpu.make_async_copy(at(total, k), at(out, k), me.send_sem.at[store[k]])

    def entering():
        yield begin
        time, sent = begin, 0
        for k in range(chunks):
            while k >= progress.parts:
                time += 0.5
                yield time
            new, sent = range(sent, progress.parts), progress.parts
            if len(new):

                @pl.when(me.end)
                def _():
                    for j in new:
                        send_in(j).start()

            time = max(time, begin + lag + 2.0) + hop
            yield time

            @pl.when(me.middle)
            def _():
                send_in(k).wait_recv()
                add_rows(at(inbox, k), at(part, k), at(inbox, k))
                send_across(k).start()

            progress.entered = k + 1
        yield time + 20.0

        @pl.when(me.end)
        def _():
            for k in range(chunks):
                send_in(k).wait_send()

        progress.sent_in.up = True

    def crossing():
        yield begin
        time = begin
        for k in range(chunks):
            while k >= progress.entered:
                time += 0.5
                yield time
            time = max(time, begin + lag + 4.0 + hop) + hop
            yield time

            @pl.when(me.middle)
            def _():
                send_across(k).wait_recv()
                add_rows(at(total, k), at(inbox, k), at(across, k))
                send_out(k).start()
                if out is not None:
                    put(k).start()

            progress.crossed = k + 1
        yield time + 10.0

        @pl.when(me.middle)
        def _():
            for k in range(chunks):
                send_across(k).wait_send()
                send_out(k).wait_send()

        progress.sent_out.up = True

    def leaving():
        yield begin
        time = begin
        for k in range(chunks):
            while k >= progress.crossed:
                time += 0.5
                yield time
            time = max(time, begin + lag + 6.0 + 2 * hop) + hop
            yield time

            @pl.when(me.end)
            def _():
                send_out(k).wait_recv()
                if out is not None:
                    put(k).start()

            progress.left = k + 1
        if out is not None:
            yield time + 2.0
            for k in range(chunks):
                put(k).wait()

    return entering(), crossing(), leaving()


def z_reduce_scatter(me, part, from_below, from_above, own, unit, begin=0.0, done=None):
    rows = part.shape[0] // 4
    z = me.z
    ups = [me.slot() for _ in range(4)]
    downs = [me.slot() for _ in range(4)]

    def at(ref, j):
        return ref.at[pl.ds(j * rows, rows)]

    def up(j, source):
        return me.again(ups[j], at(source, j), at(from_below, j), me.up())

    def down(j, source):
        return me.again(downs[j], at(source, j), at(from_above, j), me.down())

    def start(j):
        @pl.when(z == 0)
        def _():
            up(j, part).start()

        @pl.when(z == 3)
        def _():
            down(3 - j, part).start()

    def relay(j, stop):
        @pl.when(z == stop)
        def _():
            up(j, part).wait_recv()
            add_rows(at(from_below, j), at(part, j), at(from_below, j))
            up(j, from_below).start()

        @pl.when(z == 3 - stop)
        def _():
            i = 3 - j
            down(i, part).wait_recv()
            add_rows(at(from_above, i), at(part, i), at(from_above, i))
            down(i, from_above).start()

    yield begin
    start(3)
    yield begin + unit * 0.6
    start(2)
    yield begin + unit + 1.0
    relay(3, 1)
    yield begin + unit * 1.6
    start(1)
    yield begin + unit * 2 + 1.0
    relay(3, 2)
    relay(2, 1)
    yield begin + unit * 3 + 1.5
    for j in range(4):

        @pl.when(z == j)
        def _():
            if j > 0:
                up(j, part).wait_recv()
            if j < 3:
                down(j, part).wait_recv()

            def body(i, _):
                span = pl.ds(pl.multiple_of(i * 32, 32), 32)
                there = pl.ds(pl.multiple_of(j * rows + i * 32, 32), 32)
                value = part[there, :].astype(f32)
                if j > 0:
                    value = value + from_below[there, :].astype(f32)
                if j < 3:
                    value = value + from_above[there, :].astype(f32)
                own[span, :] = value
                return 0

            lax.fori_loop(0, rows // 32, body, 0)
            for i in range(4):
                if i > j:
                    up(i, part).wait_send()
                if i < j:
                    down(i, part).wait_send()

    if done is not None:
        done.up = True


def offsets_of(me, j):
    dx, dy, dc = 1 - (j % 4) // 2, 1 - j % 2, 1 - j // 4
    y = me.y + dy - 2 * me.y * dy
    x = me.x + dx - 2 * me.x * dx
    c = me.c + dc - 2 * me.c * dc
    return y * 4 + x * 2 + c


def plane_scatter_scratch(rows, cols):
    half = rows // 2
    return [
        pltpu.VMEM((8, rows, cols), bf16),
        pltpu.VMEM((4, rows, cols), bf16),
        pltpu.VMEM((2, half, cols), bf16),
        pltpu.VMEM((2, half, cols), bf16),
        pltpu.VMEM((half, cols), bf16),
        pltpu.VMEM((half, cols), bf16),
    ]


class PlaneScatter:
    def __init__(self, me, scratch):
        self.me = me
        self.blocks, self.other, self.over_x, self.over_y, self.last_y, self.last_x = scratch
        blocks, rows = self.blocks, self.blocks.shape[1]
        half = rows // 2
        self.half, self.first, self.second = half, pl.ds(0, half), pl.ds(half, half)
        first, second = self.first, self.second
        self.core = [me.copy(blocks.at[j], self.other.at[j], me.plane(1)) for j in range(4)]
        self.far_x = me.copy(blocks.at[4, first], self.over_x.at[1], me.plane(2))
        self.far_y = me.copy(blocks.at[4, second], self.over_y.at[1], me.plane(4))
        self.near_x = me.copy(blocks.at[5, first], self.over_x.at[0], me.plane(2))
        self.near_y = me.copy(blocks.at[6, second], self.over_y.at[0], me.plane(4))
        self.to_y = me.copy(blocks.at[6, first], self.last_y, me.plane(4))
        self.to_x = me.copy(blocks.at[5, second], self.last_x, me.plane(2))

    def steps(self, out, unit, begin, done, free=None):
        blocks, half, first, second = self.blocks, self.half, self.first, self.second
        for j in range(4):
            yield begin + 0.3 * j
            self.core[j].wait_recv()
            add_rows(blocks.at[4 + j], blocks.at[4 + j], self.other.at[j])
            if j == 0:
                self.far_x.start()
                self.far_y.start()
            if j == 1:
                self.near_x.start()
            if j == 2:
                self.near_y.start()
        yield begin + 3.0 + unit * 0.5
        self.far_x.wait_recv()
        add_rows(blocks.at[6, first], blocks.at[6, first], self.over_x.at[1])
        self.to_y.start()
        self.far_y.wait_recv()
        add_rows(blocks.at[5, second], blocks.at[5, second], self.over_y.at[1])
        self.to_x.start()
        yield begin + 4.0 + unit * 1.5
        for copy in (self.near_x, self.near_y, self.to_y, self.to_x):
            copy.wait_recv()

        def body(i, _):
            at = pl.ds(pl.multiple_of(i * 32, 32), 32)
            low = pl.ds(pl.multiple_of(half + i * 32, 32), 32)
            for rows, near, last in ((at, self.over_x, self.last_y), (low, self.over_y, self.last_x)):
                value = blocks[7, rows, :].astype(f32) + near[0, at, :].astype(f32)
                out[rows, :] = (value + last[at, :].astype(f32)).astype(out.dtype)
            return 0

        lax.fori_loop(0, half // 32, body, 0)
        for copy in (*self.core, self.far_x, self.far_y, self.near_x, self.near_y, self.to_y, self.to_x):
            copy.wait_send()
        done.up = True
        if free is not None:
            self.me.free_in_plane(free)


def params(number, vmem=60 * 2**20):
    return pltpu.CompilerParams(
        collective_id=number, has_side_effects=True, vmem_limit_bytes=vmem
    )


def shape(dims, kind=bf16):
    return jax.ShapeDtypeStruct(dims, kind)


def alone(flops, vmem=60 * 2**20):
    return dict(
        compiler_params=pltpu.CompilerParams(vmem_limit_bytes=vmem),
        cost_estimate=pl.CostEstimate(flops=int(flops), bytes_accessed=2**23, transcendentals=0),
    )


def gain_row(gains, which):
    return jnp.concatenate([gains[i * 8 + which : i * 8 + which + 1, :] for i in range(8)], axis=1)


def rotate_heads(values, cos, sin, inverse=False):
    out = []
    for h in range(values.shape[0] // HD):
        a = values[h * HD : h * HD + HD // 2]
        b = values[h * HD + HD // 2 : (h + 1) * HD]
        if inverse:
            out += [a * cos + b * sin, b * cos - a * sin]
        else:
            out += [a * cos - b * sin, b * cos + a * sin]
    return jnp.concatenate(out, axis=0)


def block_positions(order_ref, number, stretch_rows):
    row = lax.broadcasted_iota(jnp.int32, (stretch_rows, 128), 0)
    return jnp.concatenate(
        [row + order_ref[number * 2 + i] * stretch_rows for i in range(2)], axis=0
    )


def forward_kernel(
    order_ref, tok, w_query, w_key, w_value, gains, frequency, wo, cot, wg, wu, wd,
    tok_all, wqkv_all, gains_all, wo_all, wd_all, cot_all, kv_all, branch,
    normed_all, q_t_all, q_n_all, out_t_all, attended_all, log_sum, key_pos, query_pos, cos_t, sin_t,
    normed_two, hidden, d_gate, d_up, two_part,
    normed, q_t, q_n, out_t, attended, wqkv, gain_src, toks, wqkvs, wos, kv_own, kv, v_t, att_t, part, total, inbox, across,
    wgs, wus, wds, cots, two, ss, rs
):
    me = Here(ss, rs)
    z = me.z
    heads, hd, rows = q_t.shape
    wide = heads * hd
    keys = kv.shape[0]
    wqkv[:, :wide] = w_query[...]
    for j in range(4):

        @pl.when(z == j)
        def _():
            wqkv[:, wide : wide + hd] = w_key[:, j * hd : (j + 1) * hd]
            wqkv[:, wide + hd :] = w_value[:, j * hd : (j + 1) * hd]

    gain_src[...] = jnp.concatenate([gains[...], jnp.zeros((6, gains.shape[1]), f32)], axis=0)
    me.enter(tuple(range(1, 8)))
    lanes = att_t.shape[1]
    have_tok, have_gains, have_wqkv, have_wo = Flag(), Flag(), Flag(), Flag()
    have_wg, have_wu, have_wd, have_cot = Flag(), Flag(), Flag(), Flag()
    progress = Progress(0)
    order = Order(
        z_gather(me, tok, toks, 11.3, 0.0, have_tok),
        plane_direct(me, gain_src, gains_all, have_gains),
        plane_gather(me, wqkv, wqkvs, 7.0, 0.5, have_wqkv, 0.0),
        plane_gather(me, wo, wos, 6.0, 11.0, have_wo, 7.5),
        plane_gather(me, wg, wgs, 15.5, 20.0, have_wg, 17.0),
        z_gather(me, cot, cots, 11.3, 37.0, have_cot, 27.0),
    )
    c_number = me.x * 2 + me.c
    for i in range(4):
        x = 1 - me.x if i & 2 else me.x
        c = 1 - me.c if i & 1 else me.c
        key_pos[i * rows : (i + 1) * rows, :] = block_positions(order_ref, x * 2 + c, rows // 2)
    lane = lax.broadcasted_iota(jnp.int32, (hd // 2, rows // 2), 1)
    for i in range(2):
        span = slice(i * rows // 2, (i + 1) * rows // 2)
        position = lane + order_ref[c_number * 2 + i] * (rows // 2)
        query_pos[:, span] = position[:8]
        freq = jnp.concatenate([frequency[...]] * (rows // 256), axis=1)
        angle = position.astype(f32) * freq
        cos_t[:, span] = jnp.cos(angle)
        sin_t[:, span] = jnp.sin(angle)
    order.until(have_tok, have_gains, have_wqkv)
    saves = [me.local(toks, tok_all), me.local(wqkvs, wqkv_all)]
    for save in saves:
        save.start()
    gain = gain_row(gains_all, 0)

    def project(i):
        at = pl.ds(pl.multiple_of(i * 128, 128), 128)
        x = toks[at, :].astype(f32)
        inv = lax.rsqrt(jnp.mean(x * x, axis=1, keepdims=True) + norm_epsilon)
        low = (x * inv * gain).astype(bf16)
        normed[at, :] = low
        lin = jnp.dot(low, wqkvs[...], preferred_element_type=f32).T
        cos, sin = cos_t[:, at], sin_t[:, at]
        turned = rotate_heads(lin[: wide + hd], cos, sin)
        query = turned[:wide].astype(bf16) * bf16(1.0 / math.sqrt(hd))
        natural = query.astype(f32).T
        for h in range(heads):
            q_t[h, :, at] = query[h * hd : (h + 1) * hd]
            q_n[h, at, :] = natural[:, h * hd : (h + 1) * hd].astype(bf16)
        kv_own[at, :] = jnp.concatenate([turned[wide:], lin[wide + hd :]], axis=0).T.astype(bf16)

    order.loop(rows // 128, 1.0, project)

    def block(i):
        return kv.at[pl.ds(i * rows, rows)]

    copies = [me.copy(kv_own, block(i), me.plane(i)) for i in (1, 2, 3)]
    own = me.local(kv_own, block(0))
    for copy in (*copies, own):
        copy.start()
    order.pump(order.now + 4.0)
    order.add(plane_gather(me, wu, wus, 15.5, order.now, have_wu))
    order.add(plane_gather(me, wd, wds, 15.5, order.now + 24.0, have_wd, order.now + 14.0))
    own.wait()
    for copy in copies:
        copy.wait_recv()
    save = me.local(kv, kv_all)
    save.start()
    for i in range(keys // rows):
        span = slice(i * rows, (i + 1) * rows)
        v_t[:, span] = kv[span, :].astype(f32).T[hd:, :].astype(bf16)
    order.until(have_wo)
    save_wo = me.local(wos, wo_all)
    save_wo.start()
    for task in z_reduce_all(
        me, part, total, inbox, across, branch, 45.0, 16, progress, order.now, 18.0
    ):
        order.add(task)

    def item(i):
        r, h = i // heads, i % heads
        at = pl.ds(pl.multiple_of(r * lanes, lanes), lanes)
        s = jnp.dot(kv[:, 0:hd], q_t[h, :, at], preferred_element_type=f32)
        pos = jnp.concatenate([key_pos[...]] * (lanes // 128), axis=1)
        s = jnp.where(pos <= query_pos[0:1, at], s, masked_value)
        top = jnp.max(s, axis=0, keepdims=True)
        p = jnp.exp(s - top)
        norm = jnp.sum(p, axis=0, keepdims=True)
        o = jnp.dot(v_t[...], p.astype(bf16), preferred_element_type=f32) / norm
        out_t[h, :, at] = o
        log_sum[h, :, at] = top + jnp.log(norm)
        att_t[pl.ds(pl.multiple_of(h * hd, hd), hd), :] = o

        @pl.when(h == heads - 1)
        def _():
            natural = att_t[...].T.astype(bf16)
            attended[at, :] = natural
            part[at, :] = contract_last_dims(natural, wos[...]).astype(bf16)

    def before(k):
        progress.parts = k // heads * (lanes // 32)
        return False

    order.loop(heads * rows // lanes, 1.2, item, before)
    progress.parts = 16
    early = ((normed, normed_all), (q_t, q_t_all), (q_n, q_n_all), (out_t, out_t_all), (attended, attended_all))
    early = [me.local(*pair) for pair in early]
    for copy in early:
        copy.start()
    late = [me.local(wds, wd_all), me.local(cots, cot_all)]
    order.until(have_wg, have_wu, have_wd, have_cot)
    for copy in late:
        copy.start()
    gain_mlp = gain_row(gains_all, 1)
    half = rows // 2

    def norm_two(first):
        def body(i, _):
            at = pl.ds(pl.multiple_of(first + i * 64, 64), 64)
            h = toks[at, :].astype(f32) + total[at, :].astype(f32)
            inv = lax.rsqrt(jnp.mean(h * h, axis=1, keepdims=True) + norm_epsilon)
            normed_two[at, :] = (h * inv * gain_mlp).astype(bf16)
            return 0

        lax.fori_loop(0, half // 64, body, 0)

    def feed(at, span):
        gate = jnp.dot(normed_two[at, :], wgs[:, span], preferred_element_type=f32)
        up = jnp.dot(normed_two[at, :], wus[:, span], preferred_element_type=f32)
        grad = jnp.dot(cots[at, :], wds[:, span], preferred_element_type=f32)
        sigmoid = jax.nn.sigmoid(gate)
        silu = gate * sigmoid
        hidden[at, span] = (silu * up).astype(bf16)
        grad_gate = (grad * up * sigmoid * (1.0 + gate * (1.0 - sigmoid))).astype(bf16)
        grad_up = (grad * silu).astype(bf16)
        d_gate[at, span] = grad_gate
        d_up[at, span] = grad_up
        return contract_last_dims(grad_gate, wgs[:, span]) + contract_last_dims(grad_up, wus[:, span])

    def feed_item(j):
        @pl.when(j == 0)
        def _():
            norm_two(0)
            two[...] = jnp.zeros_like(two)

        two[...] += feed(slice(0, half), pl.ds(pl.multiple_of(j * 128, 128), 128))

    order.loop(hidden.shape[1] // 128, 1.8, feed_item, lambda k: progress.whole() < 8)
    two_part[:half, :] = two[...].astype(bf16)
    while progress.whole() < 16:
        order.step()
    norm_two(half)
    two_part[half:, :] = feed(slice(half, rows), slice(None)).astype(bf16)
    order.finish()
    for copy in copies:
        copy.wait_send()
    for copy in (save, save_wo, *saves, *early, *late):
        copy.wait()


def forward(stretch_order, tok, w_query, w_key, w_value, gains, frequency, wo, cot, wg, wu, wd):
    rows = tok.shape[0] * 4
    width = tok.shape[1]
    heads = w_query.shape[1] // HD
    keys = rows * 4
    qkv = (w_query.shape[0], w_query.shape[1] + 2 * HD)

    def grown(a, n=8):
        return shape((a.shape[0] * n,) + a.shape[1:], a.dtype)

    def room(a):
        return pltpu.VMEM(a.shape, a.dtype)

    gain_block = shape((8, gains.shape[1]), f32)
    wqkv = shape(qkv)
    block = shape((rows, width))
    units = shape((rows, wg.shape[1]))
    return pl.pallas_call(
        forward_kernel,
        out_shape=(
            block, grown(wqkv), grown(gain_block), grown(wo), grown(wd), block,
            shape((keys, 2 * HD)), block,
            block,
            shape((heads, HD, rows)),
            shape((heads, rows, HD)),
            shape((heads, HD, rows), f32),
            shape((rows, heads * HD)),
            shape((heads, 1, rows), f32),
            shape((keys, 128), jnp.int32),
            shape((8, rows), jnp.int32),
            shape((HD // 2, rows), f32),
            shape((HD // 2, rows), f32),
            block, units, units, units, block,
        ),
        in_specs=[pl.BlockSpec(memory_space=pltpu.SMEM)] + [VM] * 7 + [HB] * 4,
        out_specs=[HB, HB, VM] + [HB] * 10 + [VM] * 10,
        scratch_shapes=[
            room(block),
            pltpu.VMEM((heads, HD, rows), bf16),
            pltpu.VMEM((heads, rows, HD), bf16),
            pltpu.VMEM((heads, HD, rows), f32),
            pltpu.VMEM((rows, heads * HD), bf16),
            room(wqkv), room(gain_block), room(block), room(grown(wqkv)), room(grown(wo)),
            pltpu.VMEM((rows, 2 * HD), bf16),
            pltpu.VMEM((keys, 2 * HD), bf16),
            pltpu.VMEM((HD, keys), bf16),
            pltpu.VMEM((heads * HD, 256), f32),
            room(block), room(block), room(block), room(block),
            room(grown(wg)), room(grown(wu)), room(grown(wd)), room(block), pltpu.VMEM((rows // 2, width), f32),
        ] + dma_sems(224),
        compiler_params=params(1, 67043328),
        name="forward",
    )(stretch_order, tok, w_query, w_key, w_value, gains, frequency, wo, cot, wg, wu, wd)


def contract_rows(left, right):
    return lax.dot_general(left, right, (((0,), (0,)), ((), ())), preferred_element_type=f32)


def contract_last_dims(left, right):
    return lax.dot_general(left, right, (((1,), (1,)), ((), ())), preferred_element_type=f32)


def gain_sums(me, src, out, came, mine, came_z):
    def block(i):
        return pl.ds(pl.multiple_of(me.number(i) * 8, 8), 8)

    own = block(0)
    copies = [me.copy(src.at[block(i)], came.at[i - 1], me.plane(i)) for i in range(1, 8)]
    again = [
        me.copy(mine, came_z.at[d - 1], {"head": (me.z + d) % 4}) for d in (1, 2, 3)
    ]

    def steps(begin):
        for copy in copies:
            copy.start()
        yield begin + 6.0
        value = src[own, :]
        for i, copy in enumerate(copies):
            copy.wait_recv()
            value = value + came[i]
        mine[...] = value
        for copy in again:
            copy.start()
        yield begin + 35.0
        value = mine[...]
        for d, copy in enumerate(again):
            copy.wait_recv()
            value = value + came_z[d]
        out[...] = value
        for copy in copies + again:
            copy.wait_send()

    return steps


def backward_kernel(
    part, cot_all, hidden, normed_two, d_gate, d_up, wd_all, tok_all, branch, gains, wo_all,
    out_t_all, attended_all, q_t_all, q_n_all, kv_all, wqkv_all, normed_all, log_sum, key_pos, query_pos, cos_t, sin_t,
    dwd_own, dwg_own, dwu_own, dw_own, dwkv_all, out_own, own, grad_one, gains_out,
    total, inbox, across, cot, out_part, below, above, q_t, q_n, kv, k_t, came, dq_t,
    gain_two, gain_parts, came_gain, gain_mine, gain_z, dwkv_own, came_kv, *rest
):
    scratch_d, scratch_g = rest[:6], rest[6:12]
    free_d, free_g, free_z, ss, rs = rest[12:]
    me = Here(ss, rs)
    me.enter(tuple(range(1, 8)), all_z=True)
    z = me.z
    rows, width = part.shape
    heads, hd, _ = q_t.shape
    wide = heads * hd
    lin_cols = wide + 2 * hd
    keys = kv.shape[0]
    cols = width // 8
    progress = Progress(16)
    order = Order(*z_reduce_all(me, part, total, inbox, across, None, 45.0, 16, progress))
    down, gate = PlaneScatter(me, scratch_d), PlaneScatter(me, scratch_g)
    up = PlaneScatter(me, scratch_d)
    narrow = [ref.at[(slice(None),) * (len(ref.shape) - 1) + (pl.ds(0, lin_cols + wide),)] for ref in scratch_g]
    both = PlaneScatter(me, narrow)
    down_done, gate_done, up_done, both_done, out_done, one_done = (Flag() for _ in range(6))
    cot_load = me.local(cot_all, cot)
    cot_load.start()
    later = [me.local(src, dst) for src, dst in ((kv_all, kv), (q_t_all, q_t), (q_n_all, q_n))]
    stores = [me.slot() for _ in range(5)]
    back = [
        me.copy(kv.at[pl.ds(i * rows, rows)], came.at[i - 1], me.plane(i)) for i in (1, 2, 3)
    ]
    kv_sends = [
        me.copy(dwkv_own, came_kv.at[d - 1], {"head": (z + d) % 4}) for d in (1, 2, 3)
    ]

    gains_steps = gain_sums(me, gain_parts, gains_out, came_gain, gain_mine, gain_z)

    def columns(j):
        return pl.ds(pl.multiple_of(offsets_of(me, j) * cols, cols), cols)

    def send(scatter, j):
        for k in range(4):

            @pl.when(j == k)
            def _():
                scatter.core[k].start()

    def weights(left, right_h, right_g, wd):
        pairs = ((hidden, right_h), (normed_two, left), (d_gate, right_g))
        loads = [me.local(src, dst) for src, dst in pairs]
        for load in loads:
            load.start()
        for load in later:
            load.start()
        cot_load.wait()
        loads[0].wait()
        order.pump(2.0)

        def down_item(j):
            down.blocks[j] = contract_rows(cot[:, columns(j)], right_h[...]).astype(bf16)
            send(down, j)

        order.loop(8, 0.65, down_item)
        order.add(down.steps(dwd_own, 16.5, order.now + 0.1, down_done, free_d))
        loads[1].wait()
        loads[2].wait()

        def gate_item(j):
            gate.blocks[j] = contract_rows(left[:, columns(j)], right_g[...]).astype(bf16)
            send(gate, j)

        order.loop(8, 0.75, gate_item)
        order.add(gate.steps(dwg_own, 16.5, order.now + 19.0, gate_done, free_g))

        def fetch(j):
            at = pl.ds(pl.multiple_of(j * cols, cols), cols)
            return pltpu.make_async_copy(wd_all.at[at], wd.at[j % 2], ss.at[stores[1]])

        fetch(0).start()

        def out_item(j):
            fetch(j).wait()

            @pl.when(j < 7)
            def _():
                fetch(j + 1).start()

            at = pl.ds(pl.multiple_of(j * cols, cols), cols)
            out_part[:, at] = contract_last_dims(right_h[...], wd[j % 2]).astype(bf16)

        order.loop(8, 1.2, out_item)

    units = pltpu.VMEM(hidden.shape, bf16)
    weight = pltpu.VMEM((2, cols, hidden.shape[1]), bf16)
    pl.run_scoped(weights, pltpu.VMEM(part.shape, bf16), units, units, weight)

    def attention(tok, summed, wo, out_t, attended, g_t, g_n, delta, dk, dv):
        gain = gain_row(gains, 1)

        def fetch(r):
            at = pl.ds(pl.multiple_of(r * 128, 128), 128)
            return (
                pltpu.make_async_copy(tok_all.at[at], tok, ss.at[stores[2]]),
                pltpu.make_async_copy(branch.at[at], summed, ss.at[stores[3]]),
            )

        for copy in fetch(0):
            copy.start()
        loads = [
            me.local(src, dst)
            for src, dst in ((wo_all, wo), (out_t_all, out_t), (attended_all, attended))
        ]
        for load in loads:
            load.start()
        dk[...] = jnp.zeros_like(dk)
        dv[...] = jnp.zeros_like(dv)
        for load in later:
            load.wait()
        for i in range(keys // rows):
            span = slice(i * rows, (i + 1) * rows)
            k_t[:, span] = kv[span, :].astype(f32).T[:hd, :].astype(bf16)
        for load in loads:
            load.wait()
        order.add(z_reduce_scatter(me, out_part, below, above, out_own, 12.0, 42.0, out_done), 42.0)

        def prepare(r):
            for copy in fetch(r):
                copy.wait()
            at = pl.ds(pl.multiple_of(r * 128, 128), 128)
            h = tok[...].astype(f32) + summed[...].astype(f32)
            e = total[at, :].astype(f32)
            inv = lax.rsqrt(jnp.mean(h * h, axis=1, keepdims=True) + norm_epsilon)
            u = e * gain
            inner = jnp.mean(u * h, axis=1, keepdims=True)
            grad = cot[at, :].astype(f32) + (inv * u - h * (inv * inv * inv * inner))

            @pl.when(r == z)
            def _():
                own[...] = grad
                gain_two[...] = jnp.broadcast_to(jnp.sum(e * h * inv, axis=0, keepdims=True), gain_two.shape)

            small = grad.astype(bf16)
            cot[at, :] = small
            g = jnp.dot(small, wo[...], preferred_element_type=f32).astype(bf16)
            turned = g.astype(f32).T
            for head in range(heads):
                g_n[head] = g[:, head * hd : (head + 1) * hd]
                mine = turned[head * hd : (head + 1) * hd]
                g_t[head] = mine.astype(bf16)
                delta[head] = jnp.sum(mine * out_t[head, :, at], axis=0, keepdims=True)

            @pl.when(r < rows // 128 - 1)
            def _():
                for copy in fetch(r + 1):
                    copy.start()

        def item(i):
            r, h = i // heads, i % heads

            @pl.when(h == 0)
            def _():
                prepare(r)

            at = pl.ds(pl.multiple_of(r * 128, 128), 128)
            s = jnp.dot(kv[:, 0:hd], q_t[h, :, at], preferred_element_type=f32)
            s = jnp.where(key_pos[...] <= query_pos[0:1, at], s, masked_value)
            p = jnp.exp(s - log_sum[h, :, at])
            dp = jnp.dot(kv[:, hd:], g_t[h], preferred_element_type=f32)
            ds = (p * (dp - delta[h])).astype(bf16)
            dv[...] += jnp.dot(p.astype(bf16), g_n[h], preferred_element_type=f32)
            dk[...] += jnp.dot(ds, q_n[h, at, :], preferred_element_type=f32)
            grad = jnp.dot(k_t[...], ds, preferred_element_type=f32)
            dq_t[h, :, at] = (grad * (1.0 / math.sqrt(hd))).astype(bf16)

        def before(k):
            return progress.whole() < (k // heads + 1) * 4

        order.loop(heads * rows // 128, 1.25, item, before)
        for i in range(keys // rows):
            span = slice(i * rows, (i + 1) * rows)
            kv[span, :] = jnp.concatenate([dk[span, :], dv[span, :]], axis=1).astype(bf16)
        for copy in back:
            copy.start()
        order.until(gate_done)
        pl.semaphore_wait(free_g, 3)

        def low_item(j):
            both.blocks[j, :, lin_cols:] = contract_rows(cot[:, columns(j)], attended[...]).astype(bf16)

        order.loop(8, 0.4, low_item)

    slots = pltpu.VMEM((128, width), bf16)
    pl.run_scoped(
        attention,
        slots,
        slots,
        pltpu.VMEM(wo_all.shape, bf16),
        pltpu.VMEM(out_t_all.shape, f32),
        pltpu.VMEM(attended_all.shape, bf16),
        pltpu.VMEM((heads, hd, 128), bf16),
        pltpu.VMEM((heads, 128, hd), bf16),
        pltpu.VMEM((heads, 1, 128), f32),
        pltpu.VMEM((keys, hd), f32),
        pltpu.VMEM((keys, hd), f32),
    )

    def last(left, right_u, wqkv, normed, lin, gain_one):
        tok = cot
        pairs = ((wqkv_all, wqkv), (normed_two, left), (d_up, right_u), (normed_all, normed), (tok_all, tok))
        loads = [me.local(src, dst) for src, dst in pairs]
        for load in loads:
            load.start()
        gain_one[...] = jnp.zeros_like(gain_one)
        order.until(progress.sent_in, progress.sent_out, down_done)
        pl.semaphore_wait(free_d, 3)
        loads[1].wait()
        loads[2].wait()

        def up_item(j):
            up.blocks[j] = contract_rows(left[:, columns(j)], right_u[...]).astype(bf16)
            send(up, j)

        order.loop(8, 0.75, up_item)
        order.add(up.steps(dwu_own, 16.5, order.now + 0.1, up_done))
        for copy in back:
            copy.wait_recv()
        mine = kv[0:rows, :].astype(f32)
        for i in range(keys // rows - 1):
            mine = mine + came[i].astype(f32)
        for copy in back:
            copy.wait_send()
        kv[0:rows, :] = mine.astype(bf16)
        for load in (loads[0], loads[3], loads[4]):
            load.wait()

        def finish_item(i):
            at = pl.ds(pl.multiple_of(i * 128, 128), 128)
            grads_kv = kv[at, :].astype(f32).T
            grads = jnp.concatenate(
                [dq_t[h, :, at].astype(f32) for h in range(heads)] + [grads_kv[:hd]], axis=0
            )
            grads = rotate_heads(grads, cos_t[:, at], sin_t[:, at], inverse=True)
            natural = jnp.concatenate([grads, grads_kv[hd:]], axis=0).T.astype(bf16)
            lin[at, :] = natural
            one = contract_last_dims(natural, wqkv[...])
            total[at, :] = one.astype(bf16)
            x = tok[at, :].astype(f32)
            inv = lax.rsqrt(jnp.mean(x * x, axis=1, keepdims=True) + norm_epsilon)
            gain_one[0:1, :] += jnp.sum(one * x * inv, axis=0, keepdims=True)

        order.loop(rows // 128, 2.0, finish_item)
        for i in range(8):
            span = slice(i * cols, (i + 1) * cols)
            gain_parts[i * 8 : (i + 1) * 8, :] = jnp.concatenate(
                [gain_one[0:1, span], gain_two[0:1, span], jnp.zeros((6, cols), f32)], axis=0
            )
        order.until(out_done)
        me.free_along_z(free_z)
        order.add(gains_steps(order.now))
        order.step()
        me.wait_along_z(free_z)
        order.add(z_reduce_scatter(me, total, below, above, grad_one, 12.0, order.now, one_done), order.now)

        def both_item(j):
            both.blocks[j, :, :lin_cols] = contract_rows(normed[:, columns(j)], lin[...]).astype(bf16)
            send(both, j)

        order.loop(8, 0.5, both_item)
        order.add(both.steps(dw_own, 13.0, order.now + 0.1, both_done))

    pl.run_scoped(
        last,
        pltpu.VMEM(part.shape, bf16),
        units,
        pltpu.VMEM(wqkv_all.shape, bf16),
        pltpu.VMEM(part.shape, bf16),
        pltpu.VMEM((rows, lin_cols), bf16),
        pltpu.VMEM((8, width), f32),
    )
    order.until(both_done)
    dwkv_own[...] = dw_own[:, wide:lin_cols].astype(bf16)
    for copy in kv_sends:
        copy.start()
    order.finish()
    for copy in kv_sends:
        copy.wait_recv()
    dwkv_all[0] = dwkv_own[...]
    for d in (1, 2, 3):
        dwkv_all[d] = came_kv[d - 1]
    for copy in kv_sends:
        copy.wait_send()


def backward(
    part, cot_all, hidden, normed_two, d_gate, d_up, wd_all, tok_all, branch, gains, wo_all,
    out_t, attended, q_t, q_n, kv_all, wqkv_all, normed, log_sum, key_pos, query_pos, cos_t, sin_t
):
    heads, hd, rows = q_t.shape
    keys = key_pos.shape[0]
    width = part.shape[1]
    cols = width // 8
    whole = pltpu.VMEM(part.shape, bf16)
    own = (wd_all.shape[0] // 8, wd_all.shape[1])
    narrow = wqkv_all.shape[1] + wo_all.shape[1]
    return pl.pallas_call(
        backward_kernel,
        out_shape=(
            shape(own),
            shape(own),
            shape(own),
            shape((own[0], narrow), f32),
            shape((4, own[0], 2 * hd)),
            shape((rows // 4, width), f32),
            shape((rows // 4, width), f32),
            shape((rows // 4, width), f32),
            shape((8, cols), f32),
        ),
        in_specs=[VM] + [HB] * 8 + [VM] + [HB] * 8 + [VM] * 5,
        out_specs=[VM] * 9,
        scratch_shapes=[whole] * 7
        + [
            pltpu.VMEM(q_t.shape, bf16),
            pltpu.VMEM(q_n.shape, bf16),
            pltpu.VMEM((keys, 2 * hd), bf16),
            pltpu.VMEM((hd, keys), bf16),
            pltpu.VMEM((keys // rows - 1, rows, 2 * hd), bf16),
            pltpu.VMEM(q_t.shape, bf16),
            pltpu.VMEM((8, width), f32),
            pltpu.VMEM((64, cols), f32),
            pltpu.VMEM((7, 8, cols), f32),
            pltpu.VMEM((8, cols), f32),
            pltpu.VMEM((3, 8, cols), f32),
            pltpu.VMEM((own[0], 2 * hd), bf16),
            pltpu.VMEM((3, own[0], 2 * hd), bf16),
        ]
        + plane_scatter_scratch(*own) * 2
        + [pltpu.SemaphoreType.REGULAR] * 3
        + dma_sems(224),
        compiler_params=params(4, 67043328),
        name="backward",
    )(
        part, cot_all, hidden, normed_two, d_gate, d_up, wd_all, tok_all, branch, gains, wo_all,
        out_t, attended, q_t, q_n, kv_all, wqkv_all, normed, log_sum, key_pos, query_pos, cos_t, sin_t
    )


def local_fast(
    tokens, w_query, w_key, w_value, w_out, w_gate, w_up, w_down, gain_attn, gain_mlp, stretch_order, cotangent
):
    row_count, width = tokens.shape
    groups = 4
    cols = width // 8
    contract_last = (((1,), (1,)), ((), ()))
    z = lax.axis_index("head")
    own_first = z * row_count

    def own_rows(values):
        return lax.dynamic_slice_in_dim(values, own_first, row_count, 0)

    frequency = rope_base ** (-(np.arange(HD // 2, dtype=np.float32) * np.float32(2.0 / HD)))
    frequency = jnp.asarray(np.broadcast_to(frequency.astype(np.float32)[:, None], (HD // 2, 128)))
    gains = jnp.concatenate([gain_attn[None], gain_mlp[None]]).astype(f32)
    (
        tok_all, wqkv_all, gains_all, wo_all, wd_all, cot_all, kv_all, branch,
        normed, q_t, q_n, out_t, attended, log_sum, key_pos, query_pos, cos_t, sin_t,
        normed_two, hidden, d_gate, d_up, two_part,
    ) = forward(
        stretch_order, tokens, w_query, w_key, w_value, gains, frequency, w_out, cotangent, w_gate, w_up, w_down
    )
    gain_rows = gains_all.reshape(8, 8, cols)
    gain_one = gain_rows[:, 0].reshape(width)
    dwd_own, dwg_own, dwu_own, dw_own, dwkv_all, out_own, grad_hidden_own, grad_one, gain_grads = backward(
        two_part, cot_all, hidden, normed_two, d_gate, d_up, wd_all, tok_all, branch,
        gains_all, wo_all, out_t, attended, q_t, q_n, kv_all, wqkv_all, normed, log_sum, key_pos, query_pos,
        cos_t, sin_t,
    )

    x_own = tokens.astype(f32)
    layer_low = (x_own + own_rows(branch).astype(f32) + out_own).astype(bf16)
    inv_own = lax.rsqrt(jnp.mean(x_own * x_own, axis=-1, keepdims=True) + norm_epsilon)
    grad_tokens = (grad_hidden_own + norm_input_grad(x_own, inv_own, gain_one, grad_one)).astype(bf16)
    slots = jnp.concatenate(
        [lax.dynamic_slice_in_dim(dwkv_all, (z - j) % 4, 1, 0) for j in range(4)], axis=0
    ).astype(f32)
    grad_key = slots[:, :, :HD].transpose(1, 0, 2).reshape(cols, groups * HD)
    grad_value = slots[:, :, HD:].transpose(1, 0, 2).reshape(cols, groups * HD)
    return (
        layer_low,
        grad_tokens,
        dw_own[:, : w_query.shape[1]],
        grad_key,
        grad_value,
        dw_own[:, w_query.shape[1] + 2 * HD :],
        dwg_own.astype(f32),
        dwu_own.astype(f32),
        dwd_own.astype(f32),
        gain_grads[0],
        gain_grads[1],
    )


def solution(mesh):
    sizes = (mesh.shape["fsdp"], mesh.shape["blk"], mesh.shape["head"])
    return jax.shard_map(
        local_fast if sizes == (2, 4, 4) else local,
        mesh=mesh,
        in_specs=(
            P(("fsdp", "blk", "head"), None),
            P(("fsdp", "blk"), "head"),
            P(("fsdp", "blk"), None),
            P(("fsdp", "blk"), None),
            P(("fsdp", "blk"), "head"),
            P(("fsdp", "blk"), "head"),
            P(("fsdp", "blk"), "head"),
            P(("fsdp", "blk"), "head"),
            P(("fsdp", "blk")),
            P(("fsdp", "blk")),
            P(),
            P(("fsdp", "blk", "head"), None),
        ),
        out_specs=(
            P(("fsdp", "blk", "head"), None),
            P(("fsdp", "blk", "head"), None),
            P(("fsdp", "blk"), "head"),
            P(("fsdp", "blk"), None),
            P(("fsdp", "blk"), None),
            P(("fsdp", "blk"), "head"),
            P(("fsdp", "blk"), "head"),
            P(("fsdp", "blk"), "head"),
            P(("fsdp", "blk"), "head"),
            P(("fsdp", "blk")),
            P(("fsdp", "blk")),
        ),
        check_vma=False,
    )
```

```python
import math

import jax
import jax.numpy as jnp
import numpy as np
from jax import lax
from jax.experimental import pallas as pl
from jax.experimental.pallas import tpu as pltpu
from jax.sharding import PartitionSpec as P

H = 32
KV = 4
HD = 64


norm_epsilon = 1e-05
rope_base = 10000.0
masked_value = -1e30


def rope_tables(positions, head_dim):
    half_dim = head_dim // 2
    frequency = rope_base ** (-(jnp.arange(half_dim, dtype=jnp.float32) * (2.0 / head_dim)))
    angles = positions.astype(jnp.float32)[:, None] * frequency[None, :]
    return (jnp.cos(angles), jnp.sin(angles))


def rotate(values, cosine, sine_table):
    half_dim = values.shape[-1] // 2
    first_half = values[..., :half_dim]
    second_half = values[..., half_dim:]
    cos_rows = cosine[:, None, :]
    sin_rows = sine_table[:, None, :]
    return jnp.concatenate(
        [
            first_half * cos_rows - second_half * sin_rows,
            second_half * cos_rows + first_half * sin_rows,
        ],
        axis=-1,
    )


def unrotate(values, cosine, sine_table):
    half_dim = values.shape[-1] // 2
    first_half = values[..., :half_dim]
    second_half = values[..., half_dim:]
    cos_rows = cosine[:, None, :]
    sin_rows = sine_table[:, None, :]
    return jnp.concatenate(
        [
            first_half * cos_rows + second_half * sin_rows,
            second_half * cos_rows - first_half * sin_rows,
        ],
        axis=-1,
    )


def stretch_positions(stretch_order, first_row, row_span, stretch_rows):
    storage = first_row + jnp.arange(row_span, dtype=jnp.int32)
    stretch_index = storage // stretch_rows
    match_table = (
        stretch_index[:, None] == jnp.arange(stretch_order.shape[0], dtype=jnp.int32)[None, :]
    )
    stretch_base = jnp.sum(jnp.where(match_table, stretch_order[None, :], 0), axis=1)
    return stretch_base * stretch_rows + storage % stretch_rows


def norm_input_grad(values, inverse, gain_vector, grad_normed):
    scaled = grad_normed * gain_vector
    inner = jnp.mean(scaled * values, axis=-1, keepdims=True)
    return inverse * scaled - values * inverse * inverse * inverse * inner


def gain_grad(values, inverse, grad_normed):
    return jnp.sum(grad_normed * values * inverse, axis=0)


def fold_block(
    state_now, keys_block, values_block, key_positions, query_heads, query_positions, score_scale
):
    running_max, running_sum, running_out = state_now
    scores = (
        jnp.einsum("qhd,kd->hqk", query_heads, keys_block, preferred_element_type=jnp.float32)
        * score_scale
    )
    allowed = (query_positions[:, None] >= key_positions[None, :])[None]
    scores = jnp.where(allowed, scores, masked_value)
    new_max = jnp.maximum(running_max, jnp.max(scores, axis=-1))
    weights = jnp.where(allowed, jnp.exp(scores - new_max[..., None]), 0.0)
    factor = jnp.exp(running_max - new_max)
    running_sum = running_sum * factor + jnp.sum(weights, axis=-1)
    running_out = running_out * factor[..., None] + jnp.einsum(
        "hqk,kd->hqd",
        weights.astype(jnp.bfloat16),
        values_block,
        preferred_element_type=jnp.float32,
    )
    return (new_max, running_sum, running_out)


def local(
    tokens,
    w_query,
    w_key,
    w_value,
    w_out,
    w_gate,
    w_up,
    w_down,
    gain_attn,
    gain_mlp,
    stretch_order,
    cotangent,
):
    row_count = tokens.shape[0]
    groups = lax.axis_size("head")
    blocks = lax.axis_size("blk")
    local_heads = H // groups
    repeats = groups // KV
    head_rows = row_count * groups
    stretch_rows = head_rows // 2
    score_scale = 1.0 / math.sqrt(HD)
    contract_last = (((1,), (1,)), ((), ()))
    contract_first = (((0,), (0,)), ((), ()))
    head_index = lax.axis_index("head")
    own_first = head_index * row_count
    block_first = lax.axis_index("blk") * head_rows
    positions = stretch_positions(stretch_order, block_first + own_first, row_count, stretch_rows)
    query_positions = stretch_positions(stretch_order, block_first, head_rows, stretch_rows)
    cos_own, sin_own = rope_tables(positions, HD)
    cos_block, sin_block = rope_tables(query_positions, HD)

    def layer_weights():
        return (
            lax.all_gather(w_query, ("fsdp", "blk"), axis=0, tiled=True),
            lax.all_gather(w_key, ("fsdp", "blk"), axis=0, tiled=True),
            lax.all_gather(w_value, ("fsdp", "blk"), axis=0, tiled=True),
            lax.all_gather(w_out, ("fsdp", "blk"), axis=0, tiled=True),
            lax.all_gather(w_gate, ("fsdp", "blk"), axis=0, tiled=True),
            lax.all_gather(w_up, ("fsdp", "blk"), axis=0, tiled=True),
            lax.all_gather(w_down, ("fsdp", "blk"), axis=0, tiled=True),
            lax.all_gather(gain_attn, ("fsdp", "blk"), axis=0, tiled=True),
            lax.all_gather(gain_mlp, ("fsdp", "blk"), axis=0, tiled=True),
        )

    def gather_query(columns):
        return lax.all_gather(columns, "head", axis=1, tiled=True)

    (
        query_cols,
        key_full,
        value_full,
        out_cols,
        gate_cols,
        up_cols,
        down_cols,
        gain_one,
        gain_two,
    ) = layer_weights()
    tokens_float = tokens.astype(jnp.float32)
    inv_attn = lax.rsqrt(
        jnp.mean(tokens_float * tokens_float, axis=-1, keepdims=True) + norm_epsilon
    )
    normed = (tokens_float * inv_attn * gain_one.astype(jnp.float32)).astype(jnp.bfloat16)
    normed_rows, cotangent_rows = (
        lax.all_gather(normed, "head", axis=0, tiled=True),
        lax.all_gather(cotangent, "head", axis=0, tiled=True),
    )
    query_all = gather_query(query_cols)
    query_lin = jnp.dot(normed, query_all, preferred_element_type=jnp.float32).reshape(
        row_count, H, HD
    )
    key_lin = jnp.dot(normed, key_full, preferred_element_type=jnp.float32).reshape(
        row_count, KV, HD
    )
    value_lin = jnp.dot(normed, value_full, preferred_element_type=jnp.float32).reshape(
        row_count, KV, HD
    )
    query_rot = rotate(query_lin, cos_own, sin_own).astype(jnp.bfloat16).reshape(row_count, H * HD)
    key_rot = rotate(key_lin, cos_own, sin_own).astype(jnp.bfloat16)
    key_slots = jnp.repeat(key_rot, repeats, axis=1).reshape(row_count, groups * HD)
    value_slots = jnp.repeat(value_lin.astype(jnp.bfloat16), repeats, axis=1).reshape(
        row_count, groups * HD
    )
    query_recv, key_own, value_own = (
        lax.all_to_all(query_rot, "head", split_axis=1, concat_axis=0, tiled=True),
        lax.all_to_all(key_slots, "head", split_axis=1, concat_axis=0, tiled=True),
        lax.all_to_all(value_slots, "head", split_axis=1, concat_axis=0, tiled=True),
    )
    query_heads = query_recv.reshape(head_rows, local_heads, HD)
    initial = (
        jnp.full((local_heads, head_rows), masked_value, jnp.float32),
        jnp.zeros((local_heads, head_rows), jnp.float32),
        jnp.zeros((local_heads, head_rows, HD), jnp.float32),
    )
    state_now = initial
    keys_piece = lax.all_gather(key_own, "blk", axis=0, tiled=True)
    values_piece = lax.all_gather(value_own, "blk", axis=0, tiled=True)
    piece_rows = keys_piece.shape[0]

    def scan_step(state_inner, step_index):
        offset = step_index * head_rows
        keys_block = lax.dynamic_slice_in_dim(keys_piece, offset, head_rows, 0)
        values_block = lax.dynamic_slice_in_dim(values_piece, offset, head_rows, 0)
        key_positions = stretch_positions(stretch_order, offset, head_rows, stretch_rows)
        return (
            fold_block(
                state_inner,
                keys_block,
                values_block,
                key_positions,
                query_heads,
                query_positions,
                score_scale,
            ),
            None,
        )

    state_now, unused = lax.scan(
        scan_step, state_now, jnp.arange(piece_rows // head_rows, dtype=jnp.int32)
    )
    running_max, running_sum, running_out = state_now
    attended_float = running_out / running_sum[..., None]
    log_sum = running_max + jnp.log(running_sum)
    attended_heads = (
        attended_float.astype(jnp.bfloat16).transpose(1, 0, 2).reshape(head_rows, local_heads * HD)
    )
    branch = lax.dot_general(
        attended_heads, out_cols, contract_last, preferred_element_type=jnp.float32
    )
    own_branch = lax.dynamic_slice_in_dim(branch, own_first, row_count, 0)
    partial_value = lax.dynamic_update_slice_in_dim(branch, own_branch + tokens_float, own_first, 0)
    hidden_rows = lax.psum(partial_value.astype(jnp.bfloat16), "head").astype(jnp.float32)
    inv_mlp = lax.rsqrt(jnp.mean(hidden_rows * hidden_rows, axis=-1, keepdims=True) + norm_epsilon)
    normed_two_rows = (hidden_rows * inv_mlp * gain_two.astype(jnp.float32)).astype(jnp.bfloat16)
    gate_proj = jnp.dot(normed_two_rows, gate_cols, preferred_element_type=jnp.float32)
    up_proj = jnp.dot(normed_two_rows, up_cols, preferred_element_type=jnp.float32)
    gate_sigmoid = jax.nn.sigmoid(gate_proj)
    gate_silu = gate_proj * gate_sigmoid
    hidden = (gate_silu * up_proj).astype(jnp.bfloat16)
    hidden_own = lax.dynamic_slice_in_dim(hidden_rows, own_first, row_count, 0)
    output_float = hidden_own + lax.psum_scatter(
        lax.dot_general(
            hidden, down_cols, contract_last, preferred_element_type=jnp.float32
        ).astype(jnp.bfloat16),
        "head",
        scatter_dimension=0,
        tiled=True,
    ).astype(jnp.float32)
    layer_low = output_float.astype(jnp.bfloat16)
    (
        query_cols,
        key_full,
        value_full,
        out_cols,
        gate_cols,
        up_cols,
        down_cols,
        gain_one,
        gain_two,
    ) = layer_weights()
    query_all = gather_query(query_cols)
    grad_hidden = jnp.dot(cotangent_rows, down_cols, preferred_element_type=jnp.float32)
    grad_gate_rows = (
        grad_hidden * up_proj * gate_sigmoid * (1.0 + gate_proj * (1.0 - gate_sigmoid))
    ).astype(jnp.bfloat16)
    grad_up_rows = (grad_hidden * gate_silu).astype(jnp.bfloat16)
    grad_w_down = lax.dot_general(
        cotangent_rows, hidden, contract_first, preferred_element_type=jnp.float32
    )
    grad_w_gate = lax.dot_general(
        normed_two_rows, grad_gate_rows, contract_first, preferred_element_type=jnp.float32
    )
    grad_w_up = lax.dot_general(
        normed_two_rows, grad_up_rows, contract_first, preferred_element_type=jnp.float32
    )
    normed_two_part = lax.dot_general(
        grad_gate_rows, gate_cols, contract_last, preferred_element_type=jnp.float32
    )
    normed_two_part = normed_two_part + lax.dot_general(
        grad_up_rows, up_cols, contract_last, preferred_element_type=jnp.float32
    )
    grad_normed_two = lax.psum(normed_two_part.astype(jnp.bfloat16), "head").astype(jnp.float32)
    gain_two_float = gain_two.astype(jnp.float32)
    grad_hidden_rows = cotangent_rows.astype(jnp.float32) + norm_input_grad(
        hidden_rows, inv_mlp, gain_two_float, grad_normed_two
    )
    own_grad_two = lax.dynamic_slice_in_dim(grad_normed_two, own_first, row_count, 0)
    own_inv_mlp = lax.dynamic_slice_in_dim(inv_mlp, own_first, row_count, 0)
    grad_gain_two = gain_grad(hidden_own, own_inv_mlp, own_grad_two)
    grad_low_rows = grad_hidden_rows.astype(jnp.bfloat16)
    grad_w_out = lax.dot_general(
        grad_low_rows, attended_heads, contract_first, preferred_element_type=jnp.float32
    )
    grad_heads = (
        jnp.dot(grad_low_rows, out_cols, preferred_element_type=jnp.float32)
        .astype(jnp.bfloat16)
        .reshape(head_rows, local_heads, HD)
    )
    keys_all, values_all = (
        lax.all_gather(key_own, "blk", axis=0, tiled=True),
        lax.all_gather(value_own, "blk", axis=0, tiled=True),
    )
    row_delta = jnp.sum(grad_heads.astype(jnp.float32).transpose(1, 0, 2) * attended_float, axis=-1)

    def back_block(grad_query_acc, block_index):
        offset = block_index * head_rows
        keys_block = lax.dynamic_slice_in_dim(keys_all, offset, head_rows, 0)
        values_block = lax.dynamic_slice_in_dim(values_all, offset, head_rows, 0)
        key_positions = stretch_positions(stretch_order, offset, head_rows, stretch_rows)
        scores = (
            jnp.einsum("qhd,kd->hqk", query_heads, keys_block, preferred_element_type=jnp.float32)
            * score_scale
        )
        allowed = (query_positions[:, None] >= key_positions[None, :])[None]
        probs_block = jnp.where(allowed, jnp.exp(scores - log_sum[..., None]), 0.0)
        grad_probs = jnp.einsum(
            "qhd,kd->hqk", grad_heads, values_block, preferred_element_type=jnp.float32
        )
        grad_scores = (probs_block * (grad_probs - row_delta[..., None])).astype(jnp.bfloat16)
        grad_query_acc = grad_query_acc + jnp.einsum(
            "hqk,kd->qhd", grad_scores, keys_block, preferred_element_type=jnp.float32
        )
        grad_key_part = (
            jnp.einsum("hqk,qhd->kd", grad_scores, query_heads, preferred_element_type=jnp.float32)
            * score_scale
        )
        grad_value_part = jnp.einsum(
            "hqk,qhd->kd",
            probs_block.astype(jnp.bfloat16),
            grad_heads,
            preferred_element_type=jnp.float32,
        )
        return (grad_query_acc, (grad_key_part, grad_value_part))

    grad_query_acc, (key_terms, value_terms) = lax.scan(
        back_block,
        jnp.zeros((head_rows, local_heads, HD), jnp.float32),
        jnp.arange(blocks, dtype=jnp.int32),
    )
    grad_key_sum, grad_value_sum = (
        lax.psum_scatter(
            key_terms.reshape(blocks * head_rows, HD).astype(jnp.bfloat16),
            "blk",
            scatter_dimension=0,
            tiled=True,
        ).astype(jnp.float32),
        lax.psum_scatter(
            value_terms.reshape(blocks * head_rows, HD).astype(jnp.bfloat16),
            "blk",
            scatter_dimension=0,
            tiled=True,
        ).astype(jnp.float32),
    )
    grad_query_rot = (grad_query_acc * score_scale).astype(jnp.bfloat16)
    grad_query_lin_heads = (
        unrotate(grad_query_rot.astype(jnp.float32), cos_block, sin_block)
        .astype(jnp.bfloat16)
        .reshape(head_rows, local_heads * HD)
    )
    key_slot_grad = grad_key_sum.astype(jnp.bfloat16)
    value_slot_grad = grad_value_sum.astype(jnp.bfloat16)
    grad_w_query = lax.dot_general(
        normed_rows, grad_query_lin_heads, contract_first, preferred_element_type=jnp.float32
    )
    query_back, key_back, value_back = (
        lax.all_to_all(grad_query_lin_heads, "head", split_axis=0, concat_axis=1, tiled=True),
        lax.all_to_all(key_slot_grad, "head", split_axis=0, concat_axis=1, tiled=True),
        lax.all_to_all(value_slot_grad, "head", split_axis=0, concat_axis=1, tiled=True),
    )
    key_slot_lin = (
        unrotate(key_back.astype(jnp.float32).reshape(row_count, groups, HD), cos_own, sin_own)
        .astype(jnp.bfloat16)
        .reshape(row_count, KV, repeats, HD)
    )
    value_slot_lin = value_back.reshape(row_count, KV, repeats, HD)
    grad_w_key = jnp.einsum(
        "td,tjrc->djc", normed, key_slot_lin, preferred_element_type=jnp.float32
    ).reshape(-1, KV * HD)
    grad_w_value = jnp.einsum(
        "td,tjrc->djc", normed, value_slot_lin, preferred_element_type=jnp.float32
    ).reshape(-1, KV * HD)
    grad_normed = lax.dot_general(
        query_back, query_all, contract_last, preferred_element_type=jnp.float32
    )
    grad_normed = grad_normed + jnp.einsum(
        "tjrc,djc->td",
        key_slot_lin,
        key_full.reshape(-1, KV, HD),
        preferred_element_type=jnp.float32,
    )
    grad_normed = grad_normed + jnp.einsum(
        "tjrc,djc->td",
        value_slot_lin,
        value_full.reshape(-1, KV, HD),
        preferred_element_type=jnp.float32,
    )
    gain_one_float = gain_one.astype(jnp.float32)
    grad_input_norm = norm_input_grad(tokens_float, inv_attn, gain_one_float, grad_normed)
    grad_gain_one = gain_grad(tokens_float, inv_attn, grad_normed)
    grad_hidden_own = lax.dynamic_slice_in_dim(grad_hidden_rows, own_first, row_count, 0)
    grad_tokens = (grad_hidden_own + grad_input_norm).astype(jnp.bfloat16)
    head_sums = (
        lax.psum(grad_w_key.astype(jnp.bfloat16), "head").astype(jnp.float32),
        lax.psum(grad_w_value.astype(jnp.bfloat16), "head").astype(jnp.float32),
        lax.psum(grad_gain_one.astype(jnp.bfloat16), "head").astype(jnp.float32),
        lax.psum(grad_gain_two.astype(jnp.bfloat16), "head").astype(jnp.float32),
    )
    reduced = (
        lax.psum_scatter(
            grad_w_query.astype(jnp.bfloat16), ("fsdp", "blk"), scatter_dimension=0, tiled=True
        ).astype(jnp.float32),
        lax.psum_scatter(
            head_sums[0].astype(jnp.bfloat16), ("fsdp", "blk"), scatter_dimension=0, tiled=True
        ).astype(jnp.float32),
        lax.psum_scatter(
            head_sums[1].astype(jnp.bfloat16), ("fsdp", "blk"), scatter_dimension=0, tiled=True
        ).astype(jnp.float32),
        lax.psum_scatter(
            grad_w_out.astype(jnp.bfloat16), ("fsdp", "blk"), scatter_dimension=0, tiled=True
        ).astype(jnp.float32),
        lax.psum_scatter(
            grad_w_gate.astype(jnp.bfloat16), ("fsdp", "blk"), scatter_dimension=0, tiled=True
        ).astype(jnp.float32),
        lax.psum_scatter(
            grad_w_up.astype(jnp.bfloat16), ("fsdp", "blk"), scatter_dimension=0, tiled=True
        ).astype(jnp.float32),
        lax.psum_scatter(
            grad_w_down.astype(jnp.bfloat16), ("fsdp", "blk"), scatter_dimension=0, tiled=True
        ).astype(jnp.float32),
        lax.psum_scatter(
            head_sums[2].astype(jnp.bfloat16), ("fsdp", "blk"), scatter_dimension=0, tiled=True
        ).astype(jnp.float32),
        lax.psum_scatter(
            head_sums[3].astype(jnp.bfloat16), ("fsdp", "blk"), scatter_dimension=0, tiled=True
        ).astype(jnp.float32),
    )
    return (
        layer_low,
        grad_tokens,
        reduced[0],
        reduced[1],
        reduced[2],
        reduced[3],
        reduced[4],
        reduced[5],
        reduced[6],
        reduced[7],
        reduced[8],
    )


MESH = pl.DeviceIdType.MESH
f32, bf16 = jnp.float32, jnp.bfloat16
VM = pl.BlockSpec(memory_space=pltpu.VMEM)
HB = pl.BlockSpec(memory_space=pl.ANY)


def dma_sems(n):
    return [pltpu.SemaphoreType.DMA((n,)), pltpu.SemaphoreType.DMA((n,))]


class Here:
    def __init__(self, send_sem, recv_sem):
        self.y = lax.axis_index("fsdp")
        blk = lax.axis_index("blk")
        self.x, self.c = blk // 2, blk % 2
        self.z = lax.axis_index("head")
        self.end = (self.z == 0) | (self.z == 3)
        self.middle = (self.z == 1) | (self.z == 2)
        self.inward = {"head": jnp.where(self.z < 2, self.z + 1, self.z - 1)}
        self.outward = {"head": jnp.where(self.z < 2, self.z - 1, self.z + 1)}
        self.send_sem, self.recv_sem, self.used = send_sem, recv_sem, 0

    def plane(self, i):
        y = 1 - self.y if i & 4 else self.y
        x = 1 - self.x if i & 2 else self.x
        c = 1 - self.c if i & 1 else self.c
        return {"fsdp": y, "blk": x * 2 + c}

    def number(self, i):
        at = self.plane(i)
        return at["fsdp"] * 4 + at["blk"]

    def up(self):
        return {"head": self.z + 1}

    def down(self):
        return {"head": self.z - 1}

    def copy(self, src, dst, device):
        k = self.used
        self.used += 1
        return self.again(k, src, dst, device)

    def slot(self):
        self.used += 1
        return self.used - 1

    def again(self, k, src, dst, device):
        return pltpu.make_async_remote_copy(
            src_ref=src,
            dst_ref=dst,
            send_sem=self.send_sem.at[k],
            recv_sem=self.recv_sem.at[k],
            device_id=device,
            device_id_type=MESH,
        )

    def local(self, src, dst):
        k = self.used
        self.used += 1
        return pltpu.make_async_copy(src, dst, self.send_sem.at[k])

    def free_in_plane(self, sem):
        for i in (1, 2, 4):
            pl.semaphore_signal(sem, inc=1, device_id=self.plane(i), device_id_type=MESH)

    def free_along_z(self, sem):
        @pl.when(self.z > 0)
        def _():
            pl.semaphore_signal(sem, inc=1, device_id=self.down(), device_id_type=MESH)

        @pl.when(self.z < 3)
        def _():
            pl.semaphore_signal(sem, inc=1, device_id=self.up(), device_id_type=MESH)

    def wait_along_z(self, sem):
        pl.semaphore_wait(sem, jnp.where(self.z > 0, 1, 0) + jnp.where(self.z < 3, 1, 0))

    def enter(self, offsets, along_z=True, all_z=False):
        bar = pltpu.get_barrier_semaphore()
        for i in offsets:
            pl.semaphore_signal(bar, inc=1, device_id=self.plane(i), device_id_type=MESH)
        if all_z:
            for d in (1, 2, 3):
                pl.semaphore_signal(
                    bar, inc=1, device_id={"head": (self.z + d) % 4}, device_id_type=MESH
                )
            pl.semaphore_wait(bar, len(offsets) + 3)
            return
        if along_z:

            @pl.when(self.z > 0)
            def _():
                pl.semaphore_signal(bar, inc=1, device_id=self.down(), device_id_type=MESH)

            @pl.when(self.z < 3)
            def _():
                pl.semaphore_signal(bar, inc=1, device_id=self.up(), device_id_type=MESH)

        peers = len(offsets)
        if along_z:
            peers = peers + jnp.where(self.z > 0, 1, 0) + jnp.where(self.z < 3, 1, 0)
        pl.semaphore_wait(bar, peers)


class Order:
    def __init__(self, *tasks):
        self.now, self.count, self.waiting = 0.0, 0, []
        for task in tasks:
            self.add(task)

    def add(self, task, at=None):
        self.waiting.append((self.now if at is None else at, self.count, task))
        self.count += 1

    def next_at(self):
        return min(self.waiting, default=(math.inf,))[0]

    def step(self):
        item = min(self.waiting, key=lambda entry: entry[:2])
        self.waiting.remove(item)
        at = next(item[2], None)
        if at is not None:
            self.waiting.append((max(at, item[0]), item[1], item[2]))

    def pump(self, until):
        while self.next_at() <= until:
            self.step()
        self.now = max(self.now, until)

    def until(self, *flags):
        while not all(flag.up for flag in flags):
            self.now = max(self.now, self.next_at())
            self.step()

    def finish(self):
        while self.waiting:
            self.step()

    def loop(self, n, each, item, before=None):
        start = self.now

        def body(i, _):
            for k in range(n):
                while self.waiting and (
                    self.next_at() <= start + k * each or (before is not None and before(k))
                ):

                    @pl.when(i == k)
                    def _():
                        self.step()

            item(i)
            return 0

        lax.fori_loop(0, n, body, 0)
        self.now = start + n * each


def drive(*tasks):
    Order(*tasks).finish()


class Flag:
    def __init__(self):
        self.up = False


def z_gather(me, src, dst, unit, begin=0.0, done=None, issue=None):
    rows = src.shape[0]
    half = rows // 2
    z = me.z

    def block(j, h):
        return dst.at[pl.ds(pl.multiple_of(j * rows + h * half, half), half)]

    ups = [me.slot() for _ in range(6)]
    downs = [me.slot() for _ in range(6)]
    own = me.local(src, dst.at[pl.ds(pl.multiple_of(z * rows, rows), rows)])

    def up(j, h):
        mine = src.at[pl.ds(h * half, half)] if j == 0 else block(z - j, h)
        return me.again(ups[2 * j + h], mine, block(z - j, h), me.up())

    def down(j, h):
        mine = src.at[pl.ds(h * half, half)] if j == 0 else block(z + j, h)
        return me.again(downs[2 * j + h], mine, block(z + j, h), me.down())

    def steps():
        yield begin if issue is None else issue

        @pl.when(z < 3)
        def _():
            up(0, 0).start()
            up(0, 1).start()

        @pl.when(z > 0)
        def _():
            down(0, 0).start()
            down(0, 1).start()

        own.start()
        for j in (1, 2, 3):
            for h in (0, 1):
                yield begin + unit * (j - 0.5 + h * 0.5) + 1.8 + 0.4 * j

                @pl.when(z >= j)
                def _():
                    up(j - 1, h).wait_recv()

                if j < 3:

                    @pl.when((z >= j) & (z < 3))
                    def _():
                        up(j, h).start()

                @pl.when(z <= 3 - j)
                def _():
                    down(j - 1, h).wait_recv()

                if j < 3:

                    @pl.when((z <= 3 - j) & (z > 0))
                    def _():
                        down(j, h).start()

        own.wait()
        if done is not None:
            done.up = True
        yield begin + unit * 3 + 15.0
        for j in (0, 1, 2):

            @pl.when((z >= j) & (z < 3))
            def _():
                up(j, 0).wait_send()
                up(j, 1).wait_send()

            @pl.when((z <= 3 - j) & (z > 0))
            def _():
                down(j, 0).wait_send()
                down(j, 1).wait_send()

    return steps()


def plane_gather(me, src, dst, unit, begin=0.0, done=None, issue=None):
    rows = src.shape[0]
    half = rows // 2

    def part(i, h):
        return dst.at[pl.ds(pl.multiple_of(me.number(i) * rows + h * half, half), half)]

    def block(i):
        return dst.at[pl.ds(pl.multiple_of(me.number(i) * rows, rows), rows)]

    halves = src.at[pl.ds(0, half)], src.at[pl.ds(half, half)]
    x_in = [me.copy(halves[h], part(0, h), me.plane(2)) for h in (0, 1)]
    y_in = [me.copy(halves[h], part(0, h), me.plane(4)) for h in (1, 0)]
    to_c = me.copy(src, block(0), me.plane(1))
    own = me.local(src, block(0))
    x_on = me.copy(part(2, 0), part(2, 0), me.plane(4))
    y_on = me.copy(part(4, 1), part(4, 1), me.plane(2))
    x_core = me.copy(block(2), block(2), me.plane(1))
    y_core = me.copy(block(4), block(4), me.plane(1))
    far = [me.copy(part(6, h), part(6, h), me.plane(1)) for h in (0, 1)]

    def steps():
        yield begin if issue is None else issue
        for copy in (x_in[0], y_in[0], x_in[1], y_in[1], to_c, own):
            copy.start()
        yield begin + unit * 0.5 + 2.0
        x_in[0].wait_recv()
        x_on.start()
        y_in[0].wait_recv()
        y_on.start()
        yield begin + unit + 2.5
        x_in[1].wait_recv()
        x_core.start()
        y_in[1].wait_recv()
        y_core.start()
        yield begin + unit * 1.5 + 4.5
        x_on.wait_recv()
        far[0].start()
        y_on.wait_recv()
        far[1].start()
        yield begin + unit * 1.5 + 6.5
        own.wait()
        for copy in (to_c, x_core, y_core, *far):
            copy.wait_recv()
        if done is not None:
            done.up = True
        yield begin + unit * 1.5 + 15.0
        for copy in (*x_in, *y_in, to_c, x_on, x_core, y_on, y_core, *far):
            copy.wait_send()

    return steps()


def plane_direct(me, src, dst, done):
    rows = src.shape[0]
    place = dst.at[pl.ds(pl.multiple_of(me.number(0) * rows, rows), rows)]
    copies = [me.copy(src, place, me.plane(i)) for i in range(1, 8)]
    own = me.local(src, place)

    def steps():
        for copy in (*copies, own):
            copy.start()
        yield 5.0
        own.wait()
        for copy in copies:
            copy.wait_recv()
        done.up = True
        yield 15.0
        for copy in copies:
            copy.wait_send()

    return steps()


def add_rows(dst, a, b, step=32):
    rows = a.shape[0]

    def body(i, _):
        at = pl.ds(pl.multiple_of(i * step, step), step)
        dst[at, :] = (a[at, :].astype(f32) + b[at, :].astype(f32)).astype(dst.dtype)
        return 0

    lax.fori_loop(0, rows // step, body, 0)


class Progress:
    def __init__(self, parts):
        self.parts, self.entered, self.crossed, self.left = parts, 0, 0, 0
        self.sent_in, self.sent_out = Flag(), Flag()

    def whole(self):
        return min(self.crossed, self.left)


def z_reduce_all(me, part, total, inbox, across, out, unit, chunks, progress, begin=0.0, lag=0.0):
    rows = part.shape[0] // chunks
    first = [me.slot() for _ in range(chunks)]
    second = [me.slot() for _ in range(chunks)]
    third = [me.slot() for _ in range(chunks)]
    store = [me.slot() for _ in range(chunks)]
    hop = unit / chunks

    def at(ref, k):
        return ref.at[pl.ds(k * rows, rows)]

    def send_in(k):
        return me.again(first[k], at(part, k), at(inbox, k), me.inward)

    def send_across(k):
        return me.again(second[k], at(inbox, k), at(across, k), me.inward)

    def send_out(k):
        return me.again(third[k], at(total, k), at(total, k), me.outward)

    def put(k):
        return pltpu.make_async_copy(at(total, k), at(out, k), me.send_sem.at[store[k]])

    def entering():
        yield begin
        time, sent = begin, 0
        for k in range(chunks):
            while k >= progress.parts:
                time += 0.5
                yield time
            new, sent = range(sent, progress.parts), progress.parts
            if len(new):

                @pl.when(me.end)
                def _():
                    for j in new:
                        send_in(j).start()

            time = max(time, begin + lag + 2.0) + hop
            yield time

            @pl.when(me.middle)
            def _():
                send_in(k).wait_recv()
                add_rows(at(inbox, k), at(part, k), at(inbox, k))
                send_across(k).start()

            progress.entered = k + 1
        yield time + 20.0

        @pl.when(me.end)
        def _():
            for k in range(chunks):
                send_in(k).wait_send()

        progress.sent_in.up = True

    def crossing():
        yield begin
        time = begin
        for k in range(chunks):
            while k >= progress.entered:
                time += 0.5
                yield time
            time = max(time, begin + lag + 4.0 + hop) + hop
            yield time

            @pl.when(me.middle)
            def _():
                send_across(k).wait_recv()
                add_rows(at(total, k), at(inbox, k), at(across, k))
                send_out(k).start()
                if out is not None:
                    put(k).start()

            progress.crossed = k + 1
        yield time + 10.0

        @pl.when(me.middle)
        def _():
            for k in range(chunks):
                send_across(k).wait_send()
                send_out(k).wait_send()

        progress.sent_out.up = True

    def leaving():
        yield begin
        time = begin
        for k in range(chunks):
            while k >= progress.crossed:
                time += 0.5
                yield time
            time = max(time, begin + lag + 6.0 + 2 * hop) + hop
            yield time

            @pl.when(me.end)
            def _():
                send_out(k).wait_recv()
                if out is not None:
                    put(k).start()

            progress.left = k + 1
        if out is not None:
            yield time + 2.0
            for k in range(chunks):
                put(k).wait()

    return entering(), crossing(), leaving()


def z_reduce_scatter(me, part, from_below, from_above, own, unit, begin=0.0, done=None):
    rows = part.shape[0] // 4
    z = me.z
    ups = [me.slot() for _ in range(4)]
    downs = [me.slot() for _ in range(4)]

    def at(ref, j):
        return ref.at[pl.ds(j * rows, rows)]

    def up(j, source):
        return me.again(ups[j], at(source, j), at(from_below, j), me.up())

    def down(j, source):
        return me.again(downs[j], at(source, j), at(from_above, j), me.down())

    def start(j):
        @pl.when(z == 0)
        def _():
            up(j, part).start()

        @pl.when(z == 3)
        def _():
            down(3 - j, part).start()

    def relay(j, stop):
        @pl.when(z == stop)
        def _():
            up(j, part).wait_recv()
            add_rows(at(from_below, j), at(part, j), at(from_below, j))
            up(j, from_below).start()

        @pl.when(z == 3 - stop)
        def _():
            i = 3 - j
            down(i, part).wait_recv()
            add_rows(at(from_above, i), at(part, i), at(from_above, i))
            down(i, from_above).start()

    yield begin
    start(3)
    yield begin + unit * 0.6
    start(2)
    yield begin + unit + 1.0
    relay(3, 1)
    yield begin + unit * 1.6
    start(1)
    yield begin + unit * 2 + 1.0
    relay(3, 2)
    relay(2, 1)
    yield begin + unit * 3 + 1.5
    for j in range(4):

        @pl.when(z == j)
        def _():
            if j > 0:
                up(j, part).wait_recv()
            if j < 3:
                down(j, part).wait_recv()

            def body(i, _):
                span = pl.ds(pl.multiple_of(i * 32, 32), 32)
                there = pl.ds(pl.multiple_of(j * rows + i * 32, 32), 32)
                value = part[there, :].astype(f32)
                if j > 0:
                    value = value + from_below[there, :].astype(f32)
                if j < 3:
                    value = value + from_above[there, :].astype(f32)
                own[span, :] = value
                return 0

            lax.fori_loop(0, rows // 32, body, 0)
            for i in range(4):
                if i > j:
                    up(i, part).wait_send()
                if i < j:
                    down(i, part).wait_send()

    if done is not None:
        done.up = True


def offsets_of(me, j):
    dx, dy, dc = 1 - (j % 4) // 2, 1 - j % 2, 1 - j // 4
    y = me.y + dy - 2 * me.y * dy
    x = me.x + dx - 2 * me.x * dx
    c = me.c + dc - 2 * me.c * dc
    return y * 4 + x * 2 + c


def plane_scatter_scratch(rows, cols):
    half = rows // 2
    return [
        pltpu.VMEM((8, rows, cols), bf16),
        pltpu.VMEM((4, rows, cols), bf16),
        pltpu.VMEM((2, half, cols), bf16),
        pltpu.VMEM((2, half, cols), bf16),
        pltpu.VMEM((half, cols), bf16),
        pltpu.VMEM((half, cols), bf16),
    ]


class PlaneScatter:
    def __init__(self, me, scratch):
        self.me = me
        self.blocks, self.other, self.over_x, self.over_y, self.last_y, self.last_x = scratch
        blocks, rows = self.blocks, self.blocks.shape[1]
        half = rows // 2
        self.half, self.first, self.second = half, pl.ds(0, half), pl.ds(half, half)
        first, second = self.first, self.second
        self.core = [me.copy(blocks.at[j], self.other.at[j], me.plane(1)) for j in range(4)]
        self.far_x = me.copy(blocks.at[4, first], self.over_x.at[1], me.plane(2))
        self.far_y = me.copy(blocks.at[4, second], self.over_y.at[1], me.plane(4))
        self.near_x = me.copy(blocks.at[5, first], self.over_x.at[0], me.plane(2))
        self.near_y = me.copy(blocks.at[6, second], self.over_y.at[0], me.plane(4))
        self.to_y = me.copy(blocks.at[6, first], self.last_y, me.plane(4))
        self.to_x = me.copy(blocks.at[5, second], self.last_x, me.plane(2))

    def steps(self, out, unit, begin, done, free=None):
        blocks, half, first, second = self.blocks, self.half, self.first, self.second
        for j in range(4):
            yield begin + 0.3 * j
            self.core[j].wait_recv()
            add_rows(blocks.at[4 + j], blocks.at[4 + j], self.other.at[j])
            if j == 0:
                self.far_x.start()
                self.far_y.start()
            if j == 1:
                self.near_x.start()
            if j == 2:
                self.near_y.start()
        yield begin + 3.0 + unit * 0.5
        self.far_x.wait_recv()
        add_rows(blocks.at[6, first], blocks.at[6, first], self.over_x.at[1])
        self.to_y.start()
        self.far_y.wait_recv()
        add_rows(blocks.at[5, second], blocks.at[5, second], self.over_y.at[1])
        self.to_x.start()
        yield begin + 4.0 + unit * 1.5
        for copy in (self.near_x, self.near_y, self.to_y, self.to_x):
            copy.wait_recv()

        def body(i, _):
            at = pl.ds(pl.multiple_of(i * 32, 32), 32)
            low = pl.ds(pl.multiple_of(half + i * 32, 32), 32)
            for rows, near, last in ((at, self.over_x, self.last_y), (low, self.over_y, self.last_x)):
                value = blocks[7, rows, :].astype(f32) + near[0, at, :].astype(f32)
                out[rows, :] = (value + last[at, :].astype(f32)).astype(out.dtype)
            return 0

        lax.fori_loop(0, half // 32, body, 0)
        for copy in (*self.core, self.far_x, self.far_y, self.near_x, self.near_y, self.to_y, self.to_x):
            copy.wait_send()
        done.up = True
        if free is not None:
            self.me.free_in_plane(free)


def params(number, vmem=60 * 2**20):
    return pltpu.CompilerParams(
        collective_id=number, has_side_effects=True, vmem_limit_bytes=vmem
    )


def shape(dims, kind=bf16):
    return jax.ShapeDtypeStruct(dims, kind)


def alone(flops, vmem=60 * 2**20):
    return dict(
        compiler_params=pltpu.CompilerParams(vmem_limit_bytes=vmem),
        cost_estimate=pl.CostEstimate(flops=int(flops), bytes_accessed=2**23, transcendentals=0),
    )


def gain_row(gains, which):
    return jnp.concatenate([gains[i * 8 + which : i * 8 + which + 1, :] for i in range(8)], axis=1)


def rotate_heads(values, cos, sin, inverse=False):
    out = []
    for h in range(values.shape[0] // HD):
        a = values[h * HD : h * HD + HD // 2]
        b = values[h * HD + HD // 2 : (h + 1) * HD]
        if inverse:
            out += [a * cos + b * sin, b * cos - a * sin]
        else:
            out += [a * cos - b * sin, b * cos + a * sin]
    return jnp.concatenate(out, axis=0)


def block_positions(order_ref, number, stretch_rows):
    row = lax.broadcasted_iota(jnp.int32, (stretch_rows, 128), 0)
    return jnp.concatenate(
        [row + order_ref[number * 2 + i] * stretch_rows for i in range(2)], axis=0
    )


def forward_kernel(
    order_ref, tok, w_query, w_key, w_value, gains, frequency, wo, cot, wg, wu, wd,
    tok_all, wqkv_all, gains_all, wo_all, wd_all, cot_all, kv_all, branch,
    normed_all, q_t_all, q_n_all, out_t_all, attended_all, log_sum, key_pos, query_pos, cos_t, sin_t,
    normed_two, hidden, d_gate, d_up, two_part,
    normed, q_t, q_n, out_t, attended, wqkv, gain_src, toks, wqkvs, wos, kv_own, kv, v_t, att_t, part, total, inbox, across,
    wgs, wus, wds, cots, two, ss, rs
):
    me = Here(ss, rs)
    z = me.z
    heads, hd, rows = q_t.shape
    wide = heads * hd
    keys = kv.shape[0]
    wqkv[:, :wide] = w_query[...]
    for j in range(4):

        @pl.when(z == j)
        def _():
            wqkv[:, wide : wide + hd] = w_key[:, j * hd : (j + 1) * hd]
            wqkv[:, wide + hd :] = w_value[:, j * hd : (j + 1) * hd]

    gain_src[...] = jnp.concatenate([gains[...], jnp.zeros((6, gains.shape[1]), f32)], axis=0)
    me.enter(tuple(range(1, 8)))
    lanes = att_t.shape[1]
    have_tok, have_gains, have_wqkv, have_wo = Flag(), Flag(), Flag(), Flag()
    have_wg, have_wu, have_wd, have_cot = Flag(), Flag(), Flag(), Flag()
    progress = Progress(0)
    order = Order(
        z_gather(me, tok, toks, 11.3, 0.0, have_tok),
        plane_direct(me, gain_src, gains_all, have_gains),
        plane_gather(me, wqkv, wqkvs, 7.0, 0.5, have_wqkv, 0.0),
        plane_gather(me, wo, wos, 6.0, 11.0, have_wo, 7.5),
        plane_gather(me, wg, wgs, 15.5, 20.0, have_wg, 17.0),
        z_gather(me, cot, cots, 11.3, 37.0, have_cot, 27.0),
    )
    c_number = me.x * 2 + me.c
    for i in range(4):
        x = 1 - me.x if i & 2 else me.x
        c = 1 - me.c if i & 1 else me.c
        key_pos[i * rows : (i + 1) * rows, :] = block_positions(order_ref, x * 2 + c, rows // 2)
    lane = lax.broadcasted_iota(jnp.int32, (hd // 2, rows // 2), 1)
    for i in range(2):
        span = slice(i * rows // 2, (i + 1) * rows // 2)
        position = lane + order_ref[c_number * 2 + i] * (rows // 2)
        query_pos[:, span] = position[:8]
        freq = jnp.concatenate([frequency[...]] * (rows // 256), axis=1)
        angle = position.astype(f32) * freq
        cos_t[:, span] = jnp.cos(angle)
        sin_t[:, span] = jnp.sin(angle)
    order.until(have_tok, have_gains, have_wqkv)
    saves = [me.local(toks, tok_all), me.local(wqkvs, wqkv_all)]
    for save in saves:
        save.start()
    gain = gain_row(gains_all, 0)

    def project(i):
        at = pl.ds(pl.multiple_of(i * 128, 128), 128)
        x = toks[at, :].astype(f32)
        inv = lax.rsqrt(jnp.mean(x * x, axis=1, keepdims=True) + norm_epsilon)
        low = (x * inv * gain).astype(bf16)
        normed[at, :] = low
        lin = jnp.dot(low, wqkvs[...], preferred_element_type=f32).T
        cos, sin = cos_t[:, at], sin_t[:, at]
        turned = rotate_heads(lin[: wide + hd], cos, sin)
        query = turned[:wide].astype(bf16) * bf16(1.0 / math.sqrt(hd))
        natural = query.astype(f32).T
        for h in range(heads):
            q_t[h, :, at] = query[h * hd : (h + 1) * hd]
            q_n[h, at, :] = natural[:, h * hd : (h + 1) * hd].astype(bf16)
        kv_own[at, :] = jnp.concatenate([turned[wide:], lin[wide + hd :]], axis=0).T.astype(bf16)

    order.loop(rows // 128, 1.0, project)

    def block(i):
        return kv.at[pl.ds(i * rows, rows)]

    copies = [me.copy(kv_own, block(i), me.plane(i)) for i in (1, 2, 3)]
    own = me.local(kv_own, block(0))
    for copy in (*copies, own):
        copy.start()
    order.pump(order.now + 4.0)
    order.add(plane_gather(me, wu, wus, 15.5, order.now, have_wu))
    order.add(plane_gather(me, wd, wds, 15.5, order.now + 24.0, have_wd, order.now + 14.0))
    own.wait()
    for copy in copies:
        copy.wait_recv()
    save = me.local(kv, kv_all)
    save.start()
    for i in range(keys // rows):
        span = slice(i * rows, (i + 1) * rows)
        v_t[:, span] = kv[span, :].astype(f32).T[hd:, :].astype(bf16)
    order.until(have_wo)
    save_wo = me.local(wos, wo_all)
    save_wo.start()
    for task in z_reduce_all(
        me, part, total, inbox, across, branch, 45.0, 16, progress, order.now, 18.0
    ):
        order.add(task)

    def item(i):
        r, h = i // heads, i % heads
        at = pl.ds(pl.multiple_of(r * lanes, lanes), lanes)
        s = jnp.dot(kv[:, 0:hd], q_t[h, :, at], preferred_element_type=f32)
        pos = jnp.concatenate([key_pos[...]] * (lanes // 128), axis=1)
        s = jnp.where(pos <= query_pos[0:1, at], s, masked_value)
        top = jnp.max(s, axis=0, keepdims=True)
        p = jnp.exp(s - top)
        norm = jnp.sum(p, axis=0, keepdims=True)
        o = jnp.dot(v_t[...], p.astype(bf16), preferred_element_type=f32) / norm
        out_t[h, :, at] = o
        log_sum[h, :, at] = top + jnp.log(norm)
        att_t[pl.ds(pl.multiple_of(h * hd, hd), hd), :] = o

        @pl.when(h == heads - 1)
        def _():
            natural = att_t[...].T.astype(bf16)
            attended[at, :] = natural
            part[at, :] = contract_last_dims(natural, wos[...]).astype(bf16)

    def before(k):
        progress.parts = k // heads * (lanes // 32)
        return False

    order.loop(heads * rows // lanes, 1.2, item, before)
    progress.parts = 16
    early = ((normed, normed_all), (q_t, q_t_all), (q_n, q_n_all), (out_t, out_t_all), (attended, attended_all))
    early = [me.local(*pair) for pair in early]
    for copy in early:
        copy.start()
    late = [me.local(wds, wd_all), me.local(cots, cot_all)]
    order.until(have_wg, have_wu, have_wd, have_cot)
    for copy in late:
        copy.start()
    gain_mlp = gain_row(gains_all, 1)
    half = rows // 2

    def norm_two(first):
        def body(i, _):
            at = pl.ds(pl.multiple_of(first + i * 64, 64), 64)
            h = toks[at, :].astype(f32) + total[at, :].astype(f32)
            inv = lax.rsqrt(jnp.mean(h * h, axis=1, keepdims=True) + norm_epsilon)
            normed_two[at, :] = (h * inv * gain_mlp).astype(bf16)
            return 0

        lax.fori_loop(0, half // 64, body, 0)

    def feed(at, span):
        gate = jnp.dot(normed_two[at, :], wgs[:, span], preferred_element_type=f32)
        up = jnp.dot(normed_two[at, :], wus[:, span], preferred_element_type=f32)
        grad = jnp.dot(cots[at, :], wds[:, span], preferred_element_type=f32)
        sigmoid = jax.nn.sigmoid(gate)
        silu = gate * sigmoid
        hidden[at, span] = (silu * up).astype(bf16)
        grad_gate = (grad * up * sigmoid * (1.0 + gate * (1.0 - sigmoid))).astype(bf16)
        grad_up = (grad * silu).astype(bf16)
        d_gate[at, span] = grad_gate
        d_up[at, span] = grad_up
        return contract_last_dims(grad_gate, wgs[:, span]) + contract_last_dims(grad_up, wus[:, span])

    def feed_item(j):
        @pl.when(j == 0)
        def _():
            norm_two(0)
            two[...] = jnp.zeros_like(two)

        two[...] += feed(slice(0, half), pl.ds(pl.multiple_of(j * 128, 128), 128))

    order.loop(hidden.shape[1] // 128, 1.8, feed_item, lambda k: progress.whole() < 8)
    two_part[:half, :] = two[...].astype(bf16)
    while progress.whole() < 16:
        order.step()
    norm_two(half)
    two_part[half:, :] = feed(slice(half, rows), slice(None)).astype(bf16)
    order.finish()
    for copy in copies:
        copy.wait_send()
    for copy in (save, save_wo, *saves, *early, *late):
        copy.wait()


def forward(stretch_order, tok, w_query, w_key, w_value, gains, frequency, wo, cot, wg, wu, wd):
    rows = tok.shape[0] * 4
    width = tok.shape[1]
    heads = w_query.shape[1] // HD
    keys = rows * 4
    qkv = (w_query.shape[0], w_query.shape[1] + 2 * HD)

    def grown(a, n=8):
        return shape((a.shape[0] * n,) + a.shape[1:], a.dtype)

    def room(a):
        return pltpu.VMEM(a.shape, a.dtype)

    gain_block = shape((8, gains.shape[1]), f32)
    wqkv = shape(qkv)
    block = shape((rows, width))
    units = shape((rows, wg.shape[1]))
    return pl.pallas_call(
        forward_kernel,
        out_shape=(
            block, grown(wqkv), grown(gain_block), grown(wo), grown(wd), block,
            shape((keys, 2 * HD)), block,
            block,
            shape((heads, HD, rows)),
            shape((heads, rows, HD)),
            shape((heads, HD, rows), f32),
            shape((rows, heads * HD)),
            shape((heads, 1, rows), f32),
            shape((keys, 128), jnp.int32),
            shape((8, rows), jnp.int32),
            shape((HD // 2, rows), f32),
            shape((HD // 2, rows), f32),
            block, units, units, units, block,
        ),
        in_specs=[pl.BlockSpec(memory_space=pltpu.SMEM)] + [VM] * 7 + [HB] * 4,
        out_specs=[HB, HB, VM] + [HB] * 10 + [VM] * 10,
        scratch_shapes=[
            room(block),
            pltpu.VMEM((heads, HD, rows), bf16),
            pltpu.VMEM((heads, rows, HD), bf16),
            pltpu.VMEM((heads, HD, rows), f32),
            pltpu.VMEM((rows, heads * HD), bf16),
            room(wqkv), room(gain_block), room(block), room(grown(wqkv)), room(grown(wo)),
            pltpu.VMEM((rows, 2 * HD), bf16),
            pltpu.VMEM((keys, 2 * HD), bf16),
            pltpu.VMEM((HD, keys), bf16),
            pltpu.VMEM((heads * HD, 256), f32),
            room(block), room(block), room(block), room(block),
            room(grown(wg)), room(grown(wu)), room(grown(wd)), room(block), pltpu.VMEM((rows // 2, width), f32),
        ] + dma_sems(224),
        compiler_params=params(1, 67043328),
        name="forward",
    )(stretch_order, tok, w_query, w_key, w_value, gains, frequency, wo, cot, wg, wu, wd)


def contract_rows(left, right):
    return lax.dot_general(left, right, (((0,), (0,)), ((), ())), preferred_element_type=f32)


def contract_last_dims(left, right):
    return lax.dot_general(left, right, (((1,), (1,)), ((), ())), preferred_element_type=f32)


def gain_sums(me, src, out, came, mine, came_z):
    def block(i):
        return pl.ds(pl.multiple_of(me.number(i) * 8, 8), 8)

    own = block(0)
    copies = [me.copy(src.at[block(i)], came.at[i - 1], me.plane(i)) for i in range(1, 8)]
    again = [
        me.copy(mine, came_z.at[d - 1], {"head": (me.z + d) % 4}) for d in (1, 2, 3)
    ]

    def steps(begin):
        for copy in copies:
            copy.start()
        yield begin + 13.0
        value = src[own, :]
        for i, copy in enumerate(copies):
            copy.wait_recv()
            value = value + came[i]
        mine[...] = value
        for copy in again:
            copy.start()
        yield begin + 40.0
        value = mine[...]
        for d, copy in enumerate(again):
            copy.wait_recv()
            value = value + came_z[d]
        out[...] = value
        for copy in copies + again:
            copy.wait_send()

    return steps


def backward_kernel(
    part, cot_all, hidden, normed_two, d_gate, d_up, wd_all, tok_all, branch, gains, wo_all,
    out_t_all, attended_all, q_t_all, q_n_all, kv_all, wqkv_all, normed_all, log_sum, key_pos, query_pos, cos_t, sin_t,
    dwd_own, dwg_own, dwu_own, dw_own, dwkv_all, out_own, own, grad_one, gains_out,
    total, inbox, across, cot, out_part, below, above, q_t, q_n, kv, k_t, came, dq_t,
    gain_two, gain_parts, came_gain, gain_mine, gain_z, dwkv_own, came_kv, *rest
):
    scratch_d, scratch_g = rest[:6], rest[6:12]
    free_d, free_g, free_z, ss, rs = rest[12:]
    me = Here(ss, rs)
    me.enter(tuple(range(1, 8)), all_z=True)
    z = me.z
    rows, width = part.shape
    heads, hd, _ = q_t.shape
    wide = heads * hd
    lin_cols = wide + 2 * hd
    keys = kv.shape[0]
    cols = width // 8
    progress = Progress(16)
    order = Order(*z_reduce_all(me, part, total, inbox, across, None, 45.0, 16, progress))
    down, gate = PlaneScatter(me, scratch_d), PlaneScatter(me, scratch_g)
    up = PlaneScatter(me, scratch_d)
    narrow = [ref.at[(slice(None),) * (len(ref.shape) - 1) + (pl.ds(0, lin_cols + wide),)] for ref in scratch_g]
    both = PlaneScatter(me, narrow)
    down_done, gate_done, up_done, both_done, out_done, one_done = (Flag() for _ in range(6))
    cot_load = me.local(cot_all, cot)
    cot_load.start()
    later = [me.local(src, dst) for src, dst in ((kv_all, kv), (q_t_all, q_t), (q_n_all, q_n))]
    stores = [me.slot() for _ in range(5)]
    back = [
        me.copy(kv.at[pl.ds(i * rows, rows)], came.at[i - 1], me.plane(i)) for i in (1, 2, 3)
    ]
    kv_sends = [
        me.copy(dwkv_own, came_kv.at[d - 1], {"head": (z + d) % 4}) for d in (1, 2, 3)
    ]

    gains_steps = gain_sums(me, gain_parts, gains_out, came_gain, gain_mine, gain_z)

    def columns(j):
        return pl.ds(pl.multiple_of(offsets_of(me, j) * cols, cols), cols)

    def send(scatter, j):
        for k in range(4):

            @pl.when(j == k)
            def _():
                scatter.core[k].start()

    def weights(left, right_h, right_g, wd):
        pairs = ((hidden, right_h), (normed_two, left), (d_gate, right_g))
        loads = [me.local(src, dst) for src, dst in pairs]
        for load in loads:
            load.start()
        for load in later:
            load.start()
        cot_load.wait()
        loads[0].wait()
        order.pump(2.0)

        def down_item(j):
            down.blocks[j] = contract_rows(cot[:, columns(j)], right_h[...]).astype(bf16)
            send(down, j)

        order.loop(8, 0.65, down_item)
        order.add(down.steps(dwd_own, 16.5, order.now + 0.1, down_done, free_d))
        loads[1].wait()
        loads[2].wait()

        def gate_item(j):
            gate.blocks[j] = contract_rows(left[:, columns(j)], right_g[...]).astype(bf16)
            send(gate, j)

        order.loop(8, 0.75, gate_item)
        order.add(gate.steps(dwg_own, 16.5, order.now + 19.0, gate_done, free_g))

        def fetch(j):
            at = pl.ds(pl.multiple_of(j * cols, cols), cols)
            return pltpu.make_async_copy(wd_all.at[at], wd.at[j % 2], ss.at[stores[1]])

        fetch(0).start()

        def out_item(j):
            fetch(j).wait()

            @pl.when(j < 7)
            def _():
                fetch(j + 1).start()

            at = pl.ds(pl.multiple_of(j * cols, cols), cols)
            out_part[:, at] = contract_last_dims(right_h[...], wd[j % 2]).astype(bf16)

        order.loop(8, 1.2, out_item)

    units = pltpu.VMEM(hidden.shape, bf16)
    weight = pltpu.VMEM((2, cols, hidden.shape[1]), bf16)
    pl.run_scoped(weights, pltpu.VMEM(part.shape, bf16), units, units, weight)

    def attention(tok, summed, wo, out_t, attended, g_t, g_n, delta, dk, dv):
        gain = gain_row(gains, 1)

        def fetch(r):
            at = pl.ds(pl.multiple_of(r * 128, 128), 128)
            return (
                pltpu.make_async_copy(tok_all.at[at], tok, ss.at[stores[2]]),
                pltpu.make_async_copy(branch.at[at], summed, ss.at[stores[3]]),
            )

        for copy in fetch(0):
            copy.start()
        loads = [
            me.local(src, dst)
            for src, dst in ((wo_all, wo), (out_t_all, out_t), (attended_all, attended))
        ]
        for load in loads:
            load.start()
        dk[...] = jnp.zeros_like(dk)
        dv[...] = jnp.zeros_like(dv)
        for load in later:
            load.wait()
        for i in range(keys // rows):
            span = slice(i * rows, (i + 1) * rows)
            k_t[:, span] = kv[span, :].astype(f32).T[:hd, :].astype(bf16)
        for load in loads:
            load.wait()
        order.add(z_reduce_scatter(me, out_part, below, above, out_own, 12.0, 42.0, out_done), 42.0)

        def prepare(r):
            for copy in fetch(r):
                copy.wait()
            at = pl.ds(pl.multiple_of(r * 128, 128), 128)
            h = tok[...].astype(f32) + summed[...].astype(f32)
            e = total[at, :].astype(f32)
            inv = lax.rsqrt(jnp.mean(h * h, axis=1, keepdims=True) + norm_epsilon)
            u = e * gain
            inner = jnp.mean(u * h, axis=1, keepdims=True)
            grad = cot[at, :].astype(f32) + (inv * u - h * (inv * inv * inv * inner))

            @pl.when(r == z)
            def _():
                own[...] = grad
                gain_two[...] = jnp.broadcast_to(jnp.sum(e * h * inv, axis=0, keepdims=True), gain_two.shape)

            small = grad.astype(bf16)
            cot[at, :] = small
            g = jnp.dot(small, wo[...], preferred_element_type=f32).astype(bf16)
            turned = g.astype(f32).T
            for head in range(heads):
                g_n[head] = g[:, head * hd : (head + 1) * hd]
                mine = turned[head * hd : (head + 1) * hd]
                g_t[head] = mine.astype(bf16)
                delta[head] = jnp.sum(mine * out_t[head, :, at], axis=0, keepdims=True)

            @pl.when(r < rows // 128 - 1)
            def _():
                for copy in fetch(r + 1):
                    copy.start()

        def item(i):
            r, h = i // heads, i % heads

            @pl.when(h == 0)
            def _():
                prepare(r)

            at = pl.ds(pl.multiple_of(r * 128, 128), 128)
            s = jnp.dot(kv[:, 0:hd], q_t[h, :, at], preferred_element_type=f32)
            s = jnp.where(key_pos[...] <= query_pos[0:1, at], s, masked_value)
            p = jnp.exp(s - log_sum[h, :, at])
            dp = jnp.dot(kv[:, hd:], g_t[h], preferred_element_type=f32)
            ds = (p * (dp - delta[h])).astype(bf16)
            dv[...] += jnp.dot(p.astype(bf16), g_n[h], preferred_element_type=f32)
            dk[...] += jnp.dot(ds, q_n[h, at, :], preferred_element_type=f32)
            grad = jnp.dot(k_t[...], ds, preferred_element_type=f32)
            dq_t[h, :, at] = (grad * (1.0 / math.sqrt(hd))).astype(bf16)

        def before(k):
            return progress.whole() < (k // heads + 1) * 4

        order.loop(heads * rows // 128, 1.25, item, before)
        for i in range(keys // rows):
            span = slice(i * rows, (i + 1) * rows)
            kv[span, :] = jnp.concatenate([dk[span, :], dv[span, :]], axis=1).astype(bf16)
        for copy in back:
            copy.start()
        order.until(gate_done)
        pl.semaphore_wait(free_g, 3)

        def low_item(j):
            both.blocks[j, :, lin_cols:] = contract_rows(cot[:, columns(j)], attended[...]).astype(bf16)

        order.loop(8, 0.4, low_item)

    slots = pltpu.VMEM((128, width), bf16)
    pl.run_scoped(
        attention,
        slots,
        slots,
        pltpu.VMEM(wo_all.shape, bf16),
        pltpu.VMEM(out_t_all.shape, f32),
        pltpu.VMEM(attended_all.shape, bf16),
        pltpu.VMEM((heads, hd, 128), bf16),
        pltpu.VMEM((heads, 128, hd), bf16),
        pltpu.VMEM((heads, 1, 128), f32),
        pltpu.VMEM((keys, hd), f32),
        pltpu.VMEM((keys, hd), f32),
    )

    def last(left, right_u, wqkv, normed, lin, gain_one):
        tok = cot
        pairs = ((wqkv_all, wqkv), (normed_two, left), (d_up, right_u), (normed_all, normed), (tok_all, tok))
        loads = [me.local(src, dst) for src, dst in pairs]
        for load in loads:
            load.start()
        gain_one[...] = jnp.zeros_like(gain_one)
        order.until(progress.sent_in, progress.sent_out)
        for copy in back:
            copy.wait_recv()
        mine = kv[0:rows, :].astype(f32)
        for i in range(keys // rows - 1):
            mine = mine + came[i].astype(f32)
        for copy in back:
            copy.wait_send()
        kv[0:rows, :] = mine.astype(bf16)
        for load in (loads[0], loads[3], loads[4]):
            load.wait()

        def finish_item(i):
            at = pl.ds(pl.multiple_of(i * 128, 128), 128)
            grads_kv = kv[at, :].astype(f32).T
            grads = jnp.concatenate(
                [dq_t[h, :, at].astype(f32) for h in range(heads)] + [grads_kv[:hd]], axis=0
            )
            grads = rotate_heads(grads, cos_t[:, at], sin_t[:, at], inverse=True)
            natural = jnp.concatenate([grads, grads_kv[hd:]], axis=0).T.astype(bf16)
            lin[at, :] = natural
            one = contract_last_dims(natural, wqkv[...])
            total[at, :] = one.astype(bf16)
            x = tok[at, :].astype(f32)
            inv = lax.rsqrt(jnp.mean(x * x, axis=1, keepdims=True) + norm_epsilon)
            gain_one[0:1, :] += jnp.sum(one * x * inv, axis=0, keepdims=True)

        order.loop(rows // 128, 2.0, finish_item)
        for i in range(8):
            span = slice(i * cols, (i + 1) * cols)
            gain_parts[i * 8 : (i + 1) * 8, :] = jnp.concatenate(
                [gain_one[0:1, span], gain_two[0:1, span], jnp.zeros((6, cols), f32)], axis=0
            )
        order.until(out_done)
        me.free_along_z(free_z)
        order.add(gains_steps(order.now))
        order.step()
        me.wait_along_z(free_z)
        order.add(z_reduce_scatter(me, total, below, above, grad_one, 12.0, order.now, one_done), order.now)

        order.until(down_done)
        pl.semaphore_wait(free_d, 3)
        loads[1].wait()
        loads[2].wait()

        def up_item(j):
            up.blocks[j] = contract_rows(left[:, columns(j)], right_u[...]).astype(bf16)
            send(up, j)

        order.loop(8, 0.75, up_item)
        order.add(up.steps(dwu_own, 16.5, order.now + 0.1, up_done))
        def both_item(j):
            both.blocks[j, :, :lin_cols] = contract_rows(normed[:, columns(j)], lin[...]).astype(bf16)
            send(both, j)

        order.loop(8, 0.5, both_item)
        order.add(both.steps(dw_own, 13.0, order.now + 0.1, both_done))

    pl.run_scoped(
        last,
        pltpu.VMEM(part.shape, bf16),
        units,
        pltpu.VMEM(wqkv_all.shape, bf16),
        pltpu.VMEM(part.shape, bf16),
        pltpu.VMEM((rows, lin_cols), bf16),
        pltpu.VMEM((8, width), f32),
    )
    order.until(both_done)
    dwkv_own[...] = dw_own[:, wide:lin_cols].astype(bf16)
    for copy in kv_sends:
        copy.start()
    order.finish()
    for copy in kv_sends:
        copy.wait_recv()
    dwkv_all[0] = dwkv_own[...]
    for d in (1, 2, 3):
        dwkv_all[d] = came_kv[d - 1]
    for copy in kv_sends:
        copy.wait_send()


def backward(
    part, cot_all, hidden, normed_two, d_gate, d_up, wd_all, tok_all, branch, gains, wo_all,
    out_t, attended, q_t, q_n, kv_all, wqkv_all, normed, log_sum, key_pos, query_pos, cos_t, sin_t
):
    heads, hd, rows = q_t.shape
    keys = key_pos.shape[0]
    width = part.shape[1]
    cols = width // 8
    whole = pltpu.VMEM(part.shape, bf16)
    own = (wd_all.shape[0] // 8, wd_all.shape[1])
    narrow = wqkv_all.shape[1] + wo_all.shape[1]
    return pl.pallas_call(
        backward_kernel,
        out_shape=(
            shape(own),
            shape(own),
            shape(own),
            shape((own[0], narrow), f32),
            shape((4, own[0], 2 * hd)),
            shape((rows // 4, width), f32),
            shape((rows // 4, width), f32),
            shape((rows // 4, width), f32),
            shape((8, cols), f32),
        ),
        in_specs=[VM] + [HB] * 8 + [VM] + [HB] * 8 + [VM] * 5,
        out_specs=[VM] * 9,
        scratch_shapes=[whole] * 7
        + [
            pltpu.VMEM(q_t.shape, bf16),
            pltpu.VMEM(q_n.shape, bf16),
            pltpu.VMEM((keys, 2 * hd), bf16),
            pltpu.VMEM((hd, keys), bf16),
            pltpu.VMEM((keys // rows - 1, rows, 2 * hd), bf16),
            pltpu.VMEM(q_t.shape, bf16),
            pltpu.VMEM((8, width), f32),
            pltpu.VMEM((64, cols), f32),
            pltpu.VMEM((7, 8, cols), f32),
            pltpu.VMEM((8, cols), f32),
            pltpu.VMEM((3, 8, cols), f32),
            pltpu.VMEM((own[0], 2 * hd), bf16),
            pltpu.VMEM((3, own[0], 2 * hd), bf16),
        ]
        + plane_scatter_scratch(*own) * 2
        + [pltpu.SemaphoreType.REGULAR] * 3
        + dma_sems(224),
        compiler_params=params(4, 67043328),
        name="backward",
    )(
        part, cot_all, hidden, normed_two, d_gate, d_up, wd_all, tok_all, branch, gains, wo_all,
        out_t, attended, q_t, q_n, kv_all, wqkv_all, normed, log_sum, key_pos, query_pos, cos_t, sin_t
    )


def local_fast(
    tokens, w_query, w_key, w_value, w_out, w_gate, w_up, w_down, gain_attn, gain_mlp, stretch_order, cotangent
):
    row_count, width = tokens.shape
    groups = 4
    cols = width // 8
    contract_last = (((1,), (1,)), ((), ()))
    z = lax.axis_index("head")
    own_first = z * row_count

    def own_rows(values):
        return lax.dynamic_slice_in_dim(values, own_first, row_count, 0)

    frequency = rope_base ** (-(np.arange(HD // 2, dtype=np.float32) * np.float32(2.0 / HD)))
    frequency = jnp.asarray(np.broadcast_to(frequency.astype(np.float32)[:, None], (HD // 2, 128)))
    gains = jnp.concatenate([gain_attn[None], gain_mlp[None]]).astype(f32)
    (
        tok_all, wqkv_all, gains_all, wo_all, wd_all, cot_all, kv_all, branch,
        normed, q_t, q_n, out_t, attended, log_sum, key_pos, query_pos, cos_t, sin_t,
        normed_two, hidden, d_gate, d_up, two_part,
    ) = forward(
        stretch_order, tokens, w_query, w_key, w_value, gains, frequency, w_out, cotangent, w_gate, w_up, w_down
    )
    gain_rows = gains_all.reshape(8, 8, cols)
    gain_one = gain_rows[:, 0].reshape(width)
    dwd_own, dwg_own, dwu_own, dw_own, dwkv_all, out_own, grad_hidden_own, grad_one, gain_grads = backward(
        two_part, cot_all, hidden, normed_two, d_gate, d_up, wd_all, tok_all, branch,
        gains_all, wo_all, out_t, attended, q_t, q_n, kv_all, wqkv_all, normed, log_sum, key_pos, query_pos,
        cos_t, sin_t,
    )

    x_own = tokens.astype(f32)
    layer_low = (x_own + own_rows(branch).astype(f32) + out_own).astype(bf16)
    inv_own = lax.rsqrt(jnp.mean(x_own * x_own, axis=-1, keepdims=True) + norm_epsilon)
    grad_tokens = (grad_hidden_own + norm_input_grad(x_own, inv_own, gain_one, grad_one)).astype(bf16)
    slots = jnp.concatenate(
        [lax.dynamic_slice_in_dim(dwkv_all, (z - j) % 4, 1, 0) for j in range(4)], axis=0
    ).astype(f32)
    grad_key = slots[:, :, :HD].transpose(1, 0, 2).reshape(cols, groups * HD)
    grad_value = slots[:, :, HD:].transpose(1, 0, 2).reshape(cols, groups * HD)
    return (
        layer_low,
        grad_tokens,
        dw_own[:, : w_query.shape[1]],
        grad_key,
        grad_value,
        dw_own[:, w_query.shape[1] + 2 * HD :],
        dwg_own.astype(f32),
        dwu_own.astype(f32),
        dwd_own.astype(f32),
        gain_grads[0],
        gain_grads[1],
    )


def solution(mesh):
    sizes = (mesh.shape["fsdp"], mesh.shape["blk"], mesh.shape["head"])
    return jax.shard_map(
        local_fast if sizes == (2, 4, 4) else local,
        mesh=mesh,
        in_specs=(
            P(("fsdp", "blk", "head"), None),
            P(("fsdp", "blk"), "head"),
            P(("fsdp", "blk"), None),
            P(("fsdp", "blk"), None),
            P(("fsdp", "blk"), "head"),
            P(("fsdp", "blk"), "head"),
            P(("fsdp", "blk"), "head"),
            P(("fsdp", "blk"), "head"),
            P(("fsdp", "blk")),
            P(("fsdp", "blk")),
            P(),
            P(("fsdp", "blk", "head"), None),
        ),
        out_specs=(
            P(("fsdp", "blk", "head"), None),
            P(("fsdp", "blk", "head"), None),
            P(("fsdp", "blk"), "head"),
            P(("fsdp", "blk"), None),
            P(("fsdp", "blk"), None),
            P(("fsdp", "blk"), "head"),
            P(("fsdp", "blk"), "head"),
            P(("fsdp", "blk"), "head"),
            P(("fsdp", "blk"), "head"),
            P(("fsdp", "blk")),
            P(("fsdp", "blk")),
        ),
        check_vma=False,
    )
```

```python
import math

import jax
import jax.numpy as jnp
import numpy as np
from jax import lax
from jax.experimental import pallas as pl
from jax.experimental.pallas import tpu as pltpu
from jax.sharding import PartitionSpec as P

H = 32
KV = 4
HD = 64


norm_epsilon = 1e-05
rope_base = 10000.0
masked_value = -1e30


def rope_tables(positions, head_dim):
    half_dim = head_dim // 2
    frequency = rope_base ** (-(jnp.arange(half_dim, dtype=jnp.float32) * (2.0 / head_dim)))
    angles = positions.astype(jnp.float32)[:, None] * frequency[None, :]
    return (jnp.cos(angles), jnp.sin(angles))


def rotate(values, cosine, sine_table):
    half_dim = values.shape[-1] // 2
    first_half = values[..., :half_dim]
    second_half = values[..., half_dim:]
    cos_rows = cosine[:, None, :]
    sin_rows = sine_table[:, None, :]
    return jnp.concatenate(
        [
            first_half * cos_rows - second_half * sin_rows,
            second_half * cos_rows + first_half * sin_rows,
        ],
        axis=-1,
    )


def unrotate(values, cosine, sine_table):
    half_dim = values.shape[-1] // 2
    first_half = values[..., :half_dim]
    second_half = values[..., half_dim:]
    cos_rows = cosine[:, None, :]
    sin_rows = sine_table[:, None, :]
    return jnp.concatenate(
        [
            first_half * cos_rows + second_half * sin_rows,
            second_half * cos_rows - first_half * sin_rows,
        ],
        axis=-1,
    )


def stretch_positions(stretch_order, first_row, row_span, stretch_rows):
    storage = first_row + jnp.arange(row_span, dtype=jnp.int32)
    stretch_index = storage // stretch_rows
    match_table = (
        stretch_index[:, None] == jnp.arange(stretch_order.shape[0], dtype=jnp.int32)[None, :]
    )
    stretch_base = jnp.sum(jnp.where(match_table, stretch_order[None, :], 0), axis=1)
    return stretch_base * stretch_rows + storage % stretch_rows


def norm_input_grad(values, inverse, gain_vector, grad_normed):
    scaled = grad_normed * gain_vector
    inner = jnp.mean(scaled * values, axis=-1, keepdims=True)
    return inverse * scaled - values * inverse * inverse * inverse * inner


def gain_grad(values, inverse, grad_normed):
    return jnp.sum(grad_normed * values * inverse, axis=0)


def fold_block(
    state_now, keys_block, values_block, key_positions, query_heads, query_positions, score_scale
):
    running_max, running_sum, running_out = state_now
    scores = (
        jnp.einsum("qhd,kd->hqk", query_heads, keys_block, preferred_element_type=jnp.float32)
        * score_scale
    )
    allowed = (query_positions[:, None] >= key_positions[None, :])[None]
    scores = jnp.where(allowed, scores, masked_value)
    new_max = jnp.maximum(running_max, jnp.max(scores, axis=-1))
    weights = jnp.where(allowed, jnp.exp(scores - new_max[..., None]), 0.0)
    factor = jnp.exp(running_max - new_max)
    running_sum = running_sum * factor + jnp.sum(weights, axis=-1)
    running_out = running_out * factor[..., None] + jnp.einsum(
        "hqk,kd->hqd",
        weights.astype(jnp.bfloat16),
        values_block,
        preferred_element_type=jnp.float32,
    )
    return (new_max, running_sum, running_out)


def local(
    tokens,
    w_query,
    w_key,
    w_value,
    w_out,
    w_gate,
    w_up,
    w_down,
    gain_attn,
    gain_mlp,
    stretch_order,
    cotangent,
):
    row_count = tokens.shape[0]
    groups = lax.axis_size("head")
    blocks = lax.axis_size("blk")
    local_heads = H // groups
    repeats = groups // KV
    head_rows = row_count * groups
    stretch_rows = head_rows // 2
    score_scale = 1.0 / math.sqrt(HD)
    contract_last = (((1,), (1,)), ((), ()))
    contract_first = (((0,), (0,)), ((), ()))
    head_index = lax.axis_index("head")
    own_first = head_index * row_count
    block_first = lax.axis_index("blk") * head_rows
    positions = stretch_positions(stretch_order, block_first + own_first, row_count, stretch_rows)
    query_positions = stretch_positions(stretch_order, block_first, head_rows, stretch_rows)
    cos_own, sin_own = rope_tables(positions, HD)
    cos_block, sin_block = rope_tables(query_positions, HD)

    def layer_weights():
        return (
            lax.all_gather(w_query, ("fsdp", "blk"), axis=0, tiled=True),
            lax.all_gather(w_key, ("fsdp", "blk"), axis=0, tiled=True),
            lax.all_gather(w_value, ("fsdp", "blk"), axis=0, tiled=True),
            lax.all_gather(w_out, ("fsdp", "blk"), axis=0, tiled=True),
            lax.all_gather(w_gate, ("fsdp", "blk"), axis=0, tiled=True),
            lax.all_gather(w_up, ("fsdp", "blk"), axis=0, tiled=True),
            lax.all_gather(w_down, ("fsdp", "blk"), axis=0, tiled=True),
            lax.all_gather(gain_attn, ("fsdp", "blk"), axis=0, tiled=True),
            lax.all_gather(gain_mlp, ("fsdp", "blk"), axis=0, tiled=True),
        )

    def gather_query(columns):
        return lax.all_gather(columns, "head", axis=1, tiled=True)

    (
        query_cols,
        key_full,
        value_full,
        out_cols,
        gate_cols,
        up_cols,
        down_cols,
        gain_one,
        gain_two,
    ) = layer_weights()
    tokens_float = tokens.astype(jnp.float32)
    inv_attn = lax.rsqrt(
        jnp.mean(tokens_float * tokens_float, axis=-1, keepdims=True) + norm_epsilon
    )
    normed = (tokens_float * inv_attn * gain_one.astype(jnp.float32)).astype(jnp.bfloat16)
    normed_rows, cotangent_rows = (
        lax.all_gather(normed, "head", axis=0, tiled=True),
        lax.all_gather(cotangent, "head", axis=0, tiled=True),
    )
    query_all = gather_query(query_cols)
    query_lin = jnp.dot(normed, query_all, preferred_element_type=jnp.float32).reshape(
        row_count, H, HD
    )
    key_lin = jnp.dot(normed, key_full, preferred_element_type=jnp.float32).reshape(
        row_count, KV, HD
    )
    value_lin = jnp.dot(normed, value_full, preferred_element_type=jnp.float32).reshape(
        row_count, KV, HD
    )
    query_rot = rotate(query_lin, cos_own, sin_own).astype(jnp.bfloat16).reshape(row_count, H * HD)
    key_rot = rotate(key_lin, cos_own, sin_own).astype(jnp.bfloat16)
    key_slots = jnp.repeat(key_rot, repeats, axis=1).reshape(row_count, groups * HD)
    value_slots = jnp.repeat(value_lin.astype(jnp.bfloat16), repeats, axis=1).reshape(
        row_count, groups * HD
    )
    query_recv, key_own, value_own = (
        lax.all_to_all(query_rot, "head", split_axis=1, concat_axis=0, tiled=True),
        lax.all_to_all(key_slots, "head", split_axis=1, concat_axis=0, tiled=True),
        lax.all_to_all(value_slots, "head", split_axis=1, concat_axis=0, tiled=True),
    )
    query_heads = query_recv.reshape(head_rows, local_heads, HD)
    initial = (
        jnp.full((local_heads, head_rows), masked_value, jnp.float32),
        jnp.zeros((local_heads, head_rows), jnp.float32),
        jnp.zeros((local_heads, head_rows, HD), jnp.float32),
    )
    state_now = initial
    keys_piece = lax.all_gather(key_own, "blk", axis=0, tiled=True)
    values_piece = lax.all_gather(value_own, "blk", axis=0, tiled=True)
    piece_rows = keys_piece.shape[0]

    def scan_step(state_inner, step_index):
        offset = step_index * head_rows
        keys_block = lax.dynamic_slice_in_dim(keys_piece, offset, head_rows, 0)
        values_block = lax.dynamic_slice_in_dim(values_piece, offset, head_rows, 0)
        key_positions = stretch_positions(stretch_order, offset, head_rows, stretch_rows)
        return (
            fold_block(
                state_inner,
                keys_block,
                values_block,
                key_positions,
                query_heads,
                query_positions,
                score_scale,
            ),
            None,
        )

    state_now, unused = lax.scan(
        scan_step, state_now, jnp.arange(piece_rows // head_rows, dtype=jnp.int32)
    )
    running_max, running_sum, running_out = state_now
    attended_float = running_out / running_sum[..., None]
    log_sum = running_max + jnp.log(running_sum)
    attended_heads = (
        attended_float.astype(jnp.bfloat16).transpose(1, 0, 2).reshape(head_rows, local_heads * HD)
    )
    branch = lax.dot_general(
        attended_heads, out_cols, contract_last, preferred_element_type=jnp.float32
    )
    own_branch = lax.dynamic_slice_in_dim(branch, own_first, row_count, 0)
    partial_value = lax.dynamic_update_slice_in_dim(branch, own_branch + tokens_float, own_first, 0)
    hidden_rows = lax.psum(partial_value.astype(jnp.bfloat16), "head").astype(jnp.float32)
    inv_mlp = lax.rsqrt(jnp.mean(hidden_rows * hidden_rows, axis=-1, keepdims=True) + norm_epsilon)
    normed_two_rows = (hidden_rows * inv_mlp * gain_two.astype(jnp.float32)).astype(jnp.bfloat16)
    gate_proj = jnp.dot(normed_two_rows, gate_cols, preferred_element_type=jnp.float32)
    up_proj = jnp.dot(normed_two_rows, up_cols, preferred_element_type=jnp.float32)
    gate_sigmoid = jax.nn.sigmoid(gate_proj)
    gate_silu = gate_proj * gate_sigmoid
    hidden = (gate_silu * up_proj).astype(jnp.bfloat16)
    hidden_own = lax.dynamic_slice_in_dim(hidden_rows, own_first, row_count, 0)
    output_float = hidden_own + lax.psum_scatter(
        lax.dot_general(
            hidden, down_cols, contract_last, preferred_element_type=jnp.float32
        ).astype(jnp.bfloat16),
        "head",
        scatter_dimension=0,
        tiled=True,
    ).astype(jnp.float32)
    layer_low = output_float.astype(jnp.bfloat16)
    (
        query_cols,
        key_full,
        value_full,
        out_cols,
        gate_cols,
        up_cols,
        down_cols,
        gain_one,
        gain_two,
    ) = layer_weights()
    query_all = gather_query(query_cols)
    grad_hidden = jnp.dot(cotangent_rows, down_cols, preferred_element_type=jnp.float32)
    grad_gate_rows = (
        grad_hidden * up_proj * gate_sigmoid * (1.0 + gate_proj * (1.0 - gate_sigmoid))
    ).astype(jnp.bfloat16)
    grad_up_rows = (grad_hidden * gate_silu).astype(jnp.bfloat16)
    grad_w_down = lax.dot_general(
        cotangent_rows, hidden, contract_first, preferred_element_type=jnp.float32
    )
    grad_w_gate = lax.dot_general(
        normed_two_rows, grad_gate_rows, contract_first, preferred_element_type=jnp.float32
    )
    grad_w_up = lax.dot_general(
        normed_two_rows, grad_up_rows, contract_first, preferred_element_type=jnp.float32
    )
    normed_two_part = lax.dot_general(
        grad_gate_rows, gate_cols, contract_last, preferred_element_type=jnp.float32
    )
    normed_two_part = normed_two_part + lax.dot_general(
        grad_up_rows, up_cols, contract_last, preferred_element_type=jnp.float32
    )
    grad_normed_two = lax.psum(normed_two_part.astype(jnp.bfloat16), "head").astype(jnp.float32)
    gain_two_float = gain_two.astype(jnp.float32)
    grad_hidden_rows = cotangent_rows.astype(jnp.float32) + norm_input_grad(
        hidden_rows, inv_mlp, gain_two_float, grad_normed_two
    )
    own_grad_two = lax.dynamic_slice_in_dim(grad_normed_two, own_first, row_count, 0)
    own_inv_mlp = lax.dynamic_slice_in_dim(inv_mlp, own_first, row_count, 0)
    grad_gain_two = gain_grad(hidden_own, own_inv_mlp, own_grad_two)
    grad_low_rows = grad_hidden_rows.astype(jnp.bfloat16)
    grad_w_out = lax.dot_general(
        grad_low_rows, attended_heads, contract_first, preferred_element_type=jnp.float32
    )
    grad_heads = (
        jnp.dot(grad_low_rows, out_cols, preferred_element_type=jnp.float32)
        .astype(jnp.bfloat16)
        .reshape(head_rows, local_heads, HD)
    )
    keys_all, values_all = (
        lax.all_gather(key_own, "blk", axis=0, tiled=True),
        lax.all_gather(value_own, "blk", axis=0, tiled=True),
    )
    row_delta = jnp.sum(grad_heads.astype(jnp.float32).transpose(1, 0, 2) * attended_float, axis=-1)

    def back_block(grad_query_acc, block_index):
        offset = block_index * head_rows
        keys_block = lax.dynamic_slice_in_dim(keys_all, offset, head_rows, 0)
        values_block = lax.dynamic_slice_in_dim(values_all, offset, head_rows, 0)
        key_positions = stretch_positions(stretch_order, offset, head_rows, stretch_rows)
        scores = (
            jnp.einsum("qhd,kd->hqk", query_heads, keys_block, preferred_element_type=jnp.float32)
            * score_scale
        )
        allowed = (query_positions[:, None] >= key_positions[None, :])[None]
        probs_block = jnp.where(allowed, jnp.exp(scores - log_sum[..., None]), 0.0)
        grad_probs = jnp.einsum(
            "qhd,kd->hqk", grad_heads, values_block, preferred_element_type=jnp.float32
        )
        grad_scores = (probs_block * (grad_probs - row_delta[..., None])).astype(jnp.bfloat16)
        grad_query_acc = grad_query_acc + jnp.einsum(
            "hqk,kd->qhd", grad_scores, keys_block, preferred_element_type=jnp.float32
        )
        grad_key_part = (
            jnp.einsum("hqk,qhd->kd", grad_scores, query_heads, preferred_element_type=jnp.float32)
            * score_scale
        )
        grad_value_part = jnp.einsum(
            "hqk,qhd->kd",
            probs_block.astype(jnp.bfloat16),
            grad_heads,
            preferred_element_type=jnp.float32,
        )
        return (grad_query_acc, (grad_key_part, grad_value_part))

    grad_query_acc, (key_terms, value_terms) = lax.scan(
        back_block,
        jnp.zeros((head_rows, local_heads, HD), jnp.float32),
        jnp.arange(blocks, dtype=jnp.int32),
    )
    grad_key_sum, grad_value_sum = (
        lax.psum_scatter(
            key_terms.reshape(blocks * head_rows, HD).astype(jnp.bfloat16),
            "blk",
            scatter_dimension=0,
            tiled=True,
        ).astype(jnp.float32),
        lax.psum_scatter(
            value_terms.reshape(blocks * head_rows, HD).astype(jnp.bfloat16),
            "blk",
            scatter_dimension=0,
            tiled=True,
        ).astype(jnp.float32),
    )
    grad_query_rot = (grad_query_acc * score_scale).astype(jnp.bfloat16)
    grad_query_lin_heads = (
        unrotate(grad_query_rot.astype(jnp.float32), cos_block, sin_block)
        .astype(jnp.bfloat16)
        .reshape(head_rows, local_heads * HD)
    )
    key_slot_grad = grad_key_sum.astype(jnp.bfloat16)
    value_slot_grad = grad_value_sum.astype(jnp.bfloat16)
    grad_w_query = lax.dot_general(
        normed_rows, grad_query_lin_heads, contract_first, preferred_element_type=jnp.float32
    )
    query_back, key_back, value_back = (
        lax.all_to_all(grad_query_lin_heads, "head", split_axis=0, concat_axis=1, tiled=True),
        lax.all_to_all(key_slot_grad, "head", split_axis=0, concat_axis=1, tiled=True),
        lax.all_to_all(value_slot_grad, "head", split_axis=0, concat_axis=1, tiled=True),
    )
    key_slot_lin = (
        unrotate(key_back.astype(jnp.float32).reshape(row_count, groups, HD), cos_own, sin_own)
        .astype(jnp.bfloat16)
        .reshape(row_count, KV, repeats, HD)
    )
    value_slot_lin = value_back.reshape(row_count, KV, repeats, HD)
    grad_w_key = jnp.einsum(
        "td,tjrc->djc", normed, key_slot_lin, preferred_element_type=jnp.float32
    ).reshape(-1, KV * HD)
    grad_w_value = jnp.einsum(
        "td,tjrc->djc", normed, value_slot_lin, preferred_element_type=jnp.float32
    ).reshape(-1, KV * HD)
    grad_normed = lax.dot_general(
        query_back, query_all, contract_last, preferred_element_type=jnp.float32
    )
    grad_normed = grad_normed + jnp.einsum(
        "tjrc,djc->td",
        key_slot_lin,
        key_full.reshape(-1, KV, HD),
        preferred_element_type=jnp.float32,
    )
    grad_normed = grad_normed + jnp.einsum(
        "tjrc,djc->td",
        value_slot_lin,
        value_full.reshape(-1, KV, HD),
        preferred_element_type=jnp.float32,
    )
    gain_one_float = gain_one.astype(jnp.float32)
    grad_input_norm = norm_input_grad(tokens_float, inv_attn, gain_one_float, grad_normed)
    grad_gain_one = gain_grad(tokens_float, inv_attn, grad_normed)
    grad_hidden_own = lax.dynamic_slice_in_dim(grad_hidden_rows, own_first, row_count, 0)
    grad_tokens = (grad_hidden_own + grad_input_norm).astype(jnp.bfloat16)
    head_sums = (
        lax.psum(grad_w_key.astype(jnp.bfloat16), "head").astype(jnp.float32),
        lax.psum(grad_w_value.astype(jnp.bfloat16), "head").astype(jnp.float32),
        lax.psum(grad_gain_one.astype(jnp.bfloat16), "head").astype(jnp.float32),
        lax.psum(grad_gain_two.astype(jnp.bfloat16), "head").astype(jnp.float32),
    )
    reduced = (
        lax.psum_scatter(
            grad_w_query.astype(jnp.bfloat16), ("fsdp", "blk"), scatter_dimension=0, tiled=True
        ).astype(jnp.float32),
        lax.psum_scatter(
            head_sums[0].astype(jnp.bfloat16), ("fsdp", "blk"), scatter_dimension=0, tiled=True
        ).astype(jnp.float32),
        lax.psum_scatter(
            head_sums[1].astype(jnp.bfloat16), ("fsdp", "blk"), scatter_dimension=0, tiled=True
        ).astype(jnp.float32),
        lax.psum_scatter(
            grad_w_out.astype(jnp.bfloat16), ("fsdp", "blk"), scatter_dimension=0, tiled=True
        ).astype(jnp.float32),
        lax.psum_scatter(
            grad_w_gate.astype(jnp.bfloat16), ("fsdp", "blk"), scatter_dimension=0, tiled=True
        ).astype(jnp.float32),
        lax.psum_scatter(
            grad_w_up.astype(jnp.bfloat16), ("fsdp", "blk"), scatter_dimension=0, tiled=True
        ).astype(jnp.float32),
        lax.psum_scatter(
            grad_w_down.astype(jnp.bfloat16), ("fsdp", "blk"), scatter_dimension=0, tiled=True
        ).astype(jnp.float32),
        lax.psum_scatter(
            head_sums[2].astype(jnp.bfloat16), ("fsdp", "blk"), scatter_dimension=0, tiled=True
        ).astype(jnp.float32),
        lax.psum_scatter(
            head_sums[3].astype(jnp.bfloat16), ("fsdp", "blk"), scatter_dimension=0, tiled=True
        ).astype(jnp.float32),
    )
    return (
        layer_low,
        grad_tokens,
        reduced[0],
        reduced[1],
        reduced[2],
        reduced[3],
        reduced[4],
        reduced[5],
        reduced[6],
        reduced[7],
        reduced[8],
    )


MESH = pl.DeviceIdType.MESH
f32, bf16 = jnp.float32, jnp.bfloat16
VM = pl.BlockSpec(memory_space=pltpu.VMEM)
HB = pl.BlockSpec(memory_space=pl.ANY)


def dma_sems(n):
    return [pltpu.SemaphoreType.DMA((n,)), pltpu.SemaphoreType.DMA((n,))]


class Here:
    def __init__(self, send_sem, recv_sem):
        self.y = lax.axis_index("fsdp")
        blk = lax.axis_index("blk")
        self.x, self.c = blk // 2, blk % 2
        self.z = lax.axis_index("head")
        self.end = (self.z == 0) | (self.z == 3)
        self.middle = (self.z == 1) | (self.z == 2)
        self.inward = {"head": jnp.where(self.z < 2, self.z + 1, self.z - 1)}
        self.outward = {"head": jnp.where(self.z < 2, self.z - 1, self.z + 1)}
        self.send_sem, self.recv_sem, self.used = send_sem, recv_sem, 0

    def plane(self, i):
        y = 1 - self.y if i & 4 else self.y
        x = 1 - self.x if i & 2 else self.x
        c = 1 - self.c if i & 1 else self.c
        return {"fsdp": y, "blk": x * 2 + c}

    def number(self, i):
        at = self.plane(i)
        return at["fsdp"] * 4 + at["blk"]

    def up(self):
        return {"head": self.z + 1}

    def down(self):
        return {"head": self.z - 1}

    def copy(self, src, dst, device):
        k = self.used
        self.used += 1
        return self.again(k, src, dst, device)

    def slot(self):
        self.used += 1
        return self.used - 1

    def again(self, k, src, dst, device):
        return pltpu.make_async_remote_copy(
            src_ref=src,
            dst_ref=dst,
            send_sem=self.send_sem.at[k],
            recv_sem=self.recv_sem.at[k],
            device_id=device,
            device_id_type=MESH,
        )

    def local(self, src, dst):
        k = self.used
        self.used += 1
        return pltpu.make_async_copy(src, dst, self.send_sem.at[k])

    def free_in_plane(self, sem):
        for i in (1, 2, 4):
            pl.semaphore_signal(sem, inc=1, device_id=self.plane(i), device_id_type=MESH)

    def free_along_z(self, sem):
        @pl.when(self.z > 0)
        def _():
            pl.semaphore_signal(sem, inc=1, device_id=self.down(), device_id_type=MESH)

        @pl.when(self.z < 3)
        def _():
            pl.semaphore_signal(sem, inc=1, device_id=self.up(), device_id_type=MESH)

    def wait_along_z(self, sem):
        pl.semaphore_wait(sem, jnp.where(self.z > 0, 1, 0) + jnp.where(self.z < 3, 1, 0))

    def enter(self, offsets, along_z=True, all_z=False):
        bar = pltpu.get_barrier_semaphore()
        for i in offsets:
            pl.semaphore_signal(bar, inc=1, device_id=self.plane(i), device_id_type=MESH)
        if all_z:
            for d in (1, 2, 3):
                pl.semaphore_signal(
                    bar, inc=1, device_id={"head": (self.z + d) % 4}, device_id_type=MESH
                )
            pl.semaphore_wait(bar, len(offsets) + 3)
            return
        if along_z:

            @pl.when(self.z > 0)
            def _():
                pl.semaphore_signal(bar, inc=1, device_id=self.down(), device_id_type=MESH)

            @pl.when(self.z < 3)
            def _():
                pl.semaphore_signal(bar, inc=1, device_id=self.up(), device_id_type=MESH)

        peers = len(offsets)
        if along_z:
            peers = peers + jnp.where(self.z > 0, 1, 0) + jnp.where(self.z < 3, 1, 0)
        pl.semaphore_wait(bar, peers)


class Order:
    def __init__(self, *tasks):
        self.now, self.count, self.waiting = 0.0, 0, []
        for task in tasks:
            self.add(task)

    def add(self, task, at=None):
        self.waiting.append((self.now if at is None else at, self.count, task))
        self.count += 1

    def next_at(self):
        return min(self.waiting, default=(math.inf,))[0]

    def step(self):
        item = min(self.waiting, key=lambda entry: entry[:2])
        self.waiting.remove(item)
        at = next(item[2], None)
        if at is not None:
            self.waiting.append((max(at, item[0]), item[1], item[2]))

    def pump(self, until):
        while self.next_at() <= until:
            self.step()
        self.now = max(self.now, until)

    def until(self, *flags):
        while not all(flag.up for flag in flags):
            self.now = max(self.now, self.next_at())
            self.step()

    def finish(self):
        while self.waiting:
            self.step()

    def loop(self, n, each, item, before=None):
        start = self.now

        def body(i, _):
            for k in range(n):
                while self.waiting and (
                    self.next_at() <= start + k * each or (before is not None and before(k))
                ):

                    @pl.when(i == k)
                    def _():
                        self.step()

            item(i)
            return 0

        lax.fori_loop(0, n, body, 0)
        self.now = start + n * each


def drive(*tasks):
    Order(*tasks).finish()


class Flag:
    def __init__(self):
        self.up = False


def z_gather(me, src, dst, unit, begin=0.0, done=None, issue=None):
    rows = src.shape[0]
    half = rows // 2
    z = me.z

    def block(j, h):
        return dst.at[pl.ds(pl.multiple_of(j * rows + h * half, half), half)]

    ups = [me.slot() for _ in range(6)]
    downs = [me.slot() for _ in range(6)]
    own = me.local(src, dst.at[pl.ds(pl.multiple_of(z * rows, rows), rows)])

    def up(j, h):
        mine = src.at[pl.ds(h * half, half)] if j == 0 else block(z - j, h)
        return me.again(ups[2 * j + h], mine, block(z - j, h), me.up())

    def down(j, h):
        mine = src.at[pl.ds(h * half, half)] if j == 0 else block(z + j, h)
        return me.again(downs[2 * j + h], mine, block(z + j, h), me.down())

    def steps():
        yield begin if issue is None else issue

        @pl.when(z < 3)
        def _():
            up(0, 0).start()
            up(0, 1).start()

        @pl.when(z > 0)
        def _():
            down(0, 0).start()
            down(0, 1).start()

        own.start()
        for j in (1, 2, 3):
            for h in (0, 1):
                yield begin + unit * (j - 0.5 + h * 0.5) + 1.8 + 0.4 * j

                @pl.when(z >= j)
                def _():
                    up(j - 1, h).wait_recv()

                if j < 3:

                    @pl.when((z >= j) & (z < 3))
                    def _():
                        up(j, h).start()

                @pl.when(z <= 3 - j)
                def _():
                    down(j - 1, h).wait_recv()

                if j < 3:

                    @pl.when((z <= 3 - j) & (z > 0))
                    def _():
                        down(j, h).start()

        own.wait()
        if done is not None:
            done.up = True
        yield begin + unit * 3 + 15.0
        for j in (0, 1, 2):

            @pl.when((z >= j) & (z < 3))
            def _():
                up(j, 0).wait_send()
                up(j, 1).wait_send()

            @pl.when((z <= 3 - j) & (z > 0))
            def _():
                down(j, 0).wait_send()
                down(j, 1).wait_send()

    return steps()


def plane_gather(me, src, dst, unit, begin=0.0, done=None, issue=None):
    rows = src.shape[0]
    half = rows // 2

    def part(i, h):
        return dst.at[pl.ds(pl.multiple_of(me.number(i) * rows + h * half, half), half)]

    def block(i):
        return dst.at[pl.ds(pl.multiple_of(me.number(i) * rows, rows), rows)]

    halves = src.at[pl.ds(0, half)], src.at[pl.ds(half, half)]
    x_in = [me.copy(halves[h], part(0, h), me.plane(2)) for h in (0, 1)]
    y_in = [me.copy(halves[h], part(0, h), me.plane(4)) for h in (1, 0)]
    to_c = me.copy(src, block(0), me.plane(1))
    own = me.local(src, block(0))
    x_on = me.copy(part(2, 0), part(2, 0), me.plane(4))
    y_on = me.copy(part(4, 1), part(4, 1), me.plane(2))
    x_core = me.copy(block(2), block(2), me.plane(1))
    y_core = me.copy(block(4), block(4), me.plane(1))
    far = [me.copy(part(6, h), part(6, h), me.plane(1)) for h in (0, 1)]

    def steps():
        yield begin if issue is None else issue
        for copy in (x_in[0], y_in[0], x_in[1], y_in[1], to_c, own):
            copy.start()
        yield begin + unit * 0.5 + 2.0
        x_in[0].wait_recv()
        x_on.start()
        y_in[0].wait_recv()
        y_on.start()
        yield begin + unit + 2.5
        x_in[1].wait_recv()
        x_core.start()
        y_in[1].wait_recv()
        y_core.start()
        yield begin + unit * 1.5 + 4.5
        x_on.wait_recv()
        far[0].start()
        y_on.wait_recv()
        far[1].start()
        yield begin + unit * 1.5 + 6.5
        own.wait()
        for copy in (to_c, x_core, y_core, *far):
            copy.wait_recv()
        if done is not None:
            done.up = True
        yield begin + unit * 1.5 + 15.0
        for copy in (*x_in, *y_in, to_c, x_on, x_core, y_on, y_core, *far):
            copy.wait_send()

    return steps()


def plane_direct(me, src, dst, done):
    rows = src.shape[0]
    place = dst.at[pl.ds(pl.multiple_of(me.number(0) * rows, rows), rows)]
    copies = [me.copy(src, place, me.plane(i)) for i in range(1, 8)]
    own = me.local(src, place)

    def steps():
        for copy in (*copies, own):
            copy.start()
        yield 5.0
        own.wait()
        for copy in copies:
            copy.wait_recv()
        done.up = True
        yield 15.0
        for copy in copies:
            copy.wait_send()

    return steps()


def add_rows(dst, a, b, step=32):
    rows = a.shape[0]

    def body(i, _):
        at = pl.ds(pl.multiple_of(i * step, step), step)
        dst[at, :] = (a[at, :].astype(f32) + b[at, :].astype(f32)).astype(dst.dtype)
        return 0

    lax.fori_loop(0, rows // step, body, 0)


class Progress:
    def __init__(self, parts):
        self.parts, self.entered, self.crossed, self.left = parts, 0, 0, 0
        self.sent_in, self.sent_out = Flag(), Flag()

    def whole(self):
        return min(self.crossed, self.left)


def z_reduce_all(me, part, total, inbox, across, out, unit, chunks, progress, begin=0.0, lag=0.0):
    rows = part.shape[0] // chunks
    first = [me.slot() for _ in range(chunks)]
    second = [me.slot() for _ in range(chunks)]
    third = [me.slot() for _ in range(chunks)]
    store = [me.slot() for _ in range(chunks)]
    hop = unit / chunks

    def at(ref, k):
        return ref.at[pl.ds(k * rows, rows)]

    def send_in(k):
        return me.again(first[k], at(part, k), at(inbox, k), me.inward)

    def send_across(k):
        return me.again(second[k], at(inbox, k), at(across, k), me.inward)

    def send_out(k):
        return me.again(third[k], at(total, k), at(total, k), me.outward)

    def put(k):
        return pltpu.make_async_copy(at(total, k), at(out, k), me.send_sem.at[store[k]])

    def entering():
        yield begin
        time, sent = begin, 0
        for k in range(chunks):
            while k >= progress.parts:
                time += 0.5
                yield time
            new, sent = range(sent, progress.parts), progress.parts
            if len(new):

                @pl.when(me.end)
                def _():
                    for j in new:
                        send_in(j).start()

            time = max(time, begin + lag + 2.0) + hop
            yield time

            @pl.when(me.middle)
            def _():
                send_in(k).wait_recv()
                add_rows(at(inbox, k), at(part, k), at(inbox, k))
                send_across(k).start()

            progress.entered = k + 1
        yield time + 20.0

        @pl.when(me.end)
        def _():
            for k in range(chunks):
                send_in(k).wait_send()

        progress.sent_in.up = True

    def crossing():
        yield begin
        time = begin
        for k in range(chunks):
            while k >= progress.entered:
                time += 0.5
                yield time
            time = max(time, begin + lag + 4.0 + hop) + hop
            yield time

            @pl.when(me.middle)
            def _():
                send_across(k).wait_recv()
                add_rows(at(total, k), at(inbox, k), at(across, k))
                send_out(k).start()
                if out is not None:
                    put(k).start()

            progress.crossed = k + 1
        yield time + 10.0

        @pl.when(me.middle)
        def _():
            for k in range(chunks):
                send_across(k).wait_send()
                send_out(k).wait_send()

        progress.sent_out.up = True

    def leaving():
        yield begin
        time = begin
        for k in range(chunks):
            while k >= progress.crossed:
                time += 0.5
                yield time
            time = max(time, begin + lag + 6.0 + 2 * hop) + hop
            yield time

            @pl.when(me.end)
            def _():
                send_out(k).wait_recv()
                if out is not None:
                    put(k).start()

            progress.left = k + 1
        if out is not None:
            yield time + 2.0
            for k in range(chunks):
                put(k).wait()

    return entering(), crossing(), leaving()


def z_reduce_scatter(me, part, from_below, from_above, own, unit, begin=0.0, done=None):
    rows = part.shape[0] // 4
    z = me.z
    ups = [me.slot() for _ in range(4)]
    downs = [me.slot() for _ in range(4)]

    def at(ref, j):
        return ref.at[pl.ds(j * rows, rows)]

    def up(j, source):
        return me.again(ups[j], at(source, j), at(from_below, j), me.up())

    def down(j, source):
        return me.again(downs[j], at(source, j), at(from_above, j), me.down())

    def start(j):
        @pl.when(z == 0)
        def _():
            up(j, part).start()

        @pl.when(z == 3)
        def _():
            down(3 - j, part).start()

    def relay(j, stop):
        @pl.when(z == stop)
        def _():
            up(j, part).wait_recv()
            add_rows(at(from_below, j), at(part, j), at(from_below, j))
            up(j, from_below).start()

        @pl.when(z == 3 - stop)
        def _():
            i = 3 - j
            down(i, part).wait_recv()
            add_rows(at(from_above, i), at(part, i), at(from_above, i))
            down(i, from_above).start()

    yield begin
    start(3)
    yield begin + unit * 0.6
    start(2)
    yield begin + unit + 1.0
    relay(3, 1)
    yield begin + unit * 1.6
    start(1)
    yield begin + unit * 2 + 1.0
    relay(3, 2)
    relay(2, 1)
    yield begin + unit * 3 + 1.5
    for j in range(4):

        @pl.when(z == j)
        def _():
            if j > 0:
                up(j, part).wait_recv()
            if j < 3:
                down(j, part).wait_recv()

            def body(i, _):
                span = pl.ds(pl.multiple_of(i * 32, 32), 32)
                there = pl.ds(pl.multiple_of(j * rows + i * 32, 32), 32)
                value = part[there, :].astype(f32)
                if j > 0:
                    value = value + from_below[there, :].astype(f32)
                if j < 3:
                    value = value + from_above[there, :].astype(f32)
                own[span, :] = value
                return 0

            lax.fori_loop(0, rows // 32, body, 0)
            for i in range(4):
                if i > j:
                    up(i, part).wait_send()
                if i < j:
                    down(i, part).wait_send()

    if done is not None:
        done.up = True


def offsets_of(me, j):
    dx, dy, dc = 1 - (j % 4) // 2, 1 - j % 2, 1 - j // 4
    y = me.y + dy - 2 * me.y * dy
    x = me.x + dx - 2 * me.x * dx
    c = me.c + dc - 2 * me.c * dc
    return y * 4 + x * 2 + c


def plane_scatter_scratch(rows, cols):
    half = rows // 2
    return [
        pltpu.VMEM((8, rows, cols), bf16),
        pltpu.VMEM((4, rows, cols), bf16),
        pltpu.VMEM((2, half, cols), bf16),
        pltpu.VMEM((2, half, cols), bf16),
        pltpu.VMEM((half, cols), bf16),
        pltpu.VMEM((half, cols), bf16),
    ]


class PlaneScatter:
    def __init__(self, me, scratch):
        self.me = me
        self.blocks, self.other, self.over_x, self.over_y, self.last_y, self.last_x = scratch
        blocks, rows = self.blocks, self.blocks.shape[1]
        half = rows // 2
        self.half, self.first, self.second = half, pl.ds(0, half), pl.ds(half, half)
        first, second = self.first, self.second
        self.core = [me.copy(blocks.at[j], self.other.at[j], me.plane(1)) for j in range(4)]
        self.far_x = me.copy(blocks.at[4, first], self.over_x.at[1], me.plane(2))
        self.far_y = me.copy(blocks.at[4, second], self.over_y.at[1], me.plane(4))
        self.near_x = me.copy(blocks.at[5, first], self.over_x.at[0], me.plane(2))
        self.near_y = me.copy(blocks.at[6, second], self.over_y.at[0], me.plane(4))
        self.to_y = me.copy(blocks.at[6, first], self.last_y, me.plane(4))
        self.to_x = me.copy(blocks.at[5, second], self.last_x, me.plane(2))

    def steps(self, out, unit, begin, done, free=None):
        blocks, half, first, second = self.blocks, self.half, self.first, self.second
        for j in range(4):
            yield begin + 0.3 * j
            self.core[j].wait_recv()
            add_rows(blocks.at[4 + j], blocks.at[4 + j], self.other.at[j])
            if j == 0:
                self.far_x.start()
                self.far_y.start()
            if j == 1:
                self.near_x.start()
            if j == 2:
                self.near_y.start()
        yield begin + 3.0 + unit * 0.5
        self.far_x.wait_recv()
        add_rows(blocks.at[6, first], blocks.at[6, first], self.over_x.at[1])
        self.to_y.start()
        self.far_y.wait_recv()
        add_rows(blocks.at[5, second], blocks.at[5, second], self.over_y.at[1])
        self.to_x.start()
        yield begin + 4.0 + unit * 1.5
        for copy in (self.near_x, self.near_y, self.to_y, self.to_x):
            copy.wait_recv()

        def body(i, _):
            at = pl.ds(pl.multiple_of(i * 32, 32), 32)
            low = pl.ds(pl.multiple_of(half + i * 32, 32), 32)
            for rows, near, last in ((at, self.over_x, self.last_y), (low, self.over_y, self.last_x)):
                value = blocks[7, rows, :].astype(f32) + near[0, at, :].astype(f32)
                out[rows, :] = (value + last[at, :].astype(f32)).astype(out.dtype)
            return 0

        lax.fori_loop(0, half // 32, body, 0)
        for copy in (*self.core, self.far_x, self.far_y, self.near_x, self.near_y, self.to_y, self.to_x):
            copy.wait_send()
        done.up = True
        if free is not None:
            self.me.free_in_plane(free)


def params(number, vmem=60 * 2**20):
    return pltpu.CompilerParams(
        collective_id=number, has_side_effects=True, vmem_limit_bytes=vmem
    )


def shape(dims, kind=bf16):
    return jax.ShapeDtypeStruct(dims, kind)


def alone(flops, vmem=60 * 2**20):
    return dict(
        compiler_params=pltpu.CompilerParams(vmem_limit_bytes=vmem),
        cost_estimate=pl.CostEstimate(flops=int(flops), bytes_accessed=2**23, transcendentals=0),
    )


def gain_row(gains, which):
    return jnp.concatenate([gains[i * 8 + which : i * 8 + which + 1, :] for i in range(8)], axis=1)


def rotate_heads(values, cos, sin, inverse=False):
    out = []
    for h in range(values.shape[0] // HD):
        a = values[h * HD : h * HD + HD // 2]
        b = values[h * HD + HD // 2 : (h + 1) * HD]
        if inverse:
            out += [a * cos + b * sin, b * cos - a * sin]
        else:
            out += [a * cos - b * sin, b * cos + a * sin]
    return jnp.concatenate(out, axis=0)


def block_positions(order_ref, number, stretch_rows):
    row = lax.broadcasted_iota(jnp.int32, (stretch_rows, 128), 0)
    return jnp.concatenate(
        [row + order_ref[number * 2 + i] * stretch_rows for i in range(2)], axis=0
    )


def forward_kernel(
    order_ref, tok, w_query, w_key, w_value, gains, frequency, wo, cot, wg, wu, wd,
    tok_all, wqkv_all, gains_all, wo_all, wd_all, cot_all, kv_all, branch,
    normed_all, q_t_all, q_n_all, out_t_all, attended_all, log_sum, key_pos, query_pos, cos_t, sin_t,
    normed_two, hidden, d_gate, d_up, two_part,
    normed, q_t, q_n, out_t, attended, wqkv, gain_src, toks, wqkvs, wos, kv_own, kv, v_t, att_t, part, total, inbox, across,
    wgs, wus, wds, cots, two, ss, rs
):
    me = Here(ss, rs)
    z = me.z
    heads, hd, rows = q_t.shape
    wide = heads * hd
    keys = kv.shape[0]
    wqkv[:, :wide] = w_query[...]
    for j in range(4):

        @pl.when(z == j)
        def _():
            wqkv[:, wide : wide + hd] = w_key[:, j * hd : (j + 1) * hd]
            wqkv[:, wide + hd :] = w_value[:, j * hd : (j + 1) * hd]

    gain_src[...] = jnp.concatenate([gains[...], jnp.zeros((6, gains.shape[1]), f32)], axis=0)
    me.enter(tuple(range(1, 8)))
    lanes = att_t.shape[1]
    have_tok, have_gains, have_wqkv, have_wo = Flag(), Flag(), Flag(), Flag()
    have_wg, have_wu, have_wd, have_cot = Flag(), Flag(), Flag(), Flag()
    progress = Progress(0)
    order = Order(
        z_gather(me, tok, toks, 11.3, 0.0, have_tok),
        plane_direct(me, gain_src, gains_all, have_gains),
        plane_gather(me, wqkv, wqkvs, 7.0, 0.5, have_wqkv, 0.0),
        plane_gather(me, wo, wos, 6.0, 11.0, have_wo, 7.5),
        plane_gather(me, wg, wgs, 15.5, 20.0, have_wg, 17.0),
        z_gather(me, cot, cots, 11.3, 37.0, have_cot, 27.0),
    )
    c_number = me.x * 2 + me.c
    for i in range(4):
        x = 1 - me.x if i & 2 else me.x
        c = 1 - me.c if i & 1 else me.c
        key_pos[i * rows : (i + 1) * rows, :] = block_positions(order_ref, x * 2 + c, rows // 2)
    lane = lax.broadcasted_iota(jnp.int32, (hd // 2, rows // 2), 1)
    for i in range(2):
        span = slice(i * rows // 2, (i + 1) * rows // 2)
        position = lane + order_ref[c_number * 2 + i] * (rows // 2)
        query_pos[:, span] = position[:8]
        freq = jnp.concatenate([frequency[...]] * (rows // 256), axis=1)
        angle = position.astype(f32) * freq
        cos_t[:, span] = jnp.cos(angle)
        sin_t[:, span] = jnp.sin(angle)
    order.until(have_tok, have_gains, have_wqkv)
    saves = [me.local(toks, tok_all), me.local(wqkvs, wqkv_all)]
    for save in saves:
        save.start()
    gain = gain_row(gains_all, 0)

    def project(i):
        at = pl.ds(pl.multiple_of(i * 128, 128), 128)
        x = toks[at, :].astype(f32)
        inv = lax.rsqrt(jnp.mean(x * x, axis=1, keepdims=True) + norm_epsilon)
        low = (x * inv * gain).astype(bf16)
        normed[at, :] = low
        lin = jnp.dot(low, wqkvs[...], preferred_element_type=f32).T
        cos, sin = cos_t[:, at], sin_t[:, at]
        turned = rotate_heads(lin[: wide + hd], cos, sin)
        query = turned[:wide].astype(bf16) * bf16(1.0 / math.sqrt(hd))
        natural = query.astype(f32).T
        for h in range(heads):
            q_t[h, :, at] = query[h * hd : (h + 1) * hd]
            q_n[h, at, :] = natural[:, h * hd : (h + 1) * hd].astype(bf16)
        kv_own[at, :] = jnp.concatenate([turned[wide:], lin[wide + hd :]], axis=0).T.astype(bf16)

    order.loop(rows // 128, 1.0, project)

    def block(i):
        return kv.at[pl.ds(i * rows, rows)]

    copies = [me.copy(kv_own, block(i), me.plane(i)) for i in (1, 2, 3)]
    own = me.local(kv_own, block(0))
    for copy in (*copies, own):
        copy.start()
    order.pump(order.now + 4.0)
    order.add(plane_gather(me, wu, wus, 15.5, order.now, have_wu))
    order.add(plane_gather(me, wd, wds, 15.5, order.now + 24.0, have_wd, order.now + 14.0))
    own.wait()
    for copy in copies:
        copy.wait_recv()
    save = me.local(kv, kv_all)
    save.start()
    for i in range(keys // rows):
        span = slice(i * rows, (i + 1) * rows)
        v_t[:, span] = kv[span, :].astype(f32).T[hd:, :].astype(bf16)
    order.until(have_wo)
    save_wo = me.local(wos, wo_all)
    save_wo.start()
    for task in z_reduce_all(
        me, part, total, inbox, across, branch, 45.0, 16, progress, order.now, 18.0
    ):
        order.add(task)

    def item(i):
        r, h = i // heads, i % heads
        at = pl.ds(pl.multiple_of(r * lanes, lanes), lanes)
        s = jnp.dot(kv[:, 0:hd], q_t[h, :, at], preferred_element_type=f32)
        pos = jnp.concatenate([key_pos[...]] * (lanes // 128), axis=1)
        s = jnp.where(pos <= query_pos[0:1, at], s, masked_value)
        top = jnp.max(s, axis=0, keepdims=True)
        p = jnp.exp(s - top)
        norm = jnp.sum(p, axis=0, keepdims=True)
        o = jnp.dot(v_t[...], p.astype(bf16), preferred_element_type=f32) / norm
        out_t[h, :, at] = o
        log_sum[h, :, at] = top + jnp.log(norm)
        att_t[pl.ds(pl.multiple_of(h * hd, hd), hd), :] = o

        @pl.when(h == heads - 1)
        def _():
            natural = att_t[...].T.astype(bf16)
            attended[at, :] = natural
            part[at, :] = contract_last_dims(natural, wos[...]).astype(bf16)

    def before(k):
        progress.parts = k // heads * (lanes // 32)
        return False

    order.loop(heads * rows // lanes, 1.2, item, before)
    progress.parts = 16
    early = ((normed, normed_all), (q_t, q_t_all), (q_n, q_n_all), (out_t, out_t_all), (attended, attended_all))
    early = [me.local(*pair) for pair in early]
    for copy in early:
        copy.start()
    late = [me.local(wds, wd_all), me.local(cots, cot_all)]
    order.until(have_wg, have_wu, have_wd, have_cot)
    for copy in late:
        copy.start()
    gain_mlp = gain_row(gains_all, 1)
    half = rows // 2

    def norm_two(first):
        def body(i, _):
            at = pl.ds(pl.multiple_of(first + i * 64, 64), 64)
            h = toks[at, :].astype(f32) + total[at, :].astype(f32)
            inv = lax.rsqrt(jnp.mean(h * h, axis=1, keepdims=True) + norm_epsilon)
            normed_two[at, :] = (h * inv * gain_mlp).astype(bf16)
            return 0

        lax.fori_loop(0, half // 64, body, 0)

    def feed(at, span):
        gate = jnp.dot(normed_two[at, :], wgs[:, span], preferred_element_type=f32)
        up = jnp.dot(normed_two[at, :], wus[:, span], preferred_element_type=f32)
        grad = jnp.dot(cots[at, :], wds[:, span], preferred_element_type=f32)
        sigmoid = jax.nn.sigmoid(gate)
        silu = gate * sigmoid
        hidden[at, span] = (silu * up).astype(bf16)
        grad_gate = (grad * up * sigmoid * (1.0 + gate * (1.0 - sigmoid))).astype(bf16)
        grad_up = (grad * silu).astype(bf16)
        d_gate[at, span] = grad_gate
        d_up[at, span] = grad_up
        return contract_last_dims(grad_gate, wgs[:, span]) + contract_last_dims(grad_up, wus[:, span])

    def feed_item(j):
        @pl.when(j == 0)
        def _():
            norm_two(0)
            two[...] = jnp.zeros_like(two)

        two[...] += feed(slice(0, half), pl.ds(pl.multiple_of(j * 128, 128), 128))

    order.loop(hidden.shape[1] // 128, 1.8, feed_item, lambda k: progress.whole() < 8)
    two_part[:half, :] = two[...].astype(bf16)
    while progress.whole() < 16:
        order.step()
    norm_two(half)
    two_part[half:, :] = feed(slice(half, rows), slice(None)).astype(bf16)
    order.finish()
    for copy in copies:
        copy.wait_send()
    for copy in (save, save_wo, *saves, *early, *late):
        copy.wait()


def forward(stretch_order, tok, w_query, w_key, w_value, gains, frequency, wo, cot, wg, wu, wd):
    rows = tok.shape[0] * 4
    width = tok.shape[1]
    heads = w_query.shape[1] // HD
    keys = rows * 4
    qkv = (w_query.shape[0], w_query.shape[1] + 2 * HD)

    def grown(a, n=8):
        return shape((a.shape[0] * n,) + a.shape[1:], a.dtype)

    def room(a):
        return pltpu.VMEM(a.shape, a.dtype)

    gain_block = shape((8, gains.shape[1]), f32)
    wqkv = shape(qkv)
    block = shape((rows, width))
    units = shape((rows, wg.shape[1]))
    return pl.pallas_call(
        forward_kernel,
        out_shape=(
            block, grown(wqkv), grown(gain_block), grown(wo), grown(wd), block,
            shape((keys, 2 * HD)), block,
            block,
            shape((heads, HD, rows)),
            shape((heads, rows, HD)),
            shape((heads, HD, rows), f32),
            shape((rows, heads * HD)),
            shape((heads, 1, rows), f32),
            shape((keys, 128), jnp.int32),
            shape((8, rows), jnp.int32),
            shape((HD // 2, rows), f32),
            shape((HD // 2, rows), f32),
            block, units, units, units, block,
        ),
        in_specs=[pl.BlockSpec(memory_space=pltpu.SMEM)] + [VM] * 7 + [HB] * 4,
        out_specs=[HB, HB, VM] + [HB] * 10 + [VM] * 10,
        scratch_shapes=[
            room(block),
            pltpu.VMEM((heads, HD, rows), bf16),
            pltpu.VMEM((heads, rows, HD), bf16),
            pltpu.VMEM((heads, HD, rows), f32),
            pltpu.VMEM((rows, heads * HD), bf16),
            room(wqkv), room(gain_block), room(block), room(grown(wqkv)), room(grown(wo)),
            pltpu.VMEM((rows, 2 * HD), bf16),
            pltpu.VMEM((keys, 2 * HD), bf16),
            pltpu.VMEM((HD, keys), bf16),
            pltpu.VMEM((heads * HD, 256), f32),
            room(block), room(block), room(block), room(block),
            room(grown(wg)), room(grown(wu)), room(grown(wd)), room(block), pltpu.VMEM((rows // 2, width), f32),
        ] + dma_sems(224),
        compiler_params=params(1, 67043328),
        name="forward",
    )(stretch_order, tok, w_query, w_key, w_value, gains, frequency, wo, cot, wg, wu, wd)


def contract_rows(left, right):
    return lax.dot_general(left, right, (((0,), (0,)), ((), ())), preferred_element_type=f32)


def contract_last_dims(left, right):
    return lax.dot_general(left, right, (((1,), (1,)), ((), ())), preferred_element_type=f32)


def gain_sums(me, src, out, came, mine, came_z):
    def block(i):
        return pl.ds(pl.multiple_of(me.number(i) * 8, 8), 8)

    own = block(0)
    copies = [me.copy(src.at[block(i)], came.at[i - 1], me.plane(i)) for i in range(1, 8)]
    again = [
        me.copy(mine, came_z.at[d - 1], {"head": (me.z + d) % 4}) for d in (1, 2, 3)
    ]

    def steps(begin):
        for copy in copies:
            copy.start()
        yield begin + 13.0
        value = src[own, :]
        for i, copy in enumerate(copies):
            copy.wait_recv()
            value = value + came[i]
        mine[...] = value
        for copy in again:
            copy.start()
        yield begin + 40.0
        value = mine[...]
        for d, copy in enumerate(again):
            copy.wait_recv()
            value = value + came_z[d]
        out[...] = value
        for copy in copies + again:
            copy.wait_send()

    return steps


def backward_kernel(
    part, cot_all, hidden, normed_two, d_gate, d_up, wd_all, tok_all, branch, gains, wo_all,
    out_t_all, attended_all, q_t_all, q_n_all, kv_all, wqkv_all, normed_all, log_sum, key_pos, query_pos, cos_t, sin_t,
    dwd_own, dwg_own, dwu_own, dw_own, dwkv_all, out_own, own, grad_one, gains_out,
    total, inbox, across, cot, out_part, below, above, q_t, q_n, kv, k_t, came, dq_t,
    gain_two, gain_parts, came_gain, gain_mine, gain_z, dwkv_own, came_kv, *rest
):
    scratch_d, scratch_g = rest[:6], rest[6:12]
    free_d, free_g, free_z, ss, rs = rest[12:]
    me = Here(ss, rs)
    me.enter(tuple(range(1, 8)), all_z=True)
    z = me.z
    rows, width = part.shape
    heads, hd, _ = q_t.shape
    wide = heads * hd
    lin_cols = wide + 2 * hd
    keys = kv.shape[0]
    cols = width // 8
    progress = Progress(16)
    order = Order(*z_reduce_all(me, part, total, inbox, across, None, 45.0, 16, progress))
    down, gate = PlaneScatter(me, scratch_d), PlaneScatter(me, scratch_g)
    up = PlaneScatter(me, scratch_d)
    narrow = [ref.at[(slice(None),) * (len(ref.shape) - 1) + (pl.ds(0, lin_cols + wide),)] for ref in scratch_g]
    both = PlaneScatter(me, narrow)
    down_done, gate_done, up_done, both_done, out_done, one_done = (Flag() for _ in range(6))
    cot_load = me.local(cot_all, cot)
    cot_load.start()
    later = [me.local(src, dst) for src, dst in ((kv_all, kv), (q_t_all, q_t), (q_n_all, q_n))]
    stores = [me.slot() for _ in range(5)]
    back = [
        me.copy(kv.at[pl.ds(i * rows, rows)], came.at[i - 1], me.plane(i)) for i in (1, 2, 3)
    ]
    kv_sends = [
        me.copy(dwkv_own, came_kv.at[d - 1], {"head": (z + d) % 4}) for d in (1, 2, 3)
    ]

    gains_steps = gain_sums(me, gain_parts, gains_out, came_gain, gain_mine, gain_z)

    def columns(j):
        return pl.ds(pl.multiple_of(offsets_of(me, j) * cols, cols), cols)

    def send(scatter, j):
        for k in range(4):

            @pl.when(j == k)
            def _():
                scatter.core[k].start()

    def weights(left, right_h, right_g, wd):
        pairs = ((hidden, right_h), (normed_two, left), (d_gate, right_g))
        loads = [me.local(src, dst) for src, dst in pairs]
        for load in loads:
            load.start()
        for load in later:
            load.start()
        cot_load.wait()
        loads[0].wait()
        order.pump(2.0)

        def down_item(j):
            down.blocks[j] = contract_rows(cot[:, columns(j)], right_h[...]).astype(bf16)
            send(down, j)

        order.loop(8, 0.65, down_item)
        order.add(down.steps(dwd_own, 16.5, order.now + 0.1, down_done, free_d))
        loads[1].wait()
        loads[2].wait()

        def gate_item(j):
            gate.blocks[j] = contract_rows(left[:, columns(j)], right_g[...]).astype(bf16)
            send(gate, j)

        order.loop(8, 0.75, gate_item)
        order.add(gate.steps(dwg_own, 16.5, order.now + 19.0, gate_done, free_g))

        def fetch(j):
            at = pl.ds(pl.multiple_of(j * cols, cols), cols)
            return pltpu.make_async_copy(wd_all.at[at], wd.at[j % 2], ss.at[stores[1]])

        fetch(0).start()

        def out_item(j):
            fetch(j).wait()

            @pl.when(j < 7)
            def _():
                fetch(j + 1).start()

            at = pl.ds(pl.multiple_of(j * cols, cols), cols)
            out_part[:, at] = contract_last_dims(right_h[...], wd[j % 2]).astype(bf16)

        order.loop(8, 1.2, out_item)

    units = pltpu.VMEM(hidden.shape, bf16)
    weight = pltpu.VMEM((2, cols, hidden.shape[1]), bf16)
    pl.run_scoped(weights, pltpu.VMEM(part.shape, bf16), units, units, weight)

    def attention(tok, summed, wo, out_t, attended, g_t, g_n, delta, dk, dv):
        gain = gain_row(gains, 1)

        def fetch(r):
            at = pl.ds(pl.multiple_of(r * 128, 128), 128)
            return (
                pltpu.make_async_copy(tok_all.at[at], tok, ss.at[stores[2]]),
                pltpu.make_async_copy(branch.at[at], summed, ss.at[stores[3]]),
            )

        for copy in fetch(0):
            copy.start()
        loads = [
            me.local(src, dst)
            for src, dst in ((wo_all, wo), (out_t_all, out_t), (attended_all, attended))
        ]
        for load in loads:
            load.start()
        dk[...] = jnp.zeros_like(dk)
        dv[...] = jnp.zeros_like(dv)
        for load in later:
            load.wait()
        for i in range(keys // rows):
            span = slice(i * rows, (i + 1) * rows)
            k_t[:, span] = kv[span, :].astype(f32).T[:hd, :].astype(bf16)
        for load in loads:
            load.wait()
        order.add(z_reduce_scatter(me, out_part, below, above, out_own, 12.0, 42.0, out_done), 42.0)

        def prepare(r):
            for copy in fetch(r):
                copy.wait()
            at = pl.ds(pl.multiple_of(r * 128, 128), 128)
            h = tok[...].astype(f32) + summed[...].astype(f32)
            e = total[at, :].astype(f32)
            inv = lax.rsqrt(jnp.mean(h * h, axis=1, keepdims=True) + norm_epsilon)
            u = e * gain
            inner = jnp.mean(u * h, axis=1, keepdims=True)
            grad = cot[at, :].astype(f32) + (inv * u - h * (inv * inv * inv * inner))

            @pl.when(r == z)
            def _():
                own[...] = grad
                gain_two[...] = jnp.broadcast_to(jnp.sum(e * h * inv, axis=0, keepdims=True), gain_two.shape)

            small = grad.astype(bf16)
            cot[at, :] = small
            g = jnp.dot(small, wo[...], preferred_element_type=f32).astype(bf16)
            turned = g.astype(f32).T
            for head in range(heads):
                g_n[head] = g[:, head * hd : (head + 1) * hd]
                mine = turned[head * hd : (head + 1) * hd]
                g_t[head] = mine.astype(bf16)
                delta[head] = jnp.sum(mine * out_t[head, :, at], axis=0, keepdims=True)

            @pl.when(r < rows // 128 - 1)
            def _():
                for copy in fetch(r + 1):
                    copy.start()

        def item(i):
            r, h = i // heads, i % heads

            @pl.when(h == 0)
            def _():
                prepare(r)

            at = pl.ds(pl.multiple_of(r * 128, 128), 128)
            s = jnp.dot(kv[:, 0:hd], q_t[h, :, at], preferred_element_type=f32)
            s = jnp.where(key_pos[...] <= query_pos[0:1, at], s, masked_value)
            p = jnp.exp(s - log_sum[h, :, at])
            dp = jnp.dot(kv[:, hd:], g_t[h], preferred_element_type=f32)
            ds = (p * (dp - delta[h])).astype(bf16)
            dv[...] += jnp.dot(p.astype(bf16), g_n[h], preferred_element_type=f32)
            dk[...] += jnp.dot(ds, q_n[h, at, :], preferred_element_type=f32)
            grad = jnp.dot(k_t[...], ds, preferred_element_type=f32)
            dq_t[h, :, at] = (grad * (1.0 / math.sqrt(hd))).astype(bf16)

        def before(k):
            return progress.whole() < (k // heads + 1) * 4

        order.loop(heads * rows // 128, 1.25, item, before)
        for i in range(keys // rows):
            span = slice(i * rows, (i + 1) * rows)
            kv[span, :] = jnp.concatenate([dk[span, :], dv[span, :]], axis=1).astype(bf16)
        for copy in back:
            copy.start()
        order.until(gate_done)
        pl.semaphore_wait(free_g, 3)

        def low_item(j):
            both.blocks[j, :, lin_cols:] = contract_rows(cot[:, columns(j)], attended[...]).astype(bf16)

        order.loop(8, 0.4, low_item)

    slots = pltpu.VMEM((128, width), bf16)
    pl.run_scoped(
        attention,
        slots,
        slots,
        pltpu.VMEM(wo_all.shape, bf16),
        pltpu.VMEM(out_t_all.shape, f32),
        pltpu.VMEM(attended_all.shape, bf16),
        pltpu.VMEM((heads, hd, 128), bf16),
        pltpu.VMEM((heads, 128, hd), bf16),
        pltpu.VMEM((heads, 1, 128), f32),
        pltpu.VMEM((keys, hd), f32),
        pltpu.VMEM((keys, hd), f32),
    )

    def last(left, right_u, wqkv, normed, lin, gain_one):
        tok = cot
        pairs = ((wqkv_all, wqkv), (normed_two, left), (d_up, right_u), (normed_all, normed), (tok_all, tok))
        loads = [me.local(src, dst) for src, dst in pairs]
        for load in loads:
            load.start()
        gain_one[...] = jnp.zeros_like(gain_one)
        order.until(progress.sent_in, progress.sent_out, down_done)
        pl.semaphore_wait(free_d, 3)
        loads[1].wait()
        loads[2].wait()

        def up_item(j):
            up.blocks[j] = contract_rows(left[:, columns(j)], right_u[...]).astype(bf16)
            send(up, j)

        order.loop(8, 0.75, up_item)
        order.add(up.steps(dwu_own, 16.5, order.now + 0.1, up_done))
        for copy in back:
            copy.wait_recv()
        mine = kv[0:rows, :].astype(f32)
        for i in range(keys // rows - 1):
            mine = mine + came[i].astype(f32)
        for copy in back:
            copy.wait_send()
        kv[0:rows, :] = mine.astype(bf16)
        for load in (loads[0], loads[3], loads[4]):
            load.wait()

        def finish_item(i):
            at = pl.ds(pl.multiple_of(i * 128, 128), 128)
            grads_kv = kv[at, :].astype(f32).T
            grads = jnp.concatenate(
                [dq_t[h, :, at].astype(f32) for h in range(heads)] + [grads_kv[:hd]], axis=0
            )
            grads = rotate_heads(grads, cos_t[:, at], sin_t[:, at], inverse=True)
            natural = jnp.concatenate([grads, grads_kv[hd:]], axis=0).T.astype(bf16)
            lin[at, :] = natural
            one = contract_last_dims(natural, wqkv[...])
            total[at, :] = one.astype(bf16)
            x = tok[at, :].astype(f32)
            inv = lax.rsqrt(jnp.mean(x * x, axis=1, keepdims=True) + norm_epsilon)
            gain_one[0:1, :] += jnp.sum(one * x * inv, axis=0, keepdims=True)

        order.loop(rows // 128, 2.0, finish_item)
        for i in range(8):
            span = slice(i * cols, (i + 1) * cols)
            gain_parts[i * 8 : (i + 1) * 8, :] = jnp.concatenate(
                [gain_one[0:1, span], gain_two[0:1, span], jnp.zeros((6, cols), f32)], axis=0
            )
        order.until(out_done)
        me.free_along_z(free_z)
        order.add(gains_steps(order.now))
        order.step()
        me.wait_along_z(free_z)
        order.add(z_reduce_scatter(me, total, below, above, grad_one, 12.0, order.now, one_done), order.now)

        def both_item(j):
            both.blocks[j, :, :lin_cols] = contract_rows(normed[:, columns(j)], lin[...]).astype(bf16)
            send(both, j)

        order.loop(8, 0.5, both_item)
        order.add(both.steps(dw_own, 13.0, order.now + 0.1, both_done))

    pl.run_scoped(
        last,
        pltpu.VMEM(part.shape, bf16),
        units,
        pltpu.VMEM(wqkv_all.shape, bf16),
        pltpu.VMEM(part.shape, bf16),
        pltpu.VMEM((rows, lin_cols), bf16),
        pltpu.VMEM((8, width), f32),
    )
    order.until(both_done)
    dwkv_own[...] = dw_own[:, wide:lin_cols].astype(bf16)
    for copy in kv_sends:
        copy.start()
    order.finish()
    for copy in kv_sends:
        copy.wait_recv()
    dwkv_all[0] = dwkv_own[...]
    for d in (1, 2, 3):
        dwkv_all[d] = came_kv[d - 1]
    for copy in kv_sends:
        copy.wait_send()


def backward(
    part, cot_all, hidden, normed_two, d_gate, d_up, wd_all, tok_all, branch, gains, wo_all,
    out_t, attended, q_t, q_n, kv_all, wqkv_all, normed, log_sum, key_pos, query_pos, cos_t, sin_t
):
    heads, hd, rows = q_t.shape
    keys = key_pos.shape[0]
    width = part.shape[1]
    cols = width // 8
    whole = pltpu.VMEM(part.shape, bf16)
    own = (wd_all.shape[0] // 8, wd_all.shape[1])
    narrow = wqkv_all.shape[1] + wo_all.shape[1]
    return pl.pallas_call(
        backward_kernel,
        out_shape=(
            shape(own),
            shape(own),
            shape(own),
            shape((own[0], narrow), f32),
            shape((4, own[0], 2 * hd)),
            shape((rows // 4, width), f32),
            shape((rows // 4, width), f32),
            shape((rows // 4, width), f32),
            shape((8, cols), f32),
        ),
        in_specs=[VM] + [HB] * 8 + [VM] + [HB] * 8 + [VM] * 5,
        out_specs=[VM] * 9,
        scratch_shapes=[whole] * 7
        + [
            pltpu.VMEM(q_t.shape, bf16),
            pltpu.VMEM(q_n.shape, bf16),
            pltpu.VMEM((keys, 2 * hd), bf16),
            pltpu.VMEM((hd, keys), bf16),
            pltpu.VMEM((keys // rows - 1, rows, 2 * hd), bf16),
            pltpu.VMEM(q_t.shape, bf16),
            pltpu.VMEM((8, width), f32),
            pltpu.VMEM((64, cols), f32),
            pltpu.VMEM((7, 8, cols), f32),
            pltpu.VMEM((8, cols), f32),
            pltpu.VMEM((3, 8, cols), f32),
            pltpu.VMEM((own[0], 2 * hd), bf16),
            pltpu.VMEM((3, own[0], 2 * hd), bf16),
        ]
        + plane_scatter_scratch(*own) * 2
        + [pltpu.SemaphoreType.REGULAR] * 3
        + dma_sems(224),
        compiler_params=params(4, 67043328),
        name="backward",
    )(
        part, cot_all, hidden, normed_two, d_gate, d_up, wd_all, tok_all, branch, gains, wo_all,
        out_t, attended, q_t, q_n, kv_all, wqkv_all, normed, log_sum, key_pos, query_pos, cos_t, sin_t
    )


def local_fast(
    tokens, w_query, w_key, w_value, w_out, w_gate, w_up, w_down, gain_attn, gain_mlp, stretch_order, cotangent
):
    row_count, width = tokens.shape
    groups = 4
    cols = width // 8
    contract_last = (((1,), (1,)), ((), ()))
    z = lax.axis_index("head")
    own_first = z * row_count

    def own_rows(values):
        return lax.dynamic_slice_in_dim(values, own_first, row_count, 0)

    frequency = rope_base ** (-(np.arange(HD // 2, dtype=np.float32) * np.float32(2.0 / HD)))
    frequency = jnp.asarray(np.broadcast_to(frequency.astype(np.float32)[:, None], (HD // 2, 128)))
    gains = jnp.concatenate([gain_attn[None], gain_mlp[None]]).astype(f32)
    (
        tok_all, wqkv_all, gains_all, wo_all, wd_all, cot_all, kv_all, branch,
        normed, q_t, q_n, out_t, attended, log_sum, key_pos, query_pos, cos_t, sin_t,
        normed_two, hidden, d_gate, d_up, two_part,
    ) = forward(
        stretch_order, tokens, w_query, w_key, w_value, gains, frequency, w_out, cotangent, w_gate, w_up, w_down
    )
    gain_rows = gains_all.reshape(8, 8, cols)
    gain_one = gain_rows[:, 0].reshape(width)
    dwd_own, dwg_own, dwu_own, dw_own, dwkv_all, out_own, grad_hidden_own, grad_one, gain_grads = backward(
        two_part, cot_all, hidden, normed_two, d_gate, d_up, wd_all, tok_all, branch,
        gains_all, wo_all, out_t, attended, q_t, q_n, kv_all, wqkv_all, normed, log_sum, key_pos, query_pos,
        cos_t, sin_t,
    )

    x_own = tokens.astype(f32)
    layer_low = (x_own + own_rows(branch).astype(f32) + out_own).astype(bf16)
    inv_own = lax.rsqrt(jnp.mean(x_own * x_own, axis=-1, keepdims=True) + norm_epsilon)
    grad_tokens = (grad_hidden_own + norm_input_grad(x_own, inv_own, gain_one, grad_one)).astype(bf16)
    slots = jnp.concatenate(
        [lax.dynamic_slice_in_dim(dwkv_all, (z - j) % 4, 1, 0) for j in range(4)], axis=0
    ).astype(f32)
    grad_key = slots[:, :, :HD].transpose(1, 0, 2).reshape(cols, groups * HD)
    grad_value = slots[:, :, HD:].transpose(1, 0, 2).reshape(cols, groups * HD)
    return (
        layer_low,
        grad_tokens,
        dw_own[:, : w_query.shape[1]],
        grad_key,
        grad_value,
        dw_own[:, w_query.shape[1] + 2 * HD :],
        dwg_own.astype(f32),
        dwu_own.astype(f32),
        dwd_own.astype(f32),
        gain_grads[0],
        gain_grads[1],
    )


def solution(mesh):
    sizes = (mesh.shape["fsdp"], mesh.shape["blk"], mesh.shape["head"])
    return jax.shard_map(
        local_fast if sizes == (2, 4, 4) else local,
        mesh=mesh,
        in_specs=(
            P(("fsdp", "blk", "head"), None),
            P(("fsdp", "blk"), "head"),
            P(("fsdp", "blk"), None),
            P(("fsdp", "blk"), None),
            P(("fsdp", "blk"), "head"),
            P(("fsdp", "blk"), "head"),
            P(("fsdp", "blk"), "head"),
            P(("fsdp", "blk"), "head"),
            P(("fsdp", "blk")),
            P(("fsdp", "blk")),
            P(),
            P(("fsdp", "blk", "head"), None),
        ),
        out_specs=(
            P(("fsdp", "blk", "head"), None),
            P(("fsdp", "blk", "head"), None),
            P(("fsdp", "blk"), "head"),
            P(("fsdp", "blk"), None),
            P(("fsdp", "blk"), None),
            P(("fsdp", "blk"), "head"),
            P(("fsdp", "blk"), "head"),
            P(("fsdp", "blk"), "head"),
            P(("fsdp", "blk"), "head"),
            P(("fsdp", "blk")),
            P(("fsdp", "blk")),
        ),
        check_vma=False,
    )
```
